8 devices in a mesh: dp: 1 (over z), tp: 8 (over y, x, core).
Axes of the slice: x: 2, y: 2, z: 1, core: 2. Of those that a mesh axis runs over, the one named last changes fastest.
Arguments:
- hidden: bfloat16 [12, 768, 2048], P('dp', 'tp')
- grad_out: bfloat16 [12, 768, 2048], P('dp', 'tp')
- prefix_len: int32 [12], P('dp')
- valid_len: int32 [12], P('dp')
- attn_norm: bfloat16 [2048], replicated
- w_query: bfloat16 [2048, 2048], P(None, 'tp')
- w_key: bfloat16 [2048, 256], replicated
- w_value: bfloat16 [2048, 256], replicated
- w_out: bfloat16 [2048, 2048], P('tp')
- mlp_norm: bfloat16 [2048], replicated
- w_gate: bfloat16 [2048, 16384], P(None, 'tp')
- w_up: bfloat16 [2048, 16384], P(None, 'tp')
- w_down: bfloat16 [16384, 2048], P('tp')
Outputs:
- output 1: bfloat16 [12, 768, 2048], P('dp', 'tp')
- output 2: bfloat16 [12, 768, 2048], P('dp', 'tp')
- output 3: float32 [2048], P('dp')
- output 4: float32 [2048, 2048], P('dp', 'tp')
- output 5: float32 [2048, 256], P('dp')
- output 6: float32 [2048, 256], P('dp')
- output 7: float32 [2048, 2048], P(('dp', 'tp'))
- output 8: float32 [2048], P('dp')
- output 9: float32 [2048, 16384], P('dp', 'tp')
- output 10: float32 [2048, 16384], P('dp', 'tp')
- output 11: float32 [16384, 2048], P(('dp', 'tp'))
All inputs are finite; a program needn't handle non-finite values.
Results may differ from the reference program's by a relative error of at most 0.02.
Values are sent between devices in bfloat16 or wider.
A program may use at most 1 GiB of HBM per device.

```python
import math
import jax
import jax.numpy as jnp
from jax import lax

BATCH_SIZE = 12
SEQ_LEN = 768
MODEL_DIM = 2048
NUM_HEADS = 8
HEAD_DIM = 256
FFN_DIM = 16384


def rms_norm(x_in, gain):
    x_f = x_in.astype(jnp.float32)
    inv_rms = lax.rsqrt(jnp.mean(x_f * x_f, axis=-1, keepdims=True) + 1e-6)
    return (x_f * inv_rms * (1.0 + gain.astype(jnp.float32))).astype(jnp.bfloat16)


def rope_tables(positions, head_dim):
    half_dim = head_dim // 2
    exponent = jnp.arange(half_dim, dtype=jnp.float32) * (2.0 / head_dim)
    inv_freq = jnp.exp(exponent * (-math.log(10000.0)))
    angles = positions.astype(jnp.float32)[:, None] * inv_freq[None, :]
    return jnp.cos(angles), jnp.sin(angles)


def apply_rope(x_f, cos_t, sin_t):
    half_dim = x_f.shape[-1] // 2
    first = x_f[..., :half_dim]
    second = x_f[..., half_dim:]
    return jnp.concatenate([first * cos_t - second * sin_t, second * cos_t + first * sin_t], axis=-1)


def attend_one(operands):
    query, keys, values, prefix_count, valid_count = operands
    seq_len = query.shape[0]
    scale = query.shape[-1] ** -0.5
    scores = jnp.einsum("qhd,kd->hqk", query.astype(jnp.float32), keys.astype(jnp.float32)) * scale
    q_pos = jnp.arange(seq_len)[:, None]
    k_pos = jnp.arange(seq_len)[None, :]
    visible = (k_pos < valid_count) & ((k_pos < prefix_count) | (k_pos <= q_pos))
    scores = jnp.where(visible[None], scores, -1e30)
    probs = jax.nn.softmax(scores, axis=-1).astype(jnp.bfloat16)
    mixed = jnp.einsum("hqk,kd->qhd", probs.astype(jnp.float32), values.astype(jnp.float32))
    return mixed.astype(jnp.bfloat16)


def layer_forward(hidden, prefix_len, valid_len, weights):
    attn_norm, w_query, w_key, w_value, w_out, mlp_norm, w_gate, w_up, w_down = weights
    batch, seq_len, model_dim = hidden.shape
    head_dim = w_key.shape[1]
    num_heads = w_query.shape[1] // head_dim
    num_rows = batch * seq_len
    normed = rms_norm(hidden, attn_norm).reshape(num_rows, model_dim)
    cos_t, sin_t = rope_tables(jnp.arange(seq_len), head_dim)
    q_raw = jnp.dot(normed, w_query, preferred_element_type=jnp.float32).reshape(batch, seq_len, num_heads, head_dim)
    query = apply_rope(q_raw, cos_t[:, None, :], sin_t[:, None, :]).astype(jnp.bfloat16)
    k_raw = jnp.dot(normed, w_key, preferred_element_type=jnp.float32).reshape(batch, seq_len, head_dim)
    keys = apply_rope(k_raw, cos_t, sin_t).astype(jnp.bfloat16)
    values = jnp.dot(normed, w_value, preferred_element_type=jnp.float32).astype(jnp.bfloat16).reshape(batch, seq_len, head_dim)
    mixed = lax.map(jax.checkpoint(attend_one), (query, keys, values, prefix_len, valid_len))
    attn_out = jnp.dot(mixed.reshape(num_rows, num_heads * head_dim), w_out, preferred_element_type=jnp.float32)
    resid = (hidden.astype(jnp.float32) + attn_out.reshape(batch, seq_len, model_dim)).astype(jnp.bfloat16)
    gated_in = rms_norm(resid, mlp_norm).reshape(num_rows, model_dim)
    gate = jnp.dot(gated_in, w_gate, preferred_element_type=jnp.float32)
    upper = jnp.dot(gated_in, w_up, preferred_element_type=jnp.float32)
    act = (jax.nn.gelu(gate, approximate=True) * upper).astype(jnp.bfloat16)
    mlp_out = jnp.dot(act, w_down, preferred_element_type=jnp.float32)
    return (resid.astype(jnp.float32) + mlp_out.reshape(batch, seq_len, model_dim)).astype(jnp.bfloat16)


def setup_inputs(seed: int = 0, part: int = 0) -> dict:
    base_key = jax.random.key(seed)
    part_keys = jax.random.split(jax.random.fold_in(base_key, part), 4)
    shared_keys = jax.random.split(base_key, 9)
    q_dim = NUM_HEADS * HEAD_DIM
    act_shape = (BATCH_SIZE, SEQ_LEN, MODEL_DIM)
    hidden = (0.25 * jax.random.normal(part_keys[0], act_shape, jnp.float32)).astype(jnp.bfloat16)
    grad_out = jax.random.normal(part_keys[1], act_shape, jnp.float32).astype(jnp.bfloat16)
    valid_len = jax.random.randint(part_keys[2], (BATCH_SIZE,), (3 * SEQ_LEN) // 4, SEQ_LEN + 1, dtype=jnp.int32)
    valid_len = valid_len.at[0].set(SEQ_LEN)
    prefix_len = jax.random.randint(part_keys[3], (BATCH_SIZE,), SEQ_LEN // 8, (3 * SEQ_LEN) // 4 + 1, dtype=jnp.int32)
    in_scale = 1.0 / math.sqrt(MODEL_DIM)
    out_scale = math.sqrt(SEQ_LEN / (64.0 * q_dim))
    down_scale = 1.0 / math.sqrt(FFN_DIM)
    attn_norm = (0.3 * jax.random.normal(shared_keys[0], (MODEL_DIM,), jnp.float32)).astype(jnp.bfloat16)
    w_query = (in_scale * jax.random.normal(shared_keys[1], (MODEL_DIM, q_dim), jnp.float32)).astype(jnp.bfloat16)
    w_key = (in_scale * jax.random.normal(shared_keys[2], (MODEL_DIM, HEAD_DIM), jnp.float32)).astype(jnp.bfloat16)
    w_value = (in_scale * jax.random.normal(shared_keys[3], (MODEL_DIM, HEAD_DIM), jnp.float32)).astype(jnp.bfloat16)
    w_out = (out_scale * jax.random.normal(shared_keys[4], (q_dim, MODEL_DIM), jnp.float32)).astype(jnp.bfloat16)
    mlp_norm = (0.3 * jax.random.normal(shared_keys[5], (MODEL_DIM,), jnp.float32)).astype(jnp.bfloat16)
    w_gate = (in_scale * jax.random.normal(shared_keys[6], (MODEL_DIM, FFN_DIM), jnp.float32)).astype(jnp.bfloat16)
    w_up = (in_scale * jax.random.normal(shared_keys[7], (MODEL_DIM, FFN_DIM), jnp.float32)).astype(jnp.bfloat16)
    w_down = (down_scale * jax.random.normal(shared_keys[8], (FFN_DIM, MODEL_DIM), jnp.float32)).astype(jnp.bfloat16)
    return {"hidden": hidden, "grad_out": grad_out, "prefix_len": prefix_len, "valid_len": valid_len, "attn_norm": attn_norm, "w_query": w_query, "w_key": w_key, "w_value": w_value, "w_out": w_out, "mlp_norm": mlp_norm, "w_gate": w_gate, "w_up": w_up, "w_down": w_down}


def reference(hidden, grad_out, prefix_len, valid_len, attn_norm, w_query, w_key, w_value, w_out, mlp_norm, w_gate, w_up, w_down):
    weights = (attn_norm, w_query, w_key, w_value, w_out, mlp_norm, w_gate, w_up, w_down)

    def forward(hidden_in, weights_in):
        return layer_forward(hidden_in, prefix_len, valid_len, weights_in)

    hidden_out, pullback = jax.vjp(forward, hidden, weights)
    grad_hidden, grad_weights = pullback(grad_out)
    g_attn_norm, g_query, g_key, g_value, g_out, g_mlp_norm, g_gate, g_up, g_down = grad_weights
    return (hidden_out, grad_hidden, g_attn_norm.astype(jnp.float32), g_query.astype(jnp.float32), g_key.astype(jnp.float32), g_value.astype(jnp.float32), g_out.astype(jnp.float32), g_mlp_norm.astype(jnp.float32), g_gate.astype(jnp.float32), g_up.astype(jnp.float32), g_down.astype(jnp.float32))
```

```python
import functools
import math
import jax
import jax.numpy as jnp
from jax import lax
from jax.experimental import pallas as pl
from jax.experimental.pallas import tpu as pltpu
from jax.sharding import PartitionSpec as P

NORM_EPS = 1e-6
CHUNKS = 2
F32 = jnp.float32
BF16 = jnp.bfloat16
MASKED = -1e30


def rms_norm(x_in, gain):
    x_f = x_in.astype(F32)
    inv_rms = lax.rsqrt(jnp.mean(x_f * x_f, axis=-1, keepdims=True) + NORM_EPS)
    return (x_f * inv_rms * (1.0 + gain)).astype(BF16)


def rope_tables(positions, head_dim):
    half_dim = head_dim // 2
    exponent = jnp.arange(half_dim, dtype=F32) * (2.0 / head_dim)
    inv_freq = jnp.exp(exponent * (-math.log(10000.0)))
    angles = positions.astype(F32)[:, None] * inv_freq[None, :]
    return jnp.cos(angles), jnp.sin(angles)


def apply_rope(x_f, cos_t, sin_t):
    half_dim = x_f.shape[-1] // 2
    first = x_f[..., :half_dim]
    second = x_f[..., half_dim:]
    return jnp.concatenate([first * cos_t - second * sin_t, second * cos_t + first * sin_t], axis=-1)


def gated_act(gate, upper):
    return (jax.nn.gelu(gate, approximate=True) * upper).astype(BF16)


def dot_f32(lhs, rhs, lhs_dim, rhs_dim):
    return lax.dot_general(lhs, rhs, (((lhs_dim,), (rhs_dim,)), ((), ())), preferred_element_type=F32)


def attn_fwd_kernel(prefix_s, valid_s, q_own_ref, q_oth_ref, kv_own_ref, kv_oth_ref, cos_ref, sin_ref, qpos_ref, kpos_ref,
                    o_own_ref, o_oth_ref, r_own_ref, r_oth_ref):
    b = pl.program_id(0)
    rows, width = q_own_ref.shape[1:]
    hd = kv_own_ref.shape[-1] // 2
    half = hd // 2
    heads = width // hd
    scale = hd ** -0.5
    cos_t, sin_t = cos_ref[...], sin_ref[...]
    queries = []
    for src, dst in ((q_own_ref, r_own_ref), (q_oth_ref, r_oth_ref)):
        for n in range(heads):
            first = src[0, :, n * hd:n * hd + half]
            second = src[0, :, n * hd + half:(n + 1) * hd]
            q_1 = ((first * cos_t - second * sin_t).astype(BF16) * scale).astype(BF16)
            q_2 = ((second * cos_t + first * sin_t).astype(BF16) * scale).astype(BF16)
            dst[0, :, n * hd:n * hd + half] = q_1
            dst[0, :, n * hd + half:(n + 1) * hd] = q_2
            queries.append(jnp.concatenate([q_1, q_2], axis=1))
    n_keys = kv_own_ref.shape[0] * kv_own_ref.shape[2]
    keys = jnp.concatenate([kv_own_ref[:, 0, :, :hd].reshape(n_keys, hd), kv_oth_ref[:, 0, :, :hd].reshape(n_keys, hd)], axis=0)
    values = jnp.concatenate([kv_own_ref[:, 0, :, hd:].reshape(n_keys, hd), kv_oth_ref[:, 0, :, hd:].reshape(n_keys, hd)], axis=0)
    limit = jnp.minimum(valid_s[b], jnp.maximum(prefix_s[b], qpos_ref[...] + 1))
    visible = kpos_ref[...] < limit
    for side, dst in ((0, o_own_ref), (1, o_oth_ref)):
        query = jnp.concatenate(queries[side * heads:(side + 1) * heads], axis=0)
        scores = dot_f32(query, keys, 1, 1)
        scores = jnp.where(visible, scores, MASKED)
        top = jnp.max(scores, axis=-1, keepdims=True)
        expo = jnp.exp(scores - top)
        inv = 1.0 / jnp.sum(expo, axis=-1, keepdims=True)
        probs = (expo * inv).astype(BF16)
        mixed = dot_f32(probs, values, 1, 0).astype(BF16)
        for n in range(heads):
            dst[0, :, n * hd:(n + 1) * hd] = mixed[n * rows:(n + 1) * rows]


def attn_bwd_kernel(prefix_s, valid_s, q_own_ref, q_oth_ref, g_own_ref, g_oth_ref, kv_own_ref, kv_oth_ref, cos_ref, sin_ref,
                    qpos_ref, kpos_ref, dq_own_ref, dq_oth_ref, dkv_own_ref, dkv_oth_ref):
    b = pl.program_id(0)
    rows, width = q_own_ref.shape[1:]
    hd = kv_own_ref.shape[-1] // 2
    half = hd // 2
    heads = width // hd
    scale = hd ** -0.5
    cos_t, sin_t = cos_ref[...], sin_ref[...]
    shards = kv_own_ref.shape[0]
    n_keys = shards * kv_own_ref.shape[2]
    keys = jnp.concatenate([kv_own_ref[:, 0, :, :hd].reshape(n_keys, hd), kv_oth_ref[:, 0, :, :hd].reshape(n_keys, hd)], axis=0)
    values = jnp.concatenate([kv_own_ref[:, 0, :, hd:].reshape(n_keys, hd), kv_oth_ref[:, 0, :, hd:].reshape(n_keys, hd)], axis=0)
    limit = jnp.minimum(valid_s[b], jnp.maximum(prefix_s[b], qpos_ref[...] + 1))
    visible = kpos_ref[...] < limit
    d_keys, d_values = 0.0, 0.0
    for q_ref, g_ref, dst in ((q_own_ref, g_own_ref, dq_own_ref), (q_oth_ref, g_oth_ref, dq_oth_ref)):
        query = jnp.concatenate([q_ref[0, :, n * hd:(n + 1) * hd] for n in range(heads)], axis=0)
        grad = jnp.concatenate([g_ref[0, :, n * hd:(n + 1) * hd] for n in range(heads)], axis=0)
        scores = dot_f32(keys, query, 1, 1)
        scores = jnp.where(visible, scores, MASKED)
        top = jnp.max(scores, axis=0, keepdims=True)
        expo = jnp.exp(scores - top)
        inv = 1.0 / jnp.sum(expo, axis=0, keepdims=True)
        probs = expo * inv
        d_probs = dot_f32(values, grad, 1, 1)
        delta = jnp.sum(probs * d_probs, axis=0, keepdims=True)
        d_scores = (probs * (d_probs - delta)).astype(BF16)
        d_values = d_values + dot_f32(probs.astype(BF16), grad, 1, 0)
        d_keys = d_keys + dot_f32(d_scores, query, 1, 0)
        d_query = dot_f32(d_scores, keys, 0, 0) * scale
        for n in range(heads):
            g_1 = d_query[n * rows:(n + 1) * rows, :half]
            g_2 = d_query[n * rows:(n + 1) * rows, half:]
            dst[0, :, n * hd:n * hd + half] = (g_1 * cos_t + g_2 * sin_t).astype(BF16)
            dst[0, :, n * hd + half:(n + 1) * hd] = (g_2 * cos_t - g_1 * sin_t).astype(BF16)
    d_keys = d_keys.astype(BF16)
    d_values = d_values.astype(BF16)
    span = n_keys // shards
    for side, dst in ((0, dkv_own_ref), (1, dkv_oth_ref)):
        for c in range(shards):
            at = side * n_keys + c * span
            dst[c, 0, :, :hd] = d_keys[at:at + span]
            dst[c, 0, :, hd:] = d_values[at:at + span]


def attn_specs(batch, rows, width, shards, two_hd, half):
    q_spec = pl.BlockSpec((1, rows, width), lambda b, *_: (b, 0, 0))
    kv_spec = pl.BlockSpec((shards, 1, rows, two_hd), lambda b, *_: (0, b, 0, 0))
    tab_spec = pl.BlockSpec((rows, half), lambda b, *_: (0, 0))
    return q_spec, kv_spec, tab_spec


def whole(shape):
    return pl.BlockSpec(shape, lambda b, *_: tuple(0 for _ in shape))


def attn_fwd(q_own, q_oth, kv_own, kv_oth, cos_t, sin_t, qpos, kpos, prefix_len, valid_len):
    batch, rows, width = q_own.shape
    shards, two_hd = kv_own.shape[0], kv_own.shape[3]
    q_spec, kv_spec, tab_spec = attn_specs(batch, rows, width, shards, two_hd, two_hd // 4)
    heads = width * 2 // two_hd
    out = jax.ShapeDtypeStruct((batch, rows, width), BF16)
    qpos_col = jnp.tile(qpos, heads)[:, None]
    n_keys = kpos.shape[0]
    flops = 2 * 2 * batch * rows * 2 * width * n_keys
    return pl.pallas_call(
        attn_fwd_kernel,
        out_shape=(out, out, out, out),
        grid_spec=pltpu.PrefetchScalarGridSpec(
            num_scalar_prefetch=2, grid=(batch,),
            in_specs=[q_spec, q_spec, kv_spec, kv_spec, tab_spec, tab_spec, whole((heads * rows, 1)), whole((1, n_keys))],
            out_specs=[q_spec] * 4),
        compiler_params=pltpu.CompilerParams(dimension_semantics=("arbitrary",), vmem_limit_bytes=48 << 20),
        cost_estimate=pl.CostEstimate(flops=flops, bytes_accessed=batch * rows * width * 16 + kv_own.size * 4, transcendentals=batch * rows * heads * 2 * n_keys),
        name="attn_fwd",
    )(prefix_len, valid_len, q_own, q_oth, kv_own, kv_oth, cos_t, sin_t, qpos_col, kpos[None, :])


def attn_bwd(q_own, q_oth, g_own, g_oth, kv_own, kv_oth, cos_t, sin_t, qpos, kpos, prefix_len, valid_len):
    batch, rows, width = q_own.shape
    shards, two_hd = kv_own.shape[0], kv_own.shape[3]
    q_spec, kv_spec, tab_spec = attn_specs(batch, rows, width, shards, two_hd, two_hd // 4)
    heads = width * 2 // two_hd
    out = jax.ShapeDtypeStruct((batch, rows, width), BF16)
    kv_out = jax.ShapeDtypeStruct(kv_own.shape, BF16)
    qpos_row = jnp.tile(qpos, heads)[None, :]
    n_keys = kpos.shape[0]
    flops = 2 * 5 * batch * rows * 2 * width * n_keys
    return pl.pallas_call(
        attn_bwd_kernel,
        out_shape=(out, out, kv_out, kv_out),
        grid_spec=pltpu.PrefetchScalarGridSpec(
            num_scalar_prefetch=2, grid=(batch,),
            in_specs=[q_spec, q_spec, q_spec, q_spec, kv_spec, kv_spec, tab_spec, tab_spec, whole((1, heads * rows)), whole((n_keys, 1))],
            out_specs=[q_spec, q_spec, kv_spec, kv_spec]),
        compiler_params=pltpu.CompilerParams(dimension_semantics=("arbitrary",), vmem_limit_bytes=48 << 20),
        cost_estimate=pl.CostEstimate(flops=flops, bytes_accessed=batch * rows * width * 12 + kv_own.size * 8, transcendentals=batch * rows * heads * 2 * n_keys),
        name="attn_bwd",
    )(prefix_len, valid_len, q_own, q_oth, g_own, g_oth, kv_own, kv_oth, cos_t, sin_t, qpos_row, kpos[:, None])


def solution(mesh):
    tp_size = mesh.shape["tp"]
    chips = tp_size // 2
    act_spec = P("dp", "tp", None)
    in_specs = (act_spec, act_spec, P("dp"), P("dp"), P(None), P(None, "tp"), P(None, None), P(None, None), P("tp", None), P(None), P(None, "tp"), P(None, "tp"), P("tp", None))
    out_specs = (act_spec, act_spec, P("dp"), P("dp", "tp"), P("dp", None), P("dp", None), P(("dp", "tp"), None), P("dp"), P("dp", "tp"), P("dp", "tp"), P(("dp", "tp"), None))
    same_core = [[2 * c + k for c in range(chips)] for k in range(2)]
    partner = [(i, i ^ 1) for i in range(tp_size)]

    def gather4(x_loc):
        return lax.all_gather(x_loc, "tp", axis=0, tiled=False, axis_index_groups=same_core)

    def scatter4(x_part):
        return lax.psum_scatter(x_part, "tp", scatter_dimension=0, tiled=False, axis_index_groups=same_core)

    def swap(x_loc):
        return lax.ppermute(x_loc, "tp", partner)

    def local_layer(hidden, grad_out, prefix_len, valid_len, attn_norm, w_query, w_key, w_value, w_out, mlp_norm, w_gate, w_up, w_down):
        batch, rows, dim = hidden.shape
        hd = w_key.shape[1]
        tokens = batch * rows
        me = lax.axis_index("tp")
        core = lax.rem(me, 2)
        qpos = me * rows + jnp.arange(rows, dtype=jnp.int32)
        shard_pos = jnp.arange(rows, dtype=jnp.int32)[None, :] + (jnp.arange(chips, dtype=jnp.int32) * 2 * rows)[:, None]
        kpos = jnp.concatenate([(shard_pos + core * rows).reshape(-1), (shard_pos + (1 - core) * rows).reshape(-1)])
        cos_t, sin_t = rope_tables(qpos, hd)

        def rope_single(raw_proj):
            return apply_rope(raw_proj, cos_t, sin_t).astype(BF16)

        wq_own = gather4(w_query.T).reshape(chips * hd, dim)
        normed, norm1_pull = jax.vjp(rms_norm, hidden, attn_norm.astype(F32))
        normed_flat = normed.reshape(tokens, dim)
        k_raw = dot_f32(normed_flat, w_key, 1, 0).reshape(batch, rows, hd)
        keys, key_pull = jax.vjp(rope_single, k_raw)
        values = dot_f32(normed_flat, w_value, 1, 0).astype(BF16).reshape(batch, rows, hd)
        kv_own = gather4(jnp.concatenate([keys, values], axis=-1))
        wo_own = gather4(w_out).reshape(chips * hd, dim)
        wq_oth = swap(wq_own)
        kv_oth = swap(kv_own)
        wo_oth = swap(wo_own)
        q_own = dot_f32(normed_flat, wq_own, 1, 1).reshape(batch, rows, chips * hd)
        q_oth = dot_f32(normed_flat, wq_oth, 1, 1).reshape(batch, rows, chips * hd)
        mix_own, mix_oth, q_own, q_oth = attn_fwd(q_own, q_oth, kv_own, kv_oth, cos_t, sin_t, qpos, kpos, prefix_len, valid_len)
        mix_own = mix_own.reshape(tokens, chips * hd)
        mix_oth = mix_oth.reshape(tokens, chips * hd)
        attn_sum = dot_f32(mix_own, wo_own, 1, 0) + dot_f32(mix_oth, wo_oth, 1, 0)
        resid = (hidden.astype(F32) + attn_sum.reshape(batch, rows, dim)).astype(BF16)
        gated_in, norm2_pull = jax.vjp(rms_norm, resid, mlp_norm.astype(F32))

        step = batch // CHUNKS
        g_down = g_gate = g_up = 0.0
        mlp_sums, d_gated = [], []
        for c in range(CHUNKS):
            sl = slice(c * step, (c + 1) * step)
            g_own = gather4(grad_out[sl].reshape(step * rows, dim)).reshape(-1, dim)
            g_oth = swap(g_own)
            z_own = gather4(gated_in[sl].reshape(step * rows, dim)).reshape(-1, dim)
            z_oth = swap(z_own)
            outs, backs = [], []
            for z_all, g_all in ((z_own, g_own), (z_oth, g_oth)):
                d_act = dot_f32(g_all, w_down, 1, 1).astype(BF16)
                gate = dot_f32(z_all, w_gate, 1, 0)
                upper = dot_f32(z_all, w_up, 1, 0)
                act, act_pull = jax.vjp(gated_act, gate, upper)
                d_gate, d_upper = act_pull(d_act)
                d_gate = d_gate.astype(BF16)
                d_upper = d_upper.astype(BF16)
                outs.append(dot_f32(act, w_down, 1, 0))
                backs.append(dot_f32(d_gate, w_gate, 1, 1) + dot_f32(d_upper, w_up, 1, 1))
                g_down = g_down + dot_f32(act, g_all, 0, 0)
                g_gate = g_gate + dot_f32(z_all, d_gate, 0, 0)
                g_up = g_up + dot_f32(z_all, d_upper, 0, 0)
            for (own, oth), dest in ((outs, mlp_sums), (backs, d_gated)):
                part = (own + swap(oth.astype(BF16)).astype(F32)).astype(BF16)
                dest.append(scatter4(part.reshape(chips, step * rows, dim)).reshape(step, rows, dim))
        mlp_sum = jnp.concatenate(mlp_sums, axis=0)
        hidden_out = (resid.astype(F32) + mlp_sum.astype(F32)).astype(BF16)
        d_resid_norm, g_mlp_norm_part = norm2_pull(jnp.concatenate(d_gated, axis=0))
        d_resid = (grad_out.astype(F32) + d_resid_norm.astype(F32)).astype(BF16)

        d_resid_flat = d_resid.reshape(tokens, dim)
        d_mix_own = dot_f32(d_resid_flat, wo_own, 1, 1).astype(BF16).reshape(batch, rows, chips * hd)
        d_mix_oth = dot_f32(d_resid_flat, wo_oth, 1, 1).astype(BF16).reshape(batch, rows, chips * hd)
        dq_own, dq_oth, dkv_own, dkv_oth = attn_bwd(q_own, q_oth, d_mix_own, d_mix_oth, kv_own, kv_oth, cos_t, sin_t, qpos, kpos, prefix_len, valid_len)
        dkv = scatter4((dkv_own.astype(F32) + swap(dkv_oth).astype(F32)).astype(BF16))
        d_k_raw = key_pull(dkv[..., :hd])[0].astype(BF16).reshape(tokens, hd)
        d_values = dkv[..., hd:].reshape(tokens, hd)
        dq_own = dq_own.reshape(tokens, chips * hd)
        dq_oth = dq_oth.reshape(tokens, chips * hd)

        def weight_sum(own, oth):
            return scatter4((own + swap(oth)).reshape(chips, hd, dim))

        g_out = weight_sum(dot_f32(mix_own, d_resid_flat, 0, 0), dot_f32(mix_oth, d_resid_flat, 0, 0))
        g_query = weight_sum(dot_f32(dq_own, normed_flat, 0, 0), dot_f32(dq_oth, normed_flat, 0, 0)).T
        d_normed = (dot_f32(dq_own, wq_own, 1, 0) + dot_f32(dq_oth, wq_oth, 1, 0)
                    + dot_f32(d_k_raw, w_key, 1, 1) + dot_f32(d_values, w_value, 1, 1)).astype(BF16)
        d_hidden_norm, g_attn_norm_part = norm1_pull(d_normed.reshape(batch, rows, dim))
        grad_hidden = (d_resid.astype(F32) + d_hidden_norm.astype(F32)).astype(BF16)
        g_key = lax.psum(dot_f32(normed_flat, d_k_raw, 0, 0), "tp")
        g_value = lax.psum(dot_f32(normed_flat, d_values, 0, 0), "tp")
        g_attn_norm = lax.psum(g_attn_norm_part, "tp")
        g_mlp_norm = lax.psum(g_mlp_norm_part, "tp")
        return (hidden_out, grad_hidden, g_attn_norm, g_query, g_key, g_value, g_out, g_mlp_norm, g_gate, g_up, g_down)

    return jax.shard_map(local_layer, mesh=mesh, in_specs=in_specs, out_specs=out_specs, check_vma=False)
```

```python
import functools
import math
import jax
import jax.numpy as jnp
from jax import lax
from jax.experimental import pallas as pl
from jax.experimental.pallas import tpu as pltpu
from jax.sharding import PartitionSpec as P

NORM_EPS = 1e-6
SIZES = (4, 4, 4)
F32 = jnp.float32
BF16 = jnp.bfloat16
MASKED = -1e30


def rms_norm(x_in, gain):
    x_f = x_in.astype(F32)
    inv_rms = lax.rsqrt(jnp.mean(x_f * x_f, axis=-1, keepdims=True) + NORM_EPS)
    return (x_f * inv_rms * (1.0 + gain)).astype(BF16)


def rope_tables(positions, head_dim):
    half_dim = head_dim // 2
    exponent = jnp.arange(half_dim, dtype=F32) * (2.0 / head_dim)
    inv_freq = jnp.exp(exponent * (-math.log(10000.0)))
    angles = positions.astype(F32)[:, None] * inv_freq[None, :]
    return jnp.cos(angles), jnp.sin(angles)


def apply_rope(x_f, cos_t, sin_t):
    half_dim = x_f.shape[-1] // 2
    first = x_f[..., :half_dim]
    second = x_f[..., half_dim:]
    return jnp.concatenate([first * cos_t - second * sin_t, second * cos_t + first * sin_t], axis=-1)


def dot_f32(lhs, rhs, lhs_dim, rhs_dim):
    return lax.dot_general(lhs, rhs, (((lhs_dim,), (rhs_dim,)), ((), ())), preferred_element_type=F32)


def attn_fwd_kernel(prefix_s, valid_s, q_own_ref, q_oth_ref, kv_own_ref, kv_oth_ref, cos_ref, sin_ref, qpos_ref, kpos_ref,
                    o_own_ref, o_oth_ref, r_own_ref, r_oth_ref):
    b = pl.program_id(0)
    rows, width = q_own_ref.shape[1:]
    hd = kv_own_ref.shape[-1] // 2
    half = hd // 2
    heads = width // hd
    scale = hd ** -0.5
    cos_t, sin_t = cos_ref[...], sin_ref[...]
    queries = []
    for src, dst in ((q_own_ref, r_own_ref), (q_oth_ref, r_oth_ref)):
        for n in range(heads):
            first = src[0, :, n * hd:n * hd + half]
            second = src[0, :, n * hd + half:(n + 1) * hd]
            q_1 = ((first * cos_t - second * sin_t).astype(BF16) * scale).astype(BF16)
            q_2 = ((second * cos_t + first * sin_t).astype(BF16) * scale).astype(BF16)
            dst[0, :, n * hd:n * hd + half] = q_1
            dst[0, :, n * hd + half:(n + 1) * hd] = q_2
            queries.append(jnp.concatenate([q_1, q_2], axis=1))
    n_keys = kv_own_ref.shape[0] * kv_own_ref.shape[2]
    keys = jnp.concatenate([kv_own_ref[:, 0, :, :hd].reshape(n_keys, hd), kv_oth_ref[:, 0, :, :hd].reshape(n_keys, hd)], axis=0)
    values = jnp.concatenate([kv_own_ref[:, 0, :, hd:].reshape(n_keys, hd), kv_oth_ref[:, 0, :, hd:].reshape(n_keys, hd)], axis=0)
    limit = jnp.minimum(valid_s[b], jnp.maximum(prefix_s[b], qpos_ref[...] + 1))
    visible = kpos_ref[...] < limit
    for side, dst in ((0, o_own_ref), (1, o_oth_ref)):
        query = jnp.concatenate(queries[side * heads:(side + 1) * heads], axis=0)
        scores = dot_f32(query, keys, 1, 1)
        scores = jnp.where(visible, scores, MASKED)
        top = jnp.max(scores, axis=-1, keepdims=True)
        expo = jnp.exp(scores - top)
        inv = 1.0 / jnp.sum(expo, axis=-1, keepdims=True)
        probs = (expo * inv).astype(BF16)
        mixed = dot_f32(probs, values, 1, 0).astype(BF16)
        for n in range(heads):
            dst[0, :, n * hd:(n + 1) * hd] = mixed[n * rows:(n + 1) * rows]


def attn_bwd_kernel(first, prefix_s, valid_s, q_own_ref, q_oth_ref, g_own_ref, g_oth_ref, kv_own_ref, kv_oth_ref, cos_ref, sin_ref,
                    qpos_ref, kpos_ref, dq_own_ref, dq_oth_ref, dkv_own_ref, dkv_oth_ref):
    b = pl.program_id(0) + first
    rows, width = q_own_ref.shape[1:]
    hd = kv_own_ref.shape[-1] // 2
    half = hd // 2
    heads = width // hd
    scale = hd ** -0.5
    cos_t, sin_t = cos_ref[...], sin_ref[...]
    shards = kv_own_ref.shape[0]
    n_keys = shards * kv_own_ref.shape[2]
    keys = jnp.concatenate([kv_own_ref[:, 0, :, :hd].reshape(n_keys, hd), kv_oth_ref[:, 0, :, :hd].reshape(n_keys, hd)], axis=0)
    values = jnp.concatenate([kv_own_ref[:, 0, :, hd:].reshape(n_keys, hd), kv_oth_ref[:, 0, :, hd:].reshape(n_keys, hd)], axis=0)
    limit = jnp.minimum(valid_s[b], jnp.maximum(prefix_s[b], qpos_ref[...] + 1))
    visible = kpos_ref[...] < limit
    d_keys, d_values = 0.0, 0.0
    for q_ref, g_ref, dst in ((q_own_ref, g_own_ref, dq_own_ref), (q_oth_ref, g_oth_ref, dq_oth_ref)):
        query = jnp.concatenate([q_ref[0, :, n * hd:(n + 1) * hd] for n in range(heads)], axis=0)
        grad = jnp.concatenate([g_ref[0, :, n * hd:(n + 1) * hd] for n in range(heads)], axis=0)
        scores = dot_f32(keys, query, 1, 1)
        scores = jnp.where(visible, scores, MASKED)
        top = jnp.max(scores, axis=0, keepdims=True)
        expo = jnp.exp(scores - top)
        inv = 1.0 / jnp.sum(expo, axis=0, keepdims=True)
        probs = expo * inv
        d_probs = dot_f32(values, grad, 1, 1)
        delta = jnp.sum(probs * d_probs, axis=0, keepdims=True)
        d_scores = (probs * (d_probs - delta)).astype(BF16)
        d_values = d_values + dot_f32(probs.astype(BF16), grad, 1, 0)
        d_keys = d_keys + dot_f32(d_scores, query, 1, 0)
        d_query = dot_f32(d_scores, keys, 0, 0) * scale
        for n in range(heads):
            g_1 = d_query[n * rows:(n + 1) * rows, :half]
            g_2 = d_query[n * rows:(n + 1) * rows, half:]
            dst[0, :, n * hd:n * hd + half] = (g_1 * cos_t + g_2 * sin_t).astype(BF16)
            dst[0, :, n * hd + half:(n + 1) * hd] = (g_2 * cos_t - g_1 * sin_t).astype(BF16)
    d_keys = d_keys.astype(BF16)
    d_values = d_values.astype(BF16)
    span = n_keys // shards
    for side, dst in ((0, dkv_own_ref), (1, dkv_oth_ref)):
        for c in range(shards):
            at = side * n_keys + c * span
            dst[c, 0, :, :hd] = d_keys[at:at + span]
            dst[c, 0, :, hd:] = d_values[at:at + span]


def attn_specs(rows, width, shards, two_hd, half):
    q_spec = pl.BlockSpec((1, rows, width), lambda b, *_: (b, 0, 0))
    kv_spec = pl.BlockSpec((shards, 1, rows, two_hd), lambda b, *_: (0, b, 0, 0))
    tab_spec = pl.BlockSpec((rows, half), lambda b, *_: (0, 0))
    return q_spec, kv_spec, tab_spec


def whole(shape):
    return pl.BlockSpec(shape, lambda b, *_: tuple(0 for _ in shape))


def attn_fwd(q_own, q_oth, kv_own, kv_oth, cos_t, sin_t, qpos, kpos, prefix_len, valid_len):
    batch, rows, width = q_own.shape
    shards, two_hd = kv_own.shape[0], kv_own.shape[3]
    q_spec, kv_spec, tab_spec = attn_specs(rows, width, shards, two_hd, two_hd // 4)
    heads = width * 2 // two_hd
    out = jax.ShapeDtypeStruct((batch, rows, width), BF16)
    qpos_col = jnp.tile(qpos, heads)[:, None]
    n_keys = kpos.shape[0]
    flops = 2 * 2 * batch * rows * 2 * width * n_keys
    return pl.pallas_call(
        attn_fwd_kernel,
        out_shape=(out, out, out, out),
        grid_spec=pltpu.PrefetchScalarGridSpec(
            num_scalar_prefetch=2, grid=(batch,),
            in_specs=[q_spec, q_spec, kv_spec, kv_spec, tab_spec, tab_spec, whole((heads * rows, 1)), whole((1, n_keys))],
            out_specs=[q_spec] * 4),
        compiler_params=pltpu.CompilerParams(dimension_semantics=("arbitrary",), vmem_limit_bytes=48 << 20),
        cost_estimate=pl.CostEstimate(flops=flops, bytes_accessed=batch * rows * width * 16 + kv_own.size * 4, transcendentals=batch * rows * heads * 2 * n_keys),
        name="attn_fwd",
    )(prefix_len, valid_len, q_own, q_oth, kv_own, kv_oth, cos_t, sin_t, qpos_col, kpos[None, :])


def attn_bwd(order, q_own, q_oth, g_own, g_oth, kv_own, kv_oth, cos_t, sin_t, qpos, kpos, prefix_len, valid_len, first):
    batch, rows, width = g_own.shape
    shards, two_hd = kv_own.shape[0], kv_own.shape[3]
    g_spec, kv_out_spec, tab_spec = attn_specs(rows, width, shards, two_hd, two_hd // 4)
    q_spec = pl.BlockSpec((1, rows, width), lambda b, *_: (b + first, 0, 0))
    kv_spec = pl.BlockSpec((shards, 1, rows, two_hd), lambda b, *_: (0, b + first, 0, 0))
    heads = width * 2 // two_hd
    out = jax.ShapeDtypeStruct((batch, rows, width), BF16)
    kv_out = jax.ShapeDtypeStruct((shards, batch, rows, two_hd), BF16)
    qpos_row = jnp.tile(qpos, heads)[None, :]
    n_keys = kpos.shape[0]
    flops = 2 * 5 * batch * rows * 2 * width * n_keys

    def body(*refs):
        attn_bwd_kernel(first, *refs[:12], *refs[13:])

    out = pl.pallas_call(
        body,
        out_shape=(out, out, kv_out, kv_out),
        grid_spec=pltpu.PrefetchScalarGridSpec(
            num_scalar_prefetch=2, grid=(batch,),
            in_specs=[q_spec, q_spec, g_spec, g_spec, kv_spec, kv_spec, tab_spec, tab_spec, whole((1, heads * rows)), whole((n_keys, 1)), pl.BlockSpec(memory_space=pl.ANY)],
            out_specs=[g_spec, g_spec, kv_out_spec, kv_out_spec]),
        compiler_params=pltpu.CompilerParams(dimension_semantics=("arbitrary",), vmem_limit_bytes=48 << 20),
        cost_estimate=pl.CostEstimate(flops=flops, bytes_accessed=batch * rows * width * 12 + kv_out.size * 8, transcendentals=batch * rows * heads * 2 * n_keys),
        name="attn_bwd",
    )(prefix_len, valid_len, q_own, q_oth, g_own, g_oth, kv_own, kv_oth, cos_t, sin_t, qpos_row, kpos[:, None], order.last)
    order.last = out[0]
    return out


class Order:
    def __init__(self):
        self.last = None

    def call(self, kernel, n_in, *, in_specs, **options):
        def run(*args):
            deps = () if self.last is None or any(self.last is a for a in args) else (self.last,)

            def body(*refs):
                kernel(*refs[:n_in], *refs[n_in + len(deps):])

            out = pl.pallas_call(body, in_specs=in_specs + [pl.BlockSpec(memory_space=pl.ANY)] * len(deps), **options)(*args, *deps)
            self.last = out[0] if isinstance(out, (tuple, list)) else out
            return out

        return run


def params(steps, limit=56):
    return pltpu.CompilerParams(dimension_semantics=("arbitrary",) * steps, vmem_limit_bytes=limit << 20)


def cost(flops, *arrays):
    return pl.CostEstimate(flops=flops, bytes_accessed=sum(a.size * a.dtype.itemsize for a in arrays), transcendentals=0)


def act_kernel(z_ref, g_ref, wg_ref, wu_ref, *refs, sub):
    act_ref, dg_ref, du_ref = refs[-3:]
    c_1 = math.sqrt(2.0 / math.pi)
    c_3 = 0.044715 * c_1
    for j in range(0, wg_ref.shape[1], sub):
        gate = dot_f32(z_ref[...], wg_ref[:, j:j + sub], 1, 0)
        upper = dot_f32(z_ref[...], wu_ref[:, j:j + sub], 1, 0)
        if len(refs) == 4:
            d_act = dot_f32(g_ref[...], refs[0][j:j + sub, :], 1, 1).astype(BF16).astype(F32)
        else:
            d_act = g_ref[:, j:j + sub].astype(F32)
        square = gate * gate
        half = 0.5 * jnp.tanh(gate * (c_3 * square + c_1)) + 0.5
        gelu = gate * half
        act_ref[:, j:j + sub] = (gelu * upper).astype(BF16)
        du_ref[:, j:j + sub] = (d_act * gelu).astype(BF16)
        slope = half + gelu * (1.0 - half) * (6.0 * c_3 * square + 2.0 * c_1)
        dg_ref[:, j:j + sub] = (d_act * upper * slope).astype(BF16)


def act_call(order, z_all, g_all, w_gate, w_up, w_down, tm=768, tn=512, sub=256):
    tokens, dim = z_all.shape
    width = w_gate.shape[1]
    out = jax.ShapeDtypeStruct((tokens, width), BF16)
    row = pl.BlockSpec((tm, dim), lambda j, i: (i, 0))
    col = pl.BlockSpec((dim, tn), lambda j, i: (0, j))
    tile = pl.BlockSpec((tm, tn), lambda j, i: (i, j))
    args = (z_all, g_all, w_gate, w_up) + (() if w_down is None else (w_down,))
    specs = [row, tile if w_down is None else row, col, col] + ([] if w_down is None else [pl.BlockSpec((tn, dim), lambda j, i: (j, 0))])
    return order.call(
        functools.partial(act_kernel, sub=sub), len(args), out_shape=(out, out, out), grid=(width // tn, tokens // tm),
        in_specs=specs, out_specs=[tile] * 3, compiler_params=params(2),
        cost_estimate=cost(2 * (len(args) - 2) * tokens * dim * width, *args, out, out, out), name="mlp_act",
    )(*args)


def mm_kernel(*refs, n, rhs_dim):
    total = dot_f32(refs[0][...], refs[n][...], 1, rhs_dim)
    for p in range(1, n):
        total += dot_f32(refs[p][...], refs[n + p][...], 1, rhs_dim)
    for extra in refs[2 * n:-1]:
        total += extra[...].astype(F32)
    refs[-1][...] = total.astype(refs[-1].dtype)


def mm_call(order, lhs, rhs, rhs_dim, extra=(), tm=1152, tn=512, out_dtype=BF16, name="mm"):
    n = len(lhs)
    tokens, depth = lhs[0].shape
    width = rhs[0].shape[1 - rhs_dim]
    w_shape, w_map = ((depth, tn), lambda j, i: (0, j)) if rhs_dim == 0 else ((tn, depth), lambda j, i: (j, 0))
    out = jax.ShapeDtypeStruct((tokens, width), out_dtype)
    tile = pl.BlockSpec((tm, tn), lambda j, i: (i, j))
    return order.call(
        functools.partial(mm_kernel, n=n, rhs_dim=rhs_dim), 2 * n + len(extra), out_shape=out, grid=(width // tn, tokens // tm),
        in_specs=[pl.BlockSpec((tm, depth), lambda j, i: (i, 0))] * n + [pl.BlockSpec(w_shape, w_map)] * n + [tile] * len(extra),
        out_specs=tile, compiler_params=params(2),
        cost_estimate=cost(2 * n * tokens * depth * width, *lhs, *rhs, *extra, out), name=name,
    )(*lhs, *rhs, *extra)


def wgrad_kernel(*refs, n, tf, tn, cols):
    lhs, rhs, out, l_buf, r_buf, sems = refs[:n], refs[n:2 * n], *refs[2 * n:]
    i, j, k = pl.program_id(0), pl.program_id(1), pl.program_id(2)
    step = (i * cols + j) * n + k
    slot = lax.rem(step, 2)

    def copies(s, at, p):
        row = lax.div(s, cols * n)
        col = lax.rem(lax.div(s, n), cols)
        return (pltpu.make_async_copy(lhs[p].at[:, pl.ds(pl.multiple_of(row * tf, tf), tf)], l_buf.at[at], sems.at[0, at]),
                pltpu.make_async_copy(rhs[p].at[:, pl.ds(pl.multiple_of(col * tn, tn), tn)], r_buf.at[at], sems.at[1, at]))

    def fetch(s, at):
        for p in range(n):
            @pl.when(lax.rem(s, n) == p)
            def _(p=p):
                for copy in copies(s, at, p):
                    copy.start()

    @pl.when(step == 0)
    def _():
        fetch(step, slot)

    @pl.when(step + 1 < pl.num_programs(0) * cols * n)
    def _():
        fetch(step + 1, 1 - slot)

    for copy in copies(step, slot, 0):
        copy.wait()
    part = dot_f32(l_buf[slot], r_buf[slot], 0, 0)
    out[...] = jnp.where(k == 0, part, out[...] + part)


def wgrad_call(order, lhs, rhs, tf=1024, tn=1024):
    n = len(lhs)
    tokens, rows = lhs[0].shape
    width = rhs[0].shape[1]
    cols = width // tn
    out = jax.ShapeDtypeStruct((rows, width), F32)
    return order.call(
        functools.partial(wgrad_kernel, n=n, tf=tf, tn=tn, cols=cols), 2 * n, out_shape=out, grid=(rows // tf, cols, n),
        in_specs=[pl.BlockSpec(memory_space=pl.ANY)] * (2 * n), out_specs=pl.BlockSpec((tf, tn), lambda i, j, k: (i, j)),
        scratch_shapes=[pltpu.VMEM((2, tokens, tf), BF16), pltpu.VMEM((2, tokens, tn), BF16), pltpu.SemaphoreType.DMA((2, 2))],
        compiler_params=params(3), cost_estimate=cost(2 * n * tokens * rows * width, *lhs, *rhs, out), name="wgrad",
    )(*lhs, *rhs)


def small_wgrad_kernel(l_ref, r_ref, *refs):
    total = dot_f32(l_ref[...], r_ref[...], 0, 0)
    for extra in refs[:-1]:
        total += extra[...]
    refs[-1][...] = total


def small_wgrad(order, lhs, rhs, extra=(), tf=512, tn=1024):
    tokens, rows = lhs.shape
    width = rhs.shape[1]
    out = jax.ShapeDtypeStruct((rows, width), F32)
    tile = pl.BlockSpec((tf, tn), lambda j, i: (i, j))
    return order.call(
        small_wgrad_kernel, 2 + len(extra), out_shape=out, grid=(width // tn, rows // tf),
        in_specs=[pl.BlockSpec((tokens, tf), lambda j, i: (0, i)), pl.BlockSpec((tokens, tn), lambda j, i: (0, j))] + [tile] * len(extra),
        out_specs=tile, compiler_params=params(2), cost_estimate=cost(2 * tokens * rows * width, lhs, rhs, *extra, out), name="small_wgrad",
    )(lhs, rhs, *extra)


def resid_kernel(h_ref, a_own_ref, a_oth_ref, w_own_ref, w_oth_ref, gain_ref, resid_ref, *z_refs, edges):
    i = pl.program_id(0)
    total = dot_f32(a_own_ref[...], w_own_ref[...], 1, 0) + dot_f32(a_oth_ref[...], w_oth_ref[...], 1, 0)
    resid = (h_ref[...].astype(F32) + total).astype(BF16)
    resid_ref[...] = resid
    x_f = resid.astype(F32)
    inv = lax.rsqrt(jnp.mean(x_f * x_f, axis=-1, keepdims=True) + NORM_EPS)
    z = (x_f * inv * (1.0 + gain_ref[...])).astype(BF16)
    for z_ref, lo, hi in zip(z_refs, edges[:-1], edges[1:]):
        @pl.when((i >= lo) & (i < hi))
        def _(z_ref=z_ref):
            z_ref[...] = z


def resid_call(order, hidden, mix_own, mix_oth, wo_own, wo_oth, gain, sizes, tm):
    tokens, dim = hidden.shape
    width = mix_own.shape[1]
    edges = [0]
    for size in sizes:
        edges.append(edges[-1] + size // tm)
    row = pl.BlockSpec((tm, dim), lambda i: (i, 0))
    mix = pl.BlockSpec((tm, width), lambda i: (i, 0))
    whole_w = pl.BlockSpec((width, dim), lambda i: (0, 0))
    z_specs = [pl.BlockSpec((tm, dim), lambda i, lo=lo, hi=hi: (jnp.clip(i - lo, 0, hi - lo - 1), 0)) for lo, hi in zip(edges[:-1], edges[1:])]
    outs = (jax.ShapeDtypeStruct((tokens, dim), BF16),) + tuple(jax.ShapeDtypeStruct((size, dim), BF16) for size in sizes)
    return order.call(
        functools.partial(resid_kernel, edges=tuple(edges)), 6, out_shape=outs, grid=(tokens // tm,),
        in_specs=[row, mix, mix, whole_w, whole_w, pl.BlockSpec((1, dim), lambda i: (0, 0))], out_specs=[row] + z_specs,
        compiler_params=params(1), cost_estimate=cost(4 * tokens * dim * width, hidden, mix_own, mix_oth, wo_own, wo_oth, *outs), name="resid",
    )(hidden, mix_own, mix_oth, wo_own, wo_oth, gain)


def norm_back(x_f, gain_1, d_out):
    inv = lax.rsqrt(jnp.mean(x_f * x_f, axis=-1, keepdims=True) + NORM_EPS)
    unit = x_f * inv
    scaled = d_out * gain_1
    d_x = inv * (scaled - unit * jnp.mean(scaled * unit, axis=-1, keepdims=True))
    return d_x, d_out * unit


def fold_rows(terms):
    rows, dim = terms.shape
    return jnp.sum(terms.reshape(rows // 8, 8, dim), axis=0)


def d_resid_kernel(dz_ref, x_ref, g_ref, gain_ref, w_own_ref, w_oth_ref, d_ref, own_ref, oth_ref, norm_ref):
    @pl.when(pl.program_id(0) == 0)
    def _():
        norm_ref[...] = jnp.zeros_like(norm_ref)

    d_x, terms = norm_back(x_ref[...].astype(F32), 1.0 + gain_ref[...], dz_ref[...].astype(F32))
    norm_ref[...] += fold_rows(terms)
    d_resid = (g_ref[...].astype(F32) + d_x).astype(BF16)
    d_ref[...] = d_resid
    own_ref[...] = dot_f32(d_resid, w_own_ref[...], 1, 1).astype(BF16)
    oth_ref[...] = dot_f32(d_resid, w_oth_ref[...], 1, 1).astype(BF16)


def d_resid_call(order, dz, resid, grad_out, gain, wo_own, wo_oth, first, tm):
    tokens, dim = dz.shape
    width = wo_own.shape[0]
    base = first // tm
    row = pl.BlockSpec((tm, dim), lambda i: (i, 0))
    far = pl.BlockSpec((tm, dim), lambda i: (i + base, 0))
    mix = pl.BlockSpec((tm, width), lambda i: (i, 0))
    whole_w = pl.BlockSpec((width, dim), lambda i: (0, 0))
    outs = (jax.ShapeDtypeStruct((tokens, dim), BF16), jax.ShapeDtypeStruct((tokens, width), BF16),
            jax.ShapeDtypeStruct((tokens, width), BF16), jax.ShapeDtypeStruct((8, dim), F32))
    return order.call(
        d_resid_kernel, 6, out_shape=outs, grid=(tokens // tm,),
        in_specs=[row, far, far, pl.BlockSpec((1, dim), lambda i: (0, 0)), whole_w, whole_w],
        out_specs=[row, mix, mix, pl.BlockSpec((8, dim), lambda i: (0, 0))],
        compiler_params=params(1), cost_estimate=cost(4 * tokens * dim * width, dz, dz, dz, wo_own, wo_oth, *outs), name="d_resid",
    )(dz, resid, grad_out, gain, wo_own, wo_oth)


def d_hidden_kernel(q_own_ref, q_oth_ref, dk_ref, dv_ref, x_ref, d_ref, gain_ref, wq_own_ref, wq_oth_ref, wk_ref, wv_ref, out_ref, norm_ref):
    @pl.when(pl.program_id(0) == 0)
    def _():
        norm_ref[...] = jnp.zeros_like(norm_ref)

    d_normed = (dot_f32(q_own_ref[...], wq_own_ref[...], 1, 0) + dot_f32(q_oth_ref[...], wq_oth_ref[...], 1, 0)
                + dot_f32(dk_ref[...], wk_ref[...], 1, 1) + dot_f32(dv_ref[...], wv_ref[...], 1, 1)).astype(BF16).astype(F32)
    d_x, terms = norm_back(x_ref[...].astype(F32), 1.0 + gain_ref[...], d_normed)
    norm_ref[...] += fold_rows(terms)
    out_ref[...] = (d_ref[...].astype(F32) + d_x).astype(BF16)


def d_hidden_call(order, dq_own, dq_oth, d_k, d_v, hidden, d_resid, gain, wq_own, wq_oth, w_key, w_value, tm):
    tokens, dim = hidden.shape
    width, hd = dq_own.shape[1], d_k.shape[1]
    row = pl.BlockSpec((tm, dim), lambda i: (i, 0))
    mix = pl.BlockSpec((tm, width), lambda i: (i, 0))
    one = pl.BlockSpec((tm, hd), lambda i: (i, 0))
    whole_w = pl.BlockSpec((width, dim), lambda i: (0, 0))
    whole_k = pl.BlockSpec((dim, hd), lambda i: (0, 0))
    outs = (jax.ShapeDtypeStruct((tokens, dim), BF16), jax.ShapeDtypeStruct((8, dim), F32))
    return order.call(
        d_hidden_kernel, 11, out_shape=outs, grid=(tokens // tm,),
        in_specs=[mix, mix, one, one, row, row, pl.BlockSpec((1, dim), lambda i: (0, 0)), whole_w, whole_w, whole_k, whole_k],
        out_specs=[row, pl.BlockSpec((8, dim), lambda i: (0, 0))],
        compiler_params=params(1), cost_estimate=cost(4 * tokens * dim * (width + hd), dq_own, dq_oth, hidden, d_resid, wq_own, wq_oth, *outs), name="d_hidden",
    )(dq_own, dq_oth, d_k, d_v, hidden, d_resid, gain, wq_own, wq_oth, w_key, w_value)


def solution(mesh):
    tp_size = mesh.shape["tp"]
    chips = tp_size // 2
    act_spec = P("dp", "tp", None)
    in_specs = (act_spec, act_spec, P("dp"), P("dp"), P(None), P(None, "tp"), P(None, None), P(None, None), P("tp", None), P(None), P(None, "tp"), P(None, "tp"), P("tp", None))
    out_specs = (act_spec, act_spec, P("dp"), P("dp", "tp"), P("dp", None), P("dp", None), P(("dp", "tp"), None), P("dp"), P("dp", "tp"), P("dp", "tp"), P(("dp", "tp"), None))
    same_core = [[2 * c + k for c in range(chips)] for k in range(2)]
    partner = [(i, i ^ 1) for i in range(tp_size)]

    def gather4(x_loc):
        return lax.all_gather(x_loc, "tp", axis=0, tiled=False, axis_index_groups=same_core)

    def scatter4(x_part):
        flat = x_part.reshape((-1,) + x_part.shape[2:])
        return lax.psum_scatter(flat, "tp", scatter_dimension=0, tiled=True, axis_index_groups=same_core)

    def swap(x_loc):
        return lax.ppermute(x_loc, "tp", partner)

    def flip(x_loc, bits):
        return lax.ppermute(x_loc, "tp", [(i, i ^ bits) for i in range(tp_size)])

    def gather4_direct(x_loc):
        chip = lax.axis_index("tp") // 2
        half = x_loc.shape[0] // 2
        near, far = flip(x_loc, 2), flip(x_loc, 4)
        low, high = flip(near[:half], 4), flip(far[half:], 2)
        out = jnp.zeros((chips,) + x_loc.shape, x_loc.dtype)
        for k, block in ((0, x_loc), (1, near), (2, far)):
            out = lax.dynamic_update_slice(out, block[None], (chip ^ k, 0, 0))
        out = lax.dynamic_update_slice(out, low[None], (chip ^ 3, 0, 0))
        return lax.dynamic_update_slice(out, high[None], (chip ^ 3, half, 0))

    def local_layer(hidden, grad_out, prefix_len, valid_len, attn_norm, w_query, w_key, w_value, w_out, mlp_norm, w_gate, w_up, w_down):
        batch, rows, dim = hidden.shape
        hd = w_key.shape[1]
        tokens = batch * rows
        assert sum(SIZES) == batch
        me = lax.axis_index("tp")
        core = lax.rem(me, 2)
        qpos = me * rows + jnp.arange(rows, dtype=jnp.int32)
        shard_pos = jnp.arange(rows, dtype=jnp.int32)[None, :] + (jnp.arange(chips, dtype=jnp.int32) * 2 * rows)[:, None]
        kpos = jnp.concatenate([(shard_pos + core * rows).reshape(-1), (shard_pos + (1 - core) * rows).reshape(-1)])
        cos_t, sin_t = rope_tables(qpos, hd)

        def rope_single(raw_proj):
            return apply_rope(raw_proj, cos_t, sin_t).astype(BF16)

        attn_gain = attn_norm.astype(F32)
        mlp_gain = mlp_norm.astype(F32)
        order = Order()
        wq_own = gather4_direct(w_query.T).reshape(chips * hd, dim)
        normed_flat = rms_norm(hidden, attn_gain).reshape(tokens, dim)
        k_raw = dot_f32(normed_flat, w_key, 1, 0).reshape(batch, rows, hd)
        keys, key_pull = jax.vjp(rope_single, k_raw)
        values = dot_f32(normed_flat, w_value, 1, 0).astype(BF16).reshape(batch, rows, hd)
        kv_own = gather4(jnp.concatenate([keys, values], axis=-1))
        wo_own = gather4_direct(w_out).reshape(chips * hd, dim)
        wq_oth = swap(wq_own)
        kv_oth = swap(kv_own)
        wo_oth = swap(wo_own)
        q_own = dot_f32(normed_flat, wq_own, 1, 1).reshape(batch, rows, chips * hd)
        q_oth = dot_f32(normed_flat, wq_oth, 1, 1).reshape(batch, rows, chips * hd)
        mix_own, mix_oth, q_own, q_oth = attn_fwd(q_own, q_oth, kv_own, kv_oth, cos_t, sin_t, qpos, kpos, prefix_len, valid_len)
        mix_own = mix_own.reshape(tokens, chips * hd)
        mix_oth = mix_oth.reshape(tokens, chips * hd)
        hidden_flat = hidden.reshape(tokens, dim)
        grad_flat = grad_out.reshape(tokens, dim)
        sizes = [n * rows for n in SIZES]
        firsts = [sum(SIZES[:c]) for c in range(len(SIZES))]
        resid, *z_parts = resid_call(order, hidden_flat, mix_own, mix_oth, wo_own, wo_oth, mlp_gain[None, :], sizes, 2 * rows)

        z_pieces, g_pieces, act_pieces, dg_pieces, du_pieces = [], [], [], [], []
        mlp_sums, d_gated = [], []
        for c, (first, size, z_part) in enumerate(zip(firsts, sizes, z_parts)):
            g_own = gather4(grad_flat[first * rows:first * rows + size]).reshape(-1, dim)
            g_oth = swap(g_own)
            z_own = gather4(z_part).reshape(-1, dim)
            z_oth = swap(z_own)
            tm = 1152 if (chips * size) % 1152 == 0 else 768
            if c == 0:
                d_acts = [mm_call(order, (g,), (w_down,), 1, tm=tm, name="d_act") for g in (g_own, g_oth)]
                acts = [act_call(order, z, d, w_gate, w_up, None) for z, d in zip((z_own, z_oth), d_acts)]
            else:
                acts = [act_call(order, z, g, w_gate, w_up, w_down) for z, g in ((z_own, g_own), (z_oth, g_oth))]
            (act_own, dg_own, du_own), (act_oth, dg_oth, du_oth) = acts
            back_oth = swap(mm_call(order, (dg_oth, du_oth), (w_gate, w_up), 1, tm=tm, name="d_gated"))
            out_oth = swap(mm_call(order, (act_oth,), (w_down,), 0, tm=tm, name="mlp_out"))
            back = mm_call(order, (dg_own, du_own), (w_gate, w_up), 1, (back_oth,), tm=tm, name="d_gated")
            d_gated.append(scatter4(back.reshape(chips, size, dim)).reshape(size, dim))
            out = mm_call(order, (act_own,), (w_down,), 0, (out_oth,), tm=tm, name="mlp_out")
            mlp_sums.append(scatter4(out.reshape(chips, size, dim)).reshape(size, dim))
            z_pieces += [z_own, z_oth]
            g_pieces += [g_own, g_oth]
            act_pieces += [act_own, act_oth]
            dg_pieces += [dg_own, dg_oth]
            du_pieces += [du_own, du_oth]
        hidden_out = (resid.astype(F32) + jnp.concatenate(mlp_sums, axis=0).astype(F32)).astype(BF16).reshape(batch, rows, dim)

        d_resids, dq_owns, dq_oths, dkv_owns, dkv_oths = [], [], [], [], []
        norm_terms = 0.0
        for c, (first, n, size, dz) in enumerate(zip(firsts, SIZES, sizes, d_gated)):
            if c == len(SIZES) - 1:
                g_gate = wgrad_call(order, z_pieces, dg_pieces)
            d_resid, d_own, d_oth, terms = d_resid_call(order, dz, resid, grad_flat, mlp_gain[None, :], wo_own, wo_oth, first * rows, 2 * rows)
            dq_own, dq_oth, dkv_own, dkv_oth = attn_bwd(
                order, q_own, q_oth, d_own.reshape(n, rows, -1), d_oth.reshape(n, rows, -1), kv_own, kv_oth, cos_t, sin_t, qpos, kpos, prefix_len, valid_len, first)
            norm_terms = norm_terms + terms
            d_resids.append(d_resid)
            dq_owns.append(dq_own.reshape(size, -1))
            dq_oths.append(dq_oth.reshape(size, -1))
            dkv_owns.append(dkv_own)
            dkv_oths.append(swap(dkv_oth))
        d_resid = jnp.concatenate(d_resids, axis=0)
        dq_own = jnp.concatenate(dq_owns, axis=0)
        dq_oth = jnp.concatenate(dq_oths, axis=0)
        dkv_parts = [(own.astype(F32) + oth.astype(F32)).astype(BF16) for own, oth in zip(dkv_owns, dkv_oths)]
        dkv = scatter4(jnp.concatenate(dkv_parts, axis=1))
        d_k_raw = key_pull(dkv[..., :hd].astype(BF16))[0].astype(BF16).reshape(tokens, hd)
        d_values = dkv[..., hd:].reshape(tokens, hd)

        g_out_far = swap(small_wgrad(order, mix_oth, d_resid))
        g_query_far = swap(small_wgrad(order, dq_oth, normed_flat))
        g_out_part = small_wgrad(order, mix_own, d_resid, (g_out_far,))
        g_query_part = small_wgrad(order, dq_own, normed_flat, (g_query_far,))
        g_out = scatter4(g_out_part.reshape(chips, hd, dim))
        g_query = scatter4(g_query_part.reshape(chips, hd, dim)).reshape(hd, dim).T
        g_up = wgrad_call(order, z_pieces, du_pieces)
        g_key = lax.psum(dot_f32(normed_flat, d_k_raw, 0, 0), "tp")
        g_value = lax.psum(dot_f32(normed_flat, d_values, 0, 0), "tp")
        grad_hidden, attn_terms = d_hidden_call(order, dq_own, dq_oth, d_k_raw, d_values, hidden_flat, d_resid, attn_gain[None, :], wq_own, wq_oth, w_key, w_value, 2 * rows)
        g_attn_norm = lax.psum(jnp.sum(attn_terms, axis=0), "tp")
        g_mlp_norm = lax.psum(jnp.sum(norm_terms, axis=0), "tp")
        g_down = wgrad_call(order, act_pieces, g_pieces)
        return (hidden_out, grad_hidden.reshape(batch, rows, dim), g_attn_norm, g_query, g_key, g_value, g_out.reshape(hd, dim), g_mlp_norm, g_gate, g_up, g_down)

    return jax.shard_map(local_layer, mesh=mesh, in_specs=in_specs, out_specs=out_specs, check_vma=False)
```

```python
import functools
import math
import jax
import jax.numpy as jnp
from jax import lax
from jax.experimental import pallas as pl
from jax.experimental.pallas import tpu as pltpu
from jax.sharding import PartitionSpec as P

NORM_EPS = 1e-6
CHUNKS = 3
F32 = jnp.float32
BF16 = jnp.bfloat16
MASKED = -1e30


def rms_norm(x_in, gain):
    x_f = x_in.astype(F32)
    inv_rms = lax.rsqrt(jnp.mean(x_f * x_f, axis=-1, keepdims=True) + NORM_EPS)
    return (x_f * inv_rms * (1.0 + gain)).astype(BF16)


def rope_tables(positions, head_dim):
    half_dim = head_dim // 2
    exponent = jnp.arange(half_dim, dtype=F32) * (2.0 / head_dim)
    inv_freq = jnp.exp(exponent * (-math.log(10000.0)))
    angles = positions.astype(F32)[:, None] * inv_freq[None, :]
    return jnp.cos(angles), jnp.sin(angles)


def apply_rope(x_f, cos_t, sin_t):
    half_dim = x_f.shape[-1] // 2
    first = x_f[..., :half_dim]
    second = x_f[..., half_dim:]
    return jnp.concatenate([first * cos_t - second * sin_t, second * cos_t + first * sin_t], axis=-1)


def dot_f32(lhs, rhs, lhs_dim, rhs_dim):
    return lax.dot_general(lhs, rhs, (((lhs_dim,), (rhs_dim,)), ((), ())), preferred_element_type=F32)


def own_first(kv_ref, core, lo, hi):
    shards = kv_ref.shape[0] // 2
    return jnp.concatenate([kv_ref[2 * c + side, 0, :, lo:hi] for side in (core, 1 - core) for c in range(shards)], axis=0)


def attn_fwd_kernel(prefix_s, valid_s, core_s, q_own_ref, q_oth_ref, kv_ref, cos_ref, sin_ref, qpos_ref, kpos_ref,
                    o_own_ref, o_oth_ref, r_own_ref, r_oth_ref):
    b = pl.program_id(0)
    rows, width = q_own_ref.shape[1:]
    hd = kv_ref.shape[-1] // 2
    half = hd // 2
    heads = width // hd
    scale = hd ** -0.5
    cos_t, sin_t = cos_ref[...], sin_ref[...]
    queries = []
    for src, dst in ((q_own_ref, r_own_ref), (q_oth_ref, r_oth_ref)):
        for n in range(heads):
            first = src[0, :, n * hd:n * hd + half]
            second = src[0, :, n * hd + half:(n + 1) * hd]
            q_1 = ((first * cos_t - second * sin_t).astype(BF16) * scale).astype(BF16)
            q_2 = ((second * cos_t + first * sin_t).astype(BF16) * scale).astype(BF16)
            dst[0, :, n * hd:n * hd + half] = q_1
            dst[0, :, n * hd + half:(n + 1) * hd] = q_2
            queries.append(jnp.concatenate([q_1, q_2], axis=1))
    keys = own_first(kv_ref, core_s[0], 0, hd)
    values = own_first(kv_ref, core_s[0], hd, 2 * hd)
    limit = jnp.minimum(valid_s[b], jnp.maximum(prefix_s[b], qpos_ref[...] + 1))
    visible = kpos_ref[...] < limit
    for side, dst in ((0, o_own_ref), (1, o_oth_ref)):
        query = jnp.concatenate(queries[side * heads:(side + 1) * heads], axis=0)
        scores = dot_f32(query, keys, 1, 1)
        scores = jnp.where(visible, scores, MASKED)
        top = jnp.max(scores, axis=-1, keepdims=True)
        expo = jnp.exp(scores - top)
        inv = 1.0 / jnp.sum(expo, axis=-1, keepdims=True)
        probs = (expo * inv).astype(BF16)
        mixed = dot_f32(probs, values, 1, 0).astype(BF16)
        for n in range(heads):
            dst[0, :, n * hd:(n + 1) * hd] = mixed[n * rows:(n + 1) * rows]


def attn_bwd_kernel(first, prefix_s, valid_s, core_s, q_own_ref, q_oth_ref, g_own_ref, g_oth_ref, kv_ref, cos_ref, sin_ref,
                    qpos_ref, kpos_ref, dq_own_ref, dq_oth_ref, dkv_own_ref, dkv_oth_ref):
    b = pl.program_id(0) + first
    rows, width = q_own_ref.shape[1:]
    hd = kv_ref.shape[-1] // 2
    half = hd // 2
    heads = width // hd
    scale = hd ** -0.5
    cos_t, sin_t = cos_ref[...], sin_ref[...]
    shards = kv_ref.shape[0] // 2
    n_keys = shards * kv_ref.shape[2]
    keys = own_first(kv_ref, core_s[0], 0, hd)
    values = own_first(kv_ref, core_s[0], hd, 2 * hd)
    limit = jnp.minimum(valid_s[b], jnp.maximum(prefix_s[b], qpos_ref[...] + 1))
    visible = kpos_ref[...] < limit
    d_keys, d_values = 0.0, 0.0
    for q_ref, g_ref, dst in ((q_own_ref, g_own_ref, dq_own_ref), (q_oth_ref, g_oth_ref, dq_oth_ref)):
        query = jnp.concatenate([q_ref[0, :, n * hd:(n + 1) * hd] for n in range(heads)], axis=0)
        grad = jnp.concatenate([g_ref[0, :, n * hd:(n + 1) * hd] for n in range(heads)], axis=0)
        scores = dot_f32(keys, query, 1, 1)
        scores = jnp.where(visible, scores, MASKED)
        top = jnp.max(scores, axis=0, keepdims=True)
        expo = jnp.exp(scores - top)
        inv = 1.0 / jnp.sum(expo, axis=0, keepdims=True)
        probs = expo * inv
        d_probs = dot_f32(values, grad, 1, 1)
        delta = jnp.sum(probs * d_probs, axis=0, keepdims=True)
        d_scores = (probs * (d_probs - delta)).astype(BF16)
        d_values = d_values + dot_f32(probs.astype(BF16), grad, 1, 0)
        d_keys = d_keys + dot_f32(d_scores, query, 1, 0)
        d_query = dot_f32(d_scores, keys, 0, 0) * scale
        for n in range(heads):
            g_1 = d_query[n * rows:(n + 1) * rows, :half]
            g_2 = d_query[n * rows:(n + 1) * rows, half:]
            dst[0, :, n * hd:n * hd + half] = (g_1 * cos_t + g_2 * sin_t).astype(BF16)
            dst[0, :, n * hd + half:(n + 1) * hd] = (g_2 * cos_t - g_1 * sin_t).astype(BF16)
    d_keys = d_keys.astype(BF16)
    d_values = d_values.astype(BF16)
    span = n_keys // shards
    for side, dst in ((0, dkv_own_ref), (1, dkv_oth_ref)):
        for c in range(shards):
            at = side * n_keys + c * span
            dst[c, 0, :, :hd] = d_keys[at:at + span]
            dst[c, 0, :, hd:] = d_values[at:at + span]


def attn_specs(rows, width, shards, two_hd, half):
    q_spec = pl.BlockSpec((1, rows, width), lambda b, *_: (b, 0, 0))
    kv_spec = pl.BlockSpec((shards, 1, rows, two_hd), lambda b, *_: (0, b, 0, 0))
    tab_spec = pl.BlockSpec((rows, half), lambda b, *_: (0, 0))
    return q_spec, kv_spec, tab_spec


def whole(shape):
    return pl.BlockSpec(shape, lambda b, *_: tuple(0 for _ in shape))


def attn_fwd(q_own, q_oth, kv_all, cos_t, sin_t, qpos, kpos, scalars):
    batch, rows, width = q_own.shape
    shards, two_hd = kv_all.shape[0], kv_all.shape[3]
    q_spec, kv_spec, tab_spec = attn_specs(rows, width, shards, two_hd, two_hd // 4)
    heads = width * 2 // two_hd
    out = jax.ShapeDtypeStruct((batch, rows, width), BF16)
    qpos_col = jnp.tile(qpos, heads)[:, None]
    n_keys = kpos.shape[0]
    flops = 2 * 2 * batch * rows * 2 * width * n_keys
    return pl.pallas_call(
        attn_fwd_kernel,
        out_shape=(out, out, out, out),
        grid_spec=pltpu.PrefetchScalarGridSpec(
            num_scalar_prefetch=3, grid=(batch,),
            in_specs=[q_spec, q_spec, kv_spec, tab_spec, tab_spec, whole((heads * rows, 1)), whole((1, n_keys))],
            out_specs=[q_spec] * 4),
        compiler_params=pltpu.CompilerParams(dimension_semantics=("arbitrary",), vmem_limit_bytes=40 << 20),
        cost_estimate=pl.CostEstimate(flops=flops, bytes_accessed=batch * rows * width * 16 + kv_all.size * 2, transcendentals=batch * rows * heads * 2 * n_keys),
        name="attn_fwd",
    )(*scalars, q_own, q_oth, kv_all, cos_t, sin_t, qpos_col, kpos[None, :])


def attn_bwd(order, q_own, q_oth, g_own, g_oth, kv_all, cos_t, sin_t, qpos, kpos, scalars, first, count, earlier):
    batch, rows, width = q_own.shape
    shards, two_hd = kv_all.shape[0], kv_all.shape[3]
    tab_spec = pl.BlockSpec((rows, two_hd // 4), lambda b, *_: (0, 0))
    q_spec = pl.BlockSpec((1, rows, width), lambda b, *_: (b + first, 0, 0))
    kv_spec = pl.BlockSpec((shards, 1, rows, two_hd), lambda b, *_: (0, b + first, 0, 0))
    dkv_spec = pl.BlockSpec((shards // 2, 1, rows, two_hd), lambda b, *_: (0, b + first, 0, 0))
    heads = width * 2 // two_hd
    out = jax.ShapeDtypeStruct((batch, rows, width), BF16)
    kv_out = jax.ShapeDtypeStruct((shards // 2, batch, rows, two_hd), BF16)
    qpos_row = jnp.tile(qpos, heads)[None, :]
    n_keys = kpos.shape[0]
    flops = 2 * 5 * count * rows * 2 * width * n_keys
    return order.call(
        functools.partial(attn_bwd_kernel, first), 9, len(earlier), prefetch=3,
        out_shape=(out, out, kv_out, kv_out), grid=(count,),
        in_specs=[q_spec, q_spec, q_spec, q_spec, kv_spec, tab_spec, tab_spec, whole((1, heads * rows)), whole((n_keys, 1))],
        out_specs=[q_spec, q_spec, dkv_spec, dkv_spec],
        compiler_params=pltpu.CompilerParams(dimension_semantics=("arbitrary",), vmem_limit_bytes=40 << 20),
        cost_estimate=pl.CostEstimate(flops=flops, bytes_accessed=count * rows * width * 12 + kv_all.size * 4, transcendentals=count * rows * heads * 2 * n_keys),
        name="attn_bwd",
    )(*scalars, q_own, q_oth, g_own, g_oth, kv_all, cos_t, sin_t, qpos_row, kpos[:, None], *earlier)


class Order:
    def __init__(self):
        self.last = None

    def call(self, kernel, n_in, n_kept=0, *, in_specs, out_specs, grid, prefetch=0, scratch_shapes=(), **options):
        def run(*args):
            deps = () if self.last is None or any(self.last is a for a in args) else (self.last,)
            n_args = prefetch + n_in

            def body(*refs):
                kernel(*refs[:n_args], *refs[n_args + n_kept + len(deps):])

            n_out = len(out_specs) if isinstance(out_specs, (list, tuple)) else 1
            out = pl.pallas_call(
                body,
                grid_spec=pltpu.PrefetchScalarGridSpec(
                    num_scalar_prefetch=prefetch, grid=grid, scratch_shapes=scratch_shapes, out_specs=out_specs,
                    in_specs=in_specs + [pl.BlockSpec(memory_space=pl.ANY)] * (n_kept + len(deps))),
                input_output_aliases={n_args + k: n_out - n_kept + k for k in range(n_kept)},
                **options)(*args, *deps)
            self.last = out[0] if isinstance(out, (tuple, list)) else out
            return out

        return run


def params(steps, limit=56):
    return pltpu.CompilerParams(dimension_semantics=("arbitrary",) * steps, vmem_limit_bytes=limit << 20)


def cost(flops, *arrays):
    return pl.CostEstimate(flops=flops, bytes_accessed=sum(a.size * a.dtype.itemsize for a in arrays), transcendentals=0)


def rows_of(ref):
    return ref[...].reshape(-1, ref.shape[-1])


def raw_spec(shape):
    return pl.BlockSpec((2, 1) + shape[2:], lambda j, i, core: (lax.rem(i, 2), lax.bitwise_xor(core[0], lax.div(i, 2)), 0, 0))


def d_act_kernel(core_s, g_ref, wd_ref, out_ref):
    out_ref[...] = dot_f32(rows_of(g_ref), wd_ref[...], 1, 1).astype(BF16)


def d_act_call(order, core, g_all, w_down, tn=1024):
    chips, _, rows, dim = g_all.shape
    width = w_down.shape[0]
    out = jax.ShapeDtypeStruct((chips * 2 * rows, width), BF16)
    return order.call(
        d_act_kernel, 2, prefetch=1, out_shape=out, grid=(width // tn, chips),
        in_specs=[raw_spec(g_all.shape), pl.BlockSpec((tn, dim), lambda j, i, core: (j, 0))],
        out_specs=pl.BlockSpec((2 * rows, tn), lambda j, i, core: (i, j)), compiler_params=params(2),
        cost_estimate=cost(2 * g_all.size * width, g_all, w_down, out), name="d_act",
    )(core, g_all, w_down)


def act_kernel(core_s, z_ref, g_ref, wg_ref, wu_ref, *refs, sub):
    c_1 = math.sqrt(2.0 / math.pi)
    c_3 = 0.044715 * c_1
    act_ref, dg_ref, du_ref = refs[-3:]
    z_in = rows_of(z_ref)
    for j in range(0, wg_ref.shape[1], sub):
        gate = dot_f32(z_in, wg_ref[:, j:j + sub], 1, 0)
        upper = dot_f32(z_in, wu_ref[:, j:j + sub], 1, 0)
        if len(refs) == 4:
            d_act = dot_f32(rows_of(g_ref), refs[0][j:j + sub, :], 1, 1).astype(BF16).astype(F32)
        else:
            d_act = g_ref[:, j:j + sub].astype(F32)
        square = gate * gate
        half = 0.5 * jnp.tanh(gate * (c_3 * square + c_1)) + 0.5
        gelu = gate * half
        act_ref[:, j:j + sub] = (gelu * upper).astype(BF16)
        du_ref[:, j:j + sub] = (d_act * gelu).astype(BF16)
        slope = half + gelu * (1.0 - half) * (6.0 * c_3 * square + 2.0 * c_1)
        dg_ref[:, j:j + sub] = (d_act * upper * slope).astype(BF16)


def act_call(order, core, z_all, g_all, w_gate, w_up, w_down, tn=512, sub=256):
    chips, _, rows, dim = z_all.shape
    width = w_gate.shape[1]
    out = jax.ShapeDtypeStruct((chips * 2 * rows, width), BF16)
    raw = raw_spec(z_all.shape)
    col = pl.BlockSpec((dim, tn), lambda j, i, core: (0, j))
    tile = pl.BlockSpec((2 * rows, tn), lambda j, i, core: (i, j))
    args = (z_all, g_all, w_gate, w_up) + (() if w_down is None else (w_down,))
    specs = [raw, tile if w_down is None else raw, col, col] + ([] if w_down is None else [pl.BlockSpec((tn, dim), lambda j, i, core: (j, 0))])
    return order.call(
        functools.partial(act_kernel, sub=sub), len(args), prefetch=1, out_shape=(out, out, out), grid=(width // tn, chips),
        in_specs=specs, out_specs=[tile] * 3, compiler_params=params(2),
        cost_estimate=cost(2 * (len(args) - 2) * z_all.size * width, *args, out, out, out), name="mlp_act",
    )(core, *args)


def back_kernel(dg_ref, du_ref, act_ref, wg_ref, wu_ref, wd_ref, *refs, joined):
    far, out = (refs[:len(refs) // 2], refs[len(refs) // 2:]) if len(refs) == 2 * (1 if joined else 2) else ((), refs)
    d_z = dot_f32(dg_ref[...], wg_ref[...], 1, 1) + dot_f32(du_ref[...], wu_ref[...], 1, 1)
    mlp = dot_f32(act_ref[...], wd_ref[...], 1, 0)
    for kind, total in enumerate((d_z, mlp)):
        at = (slice(None), kind) if joined else (slice(None),)
        dst = out[0 if joined else kind]
        total = total.reshape(dst[at].shape)
        if far:
            total += far[0 if joined else kind][at].astype(F32)
        dst[at] = total.astype(BF16)


def back_call(order, side, d_gate, d_upper, act, w_gate, w_up, w_down, far, joined, chips, tn=512):
    width, dim = w_down.shape
    rows = act.shape[0] // (2 * chips)
    half = chips // 2
    lhs = pl.BlockSpec((2 * rows, width), lambda j, i: (i + side * half, 0))
    row_w = pl.BlockSpec((tn, width), lambda j, i: (j, 0))
    if joined:
        outs = (jax.ShapeDtypeStruct((chips, 2, rows, dim), BF16),)
        tiles = [pl.BlockSpec((2, 2, rows, tn), lambda j, i: (i, 0, 0, j))]
    else:
        outs = (jax.ShapeDtypeStruct((chips, rows, dim), BF16),) * 2
        tiles = [pl.BlockSpec((2, rows, tn), lambda j, i: (i, 0, j))] * 2
    return order.call(
        functools.partial(back_kernel, joined=joined), 6 + len(far), out_shape=outs, grid=(dim // tn, half),
        in_specs=[lhs, lhs, lhs, row_w, row_w, pl.BlockSpec((width, tn), lambda j, i: (0, j))] + tiles[:len(far)],
        out_specs=tiles, compiler_params=params(2),
        cost_estimate=cost(3 * act.size * dim, act, act, w_gate, w_up, w_down, *outs, *outs), name="mlp_back",
    )(d_gate, d_upper, act, w_gate, w_up, w_down, *far)


def wgrad_kernel(core_s, *refs, n, tf, tn, cols):
    lhs, rhs, out, l_buf, r_buf, sems = refs[:n], refs[n:2 * n], *refs[2 * n:]
    i, j, k = pl.program_id(0), pl.program_id(1), pl.program_id(2)
    step = (i * cols + j) * n + k
    slot = lax.rem(step, 2)
    chips = l_buf.shape[1] // 2

    def copies(s, at, p):
        row = pl.multiple_of(lax.div(s, cols * n) * tf, tf)
        col = pl.multiple_of(lax.rem(lax.div(s, n), cols) * tn, tn)
        out = []
        for q, (ref, buf, lanes) in enumerate(((lhs[p], l_buf, pl.ds(row, tf)), (rhs[p], r_buf, pl.ds(col, tn)))):
            if ref.ndim == 4:
                for side in range(2):
                    src = ref.at[:, lax.bitwise_xor(core_s[0], side), :, lanes]
                    out.append(pltpu.make_async_copy(src, buf.at[at, pl.ds(side * chips, chips)], sems.at[q, side, at]))
            else:
                out.append(pltpu.make_async_copy(ref.at[:, :, lanes], buf.at[at], sems.at[q, 0, at]))
        return out

    def fetch(s, at):
        for p in range(n):
            @pl.when(lax.rem(s, n) == p)
            def _(p=p):
                for copy in copies(s, at, p):
                    copy.start()

    @pl.when(step == 0)
    def _():
        fetch(step, slot)

    @pl.when(step + 1 < pl.num_programs(0) * cols * n)
    def _():
        fetch(step + 1, 1 - slot)

    for copy in copies(step, slot, 0):
        copy.wait()
    part = dot_f32(rows_of(l_buf.at[slot]), rows_of(r_buf.at[slot]), 0, 0)
    out[...] = jnp.where(k == 0, part, out[...] + part)


def wgrad_call(order, core, lhs, rhs, tf=1024, tn=1024):
    n = len(lhs)
    rows = lhs[0].shape[-2]
    shards = lhs[0].size // (rows * lhs[0].shape[-1])
    width = rhs[0].shape[-1]
    height = lhs[0].shape[-1]
    cols = width // tn
    out = jax.ShapeDtypeStruct((height, width), F32)
    return order.call(
        functools.partial(wgrad_kernel, n=n, tf=tf, tn=tn, cols=cols), 2 * n, prefetch=1, out_shape=out, grid=(height // tf, cols, n),
        in_specs=[pl.BlockSpec(memory_space=pl.ANY)] * (2 * n), out_specs=pl.BlockSpec((tf, tn), lambda i, j, k, core: (i, j)),
        scratch_shapes=[pltpu.VMEM((2, shards, rows, tf), BF16), pltpu.VMEM((2, shards, rows, tn), BF16), pltpu.SemaphoreType.DMA((2, 2, 2))],
        compiler_params=params(3), cost_estimate=cost(2 * n * shards * rows * height * width, *lhs, *rhs, out), name="wgrad",
    )(core, *lhs, *rhs)


def small_wgrad_kernel(l_ref, r_ref, *refs):
    total = dot_f32(l_ref[...], r_ref[...], 0, 0)
    for extra in refs[:-1]:
        total += extra[...]
    refs[-1][...] = total


def small_wgrad(order, lhs, rhs, extra=(), tf=512, tn=1024):
    tokens, rows = lhs.shape
    width = rhs.shape[1]
    out = jax.ShapeDtypeStruct((rows, width), F32)
    tile = pl.BlockSpec((tf, tn), lambda j, i: (i, j))
    return order.call(
        small_wgrad_kernel, 2 + len(extra), out_shape=out, grid=(width // tn, rows // tf),
        in_specs=[pl.BlockSpec((tokens, tf), lambda j, i: (0, i)), pl.BlockSpec((tokens, tn), lambda j, i: (0, j))] + [tile] * len(extra),
        out_specs=tile, compiler_params=params(2), cost_estimate=cost(2 * tokens * rows * width, lhs, rhs, *extra, out), name="small_wgrad",
    )(lhs, rhs, *extra)


def resid_kernel(h_ref, a_own_ref, a_oth_ref, w_own_ref, w_oth_ref, gain_ref, resid_ref, *z_refs, sub):
    for c, z_ref in enumerate(z_refs):
        @pl.when(pl.program_id(0) == c)
        def _(z_ref=z_ref):
            for r in range(0, z_ref.shape[0], sub):
                at = slice(r, r + sub)
                total = dot_f32(a_own_ref[at], w_own_ref[...], 1, 0) + dot_f32(a_oth_ref[at], w_oth_ref[...], 1, 0)
                resid = (h_ref[at].astype(F32) + total).astype(BF16)
                resid_ref[at] = resid
                x_f = resid.astype(F32)
                inv = lax.rsqrt(jnp.mean(x_f * x_f, axis=-1, keepdims=True) + NORM_EPS)
                z_ref[at] = (x_f * inv * (1.0 + gain_ref[...])).astype(BF16)


def resid_call(order, hidden, mix_own, mix_oth, wo_own, wo_oth, gain, size, sub):
    tokens, dim = hidden.shape
    width = mix_own.shape[1]
    chunks = tokens // size
    row = pl.BlockSpec((size, dim), lambda i: (i, 0))
    mix = pl.BlockSpec((size, width), lambda i: (i, 0))
    whole_w = pl.BlockSpec((width, dim), lambda i: (0, 0))
    outs = (jax.ShapeDtypeStruct((tokens, dim), BF16),) + (jax.ShapeDtypeStruct((size, dim), BF16),) * chunks
    return order.call(
        functools.partial(resid_kernel, sub=sub), 6, out_shape=outs, grid=(chunks,),
        in_specs=[row, mix, mix, whole_w, whole_w, pl.BlockSpec((1, dim), lambda i: (0, 0))],
        out_specs=[row] + [pl.BlockSpec((size, dim), lambda i: (0, 0))] * chunks,
        compiler_params=params(1), cost_estimate=cost(4 * tokens * dim * width, hidden, mix_own, mix_oth, wo_own, wo_oth, *outs), name="resid",
    )(hidden, mix_own, mix_oth, wo_own, wo_oth, gain)


def norm_back(x_f, gain_1, d_out):
    inv = lax.rsqrt(jnp.mean(x_f * x_f, axis=-1, keepdims=True) + NORM_EPS)
    unit = x_f * inv
    scaled = d_out * gain_1
    d_x = inv * (scaled - unit * jnp.mean(scaled * unit, axis=-1, keepdims=True))
    return d_x, d_out * unit


def fold_rows(terms):
    rows, dim = terms.shape
    return jnp.sum(terms.reshape(rows // 8, 8, dim), axis=0)


def d_resid_kernel(*refs, n):
    dz_refs = refs[:n]
    x_ref, g_ref, gain_ref, w_own_ref, w_oth_ref, norm_ref, d_ref, own_ref, oth_ref = refs[n:]
    i = pl.program_id(0)

    @pl.when(i == 0)
    def _():
        norm_ref[...] = jnp.zeros_like(norm_ref)

    for c, dz_ref in enumerate(dz_refs):
        @pl.when(i == c)
        def _(dz_ref=dz_ref):
            d_x, terms = norm_back(x_ref[...].astype(F32), 1.0 + gain_ref[...], rows_of(dz_ref).astype(F32))
            norm_ref[...] += fold_rows(terms)
            d_ref[...] = (g_ref[...].astype(F32) + d_x).astype(BF16)
    own_ref[...] = dot_f32(d_ref[...], w_own_ref[...], 1, 1).astype(BF16)
    oth_ref[...] = dot_f32(d_ref[...], w_oth_ref[...], 1, 1).astype(BF16)


def d_resid_call(order, dz, resid, grad_out, gain, wo_own, wo_oth, first, size, earlier):
    tokens, dim = resid.shape
    n = len(dz)
    width = wo_own.shape[0]
    one = [pl.BlockSpec((1, size, dim) if a.ndim == 3 else (size, dim), lambda i, nd=a.ndim: (0,) * nd) for a in dz]
    far = pl.BlockSpec((size, dim), lambda i: (i + first, 0))
    mix = pl.BlockSpec((size, width), lambda i: (i + first, 0))
    whole_w = pl.BlockSpec((width, dim), lambda i: (0, 0))
    outs = (jax.ShapeDtypeStruct((8, dim), F32), jax.ShapeDtypeStruct((tokens, dim), BF16),
            jax.ShapeDtypeStruct((tokens, width), BF16), jax.ShapeDtypeStruct((tokens, width), BF16))
    return order.call(
        functools.partial(d_resid_kernel, n=n), n + 5, len(earlier), out_shape=outs, grid=(n,),
        in_specs=one + [far, far, pl.BlockSpec((1, dim), lambda i: (0, 0)), whole_w, whole_w],
        out_specs=[pl.BlockSpec((8, dim), lambda i: (0, 0)), far, mix, mix],
        compiler_params=params(1, 48), cost_estimate=cost(4 * n * size * dim * width, *dz, wo_own, wo_oth, outs[1]), name="d_resid",
    )(*dz, resid, grad_out, gain, wo_own, wo_oth, *earlier)


def d_hidden_kernel(q_own_ref, q_oth_ref, dkv_ref, x_ref, d_ref, gain_ref, wq_own_ref, wq_oth_ref, wkv_ref, out_ref, norm_ref, *, sub):
    @pl.when(pl.program_id(0) == 0)
    def _():
        norm_ref[...] = jnp.zeros_like(norm_ref)

    folded = 0.0
    for r in range(0, x_ref.shape[0], sub):
        at = slice(r, r + sub)
        d_normed = (dot_f32(q_own_ref[at], wq_own_ref[...], 1, 0) + dot_f32(q_oth_ref[at], wq_oth_ref[...], 1, 0)
                    + dot_f32(dkv_ref[at], wkv_ref[...], 1, 1)).astype(BF16).astype(F32)
        d_x, terms = norm_back(x_ref[at].astype(F32), 1.0 + gain_ref[...], d_normed)
        folded += fold_rows(terms)
        out_ref[at] = (d_ref[at].astype(F32) + d_x).astype(BF16)
    norm_ref[...] += folded


def d_hidden_call(order, dq_own, dq_oth, dkv, hidden, d_resid, gain, wq_own, wq_oth, w_kv, tm, sub):
    tokens, dim = hidden.shape
    width, two_hd = dq_own.shape[1], dkv.shape[1]
    row = pl.BlockSpec((tm, dim), lambda i: (i, 0))
    mix = pl.BlockSpec((tm, width), lambda i: (i, 0))
    whole_w = pl.BlockSpec((width, dim), lambda i: (0, 0))
    outs = (jax.ShapeDtypeStruct((tokens, dim), BF16), jax.ShapeDtypeStruct((8, dim), F32))
    return order.call(
        functools.partial(d_hidden_kernel, sub=sub), 9, out_shape=outs, grid=(tokens // tm,),
        in_specs=[mix, mix, pl.BlockSpec((tm, two_hd), lambda i: (i, 0)), row, row, pl.BlockSpec((1, dim), lambda i: (0, 0)), whole_w, whole_w,
                  pl.BlockSpec((dim, two_hd), lambda i: (0, 0))],
        out_specs=[row, pl.BlockSpec((8, dim), lambda i: (0, 0))],
        compiler_params=params(1), cost_estimate=cost(4 * tokens * dim * (width + two_hd), dq_own, dq_oth, hidden, d_resid, wq_own, wq_oth, *outs), name="d_hidden",
    )(dq_own, dq_oth, dkv, hidden, d_resid, gain, wq_own, wq_oth, w_kv)


def solution(mesh):
    tp_size = mesh.shape["tp"]
    chips = tp_size // 2
    act_spec = P("dp", "tp", None)
    in_specs = (act_spec, act_spec, P("dp"), P("dp"), P(None), P(None, "tp"), P(None, None), P(None, None), P("tp", None), P(None), P(None, "tp"), P(None, "tp"), P("tp", None))
    out_specs = (act_spec, act_spec, P("dp"), P("dp", "tp"), P("dp", None), P("dp", None), P(("dp", "tp"), None), P("dp"), P("dp", "tp"), P("dp", "tp"), P(("dp", "tp"), None))
    same_core = [[2 * c + k for c in range(chips)] for k in range(2)]
    partner = [(i, i ^ 1) for i in range(tp_size)]

    def scatter4(x_part):
        flat = x_part.reshape((-1,) + x_part.shape[2:])
        return lax.psum_scatter(flat, "tp", scatter_dimension=0, tiled=True, axis_index_groups=same_core)

    def gather8(x_loc):
        return lax.all_gather(x_loc, "tp", axis=0, tiled=False)

    def swap(x_loc):
        return lax.ppermute(x_loc, "tp", partner)

    def flip(x_loc, bits):
        return lax.ppermute(x_loc, "tp", [(i, i ^ bits) for i in range(tp_size)])

    def gather4_direct(x_loc):
        chip = lax.axis_index("tp") // 2
        half = x_loc.shape[0] // 2
        near, far = flip(x_loc, 2), flip(x_loc, 4)
        low, high = flip(near[:half], 4), flip(far[half:], 2)
        out = jnp.zeros((chips,) + x_loc.shape, x_loc.dtype)
        for k, block in ((0, x_loc), (1, near), (2, far)):
            out = lax.dynamic_update_slice(out, block[None], (chip ^ k, 0, 0))
        out = lax.dynamic_update_slice(out, low[None], (chip ^ 3, 0, 0))
        return lax.dynamic_update_slice(out, high[None], (chip ^ 3, half, 0))

    def local_layer(hidden, grad_out, prefix_len, valid_len, attn_norm, w_query, w_key, w_value, w_out, mlp_norm, w_gate, w_up, w_down):
        batch, rows, dim = hidden.shape
        hd = w_key.shape[1]
        tokens = batch * rows
        assert batch % CHUNKS == 0
        me = lax.axis_index("tp")
        core = lax.rem(me, 2)
        qpos = me * rows + jnp.arange(rows, dtype=jnp.int32)
        shard_pos = jnp.arange(rows, dtype=jnp.int32)[None, :] + (jnp.arange(chips, dtype=jnp.int32) * 2 * rows)[:, None]
        kpos = jnp.concatenate([(shard_pos + core * rows).reshape(-1), (shard_pos + (1 - core) * rows).reshape(-1)])
        cos_t, sin_t = rope_tables(qpos, hd)

        def rope_single(raw_proj):
            return apply_rope(raw_proj, cos_t, sin_t)

        order = Order()
        scalars = (prefix_len, valid_len, core[None])
        attn_gain = attn_norm.astype(F32)
        mlp_gain = mlp_norm.astype(F32)
        wq_own = gather4_direct(w_query.T).reshape(chips * hd, dim)
        normed_flat = rms_norm(hidden, attn_gain).reshape(tokens, dim)
        w_kv = jnp.concatenate([w_key, w_value], axis=1)
        kv_raw = dot_f32(normed_flat, w_kv, 1, 0).reshape(batch, rows, 2 * hd)
        keys, key_pull = jax.vjp(rope_single, kv_raw[..., :hd])
        kv_all = gather8(jnp.concatenate([keys, kv_raw[..., hd:]], axis=-1).astype(BF16))
        wo_own = gather4_direct(w_out).reshape(chips * hd, dim)
        wq_oth = swap(wq_own)
        wo_oth = swap(wo_own)
        q_own = dot_f32(normed_flat, wq_own, 1, 1).reshape(batch, rows, chips * hd)
        q_oth = dot_f32(normed_flat, wq_oth, 1, 1).reshape(batch, rows, chips * hd)
        mix_own, mix_oth, q_own, q_oth = attn_fwd(q_own, q_oth, kv_all, cos_t, sin_t, qpos, kpos, scalars)
        mix_own = mix_own.reshape(tokens, chips * hd)
        mix_oth = mix_oth.reshape(tokens, chips * hd)
        hidden_flat = hidden.reshape(tokens, dim)
        grad_flat = grad_out.reshape(tokens, dim)
        size = tokens // CHUNKS
        resid, *z_parts = resid_call(order, hidden_flat, mix_own, mix_oth, wo_own, wo_oth, mlp_gain[None, :], size, 2 * rows)

        g_all, z_all, acts, far = [], [], [], []
        for c in range(CHUNKS):
            g_all.append(gather8(grad_flat[c * size:(c + 1) * size]).reshape(chips, 2, size, dim))
            z_all.append(gather8(z_parts[c]).reshape(chips, 2, size, dim))
        mlp_sums, d_gated = [None] * CHUNKS, [None] * CHUNKS
        weights = (w_gate, w_up, w_down)
        core_1 = core[None]
        grads = None

        def attn_back(first, count, earlier):
            terms, d_res, d_own, d_oth = d_resid_call(
                order, d_gated[first:first + count], resid, grad_flat, mlp_gain[None, :], wo_own, wo_oth, first, size, () if earlier is None else earlier[1])
            per = batch // CHUNKS
            parts = attn_bwd(order, q_own, q_oth, d_own.reshape(batch, rows, -1), d_oth.reshape(batch, rows, -1), kv_all, cos_t, sin_t, qpos, kpos,
                             scalars, first * per, count * per, () if earlier is None else earlier[2])
            return (terms if earlier is None else earlier[0] + terms), (d_res, d_own, d_oth), parts

        def finish(c):
            joined = c < CHUNKS - 1
            parts = back_call(order, 0, acts[c][1], acts[c][2], acts[c][0], *weights, far[c], joined, chips)
            sums = [scatter4(parts[0])]
            if not joined:
                sums.append(scatter4(parts[1]))
            if joined:
                both = sums[0].reshape(2, size, dim)
                d_gated[c], mlp_sums[c] = both, both[1]
            else:
                d_gated[c], mlp_sums[c] = (a.reshape(size, dim) for a in sums)

        for c in range(CHUNKS):
            if c == 0:
                d_act = d_act_call(order, core_1, g_all[c], w_down)
                acts.append(act_call(order, core_1, z_all[c], d_act, w_gate, w_up, None))
            else:
                acts.append(act_call(order, core_1, z_all[c], g_all[c], *weights))
                finish(c - 1)
            joined = c < CHUNKS - 1
            parts = back_call(order, 1, acts[c][1], acts[c][2], acts[c][0], *weights, (), joined, chips)
            far.append(tuple(swap(a) for a in parts))
        grads = attn_back(0, 1, None)
        finish(CHUNKS - 1)
        hidden_out = (resid.astype(F32) + jnp.concatenate(mlp_sums, axis=0).astype(F32)).astype(BF16).reshape(batch, rows, dim)
        shards = [[a.reshape(2 * chips, size, -1) for a in acts[c]] for c in range(CHUNKS)]
        g_gate = wgrad_call(order, core_1, z_all, [a[1] for a in shards])

        norm_terms, (d_resid, _, _), (dq_own, dq_oth, dkv_own, dkv_oth) = attn_back(1, CHUNKS - 1, grads)
        dq_own = dq_own.reshape(tokens, chips * hd)
        dq_oth = dq_oth.reshape(tokens, chips * hd)
        dkv = scatter4((dkv_own.astype(F32) + swap(dkv_oth).astype(F32)).astype(BF16))
        g_out_far = swap(small_wgrad(order, mix_oth, d_resid))
        g_query_far = swap(small_wgrad(order, dq_oth, normed_flat))
        g_out_part = small_wgrad(order, mix_own, d_resid, (g_out_far,))
        g_query_part = small_wgrad(order, dq_own, normed_flat, (g_query_far,))
        g_out = scatter4(g_out_part.reshape(chips, hd, dim))
        g_query = scatter4(g_query_part.reshape(chips, hd, dim)).reshape(hd, dim).T
        d_k_raw = key_pull(dkv[..., :hd].astype(F32))[0]
        dkv = jnp.concatenate([d_k_raw.astype(BF16), dkv[..., hd:]], axis=-1).reshape(tokens, 2 * hd)
        grad_hidden, attn_terms = d_hidden_call(
            order, dq_own, dq_oth, dkv, hidden_flat, d_resid, attn_gain[None, :], wq_own, wq_oth, w_kv, 4 * rows, 2 * rows)
        g_kv = small_wgrad(order, normed_flat, dkv, tf=1024, tn=2 * hd)
        norms = jnp.stack([jnp.sum(attn_terms, axis=0), jnp.sum(norm_terms, axis=0)]).reshape(-1, 2 * hd)
        sums = lax.psum(jnp.concatenate([g_kv, norms], axis=0), "tp")
        g_attn_norm, g_mlp_norm = sums[dim:].reshape(2, dim)
        g_up = wgrad_call(order, core_1, z_all, [a[2] for a in shards])
        g_down = wgrad_call(order, core_1, [a[0] for a in shards], g_all)
        return (hidden_out, grad_hidden.reshape(batch, rows, dim), g_attn_norm, g_query, sums[:dim, :hd], sums[:dim, hd:], g_out.reshape(hd, dim), g_mlp_norm, g_gate, g_up, g_down)

    return jax.shard_map(local_layer, mesh=mesh, in_specs=in_specs, out_specs=out_specs, check_vma=False)
```

```python
import functools
import math
import jax
import jax.numpy as jnp
from jax import lax
from jax.experimental import pallas as pl
from jax.experimental.pallas import tpu as pltpu
from jax.sharding import PartitionSpec as P

NORM_EPS = 1e-6
CHUNKS = 3
F32 = jnp.float32
BF16 = jnp.bfloat16
MASKED = -1e30


def rms_norm(x_in, gain):
    x_f = x_in.astype(F32)
    inv_rms = lax.rsqrt(jnp.mean(x_f * x_f, axis=-1, keepdims=True) + NORM_EPS)
    return (x_f * inv_rms * (1.0 + gain)).astype(BF16)


def rope_tables(positions, head_dim):
    half_dim = head_dim // 2
    exponent = jnp.arange(half_dim, dtype=F32) * (2.0 / head_dim)
    inv_freq = jnp.exp(exponent * (-math.log(10000.0)))
    angles = positions.astype(F32)[:, None] * inv_freq[None, :]
    return jnp.cos(angles), jnp.sin(angles)


def apply_rope(x_f, cos_t, sin_t):
    half_dim = x_f.shape[-1] // 2
    first = x_f[..., :half_dim]
    second = x_f[..., half_dim:]
    return jnp.concatenate([first * cos_t - second * sin_t, second * cos_t + first * sin_t], axis=-1)


def dot_f32(lhs, rhs, lhs_dim, rhs_dim):
    return lax.dot_general(lhs, rhs, (((lhs_dim,), (rhs_dim,)), ((), ())), preferred_element_type=F32)


def own_first(kv_ref, core, lo, hi):
    shards = kv_ref.shape[0] // 2
    return jnp.concatenate([kv_ref[2 * c + side, 0, :, lo:hi] for side in (core, 1 - core) for c in range(shards)], axis=0)


def attn_fwd_kernel(prefix_s, valid_s, core_s, q_own_ref, q_oth_ref, kv_ref, cos_ref, sin_ref, qpos_ref, kpos_ref,
                    o_own_ref, o_oth_ref, r_own_ref, r_oth_ref):
    b = pl.program_id(0)
    rows, width = q_own_ref.shape[1:]
    hd = kv_ref.shape[-1] // 2
    half = hd // 2
    heads = width // hd
    scale = hd ** -0.5
    cos_t, sin_t = cos_ref[...], sin_ref[...]
    queries = []
    for src, dst in ((q_own_ref, r_own_ref), (q_oth_ref, r_oth_ref)):
        for n in range(heads):
            first = src[0, :, n * hd:n * hd + half]
            second = src[0, :, n * hd + half:(n + 1) * hd]
            q_1 = ((first * cos_t - second * sin_t).astype(BF16) * scale).astype(BF16)
            q_2 = ((second * cos_t + first * sin_t).astype(BF16) * scale).astype(BF16)
            dst[0, :, n * hd:n * hd + half] = q_1
            dst[0, :, n * hd + half:(n + 1) * hd] = q_2
            queries.append(jnp.concatenate([q_1, q_2], axis=1))
    keys = own_first(kv_ref, core_s[0], 0, hd)
    values = own_first(kv_ref, core_s[0], hd, 2 * hd)
    limit = jnp.minimum(valid_s[b], jnp.maximum(prefix_s[b], qpos_ref[...] + 1))
    visible = kpos_ref[...] < limit
    for side, dst in ((0, o_own_ref), (1, o_oth_ref)):
        query = jnp.concatenate(queries[side * heads:(side + 1) * heads], axis=0)
        scores = dot_f32(query, keys, 1, 1)
        scores = jnp.where(visible, scores, MASKED)
        top = jnp.max(scores, axis=-1, keepdims=True)
        expo = jnp.exp(scores - top)
        inv = 1.0 / jnp.sum(expo, axis=-1, keepdims=True)
        probs = (expo * inv).astype(BF16)
        mixed = dot_f32(probs, values, 1, 0).astype(BF16)
        for n in range(heads):
            dst[0, :, n * hd:(n + 1) * hd] = mixed[n * rows:(n + 1) * rows]


def attn_bwd_kernel(first, prefix_s, valid_s, core_s, q_own_ref, q_oth_ref, g_own_ref, g_oth_ref, kv_ref, cos_ref, sin_ref,
                    qpos_ref, kpos_ref, dq_own_ref, dq_oth_ref, dkv_own_ref, dkv_oth_ref):
    b = pl.program_id(0) + first
    rows, width = q_own_ref.shape[1:]
    hd = kv_ref.shape[-1] // 2
    half = hd // 2
    heads = width // hd
    scale = hd ** -0.5
    cos_t, sin_t = cos_ref[...], sin_ref[...]
    shards = kv_ref.shape[0] // 2
    n_keys = shards * kv_ref.shape[2]
    keys = own_first(kv_ref, core_s[0], 0, hd)
    values = own_first(kv_ref, core_s[0], hd, 2 * hd)
    limit = jnp.minimum(valid_s[b], jnp.maximum(prefix_s[b], qpos_ref[...] + 1))
    visible = kpos_ref[...] < limit
    d_keys, d_values = 0.0, 0.0
    for q_ref, g_ref, dst in ((q_own_ref, g_own_ref, dq_own_ref), (q_oth_ref, g_oth_ref, dq_oth_ref)):
        query = jnp.concatenate([q_ref[0, :, n * hd:(n + 1) * hd] for n in range(heads)], axis=0)
        grad = jnp.concatenate([g_ref[0, :, n * hd:(n + 1) * hd] for n in range(heads)], axis=0)
        scores = dot_f32(keys, query, 1, 1)
        scores = jnp.where(visible, scores, MASKED)
        top = jnp.max(scores, axis=0, keepdims=True)
        expo = jnp.exp(scores - top)
        inv = 1.0 / jnp.sum(expo, axis=0, keepdims=True)
        probs = expo * inv
        d_probs = dot_f32(values, grad, 1, 1)
        delta = jnp.sum(probs * d_probs, axis=0, keepdims=True)
        d_scores = (probs * (d_probs - delta)).astype(BF16)
        d_values = d_values + dot_f32(probs.astype(BF16), grad, 1, 0)
        d_keys = d_keys + dot_f32(d_scores, query, 1, 0)
        d_query = dot_f32(d_scores, keys, 0, 0) * scale
        for n in range(heads):
            g_1 = d_query[n * rows:(n + 1) * rows, :half]
            g_2 = d_query[n * rows:(n + 1) * rows, half:]
            dst[0, :, n * hd:n * hd + half] = (g_1 * cos_t + g_2 * sin_t).astype(BF16)
            dst[0, :, n * hd + half:(n + 1) * hd] = (g_2 * cos_t - g_1 * sin_t).astype(BF16)
    d_keys = d_keys.astype(BF16)
    d_values = d_values.astype(BF16)
    span = n_keys // shards
    for side, dst in ((0, dkv_own_ref), (1, dkv_oth_ref)):
        for c in range(shards):
            at = side * n_keys + c * span
            dst[c, 0, :, :hd] = d_keys[at:at + span]
            dst[c, 0, :, hd:] = d_values[at:at + span]


def attn_specs(rows, width, shards, two_hd, half):
    q_spec = pl.BlockSpec((1, rows, width), lambda b, *_: (b, 0, 0))
    kv_spec = pl.BlockSpec((shards, 1, rows, two_hd), lambda b, *_: (0, b, 0, 0))
    tab_spec = pl.BlockSpec((rows, half), lambda b, *_: (0, 0))
    return q_spec, kv_spec, tab_spec


def whole(shape):
    return pl.BlockSpec(shape, lambda b, *_: tuple(0 for _ in shape))


def attn_fwd(q_own, q_oth, kv_all, cos_t, sin_t, qpos, kpos, scalars):
    batch, rows, width = q_own.shape
    shards, two_hd = kv_all.shape[0], kv_all.shape[3]
    q_spec, kv_spec, tab_spec = attn_specs(rows, width, shards, two_hd, two_hd // 4)
    heads = width * 2 // two_hd
    out = jax.ShapeDtypeStruct((batch, rows, width), BF16)
    qpos_col = jnp.tile(qpos, heads)[:, None]
    n_keys = kpos.shape[0]
    flops = 2 * 2 * batch * rows * 2 * width * n_keys
    return pl.pallas_call(
        attn_fwd_kernel,
        out_shape=(out, out, out, out),
        grid_spec=pltpu.PrefetchScalarGridSpec(
            num_scalar_prefetch=3, grid=(batch,),
            in_specs=[q_spec, q_spec, kv_spec, tab_spec, tab_spec, whole((heads * rows, 1)), whole((1, n_keys))],
            out_specs=[q_spec] * 4),
        compiler_params=pltpu.CompilerParams(dimension_semantics=("arbitrary",), vmem_limit_bytes=40 << 20),
        cost_estimate=pl.CostEstimate(flops=flops, bytes_accessed=batch * rows * width * 16 + kv_all.size * 2, transcendentals=batch * rows * heads * 2 * n_keys),
        name="attn_fwd",
    )(*scalars, q_own, q_oth, kv_all, cos_t, sin_t, qpos_col, kpos[None, :])


def attn_bwd(order, q_own, q_oth, g_own, g_oth, kv_all, cos_t, sin_t, qpos, kpos, scalars, first, count, earlier):
    batch, rows, width = q_own.shape
    shards, two_hd = kv_all.shape[0], kv_all.shape[3]
    tab_spec = pl.BlockSpec((rows, two_hd // 4), lambda b, *_: (0, 0))
    q_spec = pl.BlockSpec((1, rows, width), lambda b, *_: (b + first, 0, 0))
    kv_spec = pl.BlockSpec((shards, 1, rows, two_hd), lambda b, *_: (0, b + first, 0, 0))
    dkv_spec = pl.BlockSpec((shards // 2, 1, rows, two_hd), lambda b, *_: (0, b + first, 0, 0))
    heads = width * 2 // two_hd
    out = jax.ShapeDtypeStruct((batch, rows, width), BF16)
    kv_out = jax.ShapeDtypeStruct((shards // 2, batch, rows, two_hd), BF16)
    qpos_row = jnp.tile(qpos, heads)[None, :]
    n_keys = kpos.shape[0]
    flops = 2 * 5 * count * rows * 2 * width * n_keys
    return order.call(
        functools.partial(attn_bwd_kernel, first), 9, len(earlier), prefetch=3,
        out_shape=(out, out, kv_out, kv_out), grid=(count,),
        in_specs=[q_spec, q_spec, q_spec, q_spec, kv_spec, tab_spec, tab_spec, whole((1, heads * rows)), whole((n_keys, 1))],
        out_specs=[q_spec, q_spec, dkv_spec, dkv_spec],
        compiler_params=pltpu.CompilerParams(dimension_semantics=("arbitrary",), vmem_limit_bytes=40 << 20),
        cost_estimate=pl.CostEstimate(flops=flops, bytes_accessed=count * rows * width * 12 + kv_all.size * 4, transcendentals=count * rows * heads * 2 * n_keys),
        name="attn_bwd",
    )(*scalars, q_own, q_oth, g_own, g_oth, kv_all, cos_t, sin_t, qpos_row, kpos[:, None], *earlier)


class Order:
    def __init__(self):
        self.last = None

    def call(self, kernel, n_in, n_kept=0, *, in_specs, out_specs, grid, prefetch=0, scratch_shapes=(), **options):
        def run(*args):
            deps = () if self.last is None or any(self.last is a for a in args) else (self.last,)
            n_args = prefetch + n_in

            def body(*refs):
                kernel(*refs[:n_args], *refs[n_args + n_kept + len(deps):])

            n_out = len(out_specs) if isinstance(out_specs, (list, tuple)) else 1
            out = pl.pallas_call(
                body,
                grid_spec=pltpu.PrefetchScalarGridSpec(
                    num_scalar_prefetch=prefetch, grid=grid, scratch_shapes=scratch_shapes, out_specs=out_specs,
                    in_specs=in_specs + [pl.BlockSpec(memory_space=pl.ANY)] * (n_kept + len(deps))),
                input_output_aliases={n_args + k: n_out - n_kept + k for k in range(n_kept)},
                **options)(*args, *deps)
            self.last = out[0] if isinstance(out, (tuple, list)) else out
            return out

        return run


def params(steps, limit=56):
    return pltpu.CompilerParams(dimension_semantics=("arbitrary",) * steps, vmem_limit_bytes=limit << 20)


def cost(flops, *arrays):
    return pl.CostEstimate(flops=flops, bytes_accessed=sum(a.size * a.dtype.itemsize for a in arrays), transcendentals=0)


def rows_of(ref):
    return ref[...].reshape(-1, ref.shape[-1])


def raw_spec(shape):
    return pl.BlockSpec((2, 1) + shape[2:], lambda j, i, core: (lax.rem(i, 2), lax.bitwise_xor(core[0], lax.div(i, 2)), 0, 0))


def d_act_kernel(core_s, g_ref, wd_ref, out_ref):
    out_ref[...] = dot_f32(rows_of(g_ref), wd_ref[...], 1, 1).astype(BF16)


def d_act_call(order, core, g_all, w_down, tn=1024):
    chips, _, rows, dim = g_all.shape
    width = w_down.shape[0]
    out = jax.ShapeDtypeStruct((chips * 2 * rows, width), BF16)
    return order.call(
        d_act_kernel, 2, prefetch=1, out_shape=out, grid=(width // tn, chips),
        in_specs=[raw_spec(g_all.shape), pl.BlockSpec((tn, dim), lambda j, i, core: (j, 0))],
        out_specs=pl.BlockSpec((2 * rows, tn), lambda j, i, core: (i, j)), compiler_params=params(2),
        cost_estimate=cost(2 * g_all.size * width, g_all, w_down, out), name="d_act",
    )(core, g_all, w_down)


def act_kernel(core_s, z_ref, g_ref, wg_ref, wu_ref, *refs, sub):
    c_1 = math.sqrt(2.0 / math.pi)
    c_3 = 0.044715 * c_1
    act_ref, dg_ref, du_ref = refs[-3:]
    z_in = rows_of(z_ref)
    for j in range(0, wg_ref.shape[1], sub):
        gate = dot_f32(z_in, wg_ref[:, j:j + sub], 1, 0)
        upper = dot_f32(z_in, wu_ref[:, j:j + sub], 1, 0)
        if len(refs) == 4:
            d_act = dot_f32(rows_of(g_ref), refs[0][j:j + sub, :], 1, 1).astype(BF16).astype(F32)
        else:
            d_act = g_ref[:, j:j + sub].astype(F32)
        square = gate * gate
        half = 0.5 * jnp.tanh(gate * (c_3 * square + c_1)) + 0.5
        gelu = gate * half
        act_ref[:, j:j + sub] = (gelu * upper).astype(BF16)
        du_ref[:, j:j + sub] = (d_act * gelu).astype(BF16)
        slope = half + gelu * (1.0 - half) * (6.0 * c_3 * square + 2.0 * c_1)
        dg_ref[:, j:j + sub] = (d_act * upper * slope).astype(BF16)


def act_call(order, core, z_all, g_all, w_gate, w_up, w_down, tn=512, sub=256):
    chips, _, rows, dim = z_all.shape
    width = w_gate.shape[1]
    out = jax.ShapeDtypeStruct((chips * 2 * rows, width), BF16)
    raw = raw_spec(z_all.shape)
    col = pl.BlockSpec((dim, tn), lambda j, i, core: (0, j))
    tile = pl.BlockSpec((2 * rows, tn), lambda j, i, core: (i, j))
    args = (z_all, g_all, w_gate, w_up) + (() if w_down is None else (w_down,))
    specs = [raw, tile if w_down is None else raw, col, col] + ([] if w_down is None else [pl.BlockSpec((tn, dim), lambda j, i, core: (j, 0))])
    return order.call(
        functools.partial(act_kernel, sub=sub), len(args), prefetch=1, out_shape=(out, out, out), grid=(width // tn, chips),
        in_specs=specs, out_specs=[tile] * 3, compiler_params=params(2),
        cost_estimate=cost(2 * (len(args) - 2) * z_all.size * width, *args, out, out, out), name="mlp_act",
    )(core, *args)


def back_kernel(dg_hbm, du_hbm, act_hbm, wg_ref, wu_ref, wd_ref, *refs, joined, base):
    *refs, dg_buf, du_buf, act_buf, sems = refs
    far, out = (refs[:len(refs) // 2], refs[len(refs) // 2:]) if len(refs) == 2 * (1 if joined else 2) else ((), refs)
    j, i = pl.program_id(0), pl.program_id(1)
    rows = dg_buf.shape[1]

    def copies(at):
        return [pltpu.make_async_copy(src.at[pl.ds((base + at) * rows, rows)], buf.at[at], sems.at[k, at])
                for k, (src, buf) in enumerate(((dg_hbm, dg_buf), (du_hbm, du_buf), (act_hbm, act_buf)))]

    @pl.when((j == 0) & (i == 0))
    def _():
        for at in range(dg_buf.shape[0]):
            for copy in copies(at):
                copy.start()

    @pl.when(j == 0)
    def _():
        for copy in copies(i):
            copy.wait()

    d_z = dot_f32(dg_buf[i], wg_ref[...], 1, 1) + dot_f32(du_buf[i], wu_ref[...], 1, 1)
    mlp = dot_f32(act_buf[i], wd_ref[...], 1, 0)
    for kind, total in enumerate((d_z, mlp)):
        at = (slice(None), kind) if joined else (slice(None),)
        dst = out[0 if joined else kind]
        total = total.reshape(dst[at].shape)
        if far:
            total += far[0 if joined else kind][at].astype(F32)
        dst[at] = total.astype(BF16)


def back_call(order, side, d_gate, d_upper, act, w_gate, w_up, w_down, far, joined, chips, tn=512):
    width, dim = w_down.shape
    rows = act.shape[0] // (2 * chips)
    half = chips // 2
    hbm = pl.BlockSpec(memory_space=pl.ANY)
    row_w = pl.BlockSpec((tn, width), lambda j, i: (j, 0))
    if joined:
        outs = (jax.ShapeDtypeStruct((chips, 2, rows, dim), BF16),)
        tiles = [pl.BlockSpec((2, 2, rows, tn), lambda j, i: (i, 0, 0, j))]
    else:
        outs = (jax.ShapeDtypeStruct((chips, rows, dim), BF16),) * 2
        tiles = [pl.BlockSpec((2, rows, tn), lambda j, i: (i, 0, j))] * 2
    return order.call(
        functools.partial(back_kernel, joined=joined, base=side * half), 6 + len(far), out_shape=outs, grid=(dim // tn, half),
        in_specs=[hbm, hbm, hbm, row_w, row_w, pl.BlockSpec((width, tn), lambda j, i: (0, j))] + tiles[:len(far)],
        out_specs=tiles, scratch_shapes=[pltpu.VMEM((half, 2 * rows, width), BF16)] * 3 + [pltpu.SemaphoreType.DMA((3, half))],
        compiler_params=params(2, 50),
        cost_estimate=cost(3 * act.size * dim, act, act, w_gate, w_up, w_down, *outs, *outs), name="mlp_back",
    )(d_gate, d_upper, act, w_gate, w_up, w_down, *far)


def wgrad_kernel(core_s, *refs, n, tf, tn, cols):
    lhs, rhs, out, l_buf, r_buf, sems = refs[:n], refs[n:2 * n], *refs[2 * n:]
    i, j, k = pl.program_id(0), pl.program_id(1), pl.program_id(2)
    step = (i * cols + j) * n + k
    slot = lax.rem(step, 2)
    chips = l_buf.shape[1] // 2

    def copies(s, at, p):
        row = pl.multiple_of(lax.div(s, cols * n) * tf, tf)
        col = pl.multiple_of(lax.rem(lax.div(s, n), cols) * tn, tn)
        out = []
        for q, (ref, buf, lanes) in enumerate(((lhs[p], l_buf, pl.ds(row, tf)), (rhs[p], r_buf, pl.ds(col, tn)))):
            if ref.ndim == 4:
                for side in range(2):
                    src = ref.at[:, lax.bitwise_xor(core_s[0], side), :, lanes]
                    out.append(pltpu.make_async_copy(src, buf.at[at, pl.ds(side * chips, chips)], sems.at[q, side, at]))
            else:
                out.append(pltpu.make_async_copy(ref.at[:, :, lanes], buf.at[at], sems.at[q, 0, at]))
        return out

    def fetch(s, at):
        for p in range(n):
            @pl.when(lax.rem(s, n) == p)
            def _(p=p):
                for copy in copies(s, at, p):
                    copy.start()

    @pl.when(step == 0)
    def _():
        fetch(step, slot)

    @pl.when(step + 1 < pl.num_programs(0) * cols * n)
    def _():
        fetch(step + 1, 1 - slot)

    for copy in copies(step, slot, 0):
        copy.wait()
    part = dot_f32(rows_of(l_buf.at[slot]), rows_of(r_buf.at[slot]), 0, 0)
    out[...] = jnp.where(k == 0, part, out[...] + part)


def wgrad_call(order, core, lhs, rhs, tf=1024, tn=1024):
    n = len(lhs)
    rows = lhs[0].shape[-2]
    shards = lhs[0].size // (rows * lhs[0].shape[-1])
    width = rhs[0].shape[-1]
    height = lhs[0].shape[-1]
    cols = width // tn
    out = jax.ShapeDtypeStruct((height, width), F32)
    return order.call(
        functools.partial(wgrad_kernel, n=n, tf=tf, tn=tn, cols=cols), 2 * n, prefetch=1, out_shape=out, grid=(height // tf, cols, n),
        in_specs=[pl.BlockSpec(memory_space=pl.ANY)] * (2 * n), out_specs=pl.BlockSpec((tf, tn), lambda i, j, k, core: (i, j)),
        scratch_shapes=[pltpu.VMEM((2, shards, rows, tf), BF16), pltpu.VMEM((2, shards, rows, tn), BF16), pltpu.SemaphoreType.DMA((2, 2, 2))],
        compiler_params=params(3), cost_estimate=cost(2 * n * shards * rows * height * width, *lhs, *rhs, out), name="wgrad",
    )(core, *lhs, *rhs)


def small_wgrad_kernel(l_ref, r_ref, *refs):
    total = dot_f32(l_ref[...], r_ref[...], 0, 0).reshape(refs[-1].shape)
    for extra in refs[:-1]:
        total += extra[...]
    refs[-1][...] = total


def small_wgrad(order, lhs, rhs, tf=1024, tn=512):
    tokens, rows = lhs.shape
    width = rhs.shape[1]
    out = jax.ShapeDtypeStruct((rows, width), F32)
    return order.call(
        small_wgrad_kernel, 2, out_shape=out, grid=(width // tn, rows // tf),
        in_specs=[pl.BlockSpec((tokens, tf), lambda j, i: (0, i)), pl.BlockSpec((tokens, tn), lambda j, i: (0, j))],
        out_specs=pl.BlockSpec((tf, tn), lambda j, i: (i, j)), compiler_params=params(2, 28),
        cost_estimate=cost(2 * tokens * rows * width, lhs, rhs, out), name="small_wgrad",
    )(lhs, rhs)


def head_wgrad(order, lhs, rhs, hd, far=(), kind=0, earlier=None, tn=1024):
    tokens, width = lhs.shape
    dim = rhs.shape[1]
    heads = width // hd
    per = 2
    plain = pl.BlockSpec((per, hd, tn), lambda j, i: (i, 0, j))
    if far:
        out = jax.ShapeDtypeStruct((heads, 2, hd, dim), F32)
        spec = pl.BlockSpec((per, None, hd, tn), lambda j, i: (i, kind, 0, j))
    else:
        out, spec = jax.ShapeDtypeStruct((heads, hd, dim), F32), plain
    kept = () if earlier is None else (earlier,)
    return order.call(
        small_wgrad_kernel, 2 + len(far), len(kept), out_shape=out, grid=(dim // tn, heads // per),
        in_specs=[pl.BlockSpec((tokens, per * hd), lambda j, i: (0, i)), pl.BlockSpec((tokens, tn), lambda j, i: (0, j))] + [plain] * len(far),
        out_specs=spec, compiler_params=params(2, 28), cost_estimate=cost(2 * tokens * width * dim, lhs, rhs, *far, out), name="head_wgrad",
    )(lhs, rhs, *far, *kept)


def resid_kernel(h_ref, a_own_ref, a_oth_ref, w_own_ref, w_oth_ref, gain_ref, resid_ref, *z_refs, sub):
    for c, z_ref in enumerate(z_refs):
        @pl.when(pl.program_id(0) == c)
        def _(z_ref=z_ref):
            for r in range(0, z_ref.shape[0], sub):
                at = slice(r, r + sub)
                total = dot_f32(a_own_ref[at], w_own_ref[...], 1, 0) + dot_f32(a_oth_ref[at], w_oth_ref[...], 1, 0)
                resid = (h_ref[at].astype(F32) + total).astype(BF16)
                resid_ref[at] = resid
                x_f = resid.astype(F32)
                inv = lax.rsqrt(jnp.mean(x_f * x_f, axis=-1, keepdims=True) + NORM_EPS)
                z_ref[at] = (x_f * inv * (1.0 + gain_ref[...])).astype(BF16)


def resid_call(order, hidden, mix_own, mix_oth, wo_own, wo_oth, gain, size, sub):
    tokens, dim = hidden.shape
    width = mix_own.shape[1]
    chunks = tokens // size
    row = pl.BlockSpec((size, dim), lambda i: (i, 0))
    mix = pl.BlockSpec((size, width), lambda i: (i, 0))
    whole_w = pl.BlockSpec((width, dim), lambda i: (0, 0))
    outs = (jax.ShapeDtypeStruct((tokens, dim), BF16),) + (jax.ShapeDtypeStruct((size, dim), BF16),) * chunks
    return order.call(
        functools.partial(resid_kernel, sub=sub), 6, out_shape=outs, grid=(chunks,),
        in_specs=[row, mix, mix, whole_w, whole_w, pl.BlockSpec((1, dim), lambda i: (0, 0))],
        out_specs=[row] + [pl.BlockSpec((size, dim), lambda i: (0, 0))] * chunks,
        compiler_params=params(1), cost_estimate=cost(4 * tokens * dim * width, hidden, mix_own, mix_oth, wo_own, wo_oth, *outs), name="resid",
    )(hidden, mix_own, mix_oth, wo_own, wo_oth, gain)


def norm_back(x_f, gain_1, d_out):
    inv = lax.rsqrt(jnp.mean(x_f * x_f, axis=-1, keepdims=True) + NORM_EPS)
    unit = x_f * inv
    scaled = d_out * gain_1
    d_x = inv * (scaled - unit * jnp.mean(scaled * unit, axis=-1, keepdims=True))
    return d_x, d_out * unit


def fold_rows(terms):
    rows, dim = terms.shape
    return jnp.sum(terms.reshape(rows // 8, 8, dim), axis=0)


def d_resid_kernel(*refs, n):
    dz_refs = refs[:n]
    x_ref, g_ref, gain_ref, w_own_ref, w_oth_ref, norm_ref, d_ref, own_ref, oth_ref = refs[n:]
    i = pl.program_id(0)

    @pl.when(i == 0)
    def _():
        norm_ref[...] = jnp.zeros_like(norm_ref)

    for c, dz_ref in enumerate(dz_refs):
        @pl.when(i == c)
        def _(dz_ref=dz_ref):
            d_x, terms = norm_back(x_ref[...].astype(F32), 1.0 + gain_ref[...], rows_of(dz_ref).astype(F32))
            norm_ref[...] += fold_rows(terms)
            d_ref[...] = (g_ref[...].astype(F32) + d_x).astype(BF16)
    own_ref[...] = dot_f32(d_ref[...], w_own_ref[...], 1, 1).astype(BF16)
    oth_ref[...] = dot_f32(d_ref[...], w_oth_ref[...], 1, 1).astype(BF16)


def d_resid_call(order, dz, resid, grad_out, gain, wo_own, wo_oth, first, size, earlier):
    tokens, dim = resid.shape
    n = len(dz)
    width = wo_own.shape[0]
    one = [pl.BlockSpec((1, size, dim) if a.ndim == 3 else (size, dim), lambda i, nd=a.ndim: (0,) * nd) for a in dz]
    far = pl.BlockSpec((size, dim), lambda i: (i + first, 0))
    mix = pl.BlockSpec((size, width), lambda i: (i + first, 0))
    whole_w = pl.BlockSpec((width, dim), lambda i: (0, 0))
    outs = (jax.ShapeDtypeStruct((8, dim), F32), jax.ShapeDtypeStruct((tokens, dim), BF16),
            jax.ShapeDtypeStruct((tokens, width), BF16), jax.ShapeDtypeStruct((tokens, width), BF16))
    return order.call(
        functools.partial(d_resid_kernel, n=n), n + 5, len(earlier), out_shape=outs, grid=(n,),
        in_specs=one + [far, far, pl.BlockSpec((1, dim), lambda i: (0, 0)), whole_w, whole_w],
        out_specs=[pl.BlockSpec((8, dim), lambda i: (0, 0)), far, mix, mix],
        compiler_params=params(1, 48), cost_estimate=cost(4 * n * size * dim * width, *dz, wo_own, wo_oth, outs[1]), name="d_resid",
    )(*dz, resid, grad_out, gain, wo_own, wo_oth, *earlier)


def d_hidden_kernel(q_own_ref, q_oth_ref, dkv_ref, x_ref, d_ref, gain_ref, wq_own_ref, wq_oth_ref, wkv_ref, out_ref, norm_ref, *, sub):
    @pl.when(pl.program_id(0) == 0)
    def _():
        norm_ref[...] = jnp.zeros_like(norm_ref)

    folded = 0.0
    for r in range(0, x_ref.shape[0], sub):
        at = slice(r, r + sub)
        d_normed = (dot_f32(q_own_ref[at], wq_own_ref[...], 1, 0) + dot_f32(q_oth_ref[at], wq_oth_ref[...], 1, 0)
                    + dot_f32(dkv_ref[at], wkv_ref[...], 1, 1)).astype(BF16).astype(F32)
        d_x, terms = norm_back(x_ref[at].astype(F32), 1.0 + gain_ref[...], d_normed)
        folded += fold_rows(terms)
        out_ref[at] = (d_ref[at].astype(F32) + d_x).astype(BF16)
    norm_ref[...] += folded


def d_hidden_call(order, dq_own, dq_oth, dkv, hidden, d_resid, gain, wq_own, wq_oth, w_kv, tm, sub):
    tokens, dim = hidden.shape
    width, two_hd = dq_own.shape[1], dkv.shape[1]
    row = pl.BlockSpec((tm, dim), lambda i: (i, 0))
    mix = pl.BlockSpec((tm, width), lambda i: (i, 0))
    whole_w = pl.BlockSpec((width, dim), lambda i: (0, 0))
    outs = (jax.ShapeDtypeStruct((tokens, dim), BF16), jax.ShapeDtypeStruct((8, dim), F32))
    return order.call(
        functools.partial(d_hidden_kernel, sub=sub), 9, out_shape=outs, grid=(tokens // tm,),
        in_specs=[mix, mix, pl.BlockSpec((tm, two_hd), lambda i: (i, 0)), row, row, pl.BlockSpec((1, dim), lambda i: (0, 0)), whole_w, whole_w,
                  pl.BlockSpec((dim, two_hd), lambda i: (0, 0))],
        out_specs=[row, pl.BlockSpec((8, dim), lambda i: (0, 0))],
        compiler_params=params(1), cost_estimate=cost(4 * tokens * dim * (width + two_hd), dq_own, dq_oth, hidden, d_resid, wq_own, wq_oth, *outs), name="d_hidden",
    )(dq_own, dq_oth, dkv, hidden, d_resid, gain, wq_own, wq_oth, w_kv)


def solution(mesh):
    tp_size = mesh.shape["tp"]
    chips = tp_size // 2
    act_spec = P("dp", "tp", None)
    in_specs = (act_spec, act_spec, P("dp"), P("dp"), P(None), P(None, "tp"), P(None, None), P(None, None), P("tp", None), P(None), P(None, "tp"), P(None, "tp"), P("tp", None))
    out_specs = (act_spec, act_spec, P("dp"), P("dp", "tp"), P("dp", None), P("dp", None), P(("dp", "tp"), None), P("dp"), P("dp", "tp"), P("dp", "tp"), P(("dp", "tp"), None))
    same_core = [[2 * c + k for c in range(chips)] for k in range(2)]
    partner = [(i, i ^ 1) for i in range(tp_size)]

    def scatter4(x_part):
        flat = x_part.reshape((-1,) + x_part.shape[2:])
        return lax.psum_scatter(flat, "tp", scatter_dimension=0, tiled=True, axis_index_groups=same_core)

    def gather8(x_loc):
        return lax.all_gather(x_loc, "tp", axis=0, tiled=False)

    def swap(x_loc):
        return lax.ppermute(x_loc, "tp", partner)

    def flip(x_loc, bits):
        return lax.ppermute(x_loc, "tp", [(i, i ^ bits) for i in range(tp_size)])

    def gather4_direct(x_loc, before=None):
        chip = lax.axis_index("tp") // 2
        half = x_loc.shape[0] // 2
        near, far = flip(x_loc, 2), flip(x_loc, 4)
        if before is not None:
            near, far, _ = lax.optimization_barrier((near, far, before))
        low, high = flip(near[:half], 4), flip(far[half:], 2)
        out = jnp.zeros((chips,) + x_loc.shape, x_loc.dtype)
        for k, block in ((0, x_loc), (1, near), (2, far)):
            out = lax.dynamic_update_slice(out, block[None], (chip ^ k, 0, 0))
        out = lax.dynamic_update_slice(out, low[None], (chip ^ 3, 0, 0))
        return lax.dynamic_update_slice(out, high[None], (chip ^ 3, half, 0))

    def local_layer(hidden, grad_out, prefix_len, valid_len, attn_norm, w_query, w_key, w_value, w_out, mlp_norm, w_gate, w_up, w_down):
        batch, rows, dim = hidden.shape
        hd = w_key.shape[1]
        tokens = batch * rows
        assert batch % CHUNKS == 0
        me = lax.axis_index("tp")
        core = lax.rem(me, 2)
        qpos = me * rows + jnp.arange(rows, dtype=jnp.int32)
        shard_pos = jnp.arange(rows, dtype=jnp.int32)[None, :] + (jnp.arange(chips, dtype=jnp.int32) * 2 * rows)[:, None]
        kpos = jnp.concatenate([(shard_pos + core * rows).reshape(-1), (shard_pos + (1 - core) * rows).reshape(-1)])
        cos_t, sin_t = rope_tables(qpos, hd)

        def rope_single(raw_proj):
            return apply_rope(raw_proj, cos_t, sin_t)

        order = Order()
        scalars = (prefix_len, valid_len, core[None])
        attn_gain = attn_norm.astype(F32)
        mlp_gain = mlp_norm.astype(F32)
        wq_own = gather4_direct(w_query.T).reshape(chips * hd, dim)
        normed_flat = rms_norm(hidden, attn_gain).reshape(tokens, dim)
        w_kv = jnp.concatenate([w_key, w_value], axis=1)
        kv_raw = dot_f32(normed_flat, w_kv, 1, 0).reshape(batch, rows, 2 * hd)
        keys, key_pull = jax.vjp(rope_single, kv_raw[..., :hd])
        kv_all = gather8(jnp.concatenate([keys, kv_raw[..., hd:]], axis=-1).astype(BF16))
        wq_oth = swap(wq_own)
        q_own = dot_f32(normed_flat, wq_own, 1, 1)
        q_oth = dot_f32(normed_flat, wq_oth, 1, 1)
        wo_own = gather4_direct(lax.optimization_barrier((w_out, q_own))[0], q_oth).reshape(chips * hd, dim)
        wo_oth = swap(wo_own)
        q_own = q_own.reshape(batch, rows, chips * hd)
        q_oth = q_oth.reshape(batch, rows, chips * hd)
        mix_own, mix_oth, q_own, q_oth = attn_fwd(q_own, q_oth, kv_all, cos_t, sin_t, qpos, kpos, scalars)
        mix_own = mix_own.reshape(tokens, chips * hd)
        mix_oth = mix_oth.reshape(tokens, chips * hd)
        hidden_flat = hidden.reshape(tokens, dim)
        grad_flat = grad_out.reshape(tokens, dim)
        size = tokens // CHUNKS
        resid, *z_parts = resid_call(order, hidden_flat, mix_own, mix_oth, wo_own, wo_oth, mlp_gain[None, :], size, 2 * rows)

        g_all, z_all, acts, far = [], [], [], []
        for c in range(CHUNKS):
            g_all.append(gather8(grad_flat[c * size:(c + 1) * size]).reshape(chips, 2, size, dim))
            z_all.append(gather8(z_parts[c]).reshape(chips, 2, size, dim))
        mlp_sums, d_gated = [None] * CHUNKS, [None] * CHUNKS
        weights = (w_gate, w_up, w_down)
        core_1 = core[None]
        grads = None

        def d_resid_of(first, count, earlier):
            return d_resid_call(order, d_gated[first:first + count], resid, grad_flat, mlp_gain[None, :], wo_own, wo_oth, first, size,
                                () if earlier is None else earlier[1])

        def attn_bwd_of(first, count, d_own, d_oth, earlier):
            per = batch // CHUNKS
            return attn_bwd(order, q_own, q_oth, d_own.reshape(batch, rows, -1), d_oth.reshape(batch, rows, -1), kv_all, cos_t, sin_t, qpos, kpos,
                            scalars, first * per, count * per, () if earlier is None else earlier[2])

        def finish(c):
            joined = c < CHUNKS - 1
            parts = back_call(order, 0, acts[c][1], acts[c][2], acts[c][0], *weights, far[c], joined, chips)
            sums = [scatter4(parts[0])]
            if not joined:
                sums.append(scatter4(parts[1]))
            if joined:
                both = sums[0].reshape(2, size, dim)
                d_gated[c], mlp_sums[c] = both, both[1]
            else:
                d_gated[c], mlp_sums[c] = (a.reshape(size, dim) for a in sums)

        for c in range(CHUNKS):
            if c < CHUNKS - 1:
                d_act = d_act_call(order, core_1, g_all[c], w_down)
                acts.append(act_call(order, core_1, z_all[c], d_act, w_gate, w_up, None))
            else:
                acts.append(act_call(order, core_1, z_all[c], g_all[c], *weights))
            if c > 0:
                finish(c - 1)
            joined = c < CHUNKS - 1
            parts = back_call(order, 1, acts[c][1], acts[c][2], acts[c][0], *weights, (), joined, chips)
            far.append(tuple(swap(a) for a in parts))
        terms, *d_parts = d_resid_of(0, 1, None)
        grads = terms, d_parts, attn_bwd_of(0, 1, d_parts[1], d_parts[2], None)
        finish(CHUNKS - 1)
        hidden_out = (resid.astype(F32) + jnp.concatenate(mlp_sums, axis=0).astype(F32)).astype(BF16).reshape(batch, rows, dim)
        shards = [[a.reshape(2 * chips, size, -1) for a in acts[c]] for c in range(CHUNKS)]
        g_gate = wgrad_call(order, core_1, z_all, [a[1] for a in shards])

        terms, d_resid, d_own, d_oth = d_resid_of(1, CHUNKS - 1, grads)
        g_out_far = swap(head_wgrad(order, mix_oth, d_resid, hd))
        norm_terms, (dq_own, dq_oth, dkv_own, dkv_oth) = grads[0] + terms, attn_bwd_of(1, CHUNKS - 1, d_own, d_oth, grads)
        dq_own = dq_own.reshape(tokens, chips * hd)
        dq_oth = dq_oth.reshape(tokens, chips * hd)
        dkv = scatter4((dkv_own.astype(F32) + swap(dkv_oth).astype(F32)).astype(BF16))
        g_query_far = swap(head_wgrad(order, dq_oth, normed_flat, hd))
        g_heads = head_wgrad(order, mix_own, d_resid, hd, (g_out_far,), 0)
        g_heads = head_wgrad(order, dq_own, normed_flat, hd, (g_query_far,), 1, g_heads)
        g_heads = scatter4(g_heads)
        g_out, g_query = g_heads[0], g_heads[1].T
        d_k_raw = key_pull(dkv[..., :hd].astype(F32))[0]
        dkv = jnp.concatenate([d_k_raw.astype(BF16), dkv[..., hd:]], axis=-1).reshape(tokens, 2 * hd)
        grad_hidden, attn_terms = d_hidden_call(
            order, dq_own, dq_oth, dkv, hidden_flat, d_resid, attn_gain[None, :], wq_own, wq_oth, w_kv, 4 * rows, 2 * rows)
        g_kv = small_wgrad(order, normed_flat, dkv, tf=1024, tn=2 * hd)
        norms = jnp.stack([jnp.sum(attn_terms, axis=0), jnp.sum(norm_terms, axis=0)]).reshape(-1, 2 * hd)
        sums = lax.psum(jnp.concatenate([g_kv, norms], axis=0), "tp")
        g_attn_norm, g_mlp_norm = sums[dim:].reshape(2, dim)
        g_up = wgrad_call(order, core_1, z_all, [a[2] for a in shards])
        g_down = wgrad_call(order, core_1, [a[0] for a in shards], g_all)
        return (hidden_out, grad_hidden.reshape(batch, rows, dim), g_attn_norm, g_query, sums[:dim, :hd], sums[:dim, hd:], g_out, g_mlp_norm, g_gate, g_up, g_down)

    return jax.shard_map(local_layer, mesh=mesh, in_specs=in_specs, out_specs=out_specs, check_vma=False)
```

```python
import functools
import math
import jax
import jax.numpy as jnp
from jax import lax
from jax.experimental import pallas as pl
from jax.experimental.pallas import tpu as pltpu
from jax.sharding import PartitionSpec as P

NORM_EPS = 1e-6
CHUNKS = 3
F32 = jnp.float32
BF16 = jnp.bfloat16
MASKED = -1e30
LARGE = 1 << 17


def rms_norm(x_in, gain):
    x_f = x_in.astype(F32)
    inv_rms = lax.rsqrt(jnp.mean(x_f * x_f, axis=-1, keepdims=True) + NORM_EPS)
    return (x_f * inv_rms * (1.0 + gain)).astype(BF16)


def rope_tables(positions, head_dim):
    half_dim = head_dim // 2
    exponent = jnp.arange(half_dim, dtype=F32) * (2.0 / head_dim)
    inv_freq = jnp.exp(exponent * (-math.log(10000.0)))
    angles = positions.astype(F32)[:, None] * inv_freq[None, :]
    return jnp.cos(angles), jnp.sin(angles)


def apply_rope(x_f, cos_t, sin_t):
    half_dim = x_f.shape[-1] // 2
    first = x_f[..., :half_dim]
    second = x_f[..., half_dim:]
    return jnp.concatenate([first * cos_t - second * sin_t, second * cos_t + first * sin_t], axis=-1)


def dot_f32(lhs, rhs, lhs_dim, rhs_dim):
    return lax.dot_general(lhs, rhs, (((lhs_dim,), (rhs_dim,)), ((), ())), preferred_element_type=F32)


def own_first(kv_ref, core, lo, hi):
    shards = kv_ref.shape[0] // 2
    return jnp.concatenate([kv_ref[2 * c + side, 0, :, lo:hi] for side in (core, 1 - core) for c in range(shards)], axis=0)


def attn_fwd_kernel(prefix_s, valid_s, core_s, q_own_ref, q_oth_ref, kv_ref, cos_ref, sin_ref, qpos_ref, kpos_ref,
                    o_own_ref, o_oth_ref, r_own_ref, r_oth_ref):
    b = pl.program_id(0)
    rows, width = q_own_ref.shape[1:]
    hd = kv_ref.shape[-1] // 2
    half = hd // 2
    heads = width // hd
    scale = hd ** -0.5
    cos_t, sin_t = cos_ref[...], sin_ref[...]
    queries = []
    for src, dst in ((q_own_ref, r_own_ref), (q_oth_ref, r_oth_ref)):
        for n in range(heads):
            first = src[0, :, n * hd:n * hd + half]
            second = src[0, :, n * hd + half:(n + 1) * hd]
            q_1 = ((first * cos_t - second * sin_t).astype(BF16) * scale).astype(BF16)
            q_2 = ((second * cos_t + first * sin_t).astype(BF16) * scale).astype(BF16)
            dst[0, :, n * hd:n * hd + half] = q_1
            dst[0, :, n * hd + half:(n + 1) * hd] = q_2
            queries.append(jnp.concatenate([q_1, q_2], axis=1))
    keys = own_first(kv_ref, core_s[0], 0, hd)
    values = own_first(kv_ref, core_s[0], hd, 2 * hd)
    limit = jnp.minimum(valid_s[b], jnp.maximum(prefix_s[b], qpos_ref[...] + 1))
    visible = kpos_ref[...] < limit
    for side, dst in ((0, o_own_ref), (1, o_oth_ref)):
        query = jnp.concatenate(queries[side * heads:(side + 1) * heads], axis=0)
        scores = dot_f32(query, keys, 1, 1)
        scores = jnp.where(visible, scores, MASKED)
        top = jnp.max(scores, axis=-1, keepdims=True)
        expo = jnp.exp(scores - top)
        inv = 1.0 / jnp.sum(expo, axis=-1, keepdims=True)
        probs = (expo * inv).astype(BF16)
        mixed = dot_f32(probs, values, 1, 0).astype(BF16)
        for n in range(heads):
            dst[0, :, n * hd:(n + 1) * hd] = mixed[n * rows:(n + 1) * rows]


def attn_bwd_kernel(first, prefix_s, valid_s, core_s, q_own_ref, q_oth_ref, g_own_ref, g_oth_ref, kv_ref, cos_ref, sin_ref,
                    qpos_ref, kpos_ref, dq_own_ref, dq_oth_ref, dkv_ref):
    b = pl.program_id(0) + first
    rows, width = q_own_ref.shape[1:]
    hd = kv_ref.shape[-1] // 2
    half = hd // 2
    heads = width // hd
    scale = hd ** -0.5
    cos_t, sin_t = cos_ref[...], sin_ref[...]
    shards = kv_ref.shape[0] // 2
    keys = own_first(kv_ref, core_s[0], 0, hd)
    values = own_first(kv_ref, core_s[0], hd, 2 * hd)
    limit = jnp.minimum(valid_s[b], jnp.maximum(prefix_s[b], qpos_ref[...] + 1))
    visible = kpos_ref[...] < limit
    d_keys, d_values = 0.0, 0.0
    for q_ref, g_ref, dst in ((q_own_ref, g_own_ref, dq_own_ref), (q_oth_ref, g_oth_ref, dq_oth_ref)):
        query = jnp.concatenate([q_ref[0, :, n * hd:(n + 1) * hd] for n in range(heads)], axis=0)
        grad = jnp.concatenate([g_ref[0, :, n * hd:(n + 1) * hd] for n in range(heads)], axis=0)
        scores = dot_f32(keys, query, 1, 1)
        scores = jnp.where(visible, scores, MASKED)
        top = jnp.max(scores, axis=0, keepdims=True)
        expo = jnp.exp(scores - top)
        inv = 1.0 / jnp.sum(expo, axis=0, keepdims=True)
        probs = expo * inv
        d_probs = dot_f32(values, grad, 1, 1)
        delta = jnp.sum(probs * d_probs, axis=0, keepdims=True)
        d_scores = (probs * (d_probs - delta)).astype(BF16)
        d_values = d_values + dot_f32(probs.astype(BF16), grad, 1, 0)
        d_keys = d_keys + dot_f32(d_scores, query, 1, 0)
        d_query = dot_f32(d_scores, keys, 0, 0) * scale
        for n in range(heads):
            g_1 = d_query[n * rows:(n + 1) * rows, :half]
            g_2 = d_query[n * rows:(n + 1) * rows, half:]
            dst[0, :, n * hd:n * hd + half] = (g_1 * cos_t + g_2 * sin_t).astype(BF16)
            dst[0, :, n * hd + half:(n + 1) * hd] = (g_2 * cos_t - g_1 * sin_t).astype(BF16)
    d_keys = d_keys.astype(BF16)
    d_values = d_values.astype(BF16)
    span = kv_ref.shape[2]
    for k, side in enumerate((core_s[0], 1 - core_s[0])):
        for c in range(shards):
            at = (k * shards + c) * span
            dkv_ref[2 * c + side, 0, :, :hd] = d_keys[at:at + span]
            dkv_ref[2 * c + side, 0, :, hd:] = d_values[at:at + span]


def attn_specs(rows, width, shards, two_hd, half):
    q_spec = pl.BlockSpec((1, rows, width), lambda b, *_: (b, 0, 0))
    kv_spec = pl.BlockSpec((shards, 1, rows, two_hd), lambda b, *_: (0, b, 0, 0))
    tab_spec = pl.BlockSpec((rows, half), lambda b, *_: (0, 0))
    return q_spec, kv_spec, tab_spec


def whole(shape):
    return pl.BlockSpec(shape, lambda b, *_: tuple(0 for _ in shape))


def attn_fwd(q_own, q_oth, kv_all, cos_t, sin_t, qpos, kpos, scalars):
    batch, rows, width = q_own.shape
    shards, two_hd = kv_all.shape[0], kv_all.shape[3]
    q_spec, kv_spec, tab_spec = attn_specs(rows, width, shards, two_hd, two_hd // 4)
    heads = width * 2 // two_hd
    out = jax.ShapeDtypeStruct((batch, rows, width), BF16)
    qpos_col = jnp.tile(qpos, heads)[:, None]
    n_keys = kpos.shape[0]
    flops = 2 * 2 * batch * rows * 2 * width * n_keys
    return pl.pallas_call(
        attn_fwd_kernel,
        out_shape=(out, out, out, out),
        grid_spec=pltpu.PrefetchScalarGridSpec(
            num_scalar_prefetch=3, grid=(batch,),
            in_specs=[q_spec, q_spec, kv_spec, tab_spec, tab_spec, whole((heads * rows, 1)), whole((1, n_keys))],
            out_specs=[q_spec] * 4),
        compiler_params=pltpu.CompilerParams(dimension_semantics=("arbitrary",), vmem_limit_bytes=30 << 20),
        cost_estimate=pl.CostEstimate(flops=flops, bytes_accessed=batch * rows * width * 16 + kv_all.size * 2, transcendentals=batch * rows * heads * 2 * n_keys),
        name="attn_fwd",
    )(*scalars, q_own, q_oth, kv_all, cos_t, sin_t, qpos_col, kpos[None, :])


def attn_bwd(order, q_own, q_oth, g_own, g_oth, kv_all, cos_t, sin_t, qpos, kpos, scalars, first, count, earlier):
    batch, rows, width = q_own.shape
    shards, two_hd = kv_all.shape[0], kv_all.shape[3]
    tab_spec = pl.BlockSpec((rows, two_hd // 4), lambda b, *_: (0, 0))
    q_spec = pl.BlockSpec((1, rows, width), lambda b, *_: (b + first, 0, 0))
    kv_spec = pl.BlockSpec((shards, 1, rows, two_hd), lambda b, *_: (0, b + first, 0, 0))
    heads = width * 2 // two_hd
    out = jax.ShapeDtypeStruct((batch, rows, width), BF16)
    kv_out = jax.ShapeDtypeStruct(kv_all.shape, BF16)
    qpos_row = jnp.tile(qpos, heads)[None, :]
    n_keys = kpos.shape[0]
    flops = 2 * 5 * count * rows * 2 * width * n_keys
    return order.call(
        functools.partial(attn_bwd_kernel, first), 9, len(earlier), prefetch=3,
        out_shape=(out, out, kv_out), grid=(count,),
        in_specs=[q_spec, q_spec, q_spec, q_spec, kv_spec, tab_spec, tab_spec, whole((1, heads * rows)), whole((n_keys, 1))],
        out_specs=[q_spec, q_spec, kv_spec],
        compiler_params=pltpu.CompilerParams(dimension_semantics=("arbitrary",), vmem_limit_bytes=30 << 20),
        cost_estimate=pl.CostEstimate(flops=flops, bytes_accessed=count * rows * width * 12 + kv_all.size * 4, transcendentals=count * rows * heads * 2 * n_keys),
        name="attn_bwd",
    )(*scalars, q_own, q_oth, g_own, g_oth, kv_all, cos_t, sin_t, qpos_row, kpos[:, None], *earlier)


class Order:
    def __init__(self):
        self.last = None

    def call(self, kernel, n_in, n_kept=0, *, in_specs, out_specs, out_shape, grid, prefetch=0, scratch_shapes=(), **options):
        def run(*args):
            deps = () if self.last is None or any(self.last is a for a in args) else (self.last,)
            args = args[:prefetch] + tuple(pltpu.with_memory_space_constraint(a, pltpu.HBM) if a.size >= LARGE else a for a in args[prefetch:])
            n_args = prefetch + n_in

            def body(*refs):
                kernel(*refs[:n_args], *refs[n_args + n_kept + len(deps):])

            single = not isinstance(out_specs, (list, tuple))
            n_out = 1 if single else len(out_specs)
            shapes = [pltpu.HBM(o.shape, o.dtype) if o.size >= LARGE else o for o in ([out_shape] if single else out_shape)]
            out = pl.pallas_call(
                body, out_shape=shapes[0] if single else shapes,
                grid_spec=pltpu.PrefetchScalarGridSpec(
                    num_scalar_prefetch=prefetch, grid=grid, scratch_shapes=scratch_shapes, out_specs=out_specs,
                    in_specs=in_specs + [pl.BlockSpec(memory_space=pl.ANY)] * (n_kept + len(deps))),
                input_output_aliases={n_args + k: n_out - n_kept + k for k in range(n_kept)},
                **options)(*args, *deps)
            self.last = out[0] if isinstance(out, (tuple, list)) else out
            return out

        return run


def params(steps, limit=56):
    return pltpu.CompilerParams(dimension_semantics=("arbitrary",) * steps, vmem_limit_bytes=limit << 20)


def cost(flops, *arrays):
    return pl.CostEstimate(flops=flops, bytes_accessed=sum(a.size * a.dtype.itemsize for a in arrays), transcendentals=0)


def rows_of(ref):
    return ref[...].reshape(-1, ref.shape[-1])


def raw_spec(shape):
    return pl.BlockSpec((2, 1) + shape[2:], lambda j, i, core: (lax.rem(i, 2), lax.bitwise_xor(core[0], lax.div(i, 2)), 0, 0))


def d_act_kernel(core_s, g_ref, wd_ref, out_ref):
    out_ref[...] = dot_f32(rows_of(g_ref), wd_ref[...], 1, 1).astype(BF16)


def d_act_call(order, core, g_all, w_down, tn=1024):
    chips, _, rows, dim = g_all.shape
    width = w_down.shape[0]
    out = jax.ShapeDtypeStruct((chips * 2 * rows, width), BF16)
    return order.call(
        d_act_kernel, 2, prefetch=1, out_shape=out, grid=(width // tn, chips),
        in_specs=[raw_spec(g_all.shape), pl.BlockSpec((tn, dim), lambda j, i, core: (j, 0))],
        out_specs=pl.BlockSpec((2 * rows, tn), lambda j, i, core: (i, j)), compiler_params=params(2),
        cost_estimate=cost(2 * g_all.size * width, g_all, w_down, out), name="d_act",
    )(core, g_all, w_down)


def act_kernel(core_s, z_ref, g_ref, wg_ref, wu_ref, *refs, sub):
    c_1 = math.sqrt(2.0 / math.pi)
    c_3 = 0.044715 * c_1
    act_ref, dg_ref, du_ref = refs[-3:]
    z_in = rows_of(z_ref)
    for j in range(0, wg_ref.shape[1], sub):
        gate = dot_f32(z_in, wg_ref[:, j:j + sub], 1, 0)
        upper = dot_f32(z_in, wu_ref[:, j:j + sub], 1, 0)
        if len(refs) == 4:
            d_act = dot_f32(rows_of(g_ref), refs[0][j:j + sub, :], 1, 1).astype(BF16).astype(F32)
        else:
            d_act = g_ref[:, j:j + sub].astype(F32)
        square = gate * gate
        half = 0.5 * jnp.tanh(gate * (c_3 * square + c_1)) + 0.5
        gelu = gate * half
        act_ref[:, j:j + sub] = (gelu * upper).astype(BF16)
        du_ref[:, j:j + sub] = (d_act * gelu).astype(BF16)
        slope = half + gelu * (1.0 - half) * (6.0 * c_3 * square + 2.0 * c_1)
        dg_ref[:, j:j + sub] = (d_act * upper * slope).astype(BF16)


def act_call(order, core, z_all, g_all, w_gate, w_up, w_down, tn=512, sub=256):
    chips, _, rows, dim = z_all.shape
    width = w_gate.shape[1]
    out = jax.ShapeDtypeStruct((chips * 2 * rows, width), BF16)
    raw = raw_spec(z_all.shape)
    col = pl.BlockSpec((dim, tn), lambda j, i, core: (0, j))
    tile = pl.BlockSpec((2 * rows, tn), lambda j, i, core: (i, j))
    args = (z_all, g_all, w_gate, w_up) + (() if w_down is None else (w_down,))
    specs = [raw, tile if w_down is None else raw, col, col] + ([] if w_down is None else [pl.BlockSpec((tn, dim), lambda j, i, core: (j, 0))])
    return order.call(
        functools.partial(act_kernel, sub=sub), len(args), prefetch=1, out_shape=(out, out, out), grid=(width // tn, chips),
        in_specs=specs, out_specs=[tile] * 3, compiler_params=params(2),
        cost_estimate=cost(2 * (len(args) - 2) * z_all.size * width, *args, out, out, out), name="mlp_act",
    )(core, *args)


def back_kernel(*refs, terms, joined, n_far, base, tn):
    n = len(terms)
    lhs, rhs, far, out = refs[:n], refs[n:2 * n], refs[2 * n:2 * n + n_far], refs[2 * n + n_far]
    l_bufs, r_bufs, (l_sems, r_sems) = refs[2 * n + n_far + 1:][:n], refs[3 * n + n_far + 1:][:n], refs[4 * n + n_far + 1:]
    j, i = pl.program_id(0), pl.program_id(1)
    blocks, rows = l_bufs[0].shape[:2]

    def left(p, at):
        return pltpu.make_async_copy(lhs[p].at[pl.ds((base + at) * rows, rows)], l_bufs[p].at[at], l_sems.at[p, at])

    def right(p, tile):
        cols = pl.ds(pl.multiple_of(tile * tn, tn), tn)
        src = rhs[p].at[:, cols] if terms[p][0] == 0 else rhs[p].at[cols]
        return pltpu.make_async_copy(src, r_bufs[p].at[lax.rem(tile, 2)], r_sems.at[p, lax.rem(tile, 2)])

    @pl.when((j == 0) & (i == 0))
    def _():
        for p in range(n):
            right(p, 0).start()
            left(p, 0).start()
        for at in range(1, blocks):
            for p in range(n):
                left(p, at).start()

    @pl.when((i == blocks - 1) & (j + 1 < pl.num_programs(0)))
    def _():
        for p in range(n):
            right(p, j + 1).start()

    def compute(ready):
        totals = {}
        for p, (dim, kind) in enumerate(terms):
            ready(p)
            part = dot_f32(l_bufs[p][i], r_bufs[p][lax.rem(j, 2)], 1, dim)
            totals[kind] = totals[kind] + part if kind in totals else part
        for kind, total in totals.items():
            at = (slice(None), kind) if joined else (slice(None),)
            total = total.reshape(out[at].shape)
            if far:
                total += far[0][at].astype(F32)
            out[at] = total.astype(BF16)

    @pl.when(j == 0)
    def _():
        def ready(p):
            @pl.when(i == 0)
            def _():
                right(p, 0).wait()

            left(p, i).wait()

        compute(ready)

    @pl.when(j > 0)
    def _():
        @pl.when(i == 0)
        def _():
            for p in range(n):
                right(p, j).wait()

        compute(lambda p: None)


def back_call(order, side, lhs, rhs, terms, far, chips, tn=512):
    dim = rhs[0].shape[0 if terms[0][0] else 1]
    rows = lhs[0].shape[0] // (2 * chips)
    half, n = chips // 2, len(terms)
    kinds = sorted({kind for _, kind in terms})
    joined = len(kinds) == 2
    hbm = pl.BlockSpec(memory_space=pl.ANY)
    both = pl.BlockSpec((2, 2, rows, tn), lambda j, i: (i, 0, 0, j))
    out = jax.ShapeDtypeStruct((chips, 2, rows, dim) if joined else (chips, rows, dim), BF16)
    far_spec = both if joined else pl.BlockSpec((2, None, rows, tn), lambda j, i: (i, kinds[0], 0, j))
    depth = lhs[0].shape[1]
    return order.call(
        functools.partial(back_kernel, terms=terms, joined=joined, n_far=len(far), base=side * half, tn=tn), 2 * n + len(far), out_shape=out,
        grid=(dim // tn, half), in_specs=[hbm] * (2 * n) + [far_spec] * len(far),
        out_specs=both if joined else pl.BlockSpec((2, rows, tn), lambda j, i: (i, 0, j)),
        scratch_shapes=[pltpu.VMEM((half, 2 * rows, depth), BF16)] * n
        + [pltpu.VMEM((2, depth, tn) if d == 0 else (2, tn, depth), BF16) for d, _ in terms]
        + [pltpu.SemaphoreType.DMA((n, half)), pltpu.SemaphoreType.DMA((n, 2))],
        compiler_params=params(2, 54),
        cost_estimate=cost(n * lhs[0].size * dim, *lhs, *rhs, out), name="mlp_back",
    )(*lhs, *rhs, *far)


def wgrad_kernel(core_s, *refs, n, tf, tn, cols, first):
    lhs, rhs, out, l_buf, r_buf, sems = refs[:n], refs[n:2 * n], *refs[2 * n:]
    i, j, k = pl.program_id(0), pl.program_id(1), pl.program_id(2)
    step = (i * cols + j) * n + k
    slot = lax.rem(step, 2)
    chips = l_buf.shape[1] // 2

    def copies(s, at, p):
        row = pl.multiple_of((lax.div(s, cols * n) + first) * tf, tf)
        col = pl.multiple_of(lax.rem(lax.div(s, n), cols) * tn, tn)
        out = []
        for q, (ref, buf, lanes) in enumerate(((lhs[p], l_buf, pl.ds(row, tf)), (rhs[p], r_buf, pl.ds(col, tn)))):
            if ref.ndim == 4:
                for side in range(2):
                    src = ref.at[:, lax.bitwise_xor(core_s[0], side), :, lanes]
                    out.append(pltpu.make_async_copy(src, buf.at[at, pl.ds(side * chips, chips)], sems.at[q, side, at]))
            else:
                out.append(pltpu.make_async_copy(ref.at[:, :, lanes], buf.at[at], sems.at[q, 0, at]))
        return out

    def fetch(s, at):
        for p in range(n):
            @pl.when(lax.rem(s, n) == p)
            def _(p=p):
                for copy in copies(s, at, p):
                    copy.start()

    @pl.when(step == 0)
    def _():
        fetch(step, slot)

    @pl.when(step + 1 < pl.num_programs(0) * cols * n)
    def _():
        fetch(step + 1, 1 - slot)

    for copy in copies(step, slot, 0):
        copy.wait()
    part = dot_f32(rows_of(l_buf.at[slot]), rows_of(r_buf.at[slot]), 0, 0)
    out[...] = jnp.where(k == 0, part, out[...] + part)


def wgrad_call(order, core, lhs, rhs, tf=1024, tn=1024, tiles=None, earlier=None):
    n = len(lhs)
    rows = lhs[0].shape[-2]
    shards = lhs[0].size // (rows * lhs[0].shape[-1])
    width = rhs[0].shape[-1]
    height = lhs[0].shape[-1]
    cols = width // tn
    first, last = tiles or (0, height // tf)
    kept = () if earlier is None else (earlier,)
    out = jax.ShapeDtypeStruct((height, width), F32)
    return order.call(
        functools.partial(wgrad_kernel, n=n, tf=tf, tn=tn, cols=cols, first=first), 2 * n, len(kept), prefetch=1, out_shape=out, grid=(last - first, cols, n),
        in_specs=[pl.BlockSpec(memory_space=pl.ANY)] * (2 * n), out_specs=pl.BlockSpec((tf, tn), lambda i, j, k, core: (i + first, j)),
        scratch_shapes=[pltpu.VMEM((2, shards, rows, tf), BF16), pltpu.VMEM((2, shards, rows, tn), BF16), pltpu.SemaphoreType.DMA((2, 2, 2))],
        compiler_params=params(3), cost_estimate=cost(2 * n * shards * rows * height * width, *lhs, *rhs, out), name="wgrad",
    )(core, *lhs, *rhs, *kept)


def small_wgrad_kernel(l_ref, r_ref, *refs):
    total = dot_f32(l_ref[...], r_ref[...], 0, 0).reshape(refs[-1].shape)
    for extra in refs[:-1]:
        total += extra[...]
    refs[-1][...] = total


def small_wgrad(order, lhs, rhs, tf=1024, tn=512):
    tokens, rows = lhs.shape
    width = rhs.shape[1]
    out = jax.ShapeDtypeStruct((rows, width), F32)
    return order.call(
        small_wgrad_kernel, 2, out_shape=out, grid=(width // tn, rows // tf),
        in_specs=[pl.BlockSpec((tokens, tf), lambda j, i: (0, i)), pl.BlockSpec((tokens, tn), lambda j, i: (0, j))],
        out_specs=pl.BlockSpec((tf, tn), lambda j, i: (i, j)), compiler_params=params(2, 28),
        cost_estimate=cost(2 * tokens * rows * width, lhs, rhs, out), name="small_wgrad",
    )(lhs, rhs)


def head_wgrad(order, lhs, rhs, hd, far=(), kind=0, earlier=None, tn=1024):
    tokens, width = lhs.shape
    dim = rhs.shape[1]
    heads = width // hd
    per = 2
    plain = pl.BlockSpec((per, hd, tn), lambda j, i: (i, 0, j))
    if far:
        out = jax.ShapeDtypeStruct((heads, 2, hd, dim), F32)
        spec = pl.BlockSpec((per, None, hd, tn), lambda j, i: (i, kind, 0, j))
    else:
        out, spec = jax.ShapeDtypeStruct((heads, hd, dim), F32), plain
    kept = () if earlier is None else (earlier,)
    return order.call(
        small_wgrad_kernel, 2 + len(far), len(kept), out_shape=out, grid=(dim // tn, heads // per),
        in_specs=[pl.BlockSpec((tokens, per * hd), lambda j, i: (0, i)), pl.BlockSpec((tokens, tn), lambda j, i: (0, j))] + [plain] * len(far),
        out_specs=spec, compiler_params=params(2, 28), cost_estimate=cost(2 * tokens * width * dim, lhs, rhs, *far, out), name="head_wgrad",
    )(lhs, rhs, *far, *kept)


def resid_kernel(h_ref, a_own_ref, a_oth_ref, w_own_ref, w_oth_ref, gain_ref, resid_ref, *z_refs, sub):
    for c, z_ref in enumerate(z_refs):
        @pl.when(pl.program_id(0) == c)
        def _(z_ref=z_ref):
            for r in range(0, z_ref.shape[0], sub):
                at = slice(r, r + sub)
                total = dot_f32(a_own_ref[at], w_own_ref[...], 1, 0) + dot_f32(a_oth_ref[at], w_oth_ref[...], 1, 0)
                resid = (h_ref[at].astype(F32) + total).astype(BF16)
                resid_ref[at] = resid
                x_f = resid.astype(F32)
                inv = lax.rsqrt(jnp.mean(x_f * x_f, axis=-1, keepdims=True) + NORM_EPS)
                z_ref[at] = (x_f * inv * (1.0 + gain_ref[...])).astype(BF16)


def resid_call(order, hidden, mix_own, mix_oth, wo_own, wo_oth, gain, size, sub):
    tokens, dim = hidden.shape
    width = mix_own.shape[1]
    chunks = tokens // size
    row = pl.BlockSpec((size, dim), lambda i: (i, 0))
    mix = pl.BlockSpec((size, width), lambda i: (i, 0))
    whole_w = pl.BlockSpec((width, dim), lambda i: (0, 0))
    outs = (jax.ShapeDtypeStruct((tokens, dim), BF16),) + (jax.ShapeDtypeStruct((size, dim), BF16),) * chunks
    return order.call(
        functools.partial(resid_kernel, sub=sub), 6, out_shape=outs, grid=(chunks,),
        in_specs=[row, mix, mix, whole_w, whole_w, pl.BlockSpec((1, dim), lambda i: (0, 0))],
        out_specs=[row] + [pl.BlockSpec((size, dim), lambda i: (0, 0))] * chunks,
        compiler_params=params(1), cost_estimate=cost(4 * tokens * dim * width, hidden, mix_own, mix_oth, wo_own, wo_oth, *outs), name="resid",
    )(hidden, mix_own, mix_oth, wo_own, wo_oth, gain)


def norm_back(x_f, gain_1, d_out):
    inv = lax.rsqrt(jnp.mean(x_f * x_f, axis=-1, keepdims=True) + NORM_EPS)
    unit = x_f * inv
    scaled = d_out * gain_1
    d_x = inv * (scaled - unit * jnp.mean(scaled * unit, axis=-1, keepdims=True))
    return d_x, d_out * unit


def fold_rows(terms):
    rows, dim = terms.shape
    return jnp.sum(terms.reshape(rows // 8, 8, dim), axis=0)


def d_resid_kernel(*refs, n):
    dz_refs = refs[:n]
    x_ref, g_ref, gain_ref, w_own_ref, w_oth_ref, norm_ref, d_ref, own_ref, oth_ref = refs[n:]
    i = pl.program_id(0)

    @pl.when(i == 0)
    def _():
        norm_ref[...] = jnp.zeros_like(norm_ref)

    for c, dz_ref in enumerate(dz_refs):
        @pl.when(i == c)
        def _(dz_ref=dz_ref):
            d_x, terms = norm_back(x_ref[...].astype(F32), 1.0 + gain_ref[...], rows_of(dz_ref).astype(F32))
            norm_ref[...] += fold_rows(terms)
            d_ref[...] = (g_ref[...].astype(F32) + d_x).astype(BF16)
    own_ref[...] = dot_f32(d_ref[...], w_own_ref[...], 1, 1).astype(BF16)
    oth_ref[...] = dot_f32(d_ref[...], w_oth_ref[...], 1, 1).astype(BF16)


def d_resid_call(order, dz, resid, grad_out, gain, wo_own, wo_oth, first, size, earlier):
    tokens, dim = resid.shape
    n = len(dz)
    width = wo_own.shape[0]
    one = [pl.BlockSpec((1, size, dim) if a.ndim == 3 else (size, dim), lambda i, nd=a.ndim: (0,) * nd) for a in dz]
    far = pl.BlockSpec((size, dim), lambda i: (i + first, 0))
    mix = pl.BlockSpec((size, width), lambda i: (i + first, 0))
    whole_w = pl.BlockSpec((width, dim), lambda i: (0, 0))
    outs = (jax.ShapeDtypeStruct((8, dim), F32), jax.ShapeDtypeStruct((tokens, dim), BF16),
            jax.ShapeDtypeStruct((tokens, width), BF16), jax.ShapeDtypeStruct((tokens, width), BF16))
    return order.call(
        functools.partial(d_resid_kernel, n=n), n + 5, len(earlier), out_shape=outs, grid=(n,),
        in_specs=one + [far, far, pl.BlockSpec((1, dim), lambda i: (0, 0)), whole_w, whole_w],
        out_specs=[pl.BlockSpec((8, dim), lambda i: (0, 0)), far, mix, mix],
        compiler_params=params(1, 48), cost_estimate=cost(4 * n * size * dim * width, *dz, wo_own, wo_oth, outs[1]), name="d_resid",
    )(*dz, resid, grad_out, gain, wo_own, wo_oth, *earlier)


def d_hidden_kernel(q_own_ref, q_oth_ref, dkv_ref, x_ref, d_ref, gain_ref, wq_own_ref, wq_oth_ref, wkv_ref, out_ref, norm_ref, *, sub):
    @pl.when(pl.program_id(0) == 0)
    def _():
        norm_ref[...] = jnp.zeros_like(norm_ref)

    folded = 0.0
    for r in range(0, x_ref.shape[0], sub):
        at = slice(r, r + sub)
        d_normed = (dot_f32(q_own_ref[at], wq_own_ref[...], 1, 0) + dot_f32(q_oth_ref[at], wq_oth_ref[...], 1, 0)
                    + dot_f32(dkv_ref[at], wkv_ref[...], 1, 1)).astype(BF16).astype(F32)
        d_x, terms = norm_back(x_ref[at].astype(F32), 1.0 + gain_ref[...], d_normed)
        folded += fold_rows(terms)
        out_ref[at] = (d_ref[at].astype(F32) + d_x).astype(BF16)
    norm_ref[...] += folded


def d_hidden_call(order, dq_own, dq_oth, dkv, hidden, d_resid, gain, wq_own, wq_oth, w_kv, tm, sub):
    tokens, dim = hidden.shape
    width, two_hd = dq_own.shape[1], dkv.shape[1]
    row = pl.BlockSpec((tm, dim), lambda i: (i, 0))
    mix = pl.BlockSpec((tm, width), lambda i: (i, 0))
    whole_w = pl.BlockSpec((width, dim), lambda i: (0, 0))
    outs = (jax.ShapeDtypeStruct((tokens, dim), BF16), jax.ShapeDtypeStruct((8, dim), F32))
    return order.call(
        functools.partial(d_hidden_kernel, sub=sub), 9, out_shape=outs, grid=(tokens // tm,),
        in_specs=[mix, mix, pl.BlockSpec((tm, two_hd), lambda i: (i, 0)), row, row, pl.BlockSpec((1, dim), lambda i: (0, 0)), whole_w, whole_w,
                  pl.BlockSpec((dim, two_hd), lambda i: (0, 0))],
        out_specs=[row, pl.BlockSpec((8, dim), lambda i: (0, 0))],
        compiler_params=params(1), cost_estimate=cost(4 * tokens * dim * (width + two_hd), dq_own, dq_oth, hidden, d_resid, wq_own, wq_oth, *outs), name="d_hidden",
    )(dq_own, dq_oth, dkv, hidden, d_resid, gain, wq_own, wq_oth, w_kv)


def solution(mesh):
    tp_size = mesh.shape["tp"]
    chips = tp_size // 2
    act_spec = P("dp", "tp", None)
    in_specs = (act_spec, act_spec, P("dp"), P("dp"), P(None), P(None, "tp"), P(None, None), P(None, None), P("tp", None), P(None), P(None, "tp"), P(None, "tp"), P("tp", None))
    out_specs = (act_spec, act_spec, P("dp"), P("dp", "tp"), P("dp", None), P("dp", None), P(("dp", "tp"), None), P("dp"), P("dp", "tp"), P("dp", "tp"), P(("dp", "tp"), None))
    same_core = [[2 * c + k for c in range(chips)] for k in range(2)]
    partner = [(i, i ^ 1) for i in range(tp_size)]

    def scatter4(x_part):
        flat = x_part.reshape((-1,) + x_part.shape[2:])
        return lax.psum_scatter(flat, "tp", scatter_dimension=0, tiled=True, axis_index_groups=same_core)

    def gather8(x_loc):
        return lax.all_gather(x_loc, "tp", axis=0, tiled=False)

    def swap(x_loc):
        return lax.ppermute(x_loc, "tp", partner)

    def flip(x_loc, bits):
        return lax.ppermute(x_loc, "tp", [(i, i ^ bits) for i in range(tp_size)])

    def gather4_direct(x_loc, before=None):
        chip = lax.axis_index("tp") // 2
        half = x_loc.shape[0] // 2
        near, far = flip(x_loc, 2), flip(x_loc, 4)
        if before is not None:
            near, far, _ = lax.optimization_barrier((near, far, before))
        low, high = flip(near[:half], 4), flip(far[half:], 2)
        out = jnp.zeros((chips,) + x_loc.shape, x_loc.dtype)
        for k, block in ((0, x_loc), (1, near), (2, far)):
            out = lax.dynamic_update_slice(out, block[None], (chip ^ k, 0, 0))
        out = lax.dynamic_update_slice(out, low[None], (chip ^ 3, 0, 0))
        return lax.dynamic_update_slice(out, high[None], (chip ^ 3, half, 0))

    def local_layer(hidden, grad_out, prefix_len, valid_len, attn_norm, w_query, w_key, w_value, w_out, mlp_norm, w_gate, w_up, w_down):
        batch, rows, dim = hidden.shape
        hd = w_key.shape[1]
        tokens = batch * rows
        assert batch % CHUNKS == 0
        me = lax.axis_index("tp")
        core = lax.rem(me, 2)
        qpos = me * rows + jnp.arange(rows, dtype=jnp.int32)
        shard_pos = jnp.arange(rows, dtype=jnp.int32)[None, :] + (jnp.arange(chips, dtype=jnp.int32) * 2 * rows)[:, None]
        kpos = jnp.concatenate([(shard_pos + core * rows).reshape(-1), (shard_pos + (1 - core) * rows).reshape(-1)])
        cos_t, sin_t = rope_tables(qpos, hd)

        def rope_single(raw_proj):
            return apply_rope(raw_proj, cos_t, sin_t)

        order = Order()
        scalars = (prefix_len, valid_len, core[None])
        attn_gain = attn_norm.astype(F32)
        mlp_gain = mlp_norm.astype(F32)
        wq_own = gather4_direct(w_query.T).reshape(chips * hd, dim)
        normed_flat = rms_norm(hidden, attn_gain).reshape(tokens, dim)
        w_kv = jnp.concatenate([w_key, w_value], axis=1)
        kv_raw = dot_f32(normed_flat, w_kv, 1, 0).reshape(batch, rows, 2 * hd)
        keys, key_pull = jax.vjp(rope_single, kv_raw[..., :hd])
        kv_all = gather8(jnp.concatenate([keys, kv_raw[..., hd:]], axis=-1).astype(BF16))
        wq_oth = swap(wq_own)
        q_own = dot_f32(normed_flat, wq_own, 1, 1)
        q_oth = dot_f32(normed_flat, wq_oth, 1, 1)
        wo_own = gather4_direct(w_out, (q_own, q_oth)).reshape(chips * hd, dim)
        wo_oth = swap(wo_own)
        q_own = q_own.reshape(batch, rows, chips * hd)
        q_oth = q_oth.reshape(batch, rows, chips * hd)
        mix_own, mix_oth, q_own, q_oth = attn_fwd(q_own, q_oth, kv_all, cos_t, sin_t, qpos, kpos, scalars)
        mix_own = mix_own.reshape(tokens, chips * hd)
        mix_oth = mix_oth.reshape(tokens, chips * hd)
        hidden_flat = hidden.reshape(tokens, dim)
        grad_flat = grad_out.reshape(tokens, dim)
        size = tokens // CHUNKS
        resid, *z_parts = resid_call(order, hidden_flat, mix_own, mix_oth, wo_own, wo_oth, mlp_gain[None, :], size, 2 * rows)

        g_all, z_all, acts, far = [], [], [], []
        for c in range(CHUNKS):
            g_all.append(gather8(grad_flat[c * size:(c + 1) * size]).reshape(chips, 2, size, dim))
            z_all.append(gather8(z_parts[c]).reshape(chips, 2, size, dim))
        mlp_sums, d_gated = [None] * CHUNKS, [None] * CHUNKS
        weights = (w_gate, w_up, w_down)
        core_1 = core[None]
        grads = None

        def d_resid_of(first, count, earlier):
            return d_resid_call(order, d_gated[first:first + count], resid, grad_flat, mlp_gain[None, :], wo_own, wo_oth, first, size,
                                () if earlier is None else earlier[1])

        def attn_bwd_of(first, count, d_own, d_oth, earlier):
            per = batch // CHUNKS
            return attn_bwd(order, q_own, q_oth, d_own.reshape(batch, rows, -1), d_oth.reshape(batch, rows, -1), kv_all, cos_t, sin_t, qpos, kpos,
                            scalars, first * per, count * per, () if earlier is None else earlier[2])

        d_z_terms, mlp_terms = ((1, 0), (1, 0)), ((0, 1),)

        def back_both(c, side, far):
            return back_call(order, side, (acts[c][1], acts[c][2], acts[c][0]), weights, d_z_terms + mlp_terms, far, chips)

        def finish(c):
            both = back_both(c, 0, (far[c],))
            both = scatter4(both).reshape(2, size, dim)
            d_gated[c], mlp_sums[c] = both, both[1]

        def finish_last(c):
            part = back_call(order, 0, acts[c][1:], weights[:2], d_z_terms, (far[c],), chips)
            d_gated[c] = scatter4(part).reshape(size, dim)
            part = back_call(order, 0, acts[c][:1], weights[2:], mlp_terms, (far[c],), chips)
            mlp_sums[c] = scatter4(part).reshape(size, dim)

        for c in range(CHUNKS):
            if c < CHUNKS - 1:
                d_act = d_act_call(order, core_1, g_all[c], w_down)
                acts.append(act_call(order, core_1, z_all[c], d_act, w_gate, w_up, None))
            else:
                acts.append(act_call(order, core_1, z_all[c], g_all[c], *weights))
            if c > 0:
                finish(c - 1)
            far.append(swap(back_both(c, 1, ())))
        terms, *d_parts = d_resid_of(0, 1, None)
        grads = terms, d_parts, attn_bwd_of(0, 1, d_parts[1], d_parts[2], None)
        finish_last(CHUNKS - 1)
        hidden_out = (resid.astype(F32) + jnp.concatenate(mlp_sums, axis=0).astype(F32)).astype(BF16).reshape(batch, rows, dim)
        shards = [[a.reshape(2 * chips, size, -1) for a in acts[c]] for c in range(CHUNKS)]
        g_gate = wgrad_call(order, core_1, z_all, [a[1] for a in shards], tiles=(0, 1))

        terms, d_resid, d_own, d_oth = d_resid_of(1, CHUNKS - 1, grads)
        g_out_far = swap(head_wgrad(order, mix_oth, d_resid, hd))
        norm_terms, (dq_own, dq_oth, dkv) = grads[0] + terms, attn_bwd_of(1, CHUNKS - 1, d_own, d_oth, grads)
        dq_own = dq_own.reshape(tokens, chips * hd)
        dq_oth = dq_oth.reshape(tokens, chips * hd)
        dkv = lax.psum_scatter(dkv.reshape(tp_size * batch, rows, 2 * hd), "tp", scatter_dimension=0, tiled=True)
        g_query_far = swap(head_wgrad(order, dq_oth, normed_flat, hd))
        g_heads = head_wgrad(order, mix_own, d_resid, hd, (g_out_far,), 0)
        g_heads = head_wgrad(order, dq_own, normed_flat, hd, (g_query_far,), 1, g_heads)
        g_heads = scatter4(g_heads)
        g_out, g_query = g_heads[0], g_heads[1].T
        d_k_raw = key_pull(dkv[..., :hd].astype(F32))[0]
        dkv = jnp.concatenate([d_k_raw.astype(BF16), dkv[..., hd:]], axis=-1).reshape(tokens, 2 * hd)
        grad_hidden, attn_terms = d_hidden_call(
            order, dq_own, dq_oth, dkv, hidden_flat, d_resid, attn_gain[None, :], wq_own, wq_oth, w_kv, 4 * rows, 2 * rows)
        g_kv = small_wgrad(order, normed_flat, dkv, tf=1024, tn=2 * hd)
        norms = jnp.stack([jnp.sum(attn_terms, axis=0), jnp.sum(norm_terms, axis=0)]).reshape(-1, 2 * hd)
        sums = lax.psum(jnp.concatenate([g_kv, norms], axis=0), "tp")
        g_attn_norm, g_mlp_norm = sums[dim:].reshape(2, dim)
        g_gate = wgrad_call(order, core_1, z_all, [a[1] for a in shards], tiles=(1, 2), earlier=g_gate)
        g_up = wgrad_call(order, core_1, z_all, [a[2] for a in shards])
        g_down = wgrad_call(order, core_1, [a[0] for a in shards], g_all)
        return (hidden_out, grad_hidden.reshape(batch, rows, dim), g_attn_norm, g_query, sums[:dim, :hd], sums[:dim, hd:], g_out, g_mlp_norm, g_gate, g_up, g_down)

    return jax.shard_map(local_layer, mesh=mesh, in_specs=in_specs, out_specs=out_specs, check_vma=False)
```

```python
import functools
import math
import jax
import jax.numpy as jnp
from jax import lax
from jax.experimental import pallas as pl
from jax.experimental.pallas import tpu as pltpu
from jax.sharding import PartitionSpec as P

NORM_EPS = 1e-6
CHUNKS = 3
F32 = jnp.float32
BF16 = jnp.bfloat16
MASKED = -1e30


def rms_norm(x_in, gain):
    x_f = x_in.astype(F32)
    inv_rms = lax.rsqrt(jnp.mean(x_f * x_f, axis=-1, keepdims=True) + NORM_EPS)
    return (x_f * inv_rms * (1.0 + gain)).astype(BF16)


def rope_tables(positions, head_dim):
    half_dim = head_dim // 2
    exponent = jnp.arange(half_dim, dtype=F32) * (2.0 / head_dim)
    inv_freq = jnp.exp(exponent * (-math.log(10000.0)))
    angles = positions.astype(F32)[:, None] * inv_freq[None, :]
    return jnp.cos(angles), jnp.sin(angles)


def apply_rope(x_f, cos_t, sin_t):
    half_dim = x_f.shape[-1] // 2
    first = x_f[..., :half_dim]
    second = x_f[..., half_dim:]
    return jnp.concatenate([first * cos_t - second * sin_t, second * cos_t + first * sin_t], axis=-1)


def dot_f32(lhs, rhs, lhs_dim, rhs_dim):
    return lax.dot_general(lhs, rhs, (((lhs_dim,), (rhs_dim,)), ((), ())), preferred_element_type=F32)


def own_first(kv_ref, core, lo, hi):
    shards = kv_ref.shape[0] // 2
    return jnp.concatenate([kv_ref[2 * c + side, 0, :, lo:hi] for side in (core, 1 - core) for c in range(shards)], axis=0)


def attn_fwd_kernel(prefix_s, valid_s, core_s, q_own_ref, q_oth_ref, kv_ref, cos_ref, sin_ref, qpos_ref, kpos_ref,
                    o_own_ref, o_oth_ref, r_own_ref, r_oth_ref):
    b = pl.program_id(0)
    rows, width = q_own_ref.shape[1:]
    hd = kv_ref.shape[-1] // 2
    half = hd // 2
    heads = width // hd
    scale = hd ** -0.5
    cos_t, sin_t = cos_ref[...], sin_ref[...]
    queries = []
    for src, dst in ((q_own_ref, r_own_ref), (q_oth_ref, r_oth_ref)):
        for n in range(heads):
            first = src[0, :, n * hd:n * hd + half]
            second = src[0, :, n * hd + half:(n + 1) * hd]
            q_1 = ((first * cos_t - second * sin_t).astype(BF16) * scale).astype(BF16)
            q_2 = ((second * cos_t + first * sin_t).astype(BF16) * scale).astype(BF16)
            dst[0, :, n * hd:n * hd + half] = q_1
            dst[0, :, n * hd + half:(n + 1) * hd] = q_2
            queries.append(jnp.concatenate([q_1, q_2], axis=1))
    keys = own_first(kv_ref, core_s[0], 0, hd)
    values = own_first(kv_ref, core_s[0], hd, 2 * hd)
    limit = jnp.minimum(valid_s[b], jnp.maximum(prefix_s[b], qpos_ref[...] + 1))
    visible = kpos_ref[...] < limit
    for side, dst in ((0, o_own_ref), (1, o_oth_ref)):
        query = jnp.concatenate(queries[side * heads:(side + 1) * heads], axis=0)
        scores = dot_f32(query, keys, 1, 1)
        scores = jnp.where(visible, scores, MASKED)
        top = jnp.max(scores, axis=-1, keepdims=True)
        expo = jnp.exp(scores - top)
        inv = 1.0 / jnp.sum(expo, axis=-1, keepdims=True)
        probs = (expo * inv).astype(BF16)
        mixed = dot_f32(probs, values, 1, 0).astype(BF16)
        for n in range(heads):
            dst[0, :, n * hd:(n + 1) * hd] = mixed[n * rows:(n + 1) * rows]


def attn_bwd_kernel(first, prefix_s, valid_s, core_s, q_own_ref, q_oth_ref, g_own_ref, g_oth_ref, kv_ref, cos_ref, sin_ref,
                    qpos_ref, kpos_ref, dq_own_ref, dq_oth_ref, dkv_ref):
    b = pl.program_id(0) + first
    rows, width = q_own_ref.shape[1:]
    hd = kv_ref.shape[-1] // 2
    half = hd // 2
    heads = width // hd
    scale = hd ** -0.5
    cos_t, sin_t = cos_ref[...], sin_ref[...]
    shards = kv_ref.shape[0] // 2
    keys = own_first(kv_ref, core_s[0], 0, hd)
    values = own_first(kv_ref, core_s[0], hd, 2 * hd)
    limit = jnp.minimum(valid_s[b], jnp.maximum(prefix_s[b], qpos_ref[...] + 1))
    visible = kpos_ref[...] < limit
    d_keys, d_values = 0.0, 0.0
    for q_ref, g_ref, dst in ((q_own_ref, g_own_ref, dq_own_ref), (q_oth_ref, g_oth_ref, dq_oth_ref)):
        query = jnp.concatenate([q_ref[0, :, n * hd:(n + 1) * hd] for n in range(heads)], axis=0)
        grad = jnp.concatenate([g_ref[0, :, n * hd:(n + 1) * hd] for n in range(heads)], axis=0)
        scores = dot_f32(keys, query, 1, 1)
        scores = jnp.where(visible, scores, MASKED)
        top = jnp.max(scores, axis=0, keepdims=True)
        expo = jnp.exp(scores - top)
        inv = 1.0 / jnp.sum(expo, axis=0, keepdims=True)
        probs = expo * inv
        d_probs = dot_f32(values, grad, 1, 1)
        delta = jnp.sum(probs * d_probs, axis=0, keepdims=True)
        d_scores = (probs * (d_probs - delta)).astype(BF16)
        d_values = d_values + dot_f32(probs.astype(BF16), grad, 1, 0)
        d_keys = d_keys + dot_f32(d_scores, query, 1, 0)
        d_query = dot_f32(d_scores, keys, 0, 0) * scale
        for n in range(heads):
            g_1 = d_query[n * rows:(n + 1) * rows, :half]
            g_2 = d_query[n * rows:(n + 1) * rows, half:]
            dst[0, :, n * hd:n * hd + half] = (g_1 * cos_t + g_2 * sin_t).astype(BF16)
            dst[0, :, n * hd + half:(n + 1) * hd] = (g_2 * cos_t - g_1 * sin_t).astype(BF16)
    d_keys = d_keys.astype(BF16)
    d_values = d_values.astype(BF16)
    span = kv_ref.shape[2]
    for k, side in enumerate((core_s[0], 1 - core_s[0])):
        for c in range(shards):
            at = (k * shards + c) * span
            dkv_ref[2 * c + side, 0, :, :hd] = d_keys[at:at + span]
            dkv_ref[2 * c + side, 0, :, hd:] = d_values[at:at + span]


def attn_specs(rows, width, shards, two_hd, half):
    q_spec = pl.BlockSpec((1, rows, width), lambda b, *_: (b, 0, 0))
    kv_spec = pl.BlockSpec((shards, 1, rows, two_hd), lambda b, *_: (0, b, 0, 0))
    tab_spec = pl.BlockSpec((rows, half), lambda b, *_: (0, 0))
    return q_spec, kv_spec, tab_spec


def whole(shape):
    return pl.BlockSpec(shape, lambda b, *_: tuple(0 for _ in shape))


def attn_fwd(q_own, q_oth, kv_all, cos_t, sin_t, qpos, kpos, scalars):
    batch, rows, width = q_own.shape
    shards, two_hd = kv_all.shape[0], kv_all.shape[3]
    q_spec, kv_spec, tab_spec = attn_specs(rows, width, shards, two_hd, two_hd // 4)
    heads = width * 2 // two_hd
    out = jax.ShapeDtypeStruct((batch, rows, width), BF16)
    qpos_col = jnp.tile(qpos, heads)[:, None]
    n_keys = kpos.shape[0]
    flops = 2 * 2 * batch * rows * 2 * width * n_keys
    return pl.pallas_call(
        attn_fwd_kernel,
        out_shape=(out, out, out, out),
        grid_spec=pltpu.PrefetchScalarGridSpec(
            num_scalar_prefetch=3, grid=(batch,),
            in_specs=[q_spec, q_spec, kv_spec, tab_spec, tab_spec, whole((heads * rows, 1)), whole((1, n_keys))],
            out_specs=[q_spec] * 4),
        compiler_params=pltpu.CompilerParams(dimension_semantics=("arbitrary",), vmem_limit_bytes=30 << 20),
        cost_estimate=pl.CostEstimate(flops=flops, bytes_accessed=batch * rows * width * 16 + kv_all.size * 2, transcendentals=batch * rows * heads * 2 * n_keys),
        name="attn_fwd",
    )(*scalars, q_own, q_oth, kv_all, cos_t, sin_t, qpos_col, kpos[None, :])


def attn_bwd(order, q_own, q_oth, g_own, g_oth, kv_all, cos_t, sin_t, qpos, kpos, scalars, first, count, earlier):
    batch, rows, width = q_own.shape
    shards, two_hd = kv_all.shape[0], kv_all.shape[3]
    tab_spec = pl.BlockSpec((rows, two_hd // 4), lambda b, *_: (0, 0))
    q_spec = pl.BlockSpec((1, rows, width), lambda b, *_: (b + first, 0, 0))
    kv_spec = pl.BlockSpec((shards, 1, rows, two_hd), lambda b, *_: (0, b + first, 0, 0))
    heads = width * 2 // two_hd
    out = jax.ShapeDtypeStruct((batch, rows, width), BF16)
    kv_out = jax.ShapeDtypeStruct(kv_all.shape, BF16)
    qpos_row = jnp.tile(qpos, heads)[None, :]
    n_keys = kpos.shape[0]
    flops = 2 * 5 * count * rows * 2 * width * n_keys
    return order.call(
        functools.partial(attn_bwd_kernel, first), 9, len(earlier), prefetch=3,
        out_shape=(out, out, kv_out), grid=(count,),
        in_specs=[q_spec, q_spec, q_spec, q_spec, kv_spec, tab_spec, tab_spec, whole((1, heads * rows)), whole((n_keys, 1))],
        out_specs=[q_spec, q_spec, kv_spec],
        compiler_params=pltpu.CompilerParams(dimension_semantics=("arbitrary",), vmem_limit_bytes=30 << 20),
        cost_estimate=pl.CostEstimate(flops=flops, bytes_accessed=count * rows * width * 12 + kv_all.size * 4, transcendentals=count * rows * heads * 2 * n_keys),
        name="attn_bwd",
    )(*scalars, q_own, q_oth, g_own, g_oth, kv_all, cos_t, sin_t, qpos_row, kpos[:, None], *earlier)


class Order:
    def __init__(self):
        self.last = None

    def call(self, kernel, n_in, n_kept=0, *, in_specs, out_specs, out_shape, grid, prefetch=0, scratch_shapes=(), **options):
        def run(*args):
            deps = () if self.last is None or any(self.last is a for a in args) else (self.last,)
            n_args = prefetch + n_in

            def body(*refs):
                kernel(*refs[:n_args], *refs[n_args + n_kept + len(deps):])

            single = not isinstance(out_specs, (list, tuple))
            n_out = 1 if single else len(out_specs)
            out = pl.pallas_call(
                body, out_shape=out_shape,
                grid_spec=pltpu.PrefetchScalarGridSpec(
                    num_scalar_prefetch=prefetch, grid=grid, scratch_shapes=scratch_shapes, out_specs=out_specs,
                    in_specs=in_specs + [pl.BlockSpec(memory_space=pl.ANY)] * (n_kept + len(deps))),
                input_output_aliases={n_args + k: n_out - n_kept + k for k in range(n_kept)},
                **options)(*args, *deps)
            self.last = out[0] if isinstance(out, (tuple, list)) else out
            return out

        return run


def params(steps, limit=56):
    return pltpu.CompilerParams(dimension_semantics=("arbitrary",) * steps, vmem_limit_bytes=limit << 20)


def cost(flops, *arrays):
    return pl.CostEstimate(flops=flops, bytes_accessed=sum(a.size * a.dtype.itemsize for a in arrays), transcendentals=0)


def rows_of(ref):
    return ref[...].reshape(-1, ref.shape[-1])


def raw_spec(shape):
    return pl.BlockSpec((2, 1) + shape[2:], lambda j, i, core: (lax.rem(i, 2), lax.bitwise_xor(core[0], lax.div(i, 2)), 0, 0))


def d_act_kernel(core_s, g_ref, wd_ref, out_ref):
    out_ref[...] = dot_f32(rows_of(g_ref), wd_ref[...], 1, 1).astype(BF16)


def d_act_call(order, core, g_all, w_down, tn=1024):
    chips, _, rows, dim = g_all.shape
    width = w_down.shape[0]
    out = jax.ShapeDtypeStruct((chips * 2 * rows, width), BF16)
    return order.call(
        d_act_kernel, 2, prefetch=1, out_shape=out, grid=(width // tn, chips),
        in_specs=[raw_spec(g_all.shape), pl.BlockSpec((tn, dim), lambda j, i, core: (j, 0))],
        out_specs=pl.BlockSpec((2 * rows, tn), lambda j, i, core: (i, j)), compiler_params=params(2),
        cost_estimate=cost(2 * g_all.size * width, g_all, w_down, out), name="d_act",
    )(core, g_all, w_down)


def act_kernel(core_s, z_ref, g_ref, wg_ref, wu_ref, *refs, sub):
    c_1 = math.sqrt(2.0 / math.pi)
    c_3 = 0.044715 * c_1
    act_ref, dg_ref, du_ref = refs[-3:]
    z_in = rows_of(z_ref)
    for j in range(0, wg_ref.shape[1], sub):
        gate = dot_f32(z_in, wg_ref[:, j:j + sub], 1, 0)
        upper = dot_f32(z_in, wu_ref[:, j:j + sub], 1, 0)
        if len(refs) == 4:
            d_act = dot_f32(rows_of(g_ref), refs[0][j:j + sub, :], 1, 1).astype(BF16).astype(F32)
        else:
            d_act = g_ref[:, j:j + sub].astype(F32)
        square = gate * gate
        half = 0.5 * jnp.tanh(gate * (c_3 * square + c_1)) + 0.5
        gelu = gate * half
        act_ref[:, j:j + sub] = (gelu * upper).astype(BF16)
        du_ref[:, j:j + sub] = (d_act * gelu).astype(BF16)
        slope = half + gelu * (1.0 - half) * (6.0 * c_3 * square + 2.0 * c_1)
        dg_ref[:, j:j + sub] = (d_act * upper * slope).astype(BF16)


def act_call(order, core, z_all, g_all, w_gate, w_up, w_down, sub=256):
    chips, _, rows, dim = z_all.shape
    width = w_gate.shape[1]
    out = jax.ShapeDtypeStruct((chips * 2 * rows, width), BF16)
    tn = 1024 if w_down is None else 512
    raw = raw_spec(z_all.shape)
    col = pl.BlockSpec((dim, tn), lambda j, i, core: (0, j))
    tile = pl.BlockSpec((2 * rows, tn), lambda j, i, core: (i, j))
    args = (z_all, g_all, w_gate, w_up) + (() if w_down is None else (w_down,))
    specs = [raw, tile if w_down is None else raw, col, col] + ([] if w_down is None else [pl.BlockSpec((tn, dim), lambda j, i, core: (j, 0))])
    return order.call(
        functools.partial(act_kernel, sub=sub), len(args), prefetch=1, out_shape=(out, out, out), grid=(width // tn, chips),
        in_specs=specs, out_specs=[tile] * 3, compiler_params=params(2),
        cost_estimate=cost(2 * (len(args) - 2) * z_all.size * width, *args, out, out, out), name="mlp_act",
    )(core, *args)


def back_kernel(*refs, terms, joined, n_far, base, tn):
    n = len(terms)
    lhs, rhs, far, out = refs[:n], refs[n:2 * n], refs[2 * n:2 * n + n_far], refs[2 * n + n_far]
    l_bufs, r_bufs, (l_sems, r_sems) = refs[2 * n + n_far + 1:][:n], refs[3 * n + n_far + 1:][:n], refs[4 * n + n_far + 1:]
    j, i = pl.program_id(0), pl.program_id(1)
    blocks, rows = l_bufs[0].shape[:2]

    def left(p, at):
        return pltpu.make_async_copy(lhs[p].at[pl.ds((base + at) * rows, rows)], l_bufs[p].at[at], l_sems.at[p, at])

    def right(p, tile):
        cols = pl.ds(pl.multiple_of(tile * tn, tn), tn)
        src = rhs[p].at[:, cols] if terms[p][0] == 0 else rhs[p].at[cols]
        return pltpu.make_async_copy(src, r_bufs[p].at[lax.rem(tile, 2)], r_sems.at[p, lax.rem(tile, 2)])

    @pl.when((j == 0) & (i == 0))
    def _():
        for p in range(n):
            right(p, 0).start()
            left(p, 0).start()
        for at in range(1, blocks):
            for p in range(n):
                left(p, at).start()

    @pl.when((i == blocks - 1) & (j + 1 < pl.num_programs(0)))
    def _():
        for p in range(n):
            right(p, j + 1).start()

    def compute(ready):
        totals = {}
        for p, (dim, kind) in enumerate(terms):
            ready(p)
            part = dot_f32(l_bufs[p][i], r_bufs[p][lax.rem(j, 2)], 1, dim)
            totals[kind] = totals[kind] + part if kind in totals else part
        for kind, total in totals.items():
            at = (slice(None), kind) if joined else (slice(None),)
            total = total.reshape(out[at].shape)
            if far:
                total += far[0][at].astype(F32)
            out[at] = total.astype(BF16)

    @pl.when(j == 0)
    def _():
        def ready(p):
            @pl.when(i == 0)
            def _():
                right(p, 0).wait()

            left(p, i).wait()

        compute(ready)

    @pl.when(j > 0)
    def _():
        @pl.when(i == 0)
        def _():
            for p in range(n):
                right(p, j).wait()

        compute(lambda p: None)


def back_call(order, side, lhs, rhs, terms, far, chips, tn=512):
    dim = rhs[0].shape[0 if terms[0][0] else 1]
    rows = lhs[0].shape[0] // (2 * chips)
    half, n = chips // 2, len(terms)
    kinds = sorted({kind for _, kind in terms})
    joined = len(kinds) == 2
    hbm = pl.BlockSpec(memory_space=pl.ANY)
    both = pl.BlockSpec((2, 2, rows, tn), lambda j, i: (i, 0, 0, j))
    out = jax.ShapeDtypeStruct((chips, 2, rows, dim) if joined else (chips, rows, dim), BF16)
    far_spec = both if joined else pl.BlockSpec((2, None, rows, tn), lambda j, i: (i, kinds[0], 0, j))
    depth = lhs[0].shape[1]
    return order.call(
        functools.partial(back_kernel, terms=terms, joined=joined, n_far=len(far), base=side * half, tn=tn), 2 * n + len(far), out_shape=out,
        grid=(dim // tn, half), in_specs=[hbm] * (2 * n) + [far_spec] * len(far),
        out_specs=both if joined else pl.BlockSpec((2, rows, tn), lambda j, i: (i, 0, j)),
        scratch_shapes=[pltpu.VMEM((half, 2 * rows, depth), BF16)] * n
        + [pltpu.VMEM((2, depth, tn) if d == 0 else (2, tn, depth), BF16) for d, _ in terms]
        + [pltpu.SemaphoreType.DMA((n, half)), pltpu.SemaphoreType.DMA((n, 2))],
        compiler_params=params(2, 54),
        cost_estimate=cost(n * lhs[0].size * dim, *lhs, *rhs, out), name="mlp_back",
    )(*lhs, *rhs, *far)


def wgrad_kernel(core_s, *refs, n, tf, tn, cols, first):
    lhs, rhs, out, l_buf, r_buf, sems = refs[:n], refs[n:2 * n], *refs[2 * n:]
    i, j, k = pl.program_id(0), pl.program_id(1), pl.program_id(2)
    step = (i * cols + j) * n + k
    slot = lax.rem(step, 2)
    chips = l_buf.shape[1] // 2

    def copies(s, at, p):
        row = pl.multiple_of((lax.div(s, cols * n) + first) * tf, tf)
        col = pl.multiple_of(lax.rem(lax.div(s, n), cols) * tn, tn)
        out = []
        for q, (ref, buf, lanes) in enumerate(((lhs[p], l_buf, pl.ds(row, tf)), (rhs[p], r_buf, pl.ds(col, tn)))):
            if ref.ndim == 4:
                for side in range(2):
                    src = ref.at[:, lax.bitwise_xor(core_s[0], side), :, lanes]
                    out.append(pltpu.make_async_copy(src, buf.at[at, pl.ds(side * chips, chips)], sems.at[q, side, at]))
            else:
                out.append(pltpu.make_async_copy(ref.at[:, :, lanes], buf.at[at], sems.at[q, 0, at]))
        return out

    def fetch(s, at):
        for p in range(n):
            @pl.when(lax.rem(s, n) == p)
            def _(p=p):
                for copy in copies(s, at, p):
                    copy.start()

    @pl.when(step == 0)
    def _():
        fetch(step, slot)

    @pl.when(step + 1 < pl.num_programs(0) * cols * n)
    def _():
        fetch(step + 1, 1 - slot)

    for copy in copies(step, slot, 0):
        copy.wait()
    part = dot_f32(rows_of(l_buf.at[slot]), rows_of(r_buf.at[slot]), 0, 0)
    out[...] = jnp.where(k == 0, part, out[...] + part)


def wgrad_call(order, core, lhs, rhs, tf=1024, tn=1024, tiles=None, earlier=None):
    n = len(lhs)
    rows = lhs[0].shape[-2]
    shards = lhs[0].size // (rows * lhs[0].shape[-1])
    width = rhs[0].shape[-1]
    height = lhs[0].shape[-1]
    cols = width // tn
    first, last = tiles or (0, height // tf)
    kept = () if earlier is None else (earlier,)
    out = jax.ShapeDtypeStruct((height, width), F32)
    return order.call(
        functools.partial(wgrad_kernel, n=n, tf=tf, tn=tn, cols=cols, first=first), 2 * n, len(kept), prefetch=1, out_shape=out, grid=(last - first, cols, n),
        in_specs=[pl.BlockSpec(memory_space=pl.ANY)] * (2 * n), out_specs=pl.BlockSpec((tf, tn), lambda i, j, k, core: (i + first, j)),
        scratch_shapes=[pltpu.VMEM((2, shards, rows, tf), BF16), pltpu.VMEM((2, shards, rows, tn), BF16), pltpu.SemaphoreType.DMA((2, 2, 2))],
        compiler_params=params(3), cost_estimate=cost(2 * n * shards * rows * height * width, *lhs, *rhs, out), name="wgrad",
    )(core, *lhs, *rhs, *kept)


def kv_wgrad_kernel(l_ref, r_ref, *refs):
    out, steps = refs[-1], pl.num_programs(0)
    width = out.shape[1]

    @pl.when(pl.program_id(0) < steps - 1)
    def _():
        out[...] = dot_f32(l_ref[...], r_ref[...], 0, 0)

    @pl.when(pl.program_id(0) == steps - 1)
    def _():
        row = 0
        for terms in refs[:-1]:
            total = jnp.sum(terms[...], axis=0, keepdims=True)
            for k in range(0, total.shape[1], width):
                out[row:row + 1] = total[:, k:k + width]
                row += 1


def kv_wgrad(order, lhs, rhs, terms, tf=512):
    tokens, rows = lhs.shape
    width = rhs.shape[1]
    extra = sum(t.shape[1] for t in terms) // width
    steps = rows // tf
    out = jax.ShapeDtypeStruct((rows + extra, width), F32)
    return order.call(
        kv_wgrad_kernel, 2 + len(terms), out_shape=out, grid=(steps + 1,),
        in_specs=[pl.BlockSpec((tokens, tf), lambda i: (0, jnp.minimum(i, steps - 1))), pl.BlockSpec((tokens, width), lambda i: (0, 0))]
        + [pl.BlockSpec(t.shape, lambda i: (0, 0)) for t in terms],
        out_specs=pl.BlockSpec((tf, width), lambda i: (i, 0)), compiler_params=params(1, 40),
        cost_estimate=cost(2 * tokens * rows * width, lhs, rhs, out), name="kv_wgrad",
    )(lhs, rhs, *terms)


def head_wgrad_kernel(*refs):
    lhs, rhs, out = refs[:2], refs[2:4], refs[-1]
    for kind in range(2):
        total = dot_f32(lhs[kind][...], rhs[kind][...], 0, 0).reshape(out.shape[0], *out.shape[2:])
        for far in refs[4:-1]:
            total += far[:, kind]
        out[:, kind] = total


def head_wgrad(order, lhs, rhs, hd, far=(), tn=512):
    tokens, width = lhs[0].shape
    dim = rhs[0].shape[1]
    heads = width // hd
    out = jax.ShapeDtypeStruct((heads, 2, hd, dim), F32)
    tile = pl.BlockSpec((heads, 2, hd, tn), lambda j: (0, 0, 0, j))
    return order.call(
        head_wgrad_kernel, 4 + len(far), out_shape=out, grid=(dim // tn,),
        in_specs=[pl.BlockSpec((tokens, width), lambda j: (0, 0), pipeline_mode=pl.Buffered(1))] * 2
        + [pl.BlockSpec((tokens, tn), lambda j: (0, j))] * 2 + [tile] * len(far),
        out_specs=tile, compiler_params=params(1, 48), cost_estimate=cost(4 * tokens * width * dim, *lhs, *rhs, *far, out), name="head_wgrad",
    )(*lhs, *rhs, *far)


def add_kernel(base_ref, *refs):
    for c, part in enumerate(refs[:-1]):
        @pl.when(pl.program_id(0) == c)
        def _(part=part):
            refs[-1][...] = (base_ref[...].astype(F32) + rows_of(part).astype(F32)).astype(BF16)


def add_call(order, base, parts):
    tokens, dim = base.shape
    size = tokens // len(parts)
    row = pl.BlockSpec((size, dim), lambda i: (i, 0))
    specs = [pl.BlockSpec((1, size, dim), lambda i, at=a.shape[0] - 1: (at, 0, 0)) if a.ndim == 3 else pl.BlockSpec((size, dim), lambda i: (0, 0)) for a in parts]
    return order.call(
        add_kernel, 1 + len(parts), out_shape=jax.ShapeDtypeStruct(base.shape, BF16), grid=(len(parts),), in_specs=[row] + specs, out_specs=row,
        compiler_params=params(1, 40), cost_estimate=cost(base.size, base, base, base), name="add",
    )(base, *parts)


def resid_kernel(h_ref, a_own_ref, a_oth_ref, w_own_ref, w_oth_ref, gain_ref, resid_ref, *z_refs, sub):
    for c, z_ref in enumerate(z_refs):
        @pl.when(pl.program_id(0) == c)
        def _(z_ref=z_ref):
            for r in range(0, z_ref.shape[0], sub):
                at = slice(r, r + sub)
                total = dot_f32(a_own_ref[at], w_own_ref[...], 1, 0) + dot_f32(a_oth_ref[at], w_oth_ref[...], 1, 0)
                resid = (h_ref[at].astype(F32) + total).astype(BF16)
                resid_ref[at] = resid
                x_f = resid.astype(F32)
                inv = lax.rsqrt(jnp.mean(x_f * x_f, axis=-1, keepdims=True) + NORM_EPS)
                z_ref[at] = (x_f * inv * (1.0 + gain_ref[...])).astype(BF16)


def resid_call(order, hidden, mix_own, mix_oth, wo_own, wo_oth, gain, size, sub):
    tokens, dim = hidden.shape
    width = mix_own.shape[1]
    chunks = tokens // size
    row = pl.BlockSpec((size, dim), lambda i: (i, 0))
    mix = pl.BlockSpec((size, width), lambda i: (i, 0))
    whole_w = pl.BlockSpec((width, dim), lambda i: (0, 0))
    outs = (jax.ShapeDtypeStruct((tokens, dim), BF16),) + (jax.ShapeDtypeStruct((size, dim), BF16),) * chunks
    return order.call(
        functools.partial(resid_kernel, sub=sub), 6, out_shape=outs, grid=(chunks,),
        in_specs=[row, mix, mix, whole_w, whole_w, pl.BlockSpec((1, dim), lambda i: (0, 0))],
        out_specs=[row] + [pl.BlockSpec((size, dim), lambda i: (0, 0))] * chunks,
        compiler_params=params(1), cost_estimate=cost(4 * tokens * dim * width, hidden, mix_own, mix_oth, wo_own, wo_oth, *outs), name="resid",
    )(hidden, mix_own, mix_oth, wo_own, wo_oth, gain)


def norm_back(x_f, gain_1, d_out):
    inv = lax.rsqrt(jnp.mean(x_f * x_f, axis=-1, keepdims=True) + NORM_EPS)
    unit = x_f * inv
    scaled = d_out * gain_1
    d_x = inv * (scaled - unit * jnp.mean(scaled * unit, axis=-1, keepdims=True))
    return d_x, d_out * unit


def fold_rows(terms):
    rows, dim = terms.shape
    return jnp.sum(terms.reshape(rows // 8, 8, dim), axis=0)


def d_resid_kernel(*refs, n):
    dz_refs = refs[:n]
    x_ref, g_ref, gain_ref, w_own_ref, w_oth_ref, norm_ref, d_ref, own_ref, oth_ref = refs[n:]
    i = pl.program_id(0)

    @pl.when(i == 0)
    def _():
        norm_ref[...] = jnp.zeros_like(norm_ref)

    for c, dz_ref in enumerate(dz_refs):
        @pl.when(i == c)
        def _(dz_ref=dz_ref):
            d_x, terms = norm_back(x_ref[...].astype(F32), 1.0 + gain_ref[...], rows_of(dz_ref).astype(F32))
            norm_ref[...] += fold_rows(terms)
            d_ref[...] = (g_ref[...].astype(F32) + d_x).astype(BF16)
    own_ref[...] = dot_f32(d_ref[...], w_own_ref[...], 1, 1).astype(BF16)
    oth_ref[...] = dot_f32(d_ref[...], w_oth_ref[...], 1, 1).astype(BF16)


def d_resid_call(order, dz, resid, grad_out, gain, wo_own, wo_oth, first, size, earlier):
    tokens, dim = resid.shape
    n = len(dz)
    width = wo_own.shape[0]
    one = [pl.BlockSpec((1, size, dim) if a.ndim == 3 else (size, dim), lambda i, nd=a.ndim: (0,) * nd) for a in dz]
    far = pl.BlockSpec((size, dim), lambda i: (i + first, 0))
    mix = pl.BlockSpec((size, width), lambda i: (i + first, 0))
    whole_w = pl.BlockSpec((width, dim), lambda i: (0, 0))
    outs = (jax.ShapeDtypeStruct((8, dim), F32), jax.ShapeDtypeStruct((tokens, dim), BF16),
            jax.ShapeDtypeStruct((tokens, width), BF16), jax.ShapeDtypeStruct((tokens, width), BF16))
    return order.call(
        functools.partial(d_resid_kernel, n=n), n + 5, len(earlier), out_shape=outs, grid=(n,),
        in_specs=one + [far, far, pl.BlockSpec((1, dim), lambda i: (0, 0)), whole_w, whole_w],
        out_specs=[pl.BlockSpec((8, dim), lambda i: (0, 0)), far, mix, mix],
        compiler_params=params(1, 48), cost_estimate=cost(4 * n * size * dim * width, *dz, wo_own, wo_oth, outs[1]), name="d_resid",
    )(*dz, resid, grad_out, gain, wo_own, wo_oth, *earlier)


def d_hidden_kernel(q_own_ref, q_oth_ref, dkv_ref, x_ref, d_ref, gain_ref, wq_own_ref, wq_oth_ref, wkv_ref, out_ref, norm_ref, *, sub):
    @pl.when(pl.program_id(0) == 0)
    def _():
        norm_ref[...] = jnp.zeros_like(norm_ref)

    folded = 0.0
    for r in range(0, x_ref.shape[0], sub):
        at = slice(r, r + sub)
        d_normed = (dot_f32(q_own_ref[at], wq_own_ref[...], 1, 0) + dot_f32(q_oth_ref[at], wq_oth_ref[...], 1, 0)
                    + dot_f32(dkv_ref[at], wkv_ref[...], 1, 1)).astype(BF16).astype(F32)
        d_x, terms = norm_back(x_ref[at].astype(F32), 1.0 + gain_ref[...], d_normed)
        folded += fold_rows(terms)
        out_ref[at] = (d_ref[at].astype(F32) + d_x).astype(BF16)
    norm_ref[...] += folded


def d_hidden_call(order, dq_own, dq_oth, dkv, hidden, d_resid, gain, wq_own, wq_oth, w_kv, tm, sub):
    tokens, dim = hidden.shape
    width, two_hd = dq_own.shape[1], dkv.shape[1]
    row = pl.BlockSpec((tm, dim), lambda i: (i, 0))
    mix = pl.BlockSpec((tm, width), lambda i: (i, 0))
    whole_w = pl.BlockSpec((width, dim), lambda i: (0, 0))
    outs = (jax.ShapeDtypeStruct((tokens, dim), BF16), jax.ShapeDtypeStruct((8, dim), F32))
    return order.call(
        functools.partial(d_hidden_kernel, sub=sub), 9, out_shape=outs, grid=(tokens // tm,),
        in_specs=[mix, mix, pl.BlockSpec((tm, two_hd), lambda i: (i, 0)), row, row, pl.BlockSpec((1, dim), lambda i: (0, 0)), whole_w, whole_w,
                  pl.BlockSpec((dim, two_hd), lambda i: (0, 0))],
        out_specs=[row, pl.BlockSpec((8, dim), lambda i: (0, 0))],
        compiler_params=params(1), cost_estimate=cost(4 * tokens * dim * (width + two_hd), dq_own, dq_oth, hidden, d_resid, wq_own, wq_oth, *outs), name="d_hidden",
    )(dq_own, dq_oth, dkv, hidden, d_resid, gain, wq_own, wq_oth, w_kv)


def solution(mesh):
    tp_size = mesh.shape["tp"]
    chips = tp_size // 2
    act_spec = P("dp", "tp", None)
    in_specs = (act_spec, act_spec, P("dp"), P("dp"), P(None), P(None, "tp"), P(None, None), P(None, None), P("tp", None), P(None), P(None, "tp"), P(None, "tp"), P("tp", None))
    out_specs = (act_spec, act_spec, P("dp"), P("dp", "tp"), P("dp", None), P("dp", None), P(("dp", "tp"), None), P("dp"), P("dp", "tp"), P("dp", "tp"), P(("dp", "tp"), None))
    same_core = [[2 * c + k for c in range(chips)] for k in range(2)]
    partner = [(i, i ^ 1) for i in range(tp_size)]

    def scatter4(x_part):
        flat = x_part.reshape((-1,) + x_part.shape[2:])
        return lax.psum_scatter(flat, "tp", scatter_dimension=0, tiled=True, axis_index_groups=same_core)

    def gather8(x_loc):
        return lax.all_gather(x_loc, "tp", axis=0, tiled=False)

    def swap(x_loc):
        return lax.ppermute(x_loc, "tp", partner)

    def flip(x_loc, bits):
        return lax.ppermute(x_loc, "tp", [(i, i ^ bits) for i in range(tp_size)])

    def gather4_direct(x_loc, before=None):
        chip = lax.axis_index("tp") // 2
        half = x_loc.shape[0] // 2
        near, far = flip(x_loc, 2), flip(x_loc, 4)
        if before is not None:
            near, far, _ = lax.optimization_barrier((near, far, before))
        low, high = flip(near[:half], 4), flip(far[half:], 2)
        out = jnp.zeros((chips,) + x_loc.shape, x_loc.dtype)
        for k, block in ((0, x_loc), (1, near), (2, far)):
            out = lax.dynamic_update_slice(out, block[None], (chip ^ k, 0, 0))
        out = lax.dynamic_update_slice(out, low[None], (chip ^ 3, 0, 0))
        return lax.dynamic_update_slice(out, high[None], (chip ^ 3, half, 0))

    def local_layer(hidden, grad_out, prefix_len, valid_len, attn_norm, w_query, w_key, w_value, w_out, mlp_norm, w_gate, w_up, w_down):
        batch, rows, dim = hidden.shape
        hd = w_key.shape[1]
        tokens = batch * rows
        assert batch % CHUNKS == 0
        me = lax.axis_index("tp")
        core = lax.rem(me, 2)
        qpos = me * rows + jnp.arange(rows, dtype=jnp.int32)
        shard_pos = jnp.arange(rows, dtype=jnp.int32)[None, :] + (jnp.arange(chips, dtype=jnp.int32) * 2 * rows)[:, None]
        kpos = jnp.concatenate([(shard_pos + core * rows).reshape(-1), (shard_pos + (1 - core) * rows).reshape(-1)])
        cos_t, sin_t = rope_tables(qpos, hd)

        def rope_single(raw_proj):
            return apply_rope(raw_proj, cos_t, sin_t)

        order = Order()
        scalars = (prefix_len, valid_len, core[None])
        attn_gain = attn_norm.astype(F32)
        mlp_gain = mlp_norm.astype(F32)
        wq_own = gather4_direct(w_query.T).reshape(chips * hd, dim)
        normed_flat = rms_norm(hidden, attn_gain).reshape(tokens, dim)
        w_kv = jnp.concatenate([w_key, w_value], axis=1)
        kv_raw = dot_f32(normed_flat, w_kv, 1, 0).reshape(batch, rows, 2 * hd)
        keys, key_pull = jax.vjp(rope_single, kv_raw[..., :hd])
        kv_all = gather8(jnp.concatenate([keys, kv_raw[..., hd:]], axis=-1).astype(BF16))
        wq_oth = swap(wq_own)
        q_own = dot_f32(normed_flat, wq_own, 1, 1)
        q_oth = dot_f32(normed_flat, wq_oth, 1, 1)
        wo_own = gather4_direct(w_out, (q_own, q_oth)).reshape(chips * hd, dim)
        wo_oth = swap(wo_own)
        q_own = q_own.reshape(batch, rows, chips * hd)
        q_oth = q_oth.reshape(batch, rows, chips * hd)
        mix_own, mix_oth, q_own, q_oth = attn_fwd(q_own, q_oth, kv_all, cos_t, sin_t, qpos, kpos, scalars)
        mix_own = mix_own.reshape(tokens, chips * hd)
        mix_oth = mix_oth.reshape(tokens, chips * hd)
        hidden_flat = hidden.reshape(tokens, dim)
        grad_flat = grad_out.reshape(tokens, dim)
        size = tokens // CHUNKS
        resid, *z_parts = resid_call(order, hidden_flat, mix_own, mix_oth, wo_own, wo_oth, mlp_gain[None, :], size, 2 * rows)

        g_all, z_all, acts, far = [], [], [], []
        for c in range(CHUNKS):
            g_all.append(gather8(grad_flat[c * size:(c + 1) * size]).reshape(chips, 2, size, dim))
            z_all.append(gather8(z_parts[c]).reshape(chips, 2, size, dim))
        mlp_sums, d_gated = [None] * CHUNKS, [None] * CHUNKS
        weights = (w_gate, w_up, w_down)
        core_1 = core[None]
        grads = None

        def d_resid_of(first, count, earlier):
            return d_resid_call(order, d_gated[first:first + count], resid, grad_flat, mlp_gain[None, :], wo_own, wo_oth, first, size,
                                () if earlier is None else earlier[1])

        def attn_bwd_of(first, count, d_own, d_oth, earlier):
            per = batch // CHUNKS
            return attn_bwd(order, q_own, q_oth, d_own.reshape(batch, rows, -1), d_oth.reshape(batch, rows, -1), kv_all, cos_t, sin_t, qpos, kpos,
                            scalars, first * per, count * per, () if earlier is None else earlier[2])

        d_z_terms, mlp_terms = ((1, 0), (1, 0)), ((0, 1),)

        def back_both(c, side, far):
            return back_call(order, side, (acts[c][1], acts[c][2], acts[c][0]), weights, d_z_terms + mlp_terms, far, chips)

        def finish(c):
            both = back_both(c, 0, (far[c],))
            both = scatter4(both).reshape(2, size, dim)
            d_gated[c] = mlp_sums[c] = both

        def finish_last(c):
            part = back_call(order, 0, acts[c][1:], weights[:2], d_z_terms, (far[c],), chips)
            d_gated[c] = scatter4(part).reshape(size, dim)
            part = back_call(order, 0, acts[c][:1], weights[2:], mlp_terms, (far[c],), chips)
            mlp_sums[c] = scatter4(part).reshape(size, dim)

        for c in range(CHUNKS):
            if c < CHUNKS - 1:
                d_act = d_act_call(order, core_1, g_all[c], w_down)
                acts.append(act_call(order, core_1, z_all[c], d_act, w_gate, w_up, None))
            else:
                acts.append(act_call(order, core_1, z_all[c], g_all[c], *weights))
            if c > 0:
                finish(c - 1)
            far.append(swap(back_both(c, 1, ())))
        terms, *d_parts = d_resid_of(0, 1, None)
        grads = terms, d_parts, attn_bwd_of(0, 1, d_parts[1], d_parts[2], None)
        finish_last(CHUNKS - 1)
        shards = [[a.reshape(2 * chips, size, -1) for a in acts[c]] for c in range(CHUNKS)]
        g_gate = wgrad_call(order, core_1, z_all, [a[1] for a in shards], tiles=(0, 1))

        terms, d_resid, d_own, d_oth = d_resid_of(1, CHUNKS - 1, grads)
        norm_terms, (dq_own, dq_oth, dkv) = grads[0] + terms, attn_bwd_of(1, CHUNKS - 1, d_own, d_oth, grads)
        dq_own = dq_own.reshape(tokens, chips * hd)
        dq_oth = dq_oth.reshape(tokens, chips * hd)
        dkv = lax.psum_scatter(dkv.reshape(tp_size * batch, rows, 2 * hd), "tp", scatter_dimension=0, tiled=True)
        heads_far = head_wgrad(order, (mix_oth, dq_oth), (d_resid, normed_flat), hd)
        heads_far = swap(heads_far)
        g_gate = wgrad_call(order, core_1, z_all, [a[1] for a in shards], tiles=(1, 2), earlier=g_gate)
        g_heads = head_wgrad(order, (mix_own, dq_own), (d_resid, normed_flat), hd, (heads_far,))
        g_heads = scatter4(g_heads)
        g_out, g_query = g_heads[0], g_heads[1].T
        d_k_raw = key_pull(dkv[..., :hd].astype(F32))[0]
        dkv = jnp.concatenate([d_k_raw.astype(BF16), dkv[..., hd:]], axis=-1).reshape(tokens, 2 * hd)
        grad_hidden, attn_terms = d_hidden_call(
            order, dq_own, dq_oth, dkv, hidden_flat, d_resid, attn_gain[None, :], wq_own, wq_oth, w_kv, 4 * rows, 2 * rows)
        sums = kv_wgrad(order, normed_flat, dkv, (attn_terms, norm_terms))
        sums = lax.psum(sums, "tp")
        g_attn_norm, g_mlp_norm = sums[dim:].reshape(2, dim)
        hidden_out = add_call(order, resid, mlp_sums).reshape(batch, rows, dim)
        g_up = wgrad_call(order, core_1, z_all, [a[2] for a in shards])
        g_down = wgrad_call(order, core_1, [a[0] for a in shards], g_all)
        return (hidden_out, grad_hidden.reshape(batch, rows, dim), g_attn_norm, g_query, sums[:dim, :hd], sums[:dim, hd:], g_out, g_mlp_norm, g_gate, g_up, g_down)

    return jax.shard_map(local_layer, mesh=mesh, in_specs=in_specs, out_specs=out_specs, check_vma=False)
```

```python
import functools
import math
import jax
import jax.numpy as jnp
from jax import lax
from jax.experimental import pallas as pl
from jax.experimental.pallas import tpu as pltpu
from jax.sharding import PartitionSpec as P

NORM_EPS = 1e-6
CHUNKS = 3
F32 = jnp.float32
BF16 = jnp.bfloat16
MASKED = -1e30


def rms_norm(x_in, gain):
    x_f = x_in.astype(F32)
    inv_rms = lax.rsqrt(jnp.mean(x_f * x_f, axis=-1, keepdims=True) + NORM_EPS)
    return (x_f * inv_rms * (1.0 + gain)).astype(BF16)


def rope_tables(positions, head_dim):
    half_dim = head_dim // 2
    exponent = jnp.arange(half_dim, dtype=F32) * (2.0 / head_dim)
    inv_freq = jnp.exp(exponent * (-math.log(10000.0)))
    angles = positions.astype(F32)[:, None] * inv_freq[None, :]
    return jnp.cos(angles), jnp.sin(angles)


def apply_rope(x_f, cos_t, sin_t):
    half_dim = x_f.shape[-1] // 2
    first = x_f[..., :half_dim]
    second = x_f[..., half_dim:]
    return jnp.concatenate([first * cos_t - second * sin_t, second * cos_t + first * sin_t], axis=-1)


def dot_f32(lhs, rhs, lhs_dim, rhs_dim):
    return lax.dot_general(lhs, rhs, (((lhs_dim,), (rhs_dim,)), ((), ())), preferred_element_type=F32)


def own_first(kv_ref, core, lo, hi):
    shards = kv_ref.shape[0] // 2
    return jnp.concatenate([kv_ref[2 * c + side, 0, :, lo:hi] for side in (core, 1 - core) for c in range(shards)], axis=0)


def attn_fwd_kernel(prefix_s, valid_s, core_s, q_own_ref, q_oth_ref, kv_ref, cos_ref, sin_ref, qpos_ref, kpos_ref,
                    o_own_ref, o_oth_ref, r_own_ref, r_oth_ref):
    b = pl.program_id(0)
    rows, width = q_own_ref.shape[1:]
    hd = kv_ref.shape[-1] // 2
    half = hd // 2
    heads = width // hd
    scale = hd ** -0.5
    cos_t, sin_t = cos_ref[...], sin_ref[...]
    queries = []
    for src, dst in ((q_own_ref, r_own_ref), (q_oth_ref, r_oth_ref)):
        for n in range(heads):
            first = src[0, :, n * hd:n * hd + half]
            second = src[0, :, n * hd + half:(n + 1) * hd]
            q_1 = ((first * cos_t - second * sin_t).astype(BF16) * scale).astype(BF16)
            q_2 = ((second * cos_t + first * sin_t).astype(BF16) * scale).astype(BF16)
            dst[0, :, n * hd:n * hd + half] = q_1
            dst[0, :, n * hd + half:(n + 1) * hd] = q_2
            queries.append(jnp.concatenate([q_1, q_2], axis=1))
    keys = own_first(kv_ref, core_s[0], 0, hd)
    values = own_first(kv_ref, core_s[0], hd, 2 * hd)
    limit = jnp.minimum(valid_s[b], jnp.maximum(prefix_s[b], qpos_ref[...] + 1))
    visible = kpos_ref[...] < limit
    for side, dst in ((0, o_own_ref), (1, o_oth_ref)):
        query = jnp.concatenate(queries[side * heads:(side + 1) * heads], axis=0)
        scores = dot_f32(query, keys, 1, 1)
        scores = jnp.where(visible, scores, MASKED)
        top = jnp.max(scores, axis=-1, keepdims=True)
        expo = jnp.exp(scores - top)
        inv = 1.0 / jnp.sum(expo, axis=-1, keepdims=True)
        probs = (expo * inv).astype(BF16)
        mixed = dot_f32(probs, values, 1, 0).astype(BF16)
        for n in range(heads):
            dst[0, :, n * hd:(n + 1) * hd] = mixed[n * rows:(n + 1) * rows]


def attn_bwd_kernel(first, prefix_s, valid_s, core_s, q_own_ref, q_oth_ref, g_own_ref, g_oth_ref, kv_ref, cos_ref, sin_ref,
                    qpos_ref, kpos_ref, dq_own_ref, dq_oth_ref, dkv_own_ref, dkv_oth_ref):
    b = pl.program_id(0) + first
    rows, width = q_own_ref.shape[1:]
    hd = kv_ref.shape[-1] // 2
    half = hd // 2
    heads = width // hd
    scale = hd ** -0.5
    cos_t, sin_t = cos_ref[...], sin_ref[...]
    shards = kv_ref.shape[0] // 2
    keys = own_first(kv_ref, core_s[0], 0, hd)
    values = own_first(kv_ref, core_s[0], hd, 2 * hd)
    limit = jnp.minimum(valid_s[b], jnp.maximum(prefix_s[b], qpos_ref[...] + 1))
    visible = kpos_ref[...] < limit
    d_keys, d_values = 0.0, 0.0
    for q_ref, g_ref, dst in ((q_own_ref, g_own_ref, dq_own_ref), (q_oth_ref, g_oth_ref, dq_oth_ref)):
        query = jnp.concatenate([q_ref[0, :, n * hd:(n + 1) * hd] for n in range(heads)], axis=0)
        grad = jnp.concatenate([g_ref[0, :, n * hd:(n + 1) * hd] for n in range(heads)], axis=0)
        scores = dot_f32(keys, query, 1, 1)
        scores = jnp.where(visible, scores, MASKED)
        top = jnp.max(scores, axis=0, keepdims=True)
        expo = jnp.exp(scores - top)
        inv = 1.0 / jnp.sum(expo, axis=0, keepdims=True)
        probs = expo * inv
        d_probs = dot_f32(values, grad, 1, 1)
        delta = jnp.sum(probs * d_probs, axis=0, keepdims=True)
        d_scores = (probs * (d_probs - delta)).astype(BF16)
        d_values = d_values + dot_f32(probs.astype(BF16), grad, 1, 0)
        d_keys = d_keys + dot_f32(d_scores, query, 1, 0)
        d_query = dot_f32(d_scores, keys, 0, 0) * scale
        for n in range(heads):
            g_1 = d_query[n * rows:(n + 1) * rows, :half]
            g_2 = d_query[n * rows:(n + 1) * rows, half:]
            dst[0, :, n * hd:n * hd + half] = (g_1 * cos_t + g_2 * sin_t).astype(BF16)
            dst[0, :, n * hd + half:(n + 1) * hd] = (g_2 * cos_t - g_1 * sin_t).astype(BF16)
    d_keys = d_keys.astype(BF16)
    d_values = d_values.astype(BF16)
    span = kv_ref.shape[2]
    for k, dst in enumerate((dkv_own_ref, dkv_oth_ref)):
        for c in range(shards):
            at = (k * shards + c) * span
            dst[c, 0, :, :hd] = d_keys[at:at + span]
            dst[c, 0, :, hd:] = d_values[at:at + span]


def attn_specs(rows, width, shards, two_hd, half):
    q_spec = pl.BlockSpec((1, rows, width), lambda b, *_: (b, 0, 0))
    kv_spec = pl.BlockSpec((shards, 1, rows, two_hd), lambda b, *_: (0, b, 0, 0))
    tab_spec = pl.BlockSpec((rows, half), lambda b, *_: (0, 0))
    return q_spec, kv_spec, tab_spec


def whole(shape):
    return pl.BlockSpec(shape, lambda b, *_: tuple(0 for _ in shape))


def attn_fwd(q_own, q_oth, kv_all, cos_t, sin_t, qpos, kpos, scalars):
    batch, rows, width = q_own.shape
    shards, two_hd = kv_all.shape[0], kv_all.shape[3]
    q_spec, kv_spec, tab_spec = attn_specs(rows, width, shards, two_hd, two_hd // 4)
    heads = width * 2 // two_hd
    out = jax.ShapeDtypeStruct((batch, rows, width), BF16)
    qpos_col = jnp.tile(qpos, heads)[:, None]
    n_keys = kpos.shape[0]
    flops = 2 * 2 * batch * rows * 2 * width * n_keys
    return pl.pallas_call(
        attn_fwd_kernel,
        out_shape=(out, out, out, out),
        grid_spec=pltpu.PrefetchScalarGridSpec(
            num_scalar_prefetch=3, grid=(batch,),
            in_specs=[q_spec, q_spec, kv_spec, tab_spec, tab_spec, whole((heads * rows, 1)), whole((1, n_keys))],
            out_specs=[q_spec] * 4),
        compiler_params=pltpu.CompilerParams(dimension_semantics=("arbitrary",), vmem_limit_bytes=30 << 20),
        cost_estimate=pl.CostEstimate(flops=flops, bytes_accessed=batch * rows * width * 16 + kv_all.size * 2, transcendentals=batch * rows * heads * 2 * n_keys),
        name="attn_fwd",
    )(*scalars, q_own, q_oth, kv_all, cos_t, sin_t, qpos_col, kpos[None, :])


def attn_bwd(order, q_own, q_oth, g_own, g_oth, kv_all, cos_t, sin_t, qpos, kpos, scalars, first, count, earlier):
    batch, rows, width = q_own.shape
    shards, two_hd = kv_all.shape[0], kv_all.shape[3]
    tab_spec = pl.BlockSpec((rows, two_hd // 4), lambda b, *_: (0, 0))
    q_spec = pl.BlockSpec((1, rows, width), lambda b, *_: (b + first, 0, 0))
    kv_spec = pl.BlockSpec((shards, 1, rows, two_hd), lambda b, *_: (0, b + first, 0, 0))
    heads = width * 2 // two_hd
    out = jax.ShapeDtypeStruct((batch, rows, width), BF16)
    dkv_spec = pl.BlockSpec((shards // 2, 1, rows, two_hd), lambda b, *_: (0, b + first, 0, 0))
    kv_out = jax.ShapeDtypeStruct((shards // 2, batch, rows, two_hd), BF16)
    qpos_row = jnp.tile(qpos, heads)[None, :]
    n_keys = kpos.shape[0]
    flops = 2 * 5 * count * rows * 2 * width * n_keys
    return order.call(
        functools.partial(attn_bwd_kernel, first), 9, len(earlier), prefetch=3, in_parts=True,
        out_shape=(out, out, kv_out, kv_out), grid=(count,),
        in_specs=[q_spec, q_spec, q_spec, q_spec, kv_spec, tab_spec, tab_spec, whole((1, heads * rows)), whole((n_keys, 1))],
        out_specs=[q_spec, q_spec, dkv_spec, dkv_spec],
        compiler_params=pltpu.CompilerParams(dimension_semantics=("arbitrary",), vmem_limit_bytes=30 << 20),
        cost_estimate=pl.CostEstimate(flops=flops, bytes_accessed=count * rows * width * 12 + kv_all.size * 4, transcendentals=count * rows * heads * 2 * n_keys),
        name="attn_bwd",
    )(*scalars, q_own, q_oth, g_own, g_oth, kv_all, cos_t, sin_t, qpos_row, kpos[:, None], *earlier)


class Order:
    def __init__(self):
        self.last = None

    def call(self, kernel, n_in, n_kept=0, *, in_specs, out_specs, out_shape, grid, in_parts=False, after=(), prefetch=0, scratch_shapes=(), **options):
        def run(*args):
            deps = (() if self.last is None or any(self.last is a for a in args) else (self.last,)) + tuple(after)
            n_args = prefetch + n_in

            def body(*refs):
                kernel(*refs[:n_args], *refs[n_args + n_kept + len(deps):])

            n_out = len(out_specs) if isinstance(out_specs, (list, tuple)) else 1
            shapes = [pltpu.HBM(o.shape, o.dtype) if in_parts and o.size > 1 << 17 else o for o in out_shape] if in_parts else out_shape
            first = n_args
            args = args[:first] + tuple(pltpu.with_memory_space_constraint(a, pltpu.HBM) for a in args[first:])
            out = pl.pallas_call(
                body, out_shape=shapes,
                grid_spec=pltpu.PrefetchScalarGridSpec(
                    num_scalar_prefetch=prefetch, grid=grid, scratch_shapes=scratch_shapes, out_specs=out_specs,
                    in_specs=in_specs + [pl.BlockSpec(memory_space=pl.ANY)] * (n_kept + len(deps))),
                input_output_aliases={n_args + k: n_out - n_kept + k for k in range(n_kept)},
                **options)(*args, *deps)
            self.last = out[0] if isinstance(out, (tuple, list)) else out
            return out

        return run


def params(steps, limit=56):
    return pltpu.CompilerParams(dimension_semantics=("arbitrary",) * steps, vmem_limit_bytes=limit << 20)


def cost(flops, *arrays):
    return pl.CostEstimate(flops=flops, bytes_accessed=sum(a.size * a.dtype.itemsize for a in arrays), transcendentals=0)


def rows_of(ref):
    return ref[...].reshape(-1, ref.shape[-1])


def raw_spec(shape):
    return pl.BlockSpec((2, 1) + shape[2:], lambda j, i, core: (lax.rem(i, 2), lax.bitwise_xor(core[0], lax.div(i, 2)), 0, 0))


def d_act_kernel(core_s, g_ref, wd_ref, out_ref):
    out_ref[...] = dot_f32(rows_of(g_ref), wd_ref[...], 1, 1).astype(BF16)


def d_act_call(order, core, g_all, w_down, tn=1024):
    chips, _, rows, dim = g_all.shape
    width = w_down.shape[0]
    out = jax.ShapeDtypeStruct((chips * 2 * rows, width), BF16)
    return order.call(
        d_act_kernel, 2, prefetch=1, out_shape=out, grid=(width // tn, chips),
        in_specs=[raw_spec(g_all.shape), pl.BlockSpec((tn, dim), lambda j, i, core: (j, 0))],
        out_specs=pl.BlockSpec((2 * rows, tn), lambda j, i, core: (i, j)), compiler_params=params(2),
        cost_estimate=cost(2 * g_all.size * width, g_all, w_down, out), name="d_act",
    )(core, g_all, w_down)


def act_kernel(core_s, z_ref, g_ref, wg_ref, wu_ref, *refs, sub):
    c_1 = math.sqrt(2.0 / math.pi)
    c_3 = 0.044715 * c_1
    act_ref, dg_ref, du_ref = refs[-3:]
    z_in = rows_of(z_ref)
    for j in range(0, wg_ref.shape[1], sub):
        gate = dot_f32(z_in, wg_ref[:, j:j + sub], 1, 0)
        upper = dot_f32(z_in, wu_ref[:, j:j + sub], 1, 0)
        if len(refs) == 4:
            d_act = dot_f32(rows_of(g_ref), refs[0][j:j + sub, :], 1, 1).astype(BF16).astype(F32)
        else:
            d_act = g_ref[:, j:j + sub].astype(F32)
        square = gate * gate
        half = 0.5 * jnp.tanh(gate * (c_3 * square + c_1)) + 0.5
        gelu = gate * half
        act_ref[:, j:j + sub] = (gelu * upper).astype(BF16)
        du_ref[:, j:j + sub] = (d_act * gelu).astype(BF16)
        slope = half + gelu * (1.0 - half) * (6.0 * c_3 * square + 2.0 * c_1)
        dg_ref[:, j:j + sub] = (d_act * upper * slope).astype(BF16)


def act_call(order, core, z_all, g_all, w_gate, w_up, w_down, sub=256):
    chips, _, rows, dim = z_all.shape
    width = w_gate.shape[1]
    out = jax.ShapeDtypeStruct((chips * 2 * rows, width), BF16)
    tn = 1024 if w_down is None else 512
    raw = raw_spec(z_all.shape)
    col = pl.BlockSpec((dim, tn), lambda j, i, core: (0, j))
    tile = pl.BlockSpec((2 * rows, tn), lambda j, i, core: (i, j))
    args = (z_all, g_all, w_gate, w_up) + (() if w_down is None else (w_down,))
    specs = [raw, tile if w_down is None else raw, col, col] + ([] if w_down is None else [pl.BlockSpec((tn, dim), lambda j, i, core: (j, 0))])
    return order.call(
        functools.partial(act_kernel, sub=sub), len(args), prefetch=1, out_shape=(out, out, out), grid=(width // tn, chips),
        in_specs=specs, out_specs=[tile] * 3, compiler_params=params(2),
        cost_estimate=cost(2 * (len(args) - 2) * z_all.size * width, *args, out, out, out), name="mlp_act",
    )(core, *args)


def back_kernel(*refs, terms, joined, n_far, base, tn):
    n = len(terms)
    lhs, rhs, far, out = refs[:n], refs[n:2 * n], refs[2 * n:2 * n + n_far], refs[2 * n + n_far]
    l_bufs, r_bufs, (l_sems, r_sems) = refs[2 * n + n_far + 1:][:n], refs[3 * n + n_far + 1:][:n], refs[4 * n + n_far + 1:]
    j, i = pl.program_id(0), pl.program_id(1)
    blocks, rows = l_bufs[0].shape[:2]

    def left(p, at):
        return pltpu.make_async_copy(lhs[p].at[pl.ds((base + at) * rows, rows)], l_bufs[p].at[at], l_sems.at[p, at])

    def right(p, tile):
        cols = pl.ds(pl.multiple_of(tile * tn, tn), tn)
        src = rhs[p].at[:, cols] if terms[p][0] == 0 else rhs[p].at[cols]
        return pltpu.make_async_copy(src, r_bufs[p].at[lax.rem(tile, 2)], r_sems.at[p, lax.rem(tile, 2)])

    @pl.when((j == 0) & (i == 0))
    def _():
        for p in range(n):
            right(p, 0).start()
            left(p, 0).start()
        for at in range(1, blocks):
            for p in range(n):
                left(p, at).start()

    @pl.when((i == blocks - 1) & (j + 1 < pl.num_programs(0)))
    def _():
        for p in range(n):
            right(p, j + 1).start()

    def compute(ready):
        totals = {}
        for p, (dim, kind) in enumerate(terms):
            ready(p)
            part = dot_f32(l_bufs[p][i], r_bufs[p][lax.rem(j, 2)], 1, dim)
            totals[kind] = totals[kind] + part if kind in totals else part
        for kind, total in totals.items():
            at = (slice(None), kind) if joined else (slice(None),)
            total = total.reshape(out[at].shape)
            if far:
                total += far[0][at].astype(F32)
            out[at] = total.astype(BF16)

    @pl.when(j == 0)
    def _():
        def ready(p):
            @pl.when(i == 0)
            def _():
                right(p, 0).wait()

            left(p, i).wait()

        compute(ready)

    @pl.when(j > 0)
    def _():
        @pl.when(i == 0)
        def _():
            for p in range(n):
                right(p, j).wait()

        compute(lambda p: None)


def back_call(order, side, lhs, rhs, terms, far, chips, tn=512):
    dim = rhs[0].shape[0 if terms[0][0] else 1]
    rows = lhs[0].shape[0] // (2 * chips)
    half, n = chips // 2, len(terms)
    kinds = sorted({kind for _, kind in terms})
    joined = len(kinds) == 2
    hbm = pl.BlockSpec(memory_space=pl.ANY)
    both = pl.BlockSpec((2, 2, rows, tn), lambda j, i: (i, 0, 0, j))
    out = jax.ShapeDtypeStruct((chips, 2, rows, dim) if joined else (chips, rows, dim), BF16)
    far_spec = both if joined else pl.BlockSpec((2, None, rows, tn), lambda j, i: (i, kinds[0], 0, j))
    depth = lhs[0].shape[1]
    return order.call(
        functools.partial(back_kernel, terms=terms, joined=joined, n_far=len(far), base=side * half, tn=tn), 2 * n + len(far), out_shape=out,
        grid=(dim // tn, half), in_specs=[hbm] * (2 * n) + [far_spec] * len(far),
        out_specs=both if joined else pl.BlockSpec((2, rows, tn), lambda j, i: (i, 0, j)),
        scratch_shapes=[pltpu.VMEM((half, 2 * rows, depth), BF16)] * n
        + [pltpu.VMEM((2, depth, tn) if d == 0 else (2, tn, depth), BF16) for d, _ in terms]
        + [pltpu.SemaphoreType.DMA((n, half)), pltpu.SemaphoreType.DMA((n, 2))],
        compiler_params=params(2, 54),
        cost_estimate=cost(n * lhs[0].size * dim, *lhs, *rhs, out), name="mlp_back",
    )(*lhs, *rhs, *far)


def wgrad_kernel(core_s, *refs, n, tf, tn, cols, first, first_col):
    lhs, rhs, out, l_buf, r_buf, sems = refs[:n], refs[n:2 * n], *refs[2 * n:]
    i, j, k = pl.program_id(0), pl.program_id(1), pl.program_id(2)
    step = (i * cols + j) * n + k
    slot = lax.rem(step, 2)
    chips = l_buf.shape[1] // 2

    def copies(s, at, p):
        row = pl.multiple_of((lax.div(s, cols * n) + first) * tf, tf)
        col = pl.multiple_of((lax.rem(lax.div(s, n), cols) + first_col) * tn, tn)
        out = []
        for q, (ref, buf, lanes) in enumerate(((lhs[p], l_buf, pl.ds(row, tf)), (rhs[p], r_buf, pl.ds(col, tn)))):
            if ref.ndim == 4:
                for side in range(2):
                    src = ref.at[:, lax.bitwise_xor(core_s[0], side), :, lanes]
                    out.append(pltpu.make_async_copy(src, buf.at[at, pl.ds(side * chips, chips)], sems.at[q, side, at]))
            else:
                out.append(pltpu.make_async_copy(ref.at[:, :, lanes], buf.at[at], sems.at[q, 0, at]))
        return out

    def fetch(s, at):
        for p in range(n):
            @pl.when(lax.rem(s, n) == p)
            def _(p=p):
                for copy in copies(s, at, p):
                    copy.start()

    @pl.when(step == 0)
    def _():
        fetch(step, slot)

    @pl.when(step + 1 < pl.num_programs(0) * cols * n)
    def _():
        fetch(step + 1, 1 - slot)

    for copy in copies(step, slot, 0):
        copy.wait()
    part = dot_f32(rows_of(l_buf.at[slot]), rows_of(r_buf.at[slot]), 0, 0)
    out[...] = jnp.where(k == 0, part, out[...] + part)


def wgrad_call(order, core, lhs, rhs, tf=1024, tn=1024, tiles=None, col_tiles=None, earlier=None, after=()):
    n = len(lhs)
    rows = lhs[0].shape[-2]
    shards = lhs[0].size // (rows * lhs[0].shape[-1])
    width = rhs[0].shape[-1]
    height = lhs[0].shape[-1]
    first_col, last_col = col_tiles or (0, width // tn)
    cols = last_col - first_col
    first, last = tiles or (0, height // tf)
    kept = () if earlier is None else (earlier,)
    out = jax.ShapeDtypeStruct((height, width), F32)
    return order.call(
        functools.partial(wgrad_kernel, n=n, tf=tf, tn=tn, cols=cols, first=first, first_col=first_col), 2 * n, len(kept), prefetch=1, after=after, out_shape=out, grid=(last - first, cols, n),
        in_specs=[pl.BlockSpec(memory_space=pl.ANY)] * (2 * n), out_specs=pl.BlockSpec((tf, tn), lambda i, j, k, core: (i + first, j + first_col)),
        scratch_shapes=[pltpu.VMEM((2, shards, rows, tf), BF16), pltpu.VMEM((2, shards, rows, tn), BF16), pltpu.SemaphoreType.DMA((2, 2, 2))],
        compiler_params=params(3), cost_estimate=cost(2 * n * shards * rows * height * width, *lhs, *rhs, out), name="wgrad",
    )(core, *lhs, *rhs, *kept)


def kv_wgrad_kernel(l_ref, r_ref, *refs):
    out, steps = refs[-1], pl.num_programs(0)
    width = out.shape[1]

    @pl.when(pl.program_id(0) < steps - 1)
    def _():
        out[...] = dot_f32(l_ref[...], r_ref[...], 0, 0)

    @pl.when(pl.program_id(0) == steps - 1)
    def _():
        row = 0
        for terms in refs[:-1]:
            total = jnp.sum(terms[...], axis=0, keepdims=True)
            for k in range(0, total.shape[1], width):
                out[row:row + 1] = total[:, k:k + width]
                row += 1


def kv_wgrad(order, lhs, rhs, terms, tf=512):
    tokens, rows = lhs.shape
    width = rhs.shape[1]
    extra = sum(t.shape[1] for t in terms) // width
    steps = rows // tf
    out = jax.ShapeDtypeStruct((rows + extra, width), F32)
    return order.call(
        kv_wgrad_kernel, 2 + len(terms), out_shape=out, grid=(steps + 1,),
        in_specs=[pl.BlockSpec((tokens, tf), lambda i: (0, jnp.minimum(i, steps - 1))), pl.BlockSpec((tokens, width), lambda i: (0, 0))]
        + [pl.BlockSpec(t.shape, lambda i: (0, 0)) for t in terms],
        out_specs=pl.BlockSpec((tf, width), lambda i: (i, 0)), compiler_params=params(1, 40),
        cost_estimate=cost(2 * tokens * rows * width, lhs, rhs, out), name="kv_wgrad",
    )(lhs, rhs, *terms)


def head_wgrad_kernel(*refs):
    lhs, rhs, out = refs[:2], refs[2:4], refs[-1]
    for kind in range(2):
        total = dot_f32(lhs[kind][...], rhs[kind][...], 0, 0).reshape(out.shape[0], *out.shape[2:])
        for far in refs[4:-1]:
            total += far[:, kind]
        out[:, kind] = total


def head_wgrad(order, lhs, rhs, hd, far=(), tn=512):
    tokens, width = lhs[0].shape
    dim = rhs[0].shape[1]
    heads = width // hd
    out = jax.ShapeDtypeStruct((heads, 2, hd, dim), F32)
    tile = pl.BlockSpec((heads, 2, hd, tn), lambda j: (0, 0, 0, j))
    return order.call(
        head_wgrad_kernel, 4 + len(far), out_shape=out, grid=(dim // tn,),
        in_specs=[pl.BlockSpec((tokens, width), lambda j: (0, 0), pipeline_mode=pl.Buffered(1))] * 2
        + [pl.BlockSpec((tokens, tn), lambda j: (0, j))] * 2 + [tile] * len(far),
        out_specs=tile, compiler_params=params(1, 48), cost_estimate=cost(4 * tokens * width * dim, *lhs, *rhs, *far, out), name="head_wgrad",
    )(*lhs, *rhs, *far)


def add_kernel(base_ref, *refs):
    for c, part in enumerate(refs[:-1]):
        @pl.when(pl.program_id(0) == c)
        def _(part=part):
            refs[-1][...] = (base_ref[...].astype(F32) + rows_of(part).astype(F32)).astype(BF16)


def add_call(order, base, parts):
    tokens, dim = base.shape
    size = tokens // len(parts)
    row = pl.BlockSpec((size, dim), lambda i: (i, 0))
    specs = [pl.BlockSpec((1, size, dim), lambda i, at=a.shape[0] - 1: (at, 0, 0)) if a.ndim == 3 else pl.BlockSpec((size, dim), lambda i: (0, 0)) for a in parts]
    return order.call(
        add_kernel, 1 + len(parts), out_shape=jax.ShapeDtypeStruct(base.shape, BF16), grid=(len(parts),), in_specs=[row] + specs, out_specs=row,
        compiler_params=params(1, 40), cost_estimate=cost(base.size, base, base, base), name="add",
    )(base, *parts)


def resid_kernel(h_ref, a_own_ref, a_oth_ref, w_own_ref, w_oth_ref, gain_ref, resid_ref, *z_refs, sub):
    for c, z_ref in enumerate(z_refs):
        @pl.when(pl.program_id(0) == c)
        def _(z_ref=z_ref):
            for r in range(0, z_ref.shape[0], sub):
                at = slice(r, r + sub)
                total = dot_f32(a_own_ref[at], w_own_ref[...], 1, 0) + dot_f32(a_oth_ref[at], w_oth_ref[...], 1, 0)
                resid = (h_ref[at].astype(F32) + total).astype(BF16)
                resid_ref[at] = resid
                x_f = resid.astype(F32)
                inv = lax.rsqrt(jnp.mean(x_f * x_f, axis=-1, keepdims=True) + NORM_EPS)
                z_ref[at] = (x_f * inv * (1.0 + gain_ref[...])).astype(BF16)


def resid_call(order, hidden, mix_own, mix_oth, wo_own, wo_oth, gain, size, sub):
    tokens, dim = hidden.shape
    width = mix_own.shape[1]
    chunks = tokens // size
    row = pl.BlockSpec((size, dim), lambda i: (i, 0))
    mix = pl.BlockSpec((size, width), lambda i: (i, 0))
    whole_w = pl.BlockSpec((width, dim), lambda i: (0, 0))
    outs = (jax.ShapeDtypeStruct((tokens, dim), BF16),) + (jax.ShapeDtypeStruct((size, dim), BF16),) * chunks
    return order.call(
        functools.partial(resid_kernel, sub=sub), 6, out_shape=outs, grid=(chunks,),
        in_specs=[row, mix, mix, whole_w, whole_w, pl.BlockSpec((1, dim), lambda i: (0, 0))],
        out_specs=[row] + [pl.BlockSpec((size, dim), lambda i: (0, 0))] * chunks,
        compiler_params=params(1), cost_estimate=cost(4 * tokens * dim * width, hidden, mix_own, mix_oth, wo_own, wo_oth, *outs), name="resid",
    )(hidden, mix_own, mix_oth, wo_own, wo_oth, gain)


def norm_back(x_f, gain_1, d_out):
    inv = lax.rsqrt(jnp.mean(x_f * x_f, axis=-1, keepdims=True) + NORM_EPS)
    unit = x_f * inv
    scaled = d_out * gain_1
    d_x = inv * (scaled - unit * jnp.mean(scaled * unit, axis=-1, keepdims=True))
    return d_x, d_out * unit


def fold_rows(terms):
    rows, dim = terms.shape
    return jnp.sum(terms.reshape(rows // 8, 8, dim), axis=0)


def d_resid_kernel(*refs, n):
    dz_refs = refs[:n]
    x_ref, g_ref, gain_ref, w_own_ref, w_oth_ref, norm_ref, d_ref, own_ref, oth_ref = refs[n:]
    i = pl.program_id(0)

    @pl.when(i == 0)
    def _():
        norm_ref[...] = jnp.zeros_like(norm_ref)

    for c, dz_ref in enumerate(dz_refs):
        @pl.when(i == c)
        def _(dz_ref=dz_ref):
            d_x, terms = norm_back(x_ref[...].astype(F32), 1.0 + gain_ref[...], rows_of(dz_ref).astype(F32))
            norm_ref[...] += fold_rows(terms)
            d_ref[...] = (g_ref[...].astype(F32) + d_x).astype(BF16)
    own_ref[...] = dot_f32(d_ref[...], w_own_ref[...], 1, 1).astype(BF16)
    oth_ref[...] = dot_f32(d_ref[...], w_oth_ref[...], 1, 1).astype(BF16)


def d_resid_call(order, dz, resid, grad_out, gain, wo_own, wo_oth, first, size, earlier):
    tokens, dim = resid.shape
    n = len(dz)
    width = wo_own.shape[0]
    one = [pl.BlockSpec((1, size, dim) if a.ndim == 3 else (size, dim), lambda i, nd=a.ndim: (0,) * nd) for a in dz]
    far = pl.BlockSpec((size, dim), lambda i: (i + first, 0))
    mix = pl.BlockSpec((size, width), lambda i: (i + first, 0))
    whole_w = pl.BlockSpec((width, dim), lambda i: (0, 0))
    outs = (jax.ShapeDtypeStruct((8, dim), F32), jax.ShapeDtypeStruct((tokens, dim), BF16),
            jax.ShapeDtypeStruct((tokens, width), BF16), jax.ShapeDtypeStruct((tokens, width), BF16))
    return order.call(
        functools.partial(d_resid_kernel, n=n), n + 5, len(earlier), in_parts=True, out_shape=outs, grid=(n,),
        in_specs=one + [far, far, pl.BlockSpec((1, dim), lambda i: (0, 0)), whole_w, whole_w],
        out_specs=[pl.BlockSpec((8, dim), lambda i: (0, 0)), far, mix, mix],
        compiler_params=params(1, 48), cost_estimate=cost(4 * n * size * dim * width, *dz, wo_own, wo_oth, outs[1]), name="d_resid",
    )(*dz, resid, grad_out, gain, wo_own, wo_oth, *earlier)


def d_hidden_kernel(q_own_ref, q_oth_ref, dkv_ref, x_ref, d_ref, gain_ref, wq_own_ref, wq_oth_ref, wkv_ref, out_ref, norm_ref, *, sub):
    @pl.when(pl.program_id(0) == 0)
    def _():
        norm_ref[...] = jnp.zeros_like(norm_ref)

    folded = 0.0
    for r in range(0, x_ref.shape[0], sub):
        at = slice(r, r + sub)
        d_normed = (dot_f32(q_own_ref[at], wq_own_ref[...], 1, 0) + dot_f32(q_oth_ref[at], wq_oth_ref[...], 1, 0)
                    + dot_f32(dkv_ref[at], wkv_ref[...], 1, 1)).astype(BF16).astype(F32)
        d_x, terms = norm_back(x_ref[at].astype(F32), 1.0 + gain_ref[...], d_normed)
        folded += fold_rows(terms)
        out_ref[at] = (d_ref[at].astype(F32) + d_x).astype(BF16)
    norm_ref[...] += folded


def d_hidden_call(order, dq_own, dq_oth, dkv, hidden, d_resid, gain, wq_own, wq_oth, w_kv, tm, sub):
    tokens, dim = hidden.shape
    width, two_hd = dq_own.shape[1], dkv.shape[1]
    row = pl.BlockSpec((tm, dim), lambda i: (i, 0))
    mix = pl.BlockSpec((tm, width), lambda i: (i, 0))
    whole_w = pl.BlockSpec((width, dim), lambda i: (0, 0))
    outs = (jax.ShapeDtypeStruct((tokens, dim), BF16), jax.ShapeDtypeStruct((8, dim), F32))
    return order.call(
        functools.partial(d_hidden_kernel, sub=sub), 9, out_shape=outs, grid=(tokens // tm,),
        in_specs=[mix, mix, pl.BlockSpec((tm, two_hd), lambda i: (i, 0)), row, row, pl.BlockSpec((1, dim), lambda i: (0, 0)), whole_w, whole_w,
                  pl.BlockSpec((dim, two_hd), lambda i: (0, 0))],
        out_specs=[row, pl.BlockSpec((8, dim), lambda i: (0, 0))],
        compiler_params=params(1), cost_estimate=cost(4 * tokens * dim * (width + two_hd), dq_own, dq_oth, hidden, d_resid, wq_own, wq_oth, *outs), name="d_hidden",
    )(dq_own, dq_oth, dkv, hidden, d_resid, gain, wq_own, wq_oth, w_kv)


def solution(mesh):
    tp_size = mesh.shape["tp"]
    chips = tp_size // 2
    act_spec = P("dp", "tp", None)
    in_specs = (act_spec, act_spec, P("dp"), P("dp"), P(None), P(None, "tp"), P(None, None), P(None, None), P("tp", None), P(None), P(None, "tp"), P(None, "tp"), P("tp", None))
    out_specs = (act_spec, act_spec, P("dp"), P("dp", "tp"), P("dp", None), P("dp", None), P(("dp", "tp"), None), P("dp"), P("dp", "tp"), P("dp", "tp"), P(("dp", "tp"), None))
    same_core = [[2 * c + k for c in range(chips)] for k in range(2)]
    partner = [(i, i ^ 1) for i in range(tp_size)]

    def scatter4(x_part):
        flat = x_part.reshape((-1,) + x_part.shape[2:])
        return lax.psum_scatter(flat, "tp", scatter_dimension=0, tiled=True, axis_index_groups=same_core)

    def gather8(x_loc):
        return lax.all_gather(x_loc, "tp", axis=0, tiled=False)

    def swap(x_loc):
        return lax.ppermute(x_loc, "tp", partner)

    def flip(x_loc, bits):
        return lax.ppermute(x_loc, "tp", [(i, i ^ bits) for i in range(tp_size)])

    def gather4_direct(x_loc, before=None, after=None):
        chip = lax.axis_index("tp") // 2
        half = x_loc.shape[0] // 2
        near, far = flip(x_loc, 2), flip(x_loc, 4)
        if before is not None:
            near, far, _ = lax.optimization_barrier((near, far, before))
        low, high = flip(near[:half], 4), flip(far[half:], 2)
        if after is not None:
            result = after()
            x_loc, near, far, low, high, _ = lax.optimization_barrier((x_loc, near, far, low, high, result[0]))
        out = jnp.zeros((chips,) + x_loc.shape, x_loc.dtype)
        for k, block in ((0, x_loc), (1, near), (2, far)):
            out = lax.dynamic_update_slice(out, block[None], (chip ^ k, 0, 0))
        out = lax.dynamic_update_slice(out, low[None], (chip ^ 3, 0, 0))
        out = lax.dynamic_update_slice(out, high[None], (chip ^ 3, half, 0))
        return out if after is None else (out, result)

    def local_layer(hidden, grad_out, prefix_len, valid_len, attn_norm, w_query, w_key, w_value, w_out, mlp_norm, w_gate, w_up, w_down):
        batch, rows, dim = hidden.shape
        hd = w_key.shape[1]
        tokens = batch * rows
        assert batch % CHUNKS == 0
        me = lax.axis_index("tp")
        core = lax.rem(me, 2)
        qpos = me * rows + jnp.arange(rows, dtype=jnp.int32)
        shard_pos = jnp.arange(rows, dtype=jnp.int32)[None, :] + (jnp.arange(chips, dtype=jnp.int32) * 2 * rows)[:, None]
        kpos = jnp.concatenate([(shard_pos + core * rows).reshape(-1), (shard_pos + (1 - core) * rows).reshape(-1)])
        cos_t, sin_t = rope_tables(qpos, hd)

        def rope_single(raw_proj):
            return apply_rope(raw_proj, cos_t, sin_t)

        order = Order()
        scalars = (prefix_len, valid_len, core[None])
        attn_gain = attn_norm.astype(F32)
        mlp_gain = mlp_norm.astype(F32)
        wq_own = gather4_direct(w_query.T).reshape(chips * hd, dim)
        normed_flat = rms_norm(hidden, attn_gain).reshape(tokens, dim)
        w_kv = jnp.concatenate([w_key, w_value], axis=1)
        kv_raw = dot_f32(normed_flat, w_kv, 1, 0).reshape(batch, rows, 2 * hd)
        keys, key_pull = jax.vjp(rope_single, kv_raw[..., :hd])
        kv_all = gather8(jnp.concatenate([keys, kv_raw[..., hd:]], axis=-1).astype(BF16))
        wq_oth = swap(wq_own)
        q_own = dot_f32(normed_flat, wq_own, 1, 1)
        q_oth = dot_f32(normed_flat, wq_oth, 1, 1)

        def attend():
            shape = batch, rows, chips * hd
            return attn_fwd(q_own.reshape(shape), q_oth.reshape(shape), kv_all, cos_t, sin_t, qpos, kpos, scalars)

        wo_own, (mix_own, mix_oth, q_own, q_oth) = gather4_direct(w_out, (q_own, q_oth), attend)
        wo_own = wo_own.reshape(chips * hd, dim)
        wo_oth = swap(wo_own)
        mix_own = mix_own.reshape(tokens, chips * hd)
        mix_oth = mix_oth.reshape(tokens, chips * hd)
        hidden_flat = hidden.reshape(tokens, dim)
        grad_flat = grad_out.reshape(tokens, dim)
        size = tokens // CHUNKS
        resid, *z_parts = resid_call(order, hidden_flat, mix_own, mix_oth, wo_own, wo_oth, mlp_gain[None, :], size, 2 * rows)

        g_all, z_all, acts, far = [], [], [], []
        for c in range(CHUNKS):
            g_all.append(gather8(grad_flat[c * size:(c + 1) * size]).reshape(chips, 2, size, dim))
            z_all.append(gather8(z_parts[c]).reshape(chips, 2, size, dim))
        mlp_sums, d_gated = [None] * CHUNKS, [None] * CHUNKS
        weights = (w_gate, w_up, w_down)
        core_1 = core[None]
        grads = None

        def d_resid_of(first, count, earlier):
            return d_resid_call(order, d_gated[first:first + count], resid, grad_flat, mlp_gain[None, :], wo_own, wo_oth, first, size,
                                () if earlier is None else earlier[1])

        def attn_bwd_of(first, count, d_own, d_oth, earlier):
            per = batch // CHUNKS
            return attn_bwd(order, q_own, q_oth, d_own.reshape(batch, rows, -1), d_oth.reshape(batch, rows, -1), kv_all, cos_t, sin_t, qpos, kpos,
                            scalars, first * per, count * per, () if earlier is None else earlier[2])

        d_z_terms, mlp_terms = ((1, 0), (1, 0)), ((0, 1),)

        def back_both(c, side, far):
            return back_call(order, side, (acts[c][1], acts[c][2], acts[c][0]), weights, d_z_terms + mlp_terms, far, chips)

        def finish(c):
            both = back_both(c, 0, (far[c],))
            both = scatter4(both).reshape(2, size, dim)
            d_gated[c] = mlp_sums[c] = both

        def finish_last(c):
            part = back_call(order, 0, acts[c][1:], weights[:2], d_z_terms, (far[c],), chips)
            d_gated[c] = scatter4(part).reshape(size, dim)
            part = back_call(order, 0, acts[c][:1], weights[2:], mlp_terms, (far[c],), chips)
            mlp_sums[c] = scatter4(part).reshape(size, dim)

        for c in range(CHUNKS):
            if c < CHUNKS - 1:
                d_act = d_act_call(order, core_1, g_all[c], w_down)
                acts.append(act_call(order, core_1, z_all[c], d_act, w_gate, w_up, None))
            else:
                acts.append(act_call(order, core_1, z_all[c], g_all[c], *weights))
            part = back_both(c, 1, ())
            far.append(swap(part))
            if c == CHUNKS - 2:
                for earlier in range(c + 1):
                    finish(earlier)
        terms, *d_parts = d_resid_of(0, 1, None)
        grads = terms, d_parts, attn_bwd_of(0, 1, d_parts[1], d_parts[2], None)
        finish_last(CHUNKS - 1)
        shards = [[a.reshape(2 * chips, size, -1) for a in acts[c]] for c in range(CHUNKS)]
        g_gate = wgrad_call(order, core_1, z_all, [a[1] for a in shards], tiles=(0, 1))

        terms, d_resid, d_own, d_oth = d_resid_of(1, CHUNKS - 1, grads)
        norm_terms, (dq_own, dq_oth, dkv_own, dkv_oth) = grads[0] + terms, attn_bwd_of(1, CHUNKS - 1, d_own, d_oth, grads)
        dq_own = dq_own.reshape(tokens, chips * hd)
        dq_oth = dq_oth.reshape(tokens, chips * hd)
        dkv_far = swap(dkv_oth)
        heads_far = head_wgrad(order, (mix_oth, dq_oth), (d_resid, normed_flat), hd)
        dkv_far, dkv_own, _ = lax.optimization_barrier((dkv_far, dkv_own, heads_far))
        dkv = scatter4((dkv_own.astype(F32) + dkv_far.astype(F32)).astype(BF16))
        heads_far = swap(heads_far)

        def gate_quarter(k, earlier):
            return wgrad_call(order, core_1, z_all, [a[1] for a in shards], tiles=(1, 2), col_tiles=(k, k + 1), earlier=earlier)

        g_gate = gate_quarter(0, g_gate)
        g_heads = head_wgrad(order, (mix_own, dq_own), (d_resid, normed_flat), hd, (heads_far,))
        g_heads = scatter4(g_heads)
        g_gate = gate_quarter(1, g_gate)
        dkv, g_gate = lax.optimization_barrier((dkv, g_gate))
        g_out, g_query = g_heads[0], g_heads[1].T
        d_k_raw = key_pull(dkv[..., :hd].astype(F32))[0]
        dkv = jnp.concatenate([d_k_raw.astype(BF16), dkv[..., hd:]], axis=-1).reshape(tokens, 2 * hd)
        grad_hidden, attn_terms = d_hidden_call(
            order, dq_own, dq_oth, dkv, hidden_flat, d_resid, attn_gain[None, :], wq_own, wq_oth, w_kv, 4 * rows, 2 * rows)
        sums = kv_wgrad(order, normed_flat, dkv, (attn_terms, norm_terms))
        sums = lax.psum(sums, "tp")
        g_attn_norm, g_mlp_norm = sums[dim:].reshape(2, dim)
        hidden_out = add_call(order, resid, mlp_sums).reshape(batch, rows, dim)
        g_up = wgrad_call(order, core_1, z_all, [a[2] for a in shards])
        g_down = wgrad_call(order, core_1, [a[0] for a in shards], g_all, tiles=(0, 1))
        g_down = wgrad_call(order, core_1, [a[0] for a in shards], g_all, tiles=(1, 2), earlier=g_down, after=(g_heads,))
        return (hidden_out, grad_hidden.reshape(batch, rows, dim), g_attn_norm, g_query, sums[:dim, :hd], sums[:dim, hd:], g_out, g_mlp_norm, g_gate, g_up, g_down)

    return jax.shard_map(local_layer, mesh=mesh, in_specs=in_specs, out_specs=out_specs, check_vma=False)
```

```python
import functools
import math
import jax
import jax.numpy as jnp
from jax import lax
from jax.experimental import pallas as pl
from jax.experimental.pallas import tpu as pltpu
from jax.sharding import PartitionSpec as P

NORM_EPS = 1e-6
CHUNKS = 3
F32 = jnp.float32
BF16 = jnp.bfloat16
MASKED = -1e30


def rms_norm(x_in, gain):
    x_f = x_in.astype(F32)
    inv_rms = lax.rsqrt(jnp.mean(x_f * x_f, axis=-1, keepdims=True) + NORM_EPS)
    return (x_f * inv_rms * (1.0 + gain)).astype(BF16)


def rope_tables(positions, head_dim):
    half_dim = head_dim // 2
    exponent = jnp.arange(half_dim, dtype=F32) * (2.0 / head_dim)
    inv_freq = jnp.exp(exponent * (-math.log(10000.0)))
    angles = positions.astype(F32)[:, None] * inv_freq[None, :]
    return jnp.cos(angles), jnp.sin(angles)


def apply_rope(x_f, cos_t, sin_t):
    half_dim = x_f.shape[-1] // 2
    first = x_f[..., :half_dim]
    second = x_f[..., half_dim:]
    return jnp.concatenate([first * cos_t - second * sin_t, second * cos_t + first * sin_t], axis=-1)


def dot_f32(lhs, rhs, lhs_dim, rhs_dim):
    return lax.dot_general(lhs, rhs, (((lhs_dim,), (rhs_dim,)), ((), ())), preferred_element_type=F32)


def own_first(kv_ref, core, lo, hi):
    shards = kv_ref.shape[0] // 2
    return jnp.concatenate([kv_ref[2 * c + side, 0, :, lo:hi] for side in (core, 1 - core) for c in range(shards)], axis=0)


def attn_fwd_kernel(prefix_s, valid_s, core_s, q_own_ref, q_oth_ref, kv_ref, cos_ref, sin_ref, qpos_ref, kpos_ref,
                    o_own_ref, o_oth_ref, r_own_ref, r_oth_ref):
    b = pl.program_id(0)
    rows, width = q_own_ref.shape[1:]
    hd = kv_ref.shape[-1] // 2
    half = hd // 2
    heads = width // hd
    scale = hd ** -0.5
    cos_t, sin_t = cos_ref[...], sin_ref[...]
    queries = []
    for src, dst in ((q_own_ref, r_own_ref), (q_oth_ref, r_oth_ref)):
        for n in range(heads):
            first = src[0, :, n * hd:n * hd + half]
            second = src[0, :, n * hd + half:(n + 1) * hd]
            q_1 = ((first * cos_t - second * sin_t).astype(BF16) * scale).astype(BF16)
            q_2 = ((second * cos_t + first * sin_t).astype(BF16) * scale).astype(BF16)
            dst[0, :, n * hd:n * hd + half] = q_1
            dst[0, :, n * hd + half:(n + 1) * hd] = q_2
            queries.append(jnp.concatenate([q_1, q_2], axis=1))
    keys = own_first(kv_ref, core_s[0], 0, hd)
    values = own_first(kv_ref, core_s[0], hd, 2 * hd)
    limit = jnp.minimum(valid_s[b], jnp.maximum(prefix_s[b], qpos_ref[...] + 1))
    visible = kpos_ref[...] < limit
    for side, dst in ((0, o_own_ref), (1, o_oth_ref)):
        query = jnp.concatenate(queries[side * heads:(side + 1) * heads], axis=0)
        scores = dot_f32(query, keys, 1, 1)
        scores = jnp.where(visible, scores, MASKED)
        top = jnp.max(scores, axis=-1, keepdims=True)
        expo = jnp.exp(scores - top)
        inv = 1.0 / jnp.sum(expo, axis=-1, keepdims=True)
        probs = (expo * inv).astype(BF16)
        mixed = dot_f32(probs, values, 1, 0).astype(BF16)
        for n in range(heads):
            dst[0, :, n * hd:(n + 1) * hd] = mixed[n * rows:(n + 1) * rows]


def attn_bwd_kernel(first, prefix_s, valid_s, core_s, q_own_ref, q_oth_ref, g_own_ref, g_oth_ref, kv_ref, cos_ref, sin_ref,
                    qpos_ref, kpos_ref, dq_own_ref, dq_oth_ref, dkv_own_ref, dkv_oth_ref):
    b = pl.program_id(0) + first
    rows, width = q_own_ref.shape[1:]
    hd = kv_ref.shape[-1] // 2
    half = hd // 2
    heads = width // hd
    scale = hd ** -0.5
    cos_t, sin_t = cos_ref[...], sin_ref[...]
    shards = kv_ref.shape[0] // 2
    keys = own_first(kv_ref, core_s[0], 0, hd)
    values = own_first(kv_ref, core_s[0], hd, 2 * hd)
    limit = jnp.minimum(valid_s[b], jnp.maximum(prefix_s[b], qpos_ref[...] + 1))
    visible = kpos_ref[...] < limit
    d_keys, d_values = 0.0, 0.0
    for q_ref, g_ref, dst in ((q_own_ref, g_own_ref, dq_own_ref), (q_oth_ref, g_oth_ref, dq_oth_ref)):
        query = jnp.concatenate([q_ref[0, :, n * hd:(n + 1) * hd] for n in range(heads)], axis=0)
        grad = jnp.concatenate([g_ref[0, :, n * hd:(n + 1) * hd] for n in range(heads)], axis=0)
        scores = dot_f32(keys, query, 1, 1)
        scores = jnp.where(visible, scores, MASKED)
        top = jnp.max(scores, axis=0, keepdims=True)
        expo = jnp.exp(scores - top)
        inv = 1.0 / jnp.sum(expo, axis=0, keepdims=True)
        probs = expo * inv
        d_probs = dot_f32(values, grad, 1, 1)
        delta = jnp.sum(probs * d_probs, axis=0, keepdims=True)
        d_scores = (probs * (d_probs - delta)).astype(BF16)
        d_values = d_values + dot_f32(probs.astype(BF16), grad, 1, 0)
        d_keys = d_keys + dot_f32(d_scores, query, 1, 0)
        d_query = dot_f32(d_scores, keys, 0, 0) * scale
        for n in range(heads):
            g_1 = d_query[n * rows:(n + 1) * rows, :half]
            g_2 = d_query[n * rows:(n + 1) * rows, half:]
            dst[0, :, n * hd:n * hd + half] = (g_1 * cos_t + g_2 * sin_t).astype(BF16)
            dst[0, :, n * hd + half:(n + 1) * hd] = (g_2 * cos_t - g_1 * sin_t).astype(BF16)
    d_keys = d_keys.astype(BF16)
    d_values = d_values.astype(BF16)
    span = kv_ref.shape[2]
    for k, dst in enumerate((dkv_own_ref, dkv_oth_ref)):
        for c in range(shards):
            at = (k * shards + c) * span
            dst[c, 0, :, :hd] = d_keys[at:at + span]
            dst[c, 0, :, hd:] = d_values[at:at + span]


def attn_specs(rows, width, shards, two_hd, half):
    q_spec = pl.BlockSpec((1, rows, width), lambda b, *_: (b, 0, 0))
    kv_spec = pl.BlockSpec((shards, 1, rows, two_hd), lambda b, *_: (0, b, 0, 0))
    tab_spec = pl.BlockSpec((rows, half), lambda b, *_: (0, 0))
    return q_spec, kv_spec, tab_spec


def whole(shape):
    return pl.BlockSpec(shape, lambda b, *_: tuple(0 for _ in shape))


def attn_fwd(q_own, q_oth, kv_all, cos_t, sin_t, qpos, kpos, scalars):
    batch, rows, width = q_own.shape
    shards, two_hd = kv_all.shape[0], kv_all.shape[3]
    q_spec, kv_spec, tab_spec = attn_specs(rows, width, shards, two_hd, two_hd // 4)
    heads = width * 2 // two_hd
    out = jax.ShapeDtypeStruct((batch, rows, width), BF16)
    qpos_col = jnp.tile(qpos, heads)[:, None]
    n_keys = kpos.shape[0]
    flops = 2 * 2 * batch * rows * 2 * width * n_keys
    return pl.pallas_call(
        attn_fwd_kernel,
        out_shape=(out, out, out, out),
        grid_spec=pltpu.PrefetchScalarGridSpec(
            num_scalar_prefetch=3, grid=(batch,),
            in_specs=[q_spec, q_spec, kv_spec, tab_spec, tab_spec, whole((heads * rows, 1)), whole((1, n_keys))],
            out_specs=[q_spec] * 4),
        compiler_params=pltpu.CompilerParams(dimension_semantics=("arbitrary",), vmem_limit_bytes=60 << 20),
        cost_estimate=pl.CostEstimate(flops=flops, bytes_accessed=batch * rows * width * 16 + kv_all.size * 2, transcendentals=batch * rows * heads * 2 * n_keys),
        name="attn_fwd",
    )(*scalars, q_own, q_oth, kv_all, cos_t, sin_t, qpos_col, kpos[None, :])


def attn_bwd(order, q_own, q_oth, g_own, g_oth, kv_all, cos_t, sin_t, qpos, kpos, scalars, first, count, earlier):
    batch, rows, width = q_own.shape
    shards, two_hd = kv_all.shape[0], kv_all.shape[3]
    tab_spec = pl.BlockSpec((rows, two_hd // 4), lambda b, *_: (0, 0))
    q_spec = pl.BlockSpec((1, rows, width), lambda b, *_: (b + first, 0, 0))
    kv_spec = pl.BlockSpec((shards, 1, rows, two_hd), lambda b, *_: (0, b + first, 0, 0))
    heads = width * 2 // two_hd
    out = jax.ShapeDtypeStruct((batch, rows, width), BF16)
    dkv_spec = pl.BlockSpec((shards // 2, 1, rows, two_hd), lambda b, *_: (0, b + first, 0, 0))
    kv_out = jax.ShapeDtypeStruct((shards // 2, batch, rows, two_hd), BF16)
    qpos_row = jnp.tile(qpos, heads)[None, :]
    n_keys = kpos.shape[0]
    flops = 2 * 5 * count * rows * 2 * width * n_keys
    return order.call(
        functools.partial(attn_bwd_kernel, first), 9, len(earlier), prefetch=3, in_parts=True,
        out_shape=(out, out, kv_out, kv_out), grid=(count,),
        in_specs=[q_spec, q_spec, q_spec, q_spec, kv_spec, tab_spec, tab_spec, whole((1, heads * rows)), whole((n_keys, 1))],
        out_specs=[q_spec, q_spec, dkv_spec, dkv_spec],
        compiler_params=pltpu.CompilerParams(dimension_semantics=("arbitrary",), vmem_limit_bytes=60 << 20),
        cost_estimate=pl.CostEstimate(flops=flops, bytes_accessed=count * rows * width * 12 + kv_all.size * 4, transcendentals=count * rows * heads * 2 * n_keys),
        name="attn_bwd",
    )(*scalars, q_own, q_oth, g_own, g_oth, kv_all, cos_t, sin_t, qpos_row, kpos[:, None], *earlier)


class Order:
    def __init__(self):
        self.last = None

    def call(self, kernel, n_in, n_kept=0, *, in_specs, out_specs, out_shape, grid, in_parts=False, after=(), prefetch=0, scratch_shapes=(), **options):
        def run(*args):
            deps = (() if self.last is None or any(self.last is a for a in args) else (self.last,)) + tuple(after)
            n_args = prefetch + n_in

            def body(*refs):
                kernel(*refs[:n_args], *refs[n_args + n_kept + len(deps):])

            n_out = len(out_specs) if isinstance(out_specs, (list, tuple)) else 1
            shapes = [pltpu.HBM(o.shape, o.dtype) if in_parts and o.size > 1 << 17 else o for o in out_shape] if in_parts else out_shape
            first = n_args
            args = args[:first] + tuple(pltpu.with_memory_space_constraint(a, pltpu.HBM) for a in args[first:])
            out = pl.pallas_call(
                body, out_shape=shapes,
                grid_spec=pltpu.PrefetchScalarGridSpec(
                    num_scalar_prefetch=prefetch, grid=grid, scratch_shapes=scratch_shapes, out_specs=out_specs,
                    in_specs=in_specs + [pl.BlockSpec(memory_space=pl.ANY)] * (n_kept + len(deps))),
                input_output_aliases={n_args + k: n_out - n_kept + k for k in range(n_kept)},
                **options)(*args, *deps)
            self.last = out[0] if isinstance(out, (tuple, list)) else out
            return out

        return run


def params(steps, limit=60):
    return pltpu.CompilerParams(dimension_semantics=("arbitrary",) * steps, vmem_limit_bytes=limit << 20)


def cost(flops, *arrays):
    return pl.CostEstimate(flops=flops, bytes_accessed=sum(a.size * a.dtype.itemsize for a in arrays), transcendentals=0)


def rows_of(ref):
    return ref[...].reshape(-1, ref.shape[-1])


def raw_spec(shape):
    return pl.BlockSpec((2, 1) + shape[2:], lambda j, i, core: (lax.rem(i, 2), lax.bitwise_xor(core[0], lax.div(i, 2)), 0, 0))


def d_act_kernel(core_s, g_ref, wd_ref, out_ref):
    out_ref[...] = dot_f32(rows_of(g_ref), wd_ref[...], 1, 1).astype(BF16)


def d_act_call(order, core, g_all, w_down, tn=1024):
    chips, _, rows, dim = g_all.shape
    width = w_down.shape[0]
    out = jax.ShapeDtypeStruct((chips * 2 * rows, width), BF16)
    return order.call(
        d_act_kernel, 2, prefetch=1, out_shape=out, grid=(width // tn, chips),
        in_specs=[raw_spec(g_all.shape), pl.BlockSpec((tn, dim), lambda j, i, core: (j, 0))],
        out_specs=pl.BlockSpec((2 * rows, tn), lambda j, i, core: (i, j)), compiler_params=params(2),
        cost_estimate=cost(2 * g_all.size * width, g_all, w_down, out), name="d_act",
    )(core, g_all, w_down)


def act_kernel(core_s, z_ref, g_ref, wg_ref, wu_ref, *refs, sub):
    c_1 = math.sqrt(2.0 / math.pi)
    c_3 = 0.044715 * c_1
    act_ref, dg_ref, du_ref = refs[-3:]
    z_in = rows_of(z_ref)
    for j in range(0, wg_ref.shape[1], sub):
        gate = dot_f32(z_in, wg_ref[:, j:j + sub], 1, 0)
        upper = dot_f32(z_in, wu_ref[:, j:j + sub], 1, 0)
        if len(refs) == 4:
            d_act = dot_f32(rows_of(g_ref), refs[0][j:j + sub, :], 1, 1).astype(BF16).astype(F32)
        else:
            d_act = g_ref[:, j:j + sub].astype(F32)
        square = gate * gate
        half = 0.5 * jnp.tanh(gate * (c_3 * square + c_1)) + 0.5
        gelu = gate * half
        act_ref[:, j:j + sub] = (gelu * upper).astype(BF16)
        du_ref[:, j:j + sub] = (d_act * gelu).astype(BF16)
        slope = half + gelu * (1.0 - half) * (6.0 * c_3 * square + 2.0 * c_1)
        dg_ref[:, j:j + sub] = (d_act * upper * slope).astype(BF16)


def act_call(order, core, z_all, g_all, w_gate, w_up, w_down, sub=256):
    chips, _, rows, dim = z_all.shape
    width = w_gate.shape[1]
    out = jax.ShapeDtypeStruct((chips * 2 * rows, width), BF16)
    tn = 1024 if w_down is None else 512
    raw = raw_spec(z_all.shape)
    col = pl.BlockSpec((dim, tn), lambda j, i, core: (0, j))
    tile = pl.BlockSpec((2 * rows, tn), lambda j, i, core: (i, j))
    args = (z_all, g_all, w_gate, w_up) + (() if w_down is None else (w_down,))
    specs = [raw, tile if w_down is None else raw, col, col] + ([] if w_down is None else [pl.BlockSpec((tn, dim), lambda j, i, core: (j, 0))])
    return order.call(
        functools.partial(act_kernel, sub=sub), len(args), prefetch=1, out_shape=(out, out, out), grid=(width // tn, chips),
        in_specs=specs, out_specs=[tile] * 3, compiler_params=params(2),
        cost_estimate=cost(2 * (len(args) - 2) * z_all.size * width, *args, out, out, out), name="mlp_act",
    )(core, *args)


def back_kernel(*refs, terms, joined, n_far, base, tn):
    n = len(terms)
    lhs, rhs, far, out = refs[:n], refs[n:2 * n], refs[2 * n:2 * n + n_far], refs[2 * n + n_far]
    l_bufs, r_bufs, (l_sems, r_sems) = refs[2 * n + n_far + 1:][:n], refs[3 * n + n_far + 1:][:n], refs[4 * n + n_far + 1:]
    j, i = pl.program_id(0), pl.program_id(1)
    blocks, rows = l_bufs[0].shape[:2]

    def left(p, at):
        return pltpu.make_async_copy(lhs[p].at[pl.ds((base + at) * rows, rows)], l_bufs[p].at[at], l_sems.at[p, at])

    def right(p, tile):
        cols = pl.ds(pl.multiple_of(tile * tn, tn), tn)
        src = rhs[p].at[:, cols] if terms[p][0] == 0 else rhs[p].at[cols]
        return pltpu.make_async_copy(src, r_bufs[p].at[lax.rem(tile, 2)], r_sems.at[p, lax.rem(tile, 2)])

    @pl.when((j == 0) & (i == 0))
    def _():
        for p in range(n):
            right(p, 0).start()
            left(p, 0).start()
        for at in range(1, blocks):
            for p in range(n):
                left(p, at).start()

    @pl.when((i == blocks - 1) & (j + 1 < pl.num_programs(0)))
    def _():
        for p in range(n):
            right(p, j + 1).start()

    def compute(ready):
        totals = {}
        for p, (dim, kind) in enumerate(terms):
            ready(p)
            part = dot_f32(l_bufs[p][i], r_bufs[p][lax.rem(j, 2)], 1, dim)
            totals[kind] = totals[kind] + part if kind in totals else part
        for kind, total in totals.items():
            at = (slice(None), kind) if joined else (slice(None),)
            total = total.reshape(out[at].shape)
            if far:
                total += far[0][at].astype(F32)
            out[at] = total.astype(BF16)

    @pl.when(j == 0)
    def _():
        def ready(p):
            @pl.when(i == 0)
            def _():
                right(p, 0).wait()

            left(p, i).wait()

        compute(ready)

    @pl.when(j > 0)
    def _():
        @pl.when(i == 0)
        def _():
            for p in range(n):
                right(p, j).wait()

        compute(lambda p: None)


def back_call(order, side, lhs, rhs, terms, far, chips, tn=512):
    dim = rhs[0].shape[0 if terms[0][0] else 1]
    rows = lhs[0].shape[0] // (2 * chips)
    half, n = chips // 2, len(terms)
    kinds = sorted({kind for _, kind in terms})
    joined = len(kinds) == 2
    hbm = pl.BlockSpec(memory_space=pl.ANY)
    both = pl.BlockSpec((2, 2, rows, tn), lambda j, i: (i, 0, 0, j))
    out = jax.ShapeDtypeStruct((chips, 2, rows, dim) if joined else (chips, rows, dim), BF16)
    far_spec = both if joined else pl.BlockSpec((2, None, rows, tn), lambda j, i: (i, kinds[0], 0, j))
    depth = lhs[0].shape[1]
    return order.call(
        functools.partial(back_kernel, terms=terms, joined=joined, n_far=len(far), base=side * half, tn=tn), 2 * n + len(far), out_shape=out,
        grid=(dim // tn, half), in_specs=[hbm] * (2 * n) + [far_spec] * len(far),
        out_specs=both if joined else pl.BlockSpec((2, rows, tn), lambda j, i: (i, 0, j)),
        scratch_shapes=[pltpu.VMEM((half, 2 * rows, depth), BF16)] * n
        + [pltpu.VMEM((2, depth, tn) if d == 0 else (2, tn, depth), BF16) for d, _ in terms]
        + [pltpu.SemaphoreType.DMA((n, half)), pltpu.SemaphoreType.DMA((n, 2))],
        compiler_params=params(2),
        cost_estimate=cost(n * lhs[0].size * dim, *lhs, *rhs, out), name="mlp_back",
    )(*lhs, *rhs, *far)


def wgrad_kernel(core_s, *refs, n, tf, tn, cols, first, first_col):
    lhs, rhs, out, l_buf, r_buf, sems = refs[:n], refs[n:2 * n], *refs[2 * n:]
    i, j, k = pl.program_id(0), pl.program_id(1), pl.program_id(2)
    step = (i * cols + j) * n + k
    slot = lax.rem(step, 2)
    chips = l_buf.shape[1] // 2

    def copies(s, at, p):
        row = pl.multiple_of((lax.div(s, cols * n) + first) * tf, tf)
        col = pl.multiple_of((lax.rem(lax.div(s, n), cols) + first_col) * tn, tn)
        out = []
        for q, (ref, buf, lanes) in enumerate(((lhs[p], l_buf, pl.ds(row, tf)), (rhs[p], r_buf, pl.ds(col, tn)))):
            if ref.ndim == 4:
                for side in range(2):
                    src = ref.at[:, lax.bitwise_xor(core_s[0], side), :, lanes]
                    out.append(pltpu.make_async_copy(src, buf.at[at, pl.ds(side * chips, chips)], sems.at[q, side, at]))
            else:
                out.append(pltpu.make_async_copy(ref.at[:, :, lanes], buf.at[at], sems.at[q, 0, at]))
        return out

    def fetch(s, at):
        for p in range(n):
            @pl.when(lax.rem(s, n) == p)
            def _(p=p):
                for copy in copies(s, at, p):
                    copy.start()

    @pl.when(step == 0)
    def _():
        fetch(step, slot)

    @pl.when(step + 1 < pl.num_programs(0) * cols * n)
    def _():
        fetch(step + 1, 1 - slot)

    for copy in copies(step, slot, 0):
        copy.wait()
    part = dot_f32(rows_of(l_buf.at[slot]), rows_of(r_buf.at[slot]), 0, 0)
    out[...] = jnp.where(k == 0, part, out[...] + part)


def wgrad_call(order, core, lhs, rhs, tf=1024, tn=1024, tiles=None, col_tiles=None, earlier=None, after=()):
    n = len(lhs)
    rows = lhs[0].shape[-2]
    shards = lhs[0].size // (rows * lhs[0].shape[-1])
    width = rhs[0].shape[-1]
    height = lhs[0].shape[-1]
    first_col, last_col = col_tiles or (0, width // tn)
    cols = last_col - first_col
    first, last = tiles or (0, height // tf)
    kept = () if earlier is None else (earlier,)
    out = jax.ShapeDtypeStruct((height, width), F32)
    return order.call(
        functools.partial(wgrad_kernel, n=n, tf=tf, tn=tn, cols=cols, first=first, first_col=first_col), 2 * n, len(kept), prefetch=1, after=after, out_shape=out, grid=(last - first, cols, n),
        in_specs=[pl.BlockSpec(memory_space=pl.ANY)] * (2 * n), out_specs=pl.BlockSpec((tf, tn), lambda i, j, k, core: (i + first, j + first_col)),
        scratch_shapes=[pltpu.VMEM((2, shards, rows, tf), BF16), pltpu.VMEM((2, shards, rows, tn), BF16), pltpu.SemaphoreType.DMA((2, 2, 2))],
        compiler_params=params(3), cost_estimate=cost(2 * n * shards * rows * height * width, *lhs, *rhs, out), name="wgrad",
    )(core, *lhs, *rhs, *kept)


def kv_wgrad_kernel(l_ref, r_ref, *refs):
    out, steps = refs[-1], pl.num_programs(0)
    width = out.shape[1]

    @pl.when(pl.program_id(0) < steps - 1)
    def _():
        out[...] = dot_f32(l_ref[...], r_ref[...], 0, 0)

    @pl.when(pl.program_id(0) == steps - 1)
    def _():
        row = 0
        for terms in refs[:-1]:
            total = jnp.sum(terms[...], axis=0, keepdims=True)
            for k in range(0, total.shape[1], width):
                out[row:row + 1] = total[:, k:k + width]
                row += 1


def kv_wgrad(order, lhs, rhs, terms, tf=512):
    tokens, rows = lhs.shape
    width = rhs.shape[1]
    extra = sum(t.shape[1] for t in terms) // width
    steps = rows // tf
    out = jax.ShapeDtypeStruct((rows + extra, width), F32)
    return order.call(
        kv_wgrad_kernel, 2 + len(terms), out_shape=out, grid=(steps + 1,),
        in_specs=[pl.BlockSpec((tokens, tf), lambda i: (0, jnp.minimum(i, steps - 1))), pl.BlockSpec((tokens, width), lambda i: (0, 0))]
        + [pl.BlockSpec(t.shape, lambda i: (0, 0)) for t in terms],
        out_specs=pl.BlockSpec((tf, width), lambda i: (i, 0)), compiler_params=params(1),
        cost_estimate=cost(2 * tokens * rows * width, lhs, rhs, out), name="kv_wgrad",
    )(lhs, rhs, *terms)


def head_wgrad_kernel(*refs):
    lhs, rhs, out = refs[:2], refs[2:4], refs[-1]
    for kind in range(2):
        total = dot_f32(lhs[kind][...], rhs[kind][...], 0, 0).reshape(out.shape[0], *out.shape[2:])
        for far in refs[4:-1]:
            total += far[:, kind]
        out[:, kind] = total


def head_wgrad(order, lhs, rhs, hd, far=(), tn=512):
    tokens, width = lhs[0].shape
    dim = rhs[0].shape[1]
    heads = width // hd
    out = jax.ShapeDtypeStruct((heads, 2, hd, dim), F32)
    tile = pl.BlockSpec((heads, 2, hd, tn), lambda j: (0, 0, 0, j))
    return order.call(
        head_wgrad_kernel, 4 + len(far), out_shape=out, grid=(dim // tn,),
        in_specs=[pl.BlockSpec((tokens, width), lambda j: (0, 0), pipeline_mode=pl.Buffered(1))] * 2
        + [pl.BlockSpec((tokens, tn), lambda j: (0, j))] * 2 + [tile] * len(far),
        out_specs=tile, compiler_params=params(1), cost_estimate=cost(4 * tokens * width * dim, *lhs, *rhs, *far, out), name="head_wgrad",
    )(*lhs, *rhs, *far)


def add_kernel(base_ref, *refs):
    for c, part in enumerate(refs[:-1]):
        @pl.when(pl.program_id(0) == c)
        def _(part=part):
            refs[-1][...] = (base_ref[...].astype(F32) + rows_of(part).astype(F32)).astype(BF16)


def add_call(order, base, parts):
    tokens, dim = base.shape
    size = tokens // len(parts)
    row = pl.BlockSpec((size, dim), lambda i: (i, 0))
    specs = [pl.BlockSpec((1, size, dim), lambda i, at=a.shape[0] - 1: (at, 0, 0)) if a.ndim == 3 else pl.BlockSpec((size, dim), lambda i: (0, 0)) for a in parts]
    return order.call(
        add_kernel, 1 + len(parts), out_shape=jax.ShapeDtypeStruct(base.shape, BF16), grid=(len(parts),), in_specs=[row] + specs, out_specs=row,
        compiler_params=params(1), cost_estimate=cost(base.size, base, base, base), name="add",
    )(base, *parts)


def resid_kernel(h_ref, a_own_ref, a_oth_ref, w_own_ref, w_oth_ref, gain_ref, resid_ref, *z_refs, sub):
    for c, z_ref in enumerate(z_refs):
        @pl.when(pl.program_id(0) == c)
        def _(z_ref=z_ref):
            for r in range(0, z_ref.shape[0], sub):
                at = slice(r, r + sub)
                total = dot_f32(a_own_ref[at], w_own_ref[...], 1, 0) + dot_f32(a_oth_ref[at], w_oth_ref[...], 1, 0)
                resid = (h_ref[at].astype(F32) + total).astype(BF16)
                resid_ref[at] = resid
                x_f = resid.astype(F32)
                inv = lax.rsqrt(jnp.mean(x_f * x_f, axis=-1, keepdims=True) + NORM_EPS)
                z_ref[at] = (x_f * inv * (1.0 + gain_ref[...])).astype(BF16)


def resid_call(order, hidden, mix_own, mix_oth, wo_own, wo_oth, gain, size, sub):
    tokens, dim = hidden.shape
    width = mix_own.shape[1]
    chunks = tokens // size
    row = pl.BlockSpec((size, dim), lambda i: (i, 0))
    mix = pl.BlockSpec((size, width), lambda i: (i, 0))
    whole_w = pl.BlockSpec((width, dim), lambda i: (0, 0))
    outs = (jax.ShapeDtypeStruct((tokens, dim), BF16),) + (jax.ShapeDtypeStruct((size, dim), BF16),) * chunks
    return order.call(
        functools.partial(resid_kernel, sub=sub), 6, out_shape=outs, grid=(chunks,),
        in_specs=[row, mix, mix, whole_w, whole_w, pl.BlockSpec((1, dim), lambda i: (0, 0))],
        out_specs=[row] + [pl.BlockSpec((size, dim), lambda i: (0, 0))] * chunks,
        compiler_params=params(1), cost_estimate=cost(4 * tokens * dim * width, hidden, mix_own, mix_oth, wo_own, wo_oth, *outs), name="resid",
    )(hidden, mix_own, mix_oth, wo_own, wo_oth, gain)


def norm_back(x_f, gain_1, d_out):
    inv = lax.rsqrt(jnp.mean(x_f * x_f, axis=-1, keepdims=True) + NORM_EPS)
    unit = x_f * inv
    scaled = d_out * gain_1
    d_x = inv * (scaled - unit * jnp.mean(scaled * unit, axis=-1, keepdims=True))
    return d_x, d_out * unit


def fold_rows(terms):
    rows, dim = terms.shape
    return jnp.sum(terms.reshape(rows // 8, 8, dim), axis=0)


def d_resid_kernel(*refs, n):
    dz_refs = refs[:n]
    x_ref, g_ref, gain_ref, w_own_ref, w_oth_ref, norm_ref, d_ref, own_ref, oth_ref = refs[n:]
    i = pl.program_id(0)

    @pl.when(i == 0)
    def _():
        norm_ref[...] = jnp.zeros_like(norm_ref)

    for c, dz_ref in enumerate(dz_refs):
        @pl.when(i == c)
        def _(dz_ref=dz_ref):
            d_x, terms = norm_back(x_ref[...].astype(F32), 1.0 + gain_ref[...], rows_of(dz_ref).astype(F32))
            norm_ref[...] += fold_rows(terms)
            d_ref[...] = (g_ref[...].astype(F32) + d_x).astype(BF16)
    own_ref[...] = dot_f32(d_ref[...], w_own_ref[...], 1, 1).astype(BF16)
    oth_ref[...] = dot_f32(d_ref[...], w_oth_ref[...], 1, 1).astype(BF16)


def d_resid_call(order, dz, resid, grad_out, gain, wo_own, wo_oth, first, size, earlier):
    tokens, dim = resid.shape
    n = len(dz)
    width = wo_own.shape[0]
    one = [pl.BlockSpec((1, size, dim) if a.ndim == 3 else (size, dim), lambda i, nd=a.ndim: (0,) * nd) for a in dz]
    far = pl.BlockSpec((size, dim), lambda i: (i + first, 0))
    mix = pl.BlockSpec((size, width), lambda i: (i + first, 0))
    whole_w = pl.BlockSpec((width, dim), lambda i: (0, 0))
    outs = (jax.ShapeDtypeStruct((8, dim), F32), jax.ShapeDtypeStruct((tokens, dim), BF16),
            jax.ShapeDtypeStruct((tokens, width), BF16), jax.ShapeDtypeStruct((tokens, width), BF16))
    return order.call(
        functools.partial(d_resid_kernel, n=n), n + 5, len(earlier), in_parts=True, out_shape=outs, grid=(n,),
        in_specs=one + [far, far, pl.BlockSpec((1, dim), lambda i: (0, 0)), whole_w, whole_w],
        out_specs=[pl.BlockSpec((8, dim), lambda i: (0, 0)), far, mix, mix],
        compiler_params=params(1), cost_estimate=cost(4 * n * size * dim * width, *dz, wo_own, wo_oth, outs[1]), name="d_resid",
    )(*dz, resid, grad_out, gain, wo_own, wo_oth, *earlier)


def d_hidden_kernel(q_own_ref, q_oth_ref, dkv_ref, x_ref, d_ref, gain_ref, wq_own_ref, wq_oth_ref, wkv_ref, out_ref, norm_ref, *, sub):
    @pl.when(pl.program_id(0) == 0)
    def _():
        norm_ref[...] = jnp.zeros_like(norm_ref)

    folded = 0.0
    for r in range(0, x_ref.shape[0], sub):
        at = slice(r, r + sub)
        d_normed = (dot_f32(q_own_ref[at], wq_own_ref[...], 1, 0) + dot_f32(q_oth_ref[at], wq_oth_ref[...], 1, 0)
                    + dot_f32(dkv_ref[at], wkv_ref[...], 1, 1)).astype(BF16).astype(F32)
        d_x, terms = norm_back(x_ref[at].astype(F32), 1.0 + gain_ref[...], d_normed)
        folded += fold_rows(terms)
        out_ref[at] = (d_ref[at].astype(F32) + d_x).astype(BF16)
    norm_ref[...] += folded


def d_hidden_call(order, dq_own, dq_oth, dkv, hidden, d_resid, gain, wq_own, wq_oth, w_kv, tm, sub):
    tokens, dim = hidden.shape
    width, two_hd = dq_own.shape[1], dkv.shape[1]
    row = pl.BlockSpec((tm, dim), lambda i: (i, 0))
    mix = pl.BlockSpec((tm, width), lambda i: (i, 0))
    whole_w = pl.BlockSpec((width, dim), lambda i: (0, 0))
    outs = (jax.ShapeDtypeStruct((tokens, dim), BF16), jax.ShapeDtypeStruct((8, dim), F32))
    return order.call(
        functools.partial(d_hidden_kernel, sub=sub), 9, out_shape=outs, grid=(tokens // tm,),
        in_specs=[mix, mix, pl.BlockSpec((tm, two_hd), lambda i: (i, 0)), row, row, pl.BlockSpec((1, dim), lambda i: (0, 0)), whole_w, whole_w,
                  pl.BlockSpec((dim, two_hd), lambda i: (0, 0))],
        out_specs=[row, pl.BlockSpec((8, dim), lambda i: (0, 0))],
        compiler_params=params(1), cost_estimate=cost(4 * tokens * dim * (width + two_hd), dq_own, dq_oth, hidden, d_resid, wq_own, wq_oth, *outs), name="d_hidden",
    )(dq_own, dq_oth, dkv, hidden, d_resid, gain, wq_own, wq_oth, w_kv)


def solution(mesh):
    tp_size = mesh.shape["tp"]
    chips = tp_size // 2
    act_spec = P("dp", "tp", None)
    in_specs = (act_spec, act_spec, P("dp"), P("dp"), P(None), P(None, "tp"), P(None, None), P(None, None), P("tp", None), P(None), P(None, "tp"), P(None, "tp"), P("tp", None))
    out_specs = (act_spec, act_spec, P("dp"), P("dp", "tp"), P("dp", None), P("dp", None), P(("dp", "tp"), None), P("dp"), P("dp", "tp"), P("dp", "tp"), P(("dp", "tp"), None))
    same_core = [[2 * c + k for c in range(chips)] for k in range(2)]
    partner = [(i, i ^ 1) for i in range(tp_size)]

    def scatter4(x_part):
        flat = x_part.reshape((-1,) + x_part.shape[2:])
        return lax.psum_scatter(flat, "tp", scatter_dimension=0, tiled=True, axis_index_groups=same_core)

    def gather8(x_loc):
        return lax.all_gather(x_loc, "tp", axis=0, tiled=False)

    def swap(x_loc):
        return lax.ppermute(x_loc, "tp", partner)

    def flip(x_loc, bits):
        return lax.ppermute(x_loc, "tp", [(i, i ^ bits) for i in range(tp_size)])

    def gather4_direct(x_loc, before=None, after=None):
        chip = lax.axis_index("tp") // 2
        half = x_loc.shape[0] // 2
        near, far = flip(x_loc, 2), flip(x_loc, 4)
        if before is not None:
            near, far, _ = lax.optimization_barrier((near, far, before))
        low, high = flip(near[:half], 4), flip(far[half:], 2)
        if after is not None:
            result = after()
            x_loc, near, far, low, high, _ = lax.optimization_barrier((x_loc, near, far, low, high, result[0]))
        out = jnp.zeros((chips,) + x_loc.shape, x_loc.dtype)
        for k, block in ((0, x_loc), (1, near), (2, far)):
            out = lax.dynamic_update_slice(out, block[None], (chip ^ k, 0, 0))
        out = lax.dynamic_update_slice(out, low[None], (chip ^ 3, 0, 0))
        out = lax.dynamic_update_slice(out, high[None], (chip ^ 3, half, 0))
        return out if after is None else (out, result)

    def local_layer(hidden, grad_out, prefix_len, valid_len, attn_norm, w_query, w_key, w_value, w_out, mlp_norm, w_gate, w_up, w_down):
        batch, rows, dim = hidden.shape
        hd = w_key.shape[1]
        tokens = batch * rows
        assert batch % CHUNKS == 0
        me = lax.axis_index("tp")
        core = lax.rem(me, 2)
        qpos = me * rows + jnp.arange(rows, dtype=jnp.int32)
        shard_pos = jnp.arange(rows, dtype=jnp.int32)[None, :] + (jnp.arange(chips, dtype=jnp.int32) * 2 * rows)[:, None]
        kpos = jnp.concatenate([(shard_pos + core * rows).reshape(-1), (shard_pos + (1 - core) * rows).reshape(-1)])
        cos_t, sin_t = rope_tables(qpos, hd)

        def rope_single(raw_proj):
            return apply_rope(raw_proj, cos_t, sin_t)

        order = Order()
        scalars = (prefix_len, valid_len, core[None])
        attn_gain = attn_norm.astype(F32)
        mlp_gain = mlp_norm.astype(F32)
        wq_own = gather4_direct(w_query.T).reshape(chips * hd, dim)
        normed_flat = rms_norm(hidden, attn_gain).reshape(tokens, dim)
        w_kv = jnp.concatenate([w_key, w_value], axis=1)
        kv_raw = dot_f32(normed_flat, w_kv, 1, 0).reshape(batch, rows, 2 * hd)
        keys, key_pull = jax.vjp(rope_single, kv_raw[..., :hd])
        kv_all = gather8(jnp.concatenate([keys, kv_raw[..., hd:]], axis=-1).astype(BF16))
        wq_oth = swap(wq_own)
        q_own = dot_f32(normed_flat, wq_own, 1, 1)
        q_oth = dot_f32(normed_flat, wq_oth, 1, 1)

        def attend():
            shape = batch, rows, chips * hd
            return attn_fwd(q_own.reshape(shape), q_oth.reshape(shape), kv_all, cos_t, sin_t, qpos, kpos, scalars)

        wo_own, (mix_own, mix_oth, q_own, q_oth) = gather4_direct(w_out, (q_own, q_oth), attend)
        wo_own = wo_own.reshape(chips * hd, dim)
        wo_oth = swap(wo_own)
        mix_own = mix_own.reshape(tokens, chips * hd)
        mix_oth = mix_oth.reshape(tokens, chips * hd)
        hidden_flat = hidden.reshape(tokens, dim)
        grad_flat = grad_out.reshape(tokens, dim)
        size = tokens // CHUNKS
        resid, *z_parts = resid_call(order, hidden_flat, mix_own, mix_oth, wo_own, wo_oth, mlp_gain[None, :], size, 2 * rows)

        g_all, z_all, acts, far = [], [], [], []
        for c in range(CHUNKS):
            g_all.append(gather8(grad_flat[c * size:(c + 1) * size]).reshape(chips, 2, size, dim))
            z_all.append(gather8(z_parts[c]).reshape(chips, 2, size, dim))
        mlp_sums, d_gated = [None] * CHUNKS, [None] * CHUNKS
        weights = (w_gate, w_up, w_down)
        core_1 = core[None]
        grads = None

        def d_resid_of(first, count, earlier):
            return d_resid_call(order, d_gated[first:first + count], resid, grad_flat, mlp_gain[None, :], wo_own, wo_oth, first, size,
                                () if earlier is None else earlier[1])

        def attn_bwd_of(first, count, d_own, d_oth, earlier):
            per = batch // CHUNKS
            return attn_bwd(order, q_own, q_oth, d_own.reshape(batch, rows, -1), d_oth.reshape(batch, rows, -1), kv_all, cos_t, sin_t, qpos, kpos,
                            scalars, first * per, count * per, () if earlier is None else earlier[2])

        d_z_terms, mlp_terms = ((1, 0), (1, 0)), ((0, 1),)

        def back_both(c, side, far):
            return back_call(order, side, (acts[c][1], acts[c][2], acts[c][0]), weights, d_z_terms + mlp_terms, far, chips)

        def finish(c):
            both = back_both(c, 0, (far[c],))
            both = scatter4(both).reshape(2, size, dim)
            d_gated[c] = mlp_sums[c] = both

        def finish_last(c):
            part = back_call(order, 0, acts[c][1:], weights[:2], d_z_terms, (far[c],), chips)
            d_gated[c] = scatter4(part).reshape(size, dim)
            part = back_call(order, 0, acts[c][:1], weights[2:], mlp_terms, (far[c],), chips)
            mlp_sums[c] = scatter4(part).reshape(size, dim)

        for c in range(CHUNKS):
            if c < CHUNKS - 1:
                d_act = d_act_call(order, core_1, g_all[c], w_down)
                acts.append(act_call(order, core_1, z_all[c], d_act, w_gate, w_up, None))
            else:
                acts.append(act_call(order, core_1, z_all[c], g_all[c], *weights))
            part = back_both(c, 1, ())
            far.append(swap(part))
            if c == CHUNKS - 2:
                for earlier in range(c + 1):
                    finish(earlier)
        terms, *d_parts = d_resid_of(0, 1, None)
        grads = terms, d_parts, attn_bwd_of(0, 1, d_parts[1], d_parts[2], None)
        finish_last(CHUNKS - 1)
        shards = [[a.reshape(2 * chips, size, -1) for a in acts[c]] for c in range(CHUNKS)]
        g_gate = wgrad_call(order, core_1, z_all, [a[1] for a in shards], tiles=(0, 1))

        terms, d_resid, d_own, d_oth = d_resid_of(1, CHUNKS - 1, grads)
        norm_terms, (dq_own, dq_oth, dkv_own, dkv_oth) = grads[0] + terms, attn_bwd_of(1, CHUNKS - 1, d_own, d_oth, grads)
        dq_own = dq_own.reshape(tokens, chips * hd)
        dq_oth = dq_oth.reshape(tokens, chips * hd)
        dkv_far = swap(dkv_oth)
        heads_far = head_wgrad(order, (mix_oth, dq_oth), (d_resid, normed_flat), hd)
        dkv_far, dkv_own, _ = lax.optimization_barrier((dkv_far, dkv_own, heads_far))
        dkv = scatter4((dkv_own.astype(F32) + dkv_far.astype(F32)).astype(BF16))
        heads_far = swap(heads_far)

        g_gate = wgrad_call(order, core_1, z_all, [a[1] for a in shards], tiles=(1, 2), earlier=g_gate)
        g_heads_part = head_wgrad(order, (mix_own, dq_own), (d_resid, normed_flat), hd, (heads_far,))
        g_heads = scatter4(g_heads_part)
        dkv, g_heads_part = lax.optimization_barrier((dkv, g_heads_part))
        g_out, g_query = g_heads[0], g_heads[1].T
        d_k_raw = key_pull(dkv[..., :hd].astype(F32))[0]
        dkv = jnp.concatenate([d_k_raw.astype(BF16), dkv[..., hd:]], axis=-1).reshape(tokens, 2 * hd)
        grad_hidden, attn_terms = d_hidden_call(
            order, dq_own, dq_oth, dkv, hidden_flat, d_resid, attn_gain[None, :], wq_own, wq_oth, w_kv, 4 * rows, 2 * rows)
        sums = kv_wgrad(order, normed_flat, dkv, (attn_terms, norm_terms))
        sums = lax.psum(sums, "tp")
        g_attn_norm, g_mlp_norm = sums[dim:].reshape(2, dim)
        hidden_out = add_call(order, resid, mlp_sums).reshape(batch, rows, dim)
        g_up = wgrad_call(order, core_1, z_all, [a[2] for a in shards])
        g_down = wgrad_call(order, core_1, [a[0] for a in shards], g_all)
        return (hidden_out, grad_hidden.reshape(batch, rows, dim), g_attn_norm, g_query, sums[:dim, :hd], sums[:dim, hd:], g_out, g_mlp_norm, g_gate, g_up, g_down)

    return jax.shard_map(local_layer, mesh=mesh, in_specs=in_specs, out_specs=out_specs, check_vma=False)
```

```python
import functools
import math
import jax
import jax.numpy as jnp
from jax import lax
from jax.experimental import pallas as pl
from jax.experimental.pallas import tpu as pltpu
from jax.sharding import PartitionSpec as P

NORM_EPS = 1e-6
CHUNKS = 3
F32 = jnp.float32
BF16 = jnp.bfloat16
MASKED = -1e30


def rms_norm(x_in, gain):
    x_f = x_in.astype(F32)
    inv_rms = lax.rsqrt(jnp.mean(x_f * x_f, axis=-1, keepdims=True) + NORM_EPS)
    return (x_f * inv_rms * (1.0 + gain)).astype(BF16)


def rope_tables(positions, head_dim):
    half_dim = head_dim // 2
    exponent = jnp.arange(half_dim, dtype=F32) * (2.0 / head_dim)
    inv_freq = jnp.exp(exponent * (-math.log(10000.0)))
    angles = positions.astype(F32)[:, None] * inv_freq[None, :]
    return jnp.cos(angles), jnp.sin(angles)


def apply_rope(x_f, cos_t, sin_t):
    half_dim = x_f.shape[-1] // 2
    first = x_f[..., :half_dim]
    second = x_f[..., half_dim:]
    return jnp.concatenate([first * cos_t - second * sin_t, second * cos_t + first * sin_t], axis=-1)


def dot_f32(lhs, rhs, lhs_dim, rhs_dim):
    return lax.dot_general(lhs, rhs, (((lhs_dim,), (rhs_dim,)), ((), ())), preferred_element_type=F32)


def own_first(kv_ref, core, lo, hi):
    shards = kv_ref.shape[0] // 2
    return jnp.concatenate([kv_ref[2 * c + side, 0, :, lo:hi] for side in (core, 1 - core) for c in range(shards)], axis=0)


def attn_fwd_kernel(prefix_s, valid_s, core_s, q_own_ref, q_oth_ref, kv_ref, cos_ref, sin_ref, qpos_ref, kpos_ref,
                    o_own_ref, o_oth_ref, r_own_ref, r_oth_ref):
    b = pl.program_id(0)
    rows, width = q_own_ref.shape[1:]
    hd = kv_ref.shape[-1] // 2
    half = hd // 2
    heads = width // hd
    scale = hd ** -0.5
    cos_t, sin_t = cos_ref[...], sin_ref[...]
    queries = []
    for src, dst in ((q_own_ref, r_own_ref), (q_oth_ref, r_oth_ref)):
        for n in range(heads):
            first = src[0, :, n * hd:n * hd + half]
            second = src[0, :, n * hd + half:(n + 1) * hd]
            q_1 = ((first * cos_t - second * sin_t).astype(BF16) * scale).astype(BF16)
            q_2 = ((second * cos_t + first * sin_t).astype(BF16) * scale).astype(BF16)
            dst[0, :, n * hd:n * hd + half] = q_1
            dst[0, :, n * hd + half:(n + 1) * hd] = q_2
            queries.append(jnp.concatenate([q_1, q_2], axis=1))
    keys = own_first(kv_ref, core_s[0], 0, hd)
    values = own_first(kv_ref, core_s[0], hd, 2 * hd)
    limit = jnp.minimum(valid_s[b], jnp.maximum(prefix_s[b], qpos_ref[...] + 1))
    visible = kpos_ref[...] < limit
    for side, dst in ((0, o_own_ref), (1, o_oth_ref)):
        query = jnp.concatenate(queries[side * heads:(side + 1) * heads], axis=0)
        scores = dot_f32(query, keys, 1, 1)
        scores = jnp.where(visible, scores, MASKED)
        top = jnp.max(scores, axis=-1, keepdims=True)
        expo = jnp.exp(scores - top)
        inv = 1.0 / jnp.sum(expo, axis=-1, keepdims=True)
        probs = (expo * inv).astype(BF16)
        mixed = dot_f32(probs, values, 1, 0).astype(BF16)
        for n in range(heads):
            dst[0, :, n * hd:(n + 1) * hd] = mixed[n * rows:(n + 1) * rows]


def attn_bwd_kernel(first, prefix_s, valid_s, core_s, q_own_ref, q_oth_ref, g_own_ref, g_oth_ref, kv_ref, cos_ref, sin_ref,
                    qpos_ref, kpos_ref, dq_own_ref, dq_oth_ref, dkv_own_ref, dkv_oth_ref):
    b = pl.program_id(0) + first
    rows, width = q_own_ref.shape[1:]
    hd = kv_ref.shape[-1] // 2
    half = hd // 2
    heads = width // hd
    scale = hd ** -0.5
    cos_t, sin_t = cos_ref[...], sin_ref[...]
    shards = kv_ref.shape[0] // 2
    keys = own_first(kv_ref, core_s[0], 0, hd)
    values = own_first(kv_ref, core_s[0], hd, 2 * hd)
    limit = jnp.minimum(valid_s[b], jnp.maximum(prefix_s[b], qpos_ref[...] + 1))
    visible = kpos_ref[...] < limit
    d_keys, d_values = 0.0, 0.0
    for q_ref, g_ref, dst in ((q_own_ref, g_own_ref, dq_own_ref), (q_oth_ref, g_oth_ref, dq_oth_ref)):
        query = jnp.concatenate([q_ref[0, :, n * hd:(n + 1) * hd] for n in range(heads)], axis=0)
        grad = jnp.concatenate([g_ref[0, :, n * hd:(n + 1) * hd] for n in range(heads)], axis=0)
        scores = dot_f32(keys, query, 1, 1)
        scores = jnp.where(visible, scores, MASKED)
        top = jnp.max(scores, axis=0, keepdims=True)
        expo = jnp.exp(scores - top)
        inv = 1.0 / jnp.sum(expo, axis=0, keepdims=True)
        probs = expo * inv
        d_probs = dot_f32(values, grad, 1, 1)
        delta = jnp.sum(probs * d_probs, axis=0, keepdims=True)
        d_scores = (probs * (d_probs - delta)).astype(BF16)
        d_values = d_values + dot_f32(probs.astype(BF16), grad, 1, 0)
        d_keys = d_keys + dot_f32(d_scores, query, 1, 0)
        d_query = dot_f32(d_scores, keys, 0, 0) * scale
        for n in range(heads):
            g_1 = d_query[n * rows:(n + 1) * rows, :half]
            g_2 = d_query[n * rows:(n + 1) * rows, half:]
            dst[0, :, n * hd:n * hd + half] = (g_1 * cos_t + g_2 * sin_t).astype(BF16)
            dst[0, :, n * hd + half:(n + 1) * hd] = (g_2 * cos_t - g_1 * sin_t).astype(BF16)
    d_keys = d_keys.astype(BF16)
    d_values = d_values.astype(BF16)
    span = kv_ref.shape[2]
    for k, dst in enumerate((dkv_own_ref, dkv_oth_ref)):
        for c in range(shards):
            at = (k * shards + c) * span
            dst[c, 0, :, :hd] = d_keys[at:at + span]
            dst[c, 0, :, hd:] = d_values[at:at + span]


def attn_specs(rows, width, shards, two_hd, half):
    q_spec = pl.BlockSpec((1, rows, width), lambda b, *_: (b, 0, 0))
    kv_spec = pl.BlockSpec((shards, 1, rows, two_hd), lambda b, *_: (0, b, 0, 0))
    tab_spec = pl.BlockSpec((rows, half), lambda b, *_: (0, 0))
    return q_spec, kv_spec, tab_spec


def whole(shape):
    return pl.BlockSpec(shape, lambda b, *_: tuple(0 for _ in shape))


def attn_fwd(q_own, q_oth, kv_all, cos_t, sin_t, qpos, kpos, scalars):
    batch, rows, width = q_own.shape
    shards, two_hd = kv_all.shape[0], kv_all.shape[3]
    q_spec, kv_spec, tab_spec = attn_specs(rows, width, shards, two_hd, two_hd // 4)
    heads = width * 2 // two_hd
    out = jax.ShapeDtypeStruct((batch, rows, width), BF16)
    qpos_col = jnp.tile(qpos, heads)[:, None]
    n_keys = kpos.shape[0]
    flops = 2 * 2 * batch * rows * 2 * width * n_keys
    return pl.pallas_call(
        attn_fwd_kernel,
        out_shape=(out, out, out, out),
        grid_spec=pltpu.PrefetchScalarGridSpec(
            num_scalar_prefetch=3, grid=(batch,),
            in_specs=[q_spec, q_spec, kv_spec, tab_spec, tab_spec, whole((heads * rows, 1)), whole((1, n_keys))],
            out_specs=[q_spec] * 4),
        compiler_params=pltpu.CompilerParams(dimension_semantics=("arbitrary",), vmem_limit_bytes=60 << 20),
        cost_estimate=pl.CostEstimate(flops=flops, bytes_accessed=batch * rows * width * 16 + kv_all.size * 2, transcendentals=batch * rows * heads * 2 * n_keys),
        name="attn_fwd",
    )(*scalars, q_own, q_oth, kv_all, cos_t, sin_t, qpos_col, kpos[None, :])


def attn_bwd(order, q_own, q_oth, g_own, g_oth, kv_all, cos_t, sin_t, qpos, kpos, scalars, first, count, earlier):
    batch, rows, width = q_own.shape
    shards, two_hd = kv_all.shape[0], kv_all.shape[3]
    tab_spec = pl.BlockSpec((rows, two_hd // 4), lambda b, *_: (0, 0))
    q_spec = pl.BlockSpec((1, rows, width), lambda b, *_: (b + first, 0, 0))
    kv_spec = pl.BlockSpec((shards, 1, rows, two_hd), lambda b, *_: (0, b + first, 0, 0))
    heads = width * 2 // two_hd
    out = jax.ShapeDtypeStruct((batch, rows, width), BF16)
    dkv_spec = pl.BlockSpec((shards // 2, 1, rows, two_hd), lambda b, *_: (0, b + first, 0, 0))
    kv_out = jax.ShapeDtypeStruct((shards // 2, batch, rows, two_hd), BF16)
    qpos_row = jnp.tile(qpos, heads)[None, :]
    n_keys = kpos.shape[0]
    flops = 2 * 5 * count * rows * 2 * width * n_keys
    return order.call(
        functools.partial(attn_bwd_kernel, first), 9, len(earlier), prefetch=3, in_parts=True,
        out_shape=(out, out, kv_out, kv_out), grid=(count,),
        in_specs=[q_spec, q_spec, q_spec, q_spec, kv_spec, tab_spec, tab_spec, whole((1, heads * rows)), whole((n_keys, 1))],
        out_specs=[q_spec, q_spec, dkv_spec, dkv_spec],
        compiler_params=pltpu.CompilerParams(dimension_semantics=("arbitrary",), vmem_limit_bytes=60 << 20),
        cost_estimate=pl.CostEstimate(flops=flops, bytes_accessed=count * rows * width * 12 + kv_all.size * 4, transcendentals=count * rows * heads * 2 * n_keys),
        name="attn_bwd",
    )(*scalars, q_own, q_oth, g_own, g_oth, kv_all, cos_t, sin_t, qpos_row, kpos[:, None], *earlier)


class Order:
    def __init__(self):
        self.last = None

    def call(self, kernel, n_in, n_kept=0, *, in_specs, out_specs, out_shape, grid, in_parts=False, after=(), prefetch=0, scratch_shapes=(), **options):
        def run(*args):
            deps = (() if self.last is None or any(self.last is a for a in args) else (self.last,)) + tuple(after)
            n_args = prefetch + n_in

            def body(*refs):
                kernel(*refs[:n_args], *refs[n_args + n_kept + len(deps):])

            n_out = len(out_specs) if isinstance(out_specs, (list, tuple)) else 1
            shapes = [pltpu.HBM(o.shape, o.dtype) if in_parts and o.size > 1 << 17 else o for o in out_shape] if in_parts else out_shape
            first = n_args
            args = args[:first] + tuple(pltpu.with_memory_space_constraint(a, pltpu.HBM) for a in args[first:])
            out = pl.pallas_call(
                body, out_shape=shapes,
                grid_spec=pltpu.PrefetchScalarGridSpec(
                    num_scalar_prefetch=prefetch, grid=grid, scratch_shapes=scratch_shapes, out_specs=out_specs,
                    in_specs=in_specs + [pl.BlockSpec(memory_space=pl.ANY)] * (n_kept + len(deps))),
                input_output_aliases={n_args + k: n_out - n_kept + k for k in range(n_kept)},
                **options)(*args, *deps)
            self.last = out[0] if isinstance(out, (tuple, list)) else out
            return out

        return run


def params(steps, limit=60):
    return pltpu.CompilerParams(dimension_semantics=("arbitrary",) * steps, vmem_limit_bytes=limit << 20)


def cost(flops, *arrays):
    return pl.CostEstimate(flops=flops, bytes_accessed=sum(a.size * a.dtype.itemsize for a in arrays), transcendentals=0)


def rows_of(ref):
    return ref[...].reshape(-1, ref.shape[-1])


def raw_spec(shape):
    return pl.BlockSpec((2, 1) + shape[2:], lambda j, i, core: (lax.rem(i, 2), lax.bitwise_xor(core[0], lax.div(i, 2)), 0, 0))


def d_act_kernel(core_s, g_ref, wd_ref, out_ref):
    out_ref[...] = dot_f32(rows_of(g_ref), wd_ref[...], 1, 1).astype(BF16)


def d_act_call(order, core, g_all, w_down, tn=1024):
    chips, _, rows, dim = g_all.shape
    width = w_down.shape[0]
    out = jax.ShapeDtypeStruct((chips * 2 * rows, width), BF16)
    return order.call(
        d_act_kernel, 2, prefetch=1, out_shape=out, grid=(width // tn, chips),
        in_specs=[raw_spec(g_all.shape), pl.BlockSpec((tn, dim), lambda j, i, core: (j, 0))],
        out_specs=pl.BlockSpec((2 * rows, tn), lambda j, i, core: (i, j)), compiler_params=params(2),
        cost_estimate=cost(2 * g_all.size * width, g_all, w_down, out), name="d_act",
    )(core, g_all, w_down)


def act_kernel(core_s, z_ref, g_ref, wg_ref, wu_ref, *refs, sub):
    c_1 = math.sqrt(2.0 / math.pi)
    c_3 = 0.044715 * c_1
    act_ref, dg_ref, du_ref = refs[-3:]
    z_in = rows_of(z_ref)
    for j in range(0, wg_ref.shape[1], sub):
        gate = dot_f32(z_in, wg_ref[:, j:j + sub], 1, 0)
        upper = dot_f32(z_in, wu_ref[:, j:j + sub], 1, 0)
        if len(refs) == 4:
            d_act = dot_f32(rows_of(g_ref), refs[0][j:j + sub, :], 1, 1).astype(BF16).astype(F32)
        else:
            d_act = g_ref[:, j:j + sub].astype(F32)
        square = gate * gate
        half = 0.5 * jnp.tanh(gate * (c_3 * square + c_1)) + 0.5
        gelu = gate * half
        act_ref[:, j:j + sub] = (gelu * upper).astype(BF16)
        du_ref[:, j:j + sub] = (d_act * gelu).astype(BF16)
        slope = half + gelu * (1.0 - half) * (6.0 * c_3 * square + 2.0 * c_1)
        dg_ref[:, j:j + sub] = (d_act * upper * slope).astype(BF16)


def act_call(order, core, z_all, g_all, w_gate, w_up, w_down, sub=256):
    chips, _, rows, dim = z_all.shape
    width = w_gate.shape[1]
    out = jax.ShapeDtypeStruct((chips * 2 * rows, width), BF16)
    tn = 1024 if w_down is None else 512
    raw = raw_spec(z_all.shape)
    col = pl.BlockSpec((dim, tn), lambda j, i, core: (0, j))
    tile = pl.BlockSpec((2 * rows, tn), lambda j, i, core: (i, j))
    args = (z_all, g_all, w_gate, w_up) + (() if w_down is None else (w_down,))
    specs = [raw, tile if w_down is None else raw, col, col] + ([] if w_down is None else [pl.BlockSpec((tn, dim), lambda j, i, core: (j, 0))])
    return order.call(
        functools.partial(act_kernel, sub=sub), len(args), prefetch=1, out_shape=(out, out, out), grid=(width // tn, chips),
        in_specs=specs, out_specs=[tile] * 3, compiler_params=params(2),
        cost_estimate=cost(2 * (len(args) - 2) * z_all.size * width, *args, out, out, out), name="mlp_act",
    )(core, *args)


def back_kernel(*refs, terms, joined, n_far, n_out, base, tn):
    n = len(terms)
    lhs, rhs, far, outs = refs[:n], refs[n:2 * n], refs[2 * n:2 * n + n_far], refs[2 * n + n_far:][:n_out]
    l_bufs, r_bufs, (l_sems, r_sems) = refs[2 * n + n_far + n_out:][:n], refs[3 * n + n_far + n_out:][:n], refs[4 * n + n_far + n_out:]
    j, i = pl.program_id(0), pl.program_id(1)
    blocks, rows = l_bufs[0].shape[:2]

    def left(p, at):
        return pltpu.make_async_copy(lhs[p].at[pl.ds((base + at) * rows, rows)], l_bufs[p].at[at], l_sems.at[p, at])

    def right(p, tile):
        cols = pl.ds(pl.multiple_of(tile * tn, tn), tn)
        src = rhs[p].at[:, cols] if terms[p][0] == 0 else rhs[p].at[cols]
        return pltpu.make_async_copy(src, r_bufs[p].at[lax.rem(tile, 2)], r_sems.at[p, lax.rem(tile, 2)])

    @pl.when((j == 0) & (i == 0))
    def _():
        for p in range(n):
            right(p, 0).start()
            left(p, 0).start()
        for at in range(1, blocks):
            for p in range(n):
                left(p, at).start()

    @pl.when((i == blocks - 1) & (j + 1 < pl.num_programs(0)))
    def _():
        for p in range(n):
            right(p, j + 1).start()

    def compute(ready):
        totals = {}
        for p, (dim, kind) in enumerate(terms):
            ready(p)
            part = dot_f32(l_bufs[p][i], r_bufs[p][lax.rem(j, 2)], 1, dim)
            totals[kind] = totals[kind] + part if kind in totals else part
        for kind, total in totals.items():
            out, at = (outs[0], (slice(None), kind)) if joined else (outs[kind], (slice(None),))
            total = total.reshape(out[at].shape)
            if far:
                total += far[0][:, kind].astype(F32)
            out[at] = total.astype(BF16)

    @pl.when(j == 0)
    def _():
        def ready(p):
            @pl.when(i == 0)
            def _():
                right(p, 0).wait()

            left(p, i).wait()

        compute(ready)

    @pl.when(j > 0)
    def _():
        @pl.when(i == 0)
        def _():
            for p in range(n):
                right(p, j).wait()

        compute(lambda p: None)


def back_call(order, side, lhs, rhs, terms, far, chips, joined, tn=512):
    dim = rhs[0].shape[0 if terms[0][0] else 1]
    rows = lhs[0].shape[0] // (2 * chips)
    half, n = chips // 2, len(terms)
    hbm = pl.BlockSpec(memory_space=pl.ANY)
    both = pl.BlockSpec((2, 2, rows, tn), lambda j, i: (i, 0, 0, j))
    outs = [jax.ShapeDtypeStruct((chips, 2, rows, dim), BF16)] if joined else [jax.ShapeDtypeStruct((chips, rows, dim), BF16)] * 2
    depth = lhs[0].shape[1]
    return order.call(
        functools.partial(back_kernel, terms=terms, joined=joined, n_far=len(far), n_out=len(outs), base=side * half, tn=tn), 2 * n + len(far), out_shape=outs,
        grid=(dim // tn, half), in_specs=[hbm] * (2 * n) + [both] * len(far),
        out_specs=[both] if joined else [pl.BlockSpec((2, rows, tn), lambda j, i: (i, 0, j))] * 2,
        scratch_shapes=[pltpu.VMEM((half, 2 * rows, depth), BF16)] * n
        + [pltpu.VMEM((2, depth, tn) if d == 0 else (2, tn, depth), BF16) for d, _ in terms]
        + [pltpu.SemaphoreType.DMA((n, half)), pltpu.SemaphoreType.DMA((n, 2))],
        compiler_params=params(2),
        cost_estimate=cost(n * lhs[0].size * dim, *lhs, *rhs, *outs), name="mlp_back",
    )(*lhs, *rhs, *far)


def wgrad_kernel(core_s, *refs, n, tf, tn, cols, first, first_col):
    lhs, rhs, out, l_buf, r_buf, sems = refs[:n], refs[n:2 * n], *refs[2 * n:]
    i, j, k = pl.program_id(0), pl.program_id(1), pl.program_id(2)
    step = (i * cols + j) * n + k
    slot = lax.rem(step, 2)
    chips = l_buf.shape[1] // 2

    def copies(s, at, p):
        row = pl.multiple_of((lax.div(s, cols * n) + first) * tf, tf)
        col = pl.multiple_of((lax.rem(lax.div(s, n), cols) + first_col) * tn, tn)
        halves = [], []
        for side in range(2):
            half = pl.ds(side * chips, chips)
            for q, (ref, buf, lanes) in enumerate(((lhs[p], l_buf, pl.ds(row, tf)), (rhs[p], r_buf, pl.ds(col, tn)))):
                src = ref.at[:, lax.bitwise_xor(core_s[0], side), :, lanes] if ref.ndim == 4 else ref.at[half, :, lanes]
                halves[side].append(pltpu.make_async_copy(src, buf.at[at, half], sems.at[q, side, at]))
        return halves

    def fetch(s, at):
        for p in range(n):
            @pl.when(lax.rem(s, n) == p)
            def _(p=p):
                for half in copies(s, at, p):
                    for copy in half:
                        copy.start()

    @pl.when(step == 0)
    def _():
        fetch(step, slot)

    @pl.when(step + 1 < pl.num_programs(0) * cols * n)
    def _():
        fetch(step + 1, 1 - slot)

    @pl.when(step == 0)
    def _():
        for side, half in enumerate(copies(step, slot, 0)):
            for copy in half:
                copy.wait()
            rows = pl.ds(side * chips, chips)
            part = dot_f32(rows_of(l_buf.at[0, rows]), rows_of(r_buf.at[0, rows]), 0, 0)
            out[...] = part if side == 0 else out[...] + part

    @pl.when(step > 0)
    def _():
        for half in copies(step, slot, 0):
            for copy in half:
                copy.wait()
        part = dot_f32(rows_of(l_buf.at[slot]), rows_of(r_buf.at[slot]), 0, 0)
        out[...] = jnp.where(k == 0, part, out[...] + part)


def wgrad_call(order, core, lhs, rhs, tf=1024, tn=1024, tiles=None, col_tiles=None, earlier=None, after=()):
    n = len(lhs)
    rows = lhs[0].shape[-2]
    shards = lhs[0].size // (rows * lhs[0].shape[-1])
    width = rhs[0].shape[-1]
    height = lhs[0].shape[-1]
    first_col, last_col = col_tiles or (0, width // tn)
    cols = last_col - first_col
    first, last = tiles or (0, height // tf)
    kept = () if earlier is None else (earlier,)
    out = jax.ShapeDtypeStruct((height, width), F32)
    return order.call(
        functools.partial(wgrad_kernel, n=n, tf=tf, tn=tn, cols=cols, first=first, first_col=first_col), 2 * n, len(kept), prefetch=1, after=after, out_shape=out, grid=(last - first, cols, n),
        in_specs=[pl.BlockSpec(memory_space=pl.ANY)] * (2 * n), out_specs=pl.BlockSpec((tf, tn), lambda i, j, k, core: (i + first, j + first_col)),
        scratch_shapes=[pltpu.VMEM((2, shards, rows, tf), BF16), pltpu.VMEM((2, shards, rows, tn), BF16), pltpu.SemaphoreType.DMA((2, 2, 2))],
        compiler_params=params(3), cost_estimate=cost(2 * n * shards * rows * height * width, *lhs, *rhs, out), name="wgrad",
    )(core, *lhs, *rhs, *kept)


def kv_wgrad_kernel(l_ref, r_ref, *refs):
    out, steps = refs[-1], pl.num_programs(0)
    width = out.shape[1]

    @pl.when(pl.program_id(0) < steps - 1)
    def _():
        out[...] = dot_f32(l_ref[...], r_ref[...], 0, 0)

    @pl.when(pl.program_id(0) == steps - 1)
    def _():
        row = 0
        for terms in refs[:-1]:
            total = jnp.sum(terms[...], axis=0, keepdims=True)
            for k in range(0, total.shape[1], width):
                out[row:row + 1] = total[:, k:k + width]
                row += 1


def kv_wgrad(order, lhs, rhs, terms, tf=512):
    tokens, rows = lhs.shape
    width = rhs.shape[1]
    extra = sum(t.shape[1] for t in terms) // width
    steps = rows // tf
    out = jax.ShapeDtypeStruct((rows + extra, width), F32)
    return order.call(
        kv_wgrad_kernel, 2 + len(terms), out_shape=out, grid=(steps + 1,),
        in_specs=[pl.BlockSpec((tokens, tf), lambda i: (0, jnp.minimum(i, steps - 1))), pl.BlockSpec((tokens, width), lambda i: (0, 0))]
        + [pl.BlockSpec(t.shape, lambda i: (0, 0)) for t in terms],
        out_specs=pl.BlockSpec((tf, width), lambda i: (i, 0)), compiler_params=params(1),
        cost_estimate=cost(2 * tokens * rows * width, lhs, rhs, out), name="kv_wgrad",
    )(lhs, rhs, *terms)


def head_wgrad_kernel(*refs):
    lhs, rhs, out = refs[:2], refs[2:4], refs[-1]
    for kind in range(2):
        total = dot_f32(lhs[kind][...], rhs[kind][...], 0, 0).reshape(out.shape[0], *out.shape[2:])
        for far in refs[4:-1]:
            total += far[:, kind]
        out[:, kind] = total


def head_wgrad(order, lhs, rhs, hd, far=(), tn=512):
    tokens, width = lhs[0].shape
    dim = rhs[0].shape[1]
    heads = width // hd
    out = jax.ShapeDtypeStruct((heads, 2, hd, dim), F32)
    tile = pl.BlockSpec((heads, 2, hd, tn), lambda j: (0, 0, 0, j))
    return order.call(
        head_wgrad_kernel, 4 + len(far), out_shape=out, grid=(dim // tn,),
        in_specs=[pl.BlockSpec((tokens, width), lambda j: (0, 0), pipeline_mode=pl.Buffered(1))] * 2
        + [pl.BlockSpec((tokens, tn), lambda j: (0, j))] * 2 + [tile] * len(far),
        out_specs=tile, compiler_params=params(1), cost_estimate=cost(4 * tokens * width * dim, *lhs, *rhs, *far, out), name="head_wgrad",
    )(*lhs, *rhs, *far)


def add_kernel(base_ref, *refs):
    for c, part in enumerate(refs[:-1]):
        @pl.when(pl.program_id(0) == c)
        def _(part=part):
            refs[-1][...] = (base_ref[...].astype(F32) + rows_of(part).astype(F32)).astype(BF16)


def add_call(order, base, parts):
    tokens, dim = base.shape
    size = tokens // len(parts)
    row = pl.BlockSpec((size, dim), lambda i: (i, 0))
    specs = [pl.BlockSpec((1, size, dim), lambda i, at=a.shape[0] - 1: (at, 0, 0)) if a.ndim == 3 else pl.BlockSpec((size, dim), lambda i: (0, 0)) for a in parts]
    return order.call(
        add_kernel, 1 + len(parts), out_shape=jax.ShapeDtypeStruct(base.shape, BF16), grid=(len(parts),), in_specs=[row] + specs, out_specs=row,
        compiler_params=params(1), cost_estimate=cost(base.size, base, base, base), name="add",
    )(base, *parts)


def resid_kernel(h_ref, a_own_ref, a_oth_ref, w_own_ref, w_oth_ref, gain_ref, resid_ref, *z_refs, sub):
    for c, z_ref in enumerate(z_refs):
        @pl.when(pl.program_id(0) == c)
        def _(z_ref=z_ref):
            for r in range(0, z_ref.shape[0], sub):
                at = slice(r, r + sub)
                total = dot_f32(a_own_ref[at], w_own_ref[...], 1, 0) + dot_f32(a_oth_ref[at], w_oth_ref[...], 1, 0)
                resid = (h_ref[at].astype(F32) + total).astype(BF16)
                resid_ref[at] = resid
                x_f = resid.astype(F32)
                inv = lax.rsqrt(jnp.mean(x_f * x_f, axis=-1, keepdims=True) + NORM_EPS)
                z_ref[at] = (x_f * inv * (1.0 + gain_ref[...])).astype(BF16)


def resid_call(order, hidden, mix_own, mix_oth, wo_own, wo_oth, gain, size, sub):
    tokens, dim = hidden.shape
    width = mix_own.shape[1]
    chunks = tokens // size
    row = pl.BlockSpec((size, dim), lambda i: (i, 0))
    mix = pl.BlockSpec((size, width), lambda i: (i, 0))
    whole_w = pl.BlockSpec((width, dim), lambda i: (0, 0))
    outs = (jax.ShapeDtypeStruct((tokens, dim), BF16),) + (jax.ShapeDtypeStruct((size, dim), BF16),) * chunks
    return order.call(
        functools.partial(resid_kernel, sub=sub), 6, out_shape=outs, grid=(chunks,),
        in_specs=[row, mix, mix, whole_w, whole_w, pl.BlockSpec((1, dim), lambda i: (0, 0))],
        out_specs=[row] + [pl.BlockSpec((size, dim), lambda i: (0, 0))] * chunks,
        compiler_params=params(1), cost_estimate=cost(4 * tokens * dim * width, hidden, mix_own, mix_oth, wo_own, wo_oth, *outs), name="resid",
    )(hidden, mix_own, mix_oth, wo_own, wo_oth, gain)


def norm_back(x_f, gain_1, d_out):
    inv = lax.rsqrt(jnp.mean(x_f * x_f, axis=-1, keepdims=True) + NORM_EPS)
    unit = x_f * inv
    scaled = d_out * gain_1
    d_x = inv * (scaled - unit * jnp.mean(scaled * unit, axis=-1, keepdims=True))
    return d_x, d_out * unit


def fold_rows(terms):
    rows, dim = terms.shape
    return jnp.sum(terms.reshape(rows // 8, 8, dim), axis=0)


def d_resid_kernel(*refs, n):
    dz_refs = refs[:n]
    x_ref, g_ref, gain_ref, w_own_ref, w_oth_ref, norm_ref, d_ref, own_ref, oth_ref = refs[n:]
    i = pl.program_id(0)

    @pl.when(i == 0)
    def _():
        norm_ref[...] = jnp.zeros_like(norm_ref)

    for c, dz_ref in enumerate(dz_refs):
        @pl.when(i == c)
        def _(dz_ref=dz_ref):
            d_x, terms = norm_back(x_ref[...].astype(F32), 1.0 + gain_ref[...], rows_of(dz_ref).astype(F32))
            norm_ref[...] += fold_rows(terms)
            d_ref[...] = (g_ref[...].astype(F32) + d_x).astype(BF16)
    own_ref[...] = dot_f32(d_ref[...], w_own_ref[...], 1, 1).astype(BF16)
    oth_ref[...] = dot_f32(d_ref[...], w_oth_ref[...], 1, 1).astype(BF16)


def d_resid_call(order, dz, resid, grad_out, gain, wo_own, wo_oth, first, size, earlier):
    tokens, dim = resid.shape
    n = len(dz)
    width = wo_own.shape[0]
    one = [pl.BlockSpec((1, size, dim) if a.ndim == 3 else (size, dim), lambda i, nd=a.ndim: (0,) * nd) for a in dz]
    far = pl.BlockSpec((size, dim), lambda i: (i + first, 0))
    mix = pl.BlockSpec((size, width), lambda i: (i + first, 0))
    whole_w = pl.BlockSpec((width, dim), lambda i: (0, 0))
    outs = (jax.ShapeDtypeStruct((8, dim), F32), jax.ShapeDtypeStruct((tokens, dim), BF16),
            jax.ShapeDtypeStruct((tokens, width), BF16), jax.ShapeDtypeStruct((tokens, width), BF16))
    return order.call(
        functools.partial(d_resid_kernel, n=n), n + 5, len(earlier), in_parts=True, out_shape=outs, grid=(n,),
        in_specs=one + [far, far, pl.BlockSpec((1, dim), lambda i: (0, 0)), whole_w, whole_w],
        out_specs=[pl.BlockSpec((8, dim), lambda i: (0, 0)), far, mix, mix],
        compiler_params=params(1), cost_estimate=cost(4 * n * size * dim * width, *dz, wo_own, wo_oth, outs[1]), name="d_resid",
    )(*dz, resid, grad_out, gain, wo_own, wo_oth, *earlier)


def d_hidden_kernel(q_own_ref, q_oth_ref, dkv_ref, x_ref, d_ref, gain_ref, wq_own_ref, wq_oth_ref, wkv_ref, out_ref, norm_ref, *, sub):
    @pl.when(pl.program_id(0) == 0)
    def _():
        norm_ref[...] = jnp.zeros_like(norm_ref)

    folded = 0.0
    for r in range(0, x_ref.shape[0], sub):
        at = slice(r, r + sub)
        d_normed = (dot_f32(q_own_ref[at], wq_own_ref[...], 1, 0) + dot_f32(q_oth_ref[at], wq_oth_ref[...], 1, 0)
                    + dot_f32(dkv_ref[at], wkv_ref[...], 1, 1)).astype(BF16).astype(F32)
        d_x, terms = norm_back(x_ref[at].astype(F32), 1.0 + gain_ref[...], d_normed)
        folded += fold_rows(terms)
        out_ref[at] = (d_ref[at].astype(F32) + d_x).astype(BF16)
    norm_ref[...] += folded


def d_hidden_call(order, dq_own, dq_oth, dkv, hidden, d_resid, gain, wq_own, wq_oth, w_kv, tm, sub):
    tokens, dim = hidden.shape
    width, two_hd = dq_own.shape[1], dkv.shape[1]
    row = pl.BlockSpec((tm, dim), lambda i: (i, 0))
    mix = pl.BlockSpec((tm, width), lambda i: (i, 0))
    whole_w = pl.BlockSpec((width, dim), lambda i: (0, 0))
    outs = (jax.ShapeDtypeStruct((tokens, dim), BF16), jax.ShapeDtypeStruct((8, dim), F32))
    return order.call(
        functools.partial(d_hidden_kernel, sub=sub), 9, out_shape=outs, grid=(tokens // tm,),
        in_specs=[mix, mix, pl.BlockSpec((tm, two_hd), lambda i: (i, 0)), row, row, pl.BlockSpec((1, dim), lambda i: (0, 0)), whole_w, whole_w,
                  pl.BlockSpec((dim, two_hd), lambda i: (0, 0))],
        out_specs=[row, pl.BlockSpec((8, dim), lambda i: (0, 0))],
        compiler_params=params(1), cost_estimate=cost(4 * tokens * dim * (width + two_hd), dq_own, dq_oth, hidden, d_resid, wq_own, wq_oth, *outs), name="d_hidden",
    )(dq_own, dq_oth, dkv, hidden, d_resid, gain, wq_own, wq_oth, w_kv)


def solution(mesh):
    tp_size = mesh.shape["tp"]
    chips = tp_size // 2
    act_spec = P("dp", "tp", None)
    in_specs = (act_spec, act_spec, P("dp"), P("dp"), P(None), P(None, "tp"), P(None, None), P(None, None), P("tp", None), P(None), P(None, "tp"), P(None, "tp"), P("tp", None))
    out_specs = (act_spec, act_spec, P("dp"), P("dp", "tp"), P("dp", None), P("dp", None), P(("dp", "tp"), None), P("dp"), P("dp", "tp"), P("dp", "tp"), P(("dp", "tp"), None))
    same_core = [[2 * c + k for c in range(chips)] for k in range(2)]
    partner = [(i, i ^ 1) for i in range(tp_size)]

    def scatter4(x_part):
        flat = x_part.reshape((-1,) + x_part.shape[2:])
        return lax.psum_scatter(flat, "tp", scatter_dimension=0, tiled=True, axis_index_groups=same_core)

    def gather8(x_loc):
        return lax.all_gather(x_loc, "tp", axis=0, tiled=False)

    def swap(x_loc):
        return lax.ppermute(x_loc, "tp", partner)

    def flip(x_loc, bits):
        return lax.ppermute(x_loc, "tp", [(i, i ^ bits) for i in range(tp_size)])

    def gather4_direct(x_loc, before=None, after=None):
        chip = lax.axis_index("tp") // 2
        half = x_loc.shape[0] // 2
        near, far = flip(x_loc, 2), flip(x_loc, 4)
        if before is not None:
            near, far, _ = lax.optimization_barrier((near, far, before))
        low, high = flip(near[:half], 4), flip(far[half:], 2)
        if after is not None:
            result = after()
            x_loc, near, far, low, high, _ = lax.optimization_barrier((x_loc, near, far, low, high, result[0]))
        out = jnp.zeros((chips,) + x_loc.shape, x_loc.dtype)
        for k, block in ((0, x_loc), (1, near), (2, far)):
            out = lax.dynamic_update_slice(out, block[None], (chip ^ k, 0, 0))
        out = lax.dynamic_update_slice(out, low[None], (chip ^ 3, 0, 0))
        out = lax.dynamic_update_slice(out, high[None], (chip ^ 3, half, 0))
        return out if after is None else (out, result)

    def local_layer(hidden, grad_out, prefix_len, valid_len, attn_norm, w_query, w_key, w_value, w_out, mlp_norm, w_gate, w_up, w_down):
        batch, rows, dim = hidden.shape
        hd = w_key.shape[1]
        tokens = batch * rows
        assert batch % CHUNKS == 0
        me = lax.axis_index("tp")
        core = lax.rem(me, 2)
        qpos = me * rows + jnp.arange(rows, dtype=jnp.int32)
        shard_pos = jnp.arange(rows, dtype=jnp.int32)[None, :] + (jnp.arange(chips, dtype=jnp.int32) * 2 * rows)[:, None]
        kpos = jnp.concatenate([(shard_pos + core * rows).reshape(-1), (shard_pos + (1 - core) * rows).reshape(-1)])
        cos_t, sin_t = rope_tables(qpos, hd)

        def rope_single(raw_proj):
            return apply_rope(raw_proj, cos_t, sin_t)

        order = Order()
        scalars = (prefix_len, valid_len, core[None])
        attn_gain = attn_norm.astype(F32)
        mlp_gain = mlp_norm.astype(F32)
        wq_own = gather4_direct(w_query.T).reshape(chips * hd, dim)
        normed_flat = rms_norm(hidden, attn_gain).reshape(tokens, dim)
        w_kv = jnp.concatenate([w_key, w_value], axis=1)
        kv_raw = dot_f32(normed_flat, w_kv, 1, 0).reshape(batch, rows, 2 * hd)
        keys, key_pull = jax.vjp(rope_single, kv_raw[..., :hd])
        kv_all = gather8(jnp.concatenate([keys, kv_raw[..., hd:]], axis=-1).astype(BF16))
        wq_oth = swap(wq_own)
        q_own = dot_f32(normed_flat, wq_own, 1, 1)
        q_oth = dot_f32(normed_flat, wq_oth, 1, 1)

        def attend():
            shape = batch, rows, chips * hd
            return attn_fwd(q_own.reshape(shape), q_oth.reshape(shape), kv_all, cos_t, sin_t, qpos, kpos, scalars)

        wo_own, (mix_own, mix_oth, q_own, q_oth) = gather4_direct(w_out, (q_own, q_oth), attend)
        wo_own = wo_own.reshape(chips * hd, dim)
        wo_oth = swap(wo_own)
        mix_own = mix_own.reshape(tokens, chips * hd)
        mix_oth = mix_oth.reshape(tokens, chips * hd)
        hidden_flat = hidden.reshape(tokens, dim)
        grad_flat = grad_out.reshape(tokens, dim)
        size = tokens // CHUNKS
        resid, *z_parts = resid_call(order, hidden_flat, mix_own, mix_oth, wo_own, wo_oth, mlp_gain[None, :], size, 2 * rows)

        g_all, z_all, acts, far = [], [], [], []
        for c in range(CHUNKS):
            g_all.append(gather8(grad_flat[c * size:(c + 1) * size]).reshape(chips, 2, size, dim))
            z_all.append(gather8(z_parts[c]).reshape(chips, 2, size, dim))
        mlp_sums, d_gated = [None] * CHUNKS, [None] * CHUNKS
        weights = (w_gate, w_up, w_down)
        core_1 = core[None]
        grads = None

        def d_resid_of(first, count, earlier):
            return d_resid_call(order, d_gated[first:first + count], resid, grad_flat, mlp_gain[None, :], wo_own, wo_oth, first, size,
                                () if earlier is None else earlier[1])

        def attn_bwd_of(first, count, d_own, d_oth, earlier):
            per = batch // CHUNKS
            return attn_bwd(order, q_own, q_oth, d_own.reshape(batch, rows, -1), d_oth.reshape(batch, rows, -1), kv_all, cos_t, sin_t, qpos, kpos,
                            scalars, first * per, count * per, () if earlier is None else earlier[2])

        def back_both(c, side, far, joined=True):
            return back_call(order, side, (acts[c][1], acts[c][2], acts[c][0]), weights, ((1, 0), (1, 0), (0, 1)), far, chips, joined)

        def finish(c):
            both, = back_both(c, 0, (far[c],))
            both = scatter4(both).reshape(2, size, dim)
            d_gated[c] = mlp_sums[c] = both

        def finish_last(c):
            parts = back_both(c, 0, (far[c],), joined=False)
            d_gated[c] = scatter4(parts[0]).reshape(size, dim)
            mlp_sums[c] = scatter4(parts[1]).reshape(size, dim)

        for c in range(CHUNKS):
            if c < CHUNKS - 1:
                d_act = d_act_call(order, core_1, g_all[c], w_down)
                acts.append(act_call(order, core_1, z_all[c], d_act, w_gate, w_up, None))
            else:
                acts.append(act_call(order, core_1, z_all[c], g_all[c], *weights))
            part, = back_both(c, 1, ())
            far.append(swap(part))
            if c == CHUNKS - 2:
                for earlier in range(c + 1):
                    finish(earlier)
        terms, *d_parts = d_resid_of(0, 1, None)
        grads = terms, d_parts, attn_bwd_of(0, 1, d_parts[1], d_parts[2], None)
        finish_last(CHUNKS - 1)
        shards = [[a.reshape(2 * chips, size, -1) for a in acts[c]] for c in range(CHUNKS)]
        g_gate = wgrad_call(order, core_1, z_all, [a[1] for a in shards], tiles=(0, 1))

        terms, d_resid, d_own, d_oth = d_resid_of(1, CHUNKS - 1, grads)
        norm_terms, (dq_own, dq_oth, dkv_own, dkv_oth) = grads[0] + terms, attn_bwd_of(1, CHUNKS - 1, d_own, d_oth, grads)
        dq_own = dq_own.reshape(tokens, chips * hd)
        dq_oth = dq_oth.reshape(tokens, chips * hd)
        dkv_far = swap(dkv_oth)
        heads_far = head_wgrad(order, (mix_oth, dq_oth), (d_resid, normed_flat), hd)
        dkv_far, dkv_own, _ = lax.optimization_barrier((dkv_far, dkv_own, heads_far))
        dkv = scatter4((dkv_own.astype(F32) + dkv_far.astype(F32)).astype(BF16))
        heads_far = swap(heads_far)

        g_gate = wgrad_call(order, core_1, z_all, [a[1] for a in shards], tiles=(1, 2), earlier=g_gate)
        g_heads_part = head_wgrad(order, (mix_own, dq_own), (d_resid, normed_flat), hd, (heads_far,))
        g_heads = scatter4(g_heads_part)
        dkv, g_heads_part = lax.optimization_barrier((dkv, g_heads_part))
        g_out, g_query = g_heads[0], g_heads[1].T
        d_k_raw = key_pull(dkv[..., :hd].astype(F32))[0]
        dkv = jnp.concatenate([d_k_raw.astype(BF16), dkv[..., hd:]], axis=-1).reshape(tokens, 2 * hd)
        grad_hidden, attn_terms = d_hidden_call(
            order, dq_own, dq_oth, dkv, hidden_flat, d_resid, attn_gain[None, :], wq_own, wq_oth, w_kv, 4 * rows, 2 * rows)
        sums = kv_wgrad(order, normed_flat, dkv, (attn_terms, norm_terms))
        sums = lax.psum(sums, "tp")
        g_attn_norm, g_mlp_norm = sums[dim:].reshape(2, dim)
        hidden_out = add_call(order, resid, mlp_sums).reshape(batch, rows, dim)
        g_up = wgrad_call(order, core_1, z_all, [a[2] for a in shards])
        g_down = wgrad_call(order, core_1, [a[0] for a in shards], g_all)
        return (hidden_out, grad_hidden.reshape(batch, rows, dim), g_attn_norm, g_query, sums[:dim, :hd], sums[:dim, hd:], g_out, g_mlp_norm, g_gate, g_up, g_down)

    return jax.shard_map(local_layer, mesh=mesh, in_specs=in_specs, out_specs=out_specs, check_vma=False)
```

```python
import functools
import math
import jax
import jax.numpy as jnp
from jax import lax
from jax.experimental import pallas as pl
from jax.experimental.pallas import tpu as pltpu
from jax.sharding import PartitionSpec as P

NORM_EPS = 1e-6
CHUNKS = 3
F32 = jnp.float32
BF16 = jnp.bfloat16
MASKED = -1e30


def rms_norm(x_in, gain):
    x_f = x_in.astype(F32)
    inv_rms = lax.rsqrt(jnp.mean(x_f * x_f, axis=-1, keepdims=True) + NORM_EPS)
    return (x_f * inv_rms * (1.0 + gain)).astype(BF16)


def rope_tables(positions, head_dim):
    half_dim = head_dim // 2
    exponent = jnp.arange(half_dim, dtype=F32) * (2.0 / head_dim)
    inv_freq = jnp.exp(exponent * (-math.log(10000.0)))
    angles = positions.astype(F32)[:, None] * inv_freq[None, :]
    return jnp.cos(angles), jnp.sin(angles)


def apply_rope(x_f, cos_t, sin_t):
    half_dim = x_f.shape[-1] // 2
    first = x_f[..., :half_dim]
    second = x_f[..., half_dim:]
    return jnp.concatenate([first * cos_t - second * sin_t, second * cos_t + first * sin_t], axis=-1)


def dot_f32(lhs, rhs, lhs_dim, rhs_dim):
    return lax.dot_general(lhs, rhs, (((lhs_dim,), (rhs_dim,)), ((), ())), preferred_element_type=F32)


def own_first(kv_ref, core, lo, hi):
    shards = kv_ref.shape[0] // 2
    return jnp.concatenate([kv_ref[2 * c + side, 0, :, lo:hi] for side in (core, 1 - core) for c in range(shards)], axis=0)


def attn_fwd_kernel(prefix_s, valid_s, core_s, q_own_ref, q_oth_ref, kv_ref, cos_ref, sin_ref, qpos_ref, kpos_ref,
                    o_own_ref, o_oth_ref, r_own_ref, r_oth_ref):
    b = pl.program_id(0)
    rows, width = q_own_ref.shape[1:]
    hd = kv_ref.shape[-1] // 2
    half = hd // 2
    heads = width // hd
    scale = hd ** -0.5
    cos_t, sin_t = cos_ref[...], sin_ref[...]
    queries = []
    for src, dst in ((q_own_ref, r_own_ref), (q_oth_ref, r_oth_ref)):
        for n in range(heads):
            first = src[0, :, n * hd:n * hd + half]
            second = src[0, :, n * hd + half:(n + 1) * hd]
            q_1 = ((first * cos_t - second * sin_t).astype(BF16) * scale).astype(BF16)
            q_2 = ((second * cos_t + first * sin_t).astype(BF16) * scale).astype(BF16)
            dst[0, :, n * hd:n * hd + half] = q_1
            dst[0, :, n * hd + half:(n + 1) * hd] = q_2
            queries.append(jnp.concatenate([q_1, q_2], axis=1))
    keys = own_first(kv_ref, core_s[0], 0, hd)
    values = own_first(kv_ref, core_s[0], hd, 2 * hd)
    limit = jnp.minimum(valid_s[b], jnp.maximum(prefix_s[b], qpos_ref[...] + 1))
    visible = kpos_ref[...] < limit
    for side, dst in ((0, o_own_ref), (1, o_oth_ref)):
        query = jnp.concatenate(queries[side * heads:(side + 1) * heads], axis=0)
        scores = dot_f32(query, keys, 1, 1)
        scores = jnp.where(visible, scores, MASKED)
        top = jnp.max(scores, axis=-1, keepdims=True)
        expo = jnp.exp(scores - top)
        inv = 1.0 / jnp.sum(expo, axis=-1, keepdims=True)
        probs = (expo * inv).astype(BF16)
        mixed = dot_f32(probs, values, 1, 0).astype(BF16)
        for n in range(heads):
            dst[0, :, n * hd:(n + 1) * hd] = mixed[n * rows:(n + 1) * rows]


def attn_bwd_kernel(first, prefix_s, valid_s, core_s, q_own_ref, q_oth_ref, g_own_ref, g_oth_ref, kv_ref, cos_ref, sin_ref,
                    qpos_ref, kpos_ref, dq_own_ref, dq_oth_ref, dkv_own_ref, dkv_oth_ref):
    b = pl.program_id(0) + first
    rows, width = q_own_ref.shape[1:]
    hd = kv_ref.shape[-1] // 2
    half = hd // 2
    heads = width // hd
    scale = hd ** -0.5
    cos_t, sin_t = cos_ref[...], sin_ref[...]
    shards = kv_ref.shape[0] // 2
    keys = own_first(kv_ref, core_s[0], 0, hd)
    values = own_first(kv_ref, core_s[0], hd, 2 * hd)
    limit = jnp.minimum(valid_s[b], jnp.maximum(prefix_s[b], qpos_ref[...] + 1))
    visible = kpos_ref[...] < limit
    d_keys, d_values = 0.0, 0.0
    for q_ref, g_ref, dst in ((q_own_ref, g_own_ref, dq_own_ref), (q_oth_ref, g_oth_ref, dq_oth_ref)):
        query = jnp.concatenate([q_ref[0, :, n * hd:(n + 1) * hd] for n in range(heads)], axis=0)
        grad = jnp.concatenate([g_ref[0, :, n * hd:(n + 1) * hd] for n in range(heads)], axis=0)
        scores = dot_f32(keys, query, 1, 1)
        scores = jnp.where(visible, scores, MASKED)
        top = jnp.max(scores, axis=0, keepdims=True)
        expo = jnp.exp(scores - top)
        inv = 1.0 / jnp.sum(expo, axis=0, keepdims=True)
        probs = expo * inv
        d_probs = dot_f32(values, grad, 1, 1)
        delta = jnp.sum(probs * d_probs, axis=0, keepdims=True)
        d_scores = (probs * (d_probs - delta)).astype(BF16)
        d_values = d_values + dot_f32(probs.astype(BF16), grad, 1, 0)
        d_keys = d_keys + dot_f32(d_scores, query, 1, 0)
        d_query = dot_f32(d_scores, keys, 0, 0) * scale
        for n in range(heads):
            g_1 = d_query[n * rows:(n + 1) * rows, :half]
            g_2 = d_query[n * rows:(n + 1) * rows, half:]
            dst[0, :, n * hd:n * hd + half] = (g_1 * cos_t + g_2 * sin_t).astype(BF16)
            dst[0, :, n * hd + half:(n + 1) * hd] = (g_2 * cos_t - g_1 * sin_t).astype(BF16)
    d_keys = d_keys.astype(BF16)
    d_values = d_values.astype(BF16)
    span = kv_ref.shape[2]
    for k, dst in enumerate((dkv_own_ref, dkv_oth_ref)):
        for c in range(shards):
            at = (k * shards + c) * span
            dst[c, 0, :, :hd] = d_keys[at:at + span]
            dst[c, 0, :, hd:] = d_values[at:at + span]


def attn_specs(rows, width, shards, two_hd, half):
    q_spec = pl.BlockSpec((1, rows, width), lambda b, *_: (b, 0, 0))
    kv_spec = pl.BlockSpec((shards, 1, rows, two_hd), lambda b, *_: (0, b, 0, 0))
    tab_spec = pl.BlockSpec((rows, half), lambda b, *_: (0, 0))
    return q_spec, kv_spec, tab_spec


def whole(shape):
    return pl.BlockSpec(shape, lambda b, *_: tuple(0 for _ in shape))


def attn_fwd(q_own, q_oth, kv_all, cos_t, sin_t, qpos, kpos, scalars):
    batch, rows, width = q_own.shape
    shards, two_hd = kv_all.shape[0], kv_all.shape[3]
    q_spec, kv_spec, tab_spec = attn_specs(rows, width, shards, two_hd, two_hd // 4)
    heads = width * 2 // two_hd
    out = jax.ShapeDtypeStruct((batch, rows, width), BF16)
    qpos_col = jnp.tile(qpos, heads)[:, None]
    n_keys = kpos.shape[0]
    flops = 2 * 2 * batch * rows * 2 * width * n_keys
    return pl.pallas_call(
        attn_fwd_kernel,
        out_shape=(out, out, out, out),
        grid_spec=pltpu.PrefetchScalarGridSpec(
            num_scalar_prefetch=3, grid=(batch,),
            in_specs=[q_spec, q_spec, kv_spec, tab_spec, tab_spec, whole((heads * rows, 1)), whole((1, n_keys))],
            out_specs=[q_spec] * 4),
        compiler_params=pltpu.CompilerParams(dimension_semantics=("arbitrary",), vmem_limit_bytes=60 << 20),
        cost_estimate=pl.CostEstimate(flops=flops, bytes_accessed=batch * rows * width * 16 + kv_all.size * 2, transcendentals=batch * rows * heads * 2 * n_keys),
        name="attn_fwd",
    )(*scalars, q_own, q_oth, kv_all, cos_t, sin_t, qpos_col, kpos[None, :])


def attn_bwd(order, q_own, q_oth, g_own, g_oth, kv_all, cos_t, sin_t, qpos, kpos, scalars, first, count, earlier):
    batch, rows, width = q_own.shape
    shards, two_hd = kv_all.shape[0], kv_all.shape[3]
    tab_spec = pl.BlockSpec((rows, two_hd // 4), lambda b, *_: (0, 0))
    q_spec = pl.BlockSpec((1, rows, width), lambda b, *_: (b + first, 0, 0))
    kv_spec = pl.BlockSpec((shards, 1, rows, two_hd), lambda b, *_: (0, b + first, 0, 0))
    heads = width * 2 // two_hd
    out = jax.ShapeDtypeStruct((batch, rows, width), BF16)
    dkv_spec = pl.BlockSpec((shards // 2, 1, rows, two_hd), lambda b, *_: (0, b + first, 0, 0))
    kv_out = jax.ShapeDtypeStruct((shards // 2, batch, rows, two_hd), BF16)
    qpos_row = jnp.tile(qpos, heads)[None, :]
    n_keys = kpos.shape[0]
    flops = 2 * 5 * count * rows * 2 * width * n_keys
    return order.call(
        functools.partial(attn_bwd_kernel, first), 9, len(earlier), prefetch=3, in_parts=True,
        out_shape=(out, out, kv_out, kv_out), grid=(count,),
        in_specs=[q_spec, q_spec, q_spec, q_spec, kv_spec, tab_spec, tab_spec, whole((1, heads * rows)), whole((n_keys, 1))],
        out_specs=[q_spec, q_spec, dkv_spec, dkv_spec],
        compiler_params=pltpu.CompilerParams(dimension_semantics=("arbitrary",), vmem_limit_bytes=60 << 20),
        cost_estimate=pl.CostEstimate(flops=flops, bytes_accessed=count * rows * width * 12 + kv_all.size * 4, transcendentals=count * rows * heads * 2 * n_keys),
        name="attn_bwd",
    )(*scalars, q_own, q_oth, g_own, g_oth, kv_all, cos_t, sin_t, qpos_row, kpos[:, None], *earlier)


class Order:
    def __init__(self):
        self.last = None

    def call(self, kernel, n_in, n_kept=0, *, in_specs, out_specs, out_shape, grid, in_parts=False, after=(), prefetch=0, scratch_shapes=(), **options):
        def run(*args):
            deps = (() if self.last is None or any(self.last is a for a in args) else (self.last,)) + tuple(after)
            n_args = prefetch + n_in

            def body(*refs):
                kernel(*refs[:n_args], *refs[n_args + n_kept + len(deps):])

            n_out = len(out_specs) if isinstance(out_specs, (list, tuple)) else 1
            shapes = [pltpu.HBM(o.shape, o.dtype) if in_parts and o.size > 1 << 17 else o for o in out_shape] if in_parts else out_shape
            first = n_args
            args = args[:first] + tuple(pltpu.with_memory_space_constraint(a, pltpu.HBM) for a in args[first:])
            out = pl.pallas_call(
                body, out_shape=shapes,
                grid_spec=pltpu.PrefetchScalarGridSpec(
                    num_scalar_prefetch=prefetch, grid=grid, scratch_shapes=scratch_shapes, out_specs=out_specs,
                    in_specs=in_specs + [pl.BlockSpec(memory_space=pl.ANY)] * (n_kept + len(deps))),
                input_output_aliases={n_args + k: n_out - n_kept + k for k in range(n_kept)},
                **options)(*args, *deps)
            self.last = out[0] if isinstance(out, (tuple, list)) else out
            return out

        return run


def params(steps, limit=60):
    return pltpu.CompilerParams(dimension_semantics=("arbitrary",) * steps, vmem_limit_bytes=limit << 20)


def cost(flops, *arrays):
    return pl.CostEstimate(flops=flops, bytes_accessed=sum(a.size * a.dtype.itemsize for a in arrays), transcendentals=0)


def rows_of(ref):
    return ref[...].reshape(-1, ref.shape[-1])


def raw_spec(shape):
    return pl.BlockSpec((2, 1) + shape[2:], lambda j, i, core: (lax.rem(i, 2), lax.bitwise_xor(core[0], lax.div(i, 2)), 0, 0))


def d_act_kernel(core_s, g_ref, wd_ref, out_ref):
    out_ref[...] = dot_f32(rows_of(g_ref), wd_ref[...], 1, 1).astype(BF16)


def d_act_call(order, core, g_all, w_down, tn=1024):
    chips, _, rows, dim = g_all.shape
    width = w_down.shape[0]
    out = jax.ShapeDtypeStruct((chips * 2 * rows, width), BF16)
    return order.call(
        d_act_kernel, 2, prefetch=1, out_shape=out, grid=(width // tn, chips),
        in_specs=[raw_spec(g_all.shape), pl.BlockSpec((tn, dim), lambda j, i, core: (j, 0))],
        out_specs=pl.BlockSpec((2 * rows, tn), lambda j, i, core: (i, j)), compiler_params=params(2),
        cost_estimate=cost(2 * g_all.size * width, g_all, w_down, out), name="d_act",
    )(core, g_all, w_down)


def act_kernel(core_s, z_ref, g_ref, wg_ref, wu_ref, *refs, sub):
    c_1 = math.sqrt(2.0 / math.pi)
    c_3 = 0.044715 * c_1
    act_ref, dg_ref, du_ref = refs[-3:]
    z_in = rows_of(z_ref)
    for j in range(0, wg_ref.shape[1], sub):
        gate = dot_f32(z_in, wg_ref[:, j:j + sub], 1, 0)
        upper = dot_f32(z_in, wu_ref[:, j:j + sub], 1, 0)
        if len(refs) == 4:
            d_act = dot_f32(rows_of(g_ref), refs[0][j:j + sub, :], 1, 1).astype(BF16).astype(F32)
        else:
            d_act = g_ref[:, j:j + sub].astype(F32)
        square = gate * gate
        half = 0.5 * jnp.tanh(gate * (c_3 * square + c_1)) + 0.5
        gelu = gate * half
        act_ref[:, j:j + sub] = (gelu * upper).astype(BF16)
        du_ref[:, j:j + sub] = (d_act * gelu).astype(BF16)
        slope = half + gelu * (1.0 - half) * (6.0 * c_3 * square + 2.0 * c_1)
        dg_ref[:, j:j + sub] = (d_act * upper * slope).astype(BF16)


def act_call(order, core, z_all, g_all, w_gate, w_up, w_down, sub=256):
    chips, _, rows, dim = z_all.shape
    width = w_gate.shape[1]
    out = jax.ShapeDtypeStruct((chips * 2 * rows, width), BF16)
    tn = 1024 if w_down is None else 512
    raw = raw_spec(z_all.shape)
    col = pl.BlockSpec((dim, tn), lambda j, i, core: (0, j))
    tile = pl.BlockSpec((2 * rows, tn), lambda j, i, core: (i, j))
    args = (z_all, g_all, w_gate, w_up) + (() if w_down is None else (w_down,))
    specs = [raw, tile if w_down is None else raw, col, col] + ([] if w_down is None else [pl.BlockSpec((tn, dim), lambda j, i, core: (j, 0))])
    return order.call(
        functools.partial(act_kernel, sub=sub), len(args), prefetch=1, out_shape=(out, out, out), grid=(width // tn, chips),
        in_specs=specs, out_specs=[tile] * 3, compiler_params=params(2),
        cost_estimate=cost(2 * (len(args) - 2) * z_all.size * width, *args, out, out, out), name="mlp_act",
    )(core, *args)


def back_kernel(*refs, terms, joined, n_far, base, tn):
    n = len(terms)
    lhs, rhs, far, out = refs[:n], refs[n:2 * n], refs[2 * n:2 * n + n_far], refs[2 * n + n_far]
    l_bufs, r_bufs, (l_sems, r_sems) = refs[2 * n + n_far + 1:][:n], refs[3 * n + n_far + 1:][:n], refs[4 * n + n_far + 1:]
    j, i = pl.program_id(0), pl.program_id(1)
    blocks, rows = l_bufs[0].shape[:2]

    def left(p, at):
        return pltpu.make_async_copy(lhs[p].at[pl.ds((base + at) * rows, rows)], l_bufs[p].at[at], l_sems.at[p, at])

    def right(p, tile):
        cols = pl.ds(pl.multiple_of(tile * tn, tn), tn)
        src = rhs[p].at[:, cols] if terms[p][0] == 0 else rhs[p].at[cols]
        return pltpu.make_async_copy(src, r_bufs[p].at[lax.rem(tile, 2)], r_sems.at[p, lax.rem(tile, 2)])

    @pl.when((j == 0) & (i == 0))
    def _():
        for p in range(n):
            right(p, 0).start()
            left(p, 0).start()
        for at in range(1, blocks):
            for p in range(n):
                left(p, at).start()

    @pl.when((i == blocks - 1) & (j + 1 < pl.num_programs(0)))
    def _():
        for p in range(n):
            right(p, j + 1).start()

    def compute(ready):
        totals = {}
        for p, (dim, kind) in enumerate(terms):
            ready(p)
            part = dot_f32(l_bufs[p][i], r_bufs[p][lax.rem(j, 2)], 1, dim)
            totals[kind] = totals[kind] + part if kind in totals else part
        for kind, total in totals.items():
            at = (slice(None), kind) if joined else (slice(None),)
            total = total.reshape(out[at].shape)
            if far:
                total += far[0][at].astype(F32)
            out[at] = total.astype(BF16)

    @pl.when(j == 0)
    def _():
        def ready(p):
            @pl.when(i == 0)
            def _():
                right(p, 0).wait()

            left(p, i).wait()

        compute(ready)

    @pl.when(j > 0)
    def _():
        @pl.when(i == 0)
        def _():
            for p in range(n):
                right(p, j).wait()

        compute(lambda p: None)


def back_call(order, side, lhs, rhs, terms, far, chips, tn=512):
    dim = rhs[0].shape[0 if terms[0][0] else 1]
    rows = lhs[0].shape[0] // (2 * chips)
    half, n = chips // 2, len(terms)
    kinds = sorted({kind for _, kind in terms})
    joined = len(kinds) == 2
    hbm = pl.BlockSpec(memory_space=pl.ANY)
    both = pl.BlockSpec((2, 2, rows, tn), lambda j, i: (i, 0, 0, j))
    out = jax.ShapeDtypeStruct((chips, 2, rows, dim) if joined else (chips, rows, dim), BF16)
    far_spec = both if joined else pl.BlockSpec((2, None, rows, tn), lambda j, i: (i, kinds[0], 0, j))
    depth = lhs[0].shape[1]
    return order.call(
        functools.partial(back_kernel, terms=terms, joined=joined, n_far=len(far), base=side * half, tn=tn), 2 * n + len(far), out_shape=out,
        grid=(dim // tn, half), in_specs=[hbm] * (2 * n) + [far_spec] * len(far),
        out_specs=both if joined else pl.BlockSpec((2, rows, tn), lambda j, i: (i, 0, j)),
        scratch_shapes=[pltpu.VMEM((half, 2 * rows, depth), BF16)] * n
        + [pltpu.VMEM((2, depth, tn) if d == 0 else (2, tn, depth), BF16) for d, _ in terms]
        + [pltpu.SemaphoreType.DMA((n, half)), pltpu.SemaphoreType.DMA((n, 2))],
        compiler_params=params(2),
        cost_estimate=cost(n * lhs[0].size * dim, *lhs, *rhs, out), name="mlp_back",
    )(*lhs, *rhs, *far)


def wgrad_kernel(core_s, *refs, n, tf, tn, cols, first, first_col):
    lhs, rhs, out, l_buf, r_buf, sems = refs[:n], refs[n:2 * n], *refs[2 * n:]
    i, j, k = pl.program_id(0), pl.program_id(1), pl.program_id(2)
    step = (i * cols + j) * n + k
    slot = lax.rem(step, 2)
    chips = l_buf.shape[1] // 2

    def copies(s, at, p):
        row = pl.multiple_of((lax.div(s, cols * n) + first) * tf, tf)
        col = pl.multiple_of((lax.rem(lax.div(s, n), cols) + first_col) * tn, tn)
        halves = [], []
        for side in range(2):
            half = pl.ds(side * chips, chips)
            for q, (ref, buf, lanes) in enumerate(((lhs[p], l_buf, pl.ds(row, tf)), (rhs[p], r_buf, pl.ds(col, tn)))):
                src = ref.at[:, lax.bitwise_xor(core_s[0], side), :, lanes] if ref.ndim == 4 else ref.at[half, :, lanes]
                halves[side].append(pltpu.make_async_copy(src, buf.at[at, half], sems.at[q, side, at]))
        return halves

    def fetch(s, at):
        for p in range(n):
            @pl.when(lax.rem(s, n) == p)
            def _(p=p):
                for half in copies(s, at, p):
                    for copy in half:
                        copy.start()

    @pl.when(step == 0)
    def _():
        fetch(step, slot)

    @pl.when(step + 1 < pl.num_programs(0) * cols * n)
    def _():
        fetch(step + 1, 1 - slot)

    @pl.when(step == 0)
    def _():
        for side, half in enumerate(copies(step, slot, 0)):
            for copy in half:
                copy.wait()
            rows = pl.ds(side * chips, chips)
            part = dot_f32(rows_of(l_buf.at[0, rows]), rows_of(r_buf.at[0, rows]), 0, 0)
            out[...] = part if side == 0 else out[...] + part

    @pl.when(step > 0)
    def _():
        for half in copies(step, slot, 0):
            for copy in half:
                copy.wait()
        part = dot_f32(rows_of(l_buf.at[slot]), rows_of(r_buf.at[slot]), 0, 0)
        out[...] = jnp.where(k == 0, part, out[...] + part)


def wgrad_call(order, core, lhs, rhs, tf=1024, tn=1024, tiles=None, col_tiles=None, earlier=None, after=()):
    n = len(lhs)
    rows = lhs[0].shape[-2]
    shards = lhs[0].size // (rows * lhs[0].shape[-1])
    width = rhs[0].shape[-1]
    height = lhs[0].shape[-1]
    first_col, last_col = col_tiles or (0, width // tn)
    cols = last_col - first_col
    first, last = tiles or (0, height // tf)
    kept = () if earlier is None else (earlier,)
    out = jax.ShapeDtypeStruct((height, width), F32)
    return order.call(
        functools.partial(wgrad_kernel, n=n, tf=tf, tn=tn, cols=cols, first=first, first_col=first_col), 2 * n, len(kept), prefetch=1, after=after, out_shape=out, grid=(last - first, cols, n),
        in_specs=[pl.BlockSpec(memory_space=pl.ANY)] * (2 * n), out_specs=pl.BlockSpec((tf, tn), lambda i, j, k, core: (i + first, j + first_col)),
        scratch_shapes=[pltpu.VMEM((2, shards, rows, tf), BF16), pltpu.VMEM((2, shards, rows, tn), BF16), pltpu.SemaphoreType.DMA((2, 2, 2))],
        compiler_params=params(3), cost_estimate=cost(2 * n * shards * rows * height * width, *lhs, *rhs, out), name="wgrad",
    )(core, *lhs, *rhs, *kept)


def kv_wgrad_kernel(l_ref, r_ref, *refs):
    out, steps = refs[-1], pl.num_programs(0)
    width = out.shape[1]

    @pl.when(pl.program_id(0) < steps - 1)
    def _():
        out[...] = dot_f32(l_ref[...], r_ref[...], 0, 0)

    @pl.when(pl.program_id(0) == steps - 1)
    def _():
        row = 0
        for terms in refs[:-1]:
            total = jnp.sum(terms[...], axis=0, keepdims=True)
            for k in range(0, total.shape[1], width):
                out[row:row + 1] = total[:, k:k + width]
                row += 1


def kv_wgrad(order, lhs, rhs, terms, tf=512):
    tokens, rows = lhs.shape
    width = rhs.shape[1]
    extra = sum(t.shape[1] for t in terms) // width
    steps = rows // tf
    out = jax.ShapeDtypeStruct((rows + extra, width), F32)
    return order.call(
        kv_wgrad_kernel, 2 + len(terms), out_shape=out, grid=(steps + 1,),
        in_specs=[pl.BlockSpec((tokens, tf), lambda i: (0, jnp.minimum(i, steps - 1))), pl.BlockSpec((tokens, width), lambda i: (0, 0))]
        + [pl.BlockSpec(t.shape, lambda i: (0, 0)) for t in terms],
        out_specs=pl.BlockSpec((tf, width), lambda i: (i, 0)), compiler_params=params(1),
        cost_estimate=cost(2 * tokens * rows * width, lhs, rhs, out), name="kv_wgrad",
    )(lhs, rhs, *terms)


def head_wgrad_kernel(*refs):
    lhs, rhs, out = refs[:2], refs[2:4], refs[-1]
    for kind in range(2):
        total = dot_f32(lhs[kind][...], rhs[kind][...], 0, 0).reshape(out.shape[0], *out.shape[2:])
        for far in refs[4:-1]:
            total += far[:, kind]
        out[:, kind] = total


def head_wgrad(order, lhs, rhs, hd, far=(), tn=512):
    tokens, width = lhs[0].shape
    dim = rhs[0].shape[1]
    heads = width // hd
    out = jax.ShapeDtypeStruct((heads, 2, hd, dim), F32)
    tile = pl.BlockSpec((heads, 2, hd, tn), lambda j: (0, 0, 0, j))
    return order.call(
        head_wgrad_kernel, 4 + len(far), out_shape=out, grid=(dim // tn,),
        in_specs=[pl.BlockSpec((tokens, width), lambda j: (0, 0), pipeline_mode=pl.Buffered(1))] * 2
        + [pl.BlockSpec((tokens, tn), lambda j: (0, j))] * 2 + [tile] * len(far),
        out_specs=tile, compiler_params=params(1), cost_estimate=cost(4 * tokens * width * dim, *lhs, *rhs, *far, out), name="head_wgrad",
    )(*lhs, *rhs, *far)


def add_kernel(base_ref, *refs):
    for c, part in enumerate(refs[:-1]):
        @pl.when(pl.program_id(0) == c)
        def _(part=part):
            refs[-1][...] = (base_ref[...].astype(F32) + rows_of(part).astype(F32)).astype(BF16)


def add_call(order, base, parts):
    tokens, dim = base.shape
    size = tokens // len(parts)
    row = pl.BlockSpec((size, dim), lambda i: (i, 0))
    specs = [pl.BlockSpec((1, size, dim), lambda i, at=a.shape[0] - 1: (at, 0, 0)) if a.ndim == 3 else pl.BlockSpec((size, dim), lambda i: (0, 0)) for a in parts]
    return order.call(
        add_kernel, 1 + len(parts), out_shape=jax.ShapeDtypeStruct(base.shape, BF16), grid=(len(parts),), in_specs=[row] + specs, out_specs=row,
        compiler_params=params(1), cost_estimate=cost(base.size, base, base, base), name="add",
    )(base, *parts)


def resid_kernel(h_ref, a_own_ref, a_oth_ref, w_own_ref, w_oth_ref, gain_ref, resid_ref, *z_refs, sub):
    for c, z_ref in enumerate(z_refs):
        @pl.when(pl.program_id(0) == c)
        def _(z_ref=z_ref):
            for r in range(0, z_ref.shape[0], sub):
                at = slice(r, r + sub)
                total = dot_f32(a_own_ref[at], w_own_ref[...], 1, 0) + dot_f32(a_oth_ref[at], w_oth_ref[...], 1, 0)
                resid = (h_ref[at].astype(F32) + total).astype(BF16)
                resid_ref[at] = resid
                x_f = resid.astype(F32)
                inv = lax.rsqrt(jnp.mean(x_f * x_f, axis=-1, keepdims=True) + NORM_EPS)
                z_ref[at] = (x_f * inv * (1.0 + gain_ref[...])).astype(BF16)


def resid_call(order, hidden, mix_own, mix_oth, wo_own, wo_oth, gain, size, sub):
    tokens, dim = hidden.shape
    width = mix_own.shape[1]
    chunks = tokens // size
    row = pl.BlockSpec((size, dim), lambda i: (i, 0))
    mix = pl.BlockSpec((size, width), lambda i: (i, 0))
    whole_w = pl.BlockSpec((width, dim), lambda i: (0, 0))
    outs = (jax.ShapeDtypeStruct((tokens, dim), BF16),) + (jax.ShapeDtypeStruct((size, dim), BF16),) * chunks
    return order.call(
        functools.partial(resid_kernel, sub=sub), 6, out_shape=outs, grid=(chunks,),
        in_specs=[row, mix, mix, whole_w, whole_w, pl.BlockSpec((1, dim), lambda i: (0, 0))],
        out_specs=[row] + [pl.BlockSpec((size, dim), lambda i: (0, 0))] * chunks,
        compiler_params=params(1), cost_estimate=cost(4 * tokens * dim * width, hidden, mix_own, mix_oth, wo_own, wo_oth, *outs), name="resid",
    )(hidden, mix_own, mix_oth, wo_own, wo_oth, gain)


def norm_back(x_f, gain_1, d_out):
    inv = lax.rsqrt(jnp.mean(x_f * x_f, axis=-1, keepdims=True) + NORM_EPS)
    unit = x_f * inv
    scaled = d_out * gain_1
    d_x = inv * (scaled - unit * jnp.mean(scaled * unit, axis=-1, keepdims=True))
    return d_x, d_out * unit


def fold_rows(terms):
    rows, dim = terms.shape
    return jnp.sum(terms.reshape(rows // 8, 8, dim), axis=0)


def d_resid_kernel(*refs, n):
    dz_refs = refs[:n]
    x_ref, g_ref, gain_ref, w_own_ref, w_oth_ref, norm_ref, d_ref, own_ref, oth_ref = refs[n:]
    i = pl.program_id(0)

    @pl.when(i == 0)
    def _():
        norm_ref[...] = jnp.zeros_like(norm_ref)

    for c, dz_ref in enumerate(dz_refs):
        @pl.when(i == c)
        def _(dz_ref=dz_ref):
            d_x, terms = norm_back(x_ref[...].astype(F32), 1.0 + gain_ref[...], rows_of(dz_ref).astype(F32))
            norm_ref[...] += fold_rows(terms)
            d_ref[...] = (g_ref[...].astype(F32) + d_x).astype(BF16)
    own_ref[...] = dot_f32(d_ref[...], w_own_ref[...], 1, 1).astype(BF16)
    oth_ref[...] = dot_f32(d_ref[...], w_oth_ref[...], 1, 1).astype(BF16)


def d_resid_call(order, dz, resid, grad_out, gain, wo_own, wo_oth, first, size, earlier):
    tokens, dim = resid.shape
    n = len(dz)
    width = wo_own.shape[0]
    one = [pl.BlockSpec((1, size, dim) if a.ndim == 3 else (size, dim), lambda i, nd=a.ndim: (0,) * nd) for a in dz]
    far = pl.BlockSpec((size, dim), lambda i: (i + first, 0))
    mix = pl.BlockSpec((size, width), lambda i: (i + first, 0))
    whole_w = pl.BlockSpec((width, dim), lambda i: (0, 0))
    outs = (jax.ShapeDtypeStruct((8, dim), F32), jax.ShapeDtypeStruct((tokens, dim), BF16),
            jax.ShapeDtypeStruct((tokens, width), BF16), jax.ShapeDtypeStruct((tokens, width), BF16))
    return order.call(
        functools.partial(d_resid_kernel, n=n), n + 5, len(earlier), in_parts=True, out_shape=outs, grid=(n,),
        in_specs=one + [far, far, pl.BlockSpec((1, dim), lambda i: (0, 0)), whole_w, whole_w],
        out_specs=[pl.BlockSpec((8, dim), lambda i: (0, 0)), far, mix, mix],
        compiler_params=params(1), cost_estimate=cost(4 * n * size * dim * width, *dz, wo_own, wo_oth, outs[1]), name="d_resid",
    )(*dz, resid, grad_out, gain, wo_own, wo_oth, *earlier)


def d_hidden_kernel(q_own_ref, q_oth_ref, dkv_ref, x_ref, d_ref, gain_ref, wq_own_ref, wq_oth_ref, wkv_ref, out_ref, norm_ref, *, sub):
    @pl.when(pl.program_id(0) == 0)
    def _():
        norm_ref[...] = jnp.zeros_like(norm_ref)

    folded = 0.0
    for r in range(0, x_ref.shape[0], sub):
        at = slice(r, r + sub)
        d_normed = (dot_f32(q_own_ref[at], wq_own_ref[...], 1, 0) + dot_f32(q_oth_ref[at], wq_oth_ref[...], 1, 0)
                    + dot_f32(dkv_ref[at], wkv_ref[...], 1, 1)).astype(BF16).astype(F32)
        d_x, terms = norm_back(x_ref[at].astype(F32), 1.0 + gain_ref[...], d_normed)
        folded += fold_rows(terms)
        out_ref[at] = (d_ref[at].astype(F32) + d_x).astype(BF16)
    norm_ref[...] += folded


def d_hidden_call(order, dq_own, dq_oth, dkv, hidden, d_resid, gain, wq_own, wq_oth, w_kv, tm, sub):
    tokens, dim = hidden.shape
    width, two_hd = dq_own.shape[1], dkv.shape[1]
    row = pl.BlockSpec((tm, dim), lambda i: (i, 0))
    mix = pl.BlockSpec((tm, width), lambda i: (i, 0))
    whole_w = pl.BlockSpec((width, dim), lambda i: (0, 0))
    outs = (jax.ShapeDtypeStruct((tokens, dim), BF16), jax.ShapeDtypeStruct((8, dim), F32))
    return order.call(
        functools.partial(d_hidden_kernel, sub=sub), 9, out_shape=outs, grid=(tokens // tm,),
        in_specs=[mix, mix, pl.BlockSpec((tm, two_hd), lambda i: (i, 0)), row, row, pl.BlockSpec((1, dim), lambda i: (0, 0)), whole_w, whole_w,
                  pl.BlockSpec((dim, two_hd), lambda i: (0, 0))],
        out_specs=[row, pl.BlockSpec((8, dim), lambda i: (0, 0))],
        compiler_params=params(1), cost_estimate=cost(4 * tokens * dim * (width + two_hd), dq_own, dq_oth, hidden, d_resid, wq_own, wq_oth, *outs), name="d_hidden",
    )(dq_own, dq_oth, dkv, hidden, d_resid, gain, wq_own, wq_oth, w_kv)


def solution(mesh):
    tp_size = mesh.shape["tp"]
    chips = tp_size // 2
    act_spec = P("dp", "tp", None)
    in_specs = (act_spec, act_spec, P("dp"), P("dp"), P(None), P(None, "tp"), P(None, None), P(None, None), P("tp", None), P(None), P(None, "tp"), P(None, "tp"), P("tp", None))
    out_specs = (act_spec, act_spec, P("dp"), P("dp", "tp"), P("dp", None), P("dp", None), P(("dp", "tp"), None), P("dp"), P("dp", "tp"), P("dp", "tp"), P(("dp", "tp"), None))
    same_core = [[2 * c + k for c in range(chips)] for k in range(2)]
    partner = [(i, i ^ 1) for i in range(tp_size)]

    def scatter4(x_part):
        flat = x_part.reshape((-1,) + x_part.shape[2:])
        return lax.psum_scatter(flat, "tp", scatter_dimension=0, tiled=True, axis_index_groups=same_core)

    def gather8(x_loc):
        return lax.all_gather(x_loc, "tp", axis=0, tiled=False)

    def swap(x_loc):
        return lax.ppermute(x_loc, "tp", partner)

    def flip(x_loc, bits):
        return lax.ppermute(x_loc, "tp", [(i, i ^ bits) for i in range(tp_size)])

    def gather4_direct(x_loc, before=None, after=None):
        chip = lax.axis_index("tp") // 2
        half = x_loc.shape[0] // 2
        near, far = flip(x_loc, 2), flip(x_loc, 4)
        if before is not None:
            near, far, _ = lax.optimization_barrier((near, far, before))
        low, high = flip(near[:half], 4), flip(far[half:], 2)
        if after is not None:
            result = after()
            x_loc, near, far, low, high, _ = lax.optimization_barrier((x_loc, near, far, low, high, result[0]))
        out = jnp.zeros((chips,) + x_loc.shape, x_loc.dtype)
        for k, block in ((0, x_loc), (1, near), (2, far)):
            out = lax.dynamic_update_slice(out, block[None], (chip ^ k, 0, 0))
        out = lax.dynamic_update_slice(out, low[None], (chip ^ 3, 0, 0))
        out = lax.dynamic_update_slice(out, high[None], (chip ^ 3, half, 0))
        return out if after is None else (out, result)

    def local_layer(hidden, grad_out, prefix_len, valid_len, attn_norm, w_query, w_key, w_value, w_out, mlp_norm, w_gate, w_up, w_down):
        batch, rows, dim = hidden.shape
        hd = w_key.shape[1]
        tokens = batch * rows
        assert batch % CHUNKS == 0
        me = lax.axis_index("tp")
        core = lax.rem(me, 2)
        qpos = me * rows + jnp.arange(rows, dtype=jnp.int32)
        shard_pos = jnp.arange(rows, dtype=jnp.int32)[None, :] + (jnp.arange(chips, dtype=jnp.int32) * 2 * rows)[:, None]
        kpos = jnp.concatenate([(shard_pos + core * rows).reshape(-1), (shard_pos + (1 - core) * rows).reshape(-1)])
        cos_t, sin_t = rope_tables(qpos, hd)

        def rope_single(raw_proj):
            return apply_rope(raw_proj, cos_t, sin_t)

        order = Order()
        scalars = (prefix_len, valid_len, core[None])
        attn_gain = attn_norm.astype(F32)
        mlp_gain = mlp_norm.astype(F32)
        wq_own = gather4_direct(w_query.T).reshape(chips * hd, dim)
        normed_flat = rms_norm(hidden, attn_gain).reshape(tokens, dim)
        w_kv = jnp.concatenate([w_key, w_value], axis=1)
        kv_raw = dot_f32(normed_flat, w_kv, 1, 0).reshape(batch, rows, 2 * hd)
        keys, key_pull = jax.vjp(rope_single, kv_raw[..., :hd])
        kv_all = gather8(jnp.concatenate([keys, kv_raw[..., hd:]], axis=-1).astype(BF16))
        wq_oth = swap(wq_own)
        q_own = dot_f32(normed_flat, wq_own, 1, 1)
        q_oth = dot_f32(normed_flat, wq_oth, 1, 1)

        def attend():
            shape = batch, rows, chips * hd
            return attn_fwd(q_own.reshape(shape), q_oth.reshape(shape), kv_all, cos_t, sin_t, qpos, kpos, scalars)

        wo_own, (mix_own, mix_oth, q_own, q_oth) = gather4_direct(w_out, (q_own, q_oth), attend)
        wo_own = wo_own.reshape(chips * hd, dim)
        wo_oth = swap(wo_own)
        mix_own = mix_own.reshape(tokens, chips * hd)
        mix_oth = mix_oth.reshape(tokens, chips * hd)
        hidden_flat = hidden.reshape(tokens, dim)
        grad_flat = grad_out.reshape(tokens, dim)
        size = tokens // CHUNKS
        resid, *z_parts = resid_call(order, hidden_flat, mix_own, mix_oth, wo_own, wo_oth, mlp_gain[None, :], size, 2 * rows)

        g_all, z_all, acts, far = [], [], [], []
        for c in range(CHUNKS):
            g_all.append(gather8(grad_flat[c * size:(c + 1) * size]).reshape(chips, 2, size, dim))
            z_all.append(gather8(z_parts[c]).reshape(chips, 2, size, dim))
        mlp_sums, d_gated = [None] * CHUNKS, [None] * CHUNKS
        weights = (w_gate, w_up, w_down)
        core_1 = core[None]
        grads = None

        def d_resid_of(first, count, earlier):
            return d_resid_call(order, d_gated[first:first + count], resid, grad_flat, mlp_gain[None, :], wo_own, wo_oth, first, size,
                                () if earlier is None else earlier[1])

        def attn_bwd_of(first, count, d_own, d_oth, earlier):
            per = batch // CHUNKS
            return attn_bwd(order, q_own, q_oth, d_own.reshape(batch, rows, -1), d_oth.reshape(batch, rows, -1), kv_all, cos_t, sin_t, qpos, kpos,
                            scalars, first * per, count * per, () if earlier is None else earlier[2])

        d_z_terms, mlp_terms = ((1, 0), (1, 0)), ((0, 1),)

        def back_both(c, side, far):
            return back_call(order, side, (acts[c][1], acts[c][2], acts[c][0]), weights, d_z_terms + mlp_terms, far, chips)

        def finish(c):
            both = back_both(c, 0, (far[c],))
            both = scatter4(both).reshape(2, size, dim)
            d_gated[c] = mlp_sums[c] = both

        def finish_last(c):
            part = back_call(order, 0, acts[c][1:], weights[:2], d_z_terms, (far[c],), chips)
            d_gated[c] = scatter4(part).reshape(size, dim)
            part = back_call(order, 0, acts[c][:1], weights[2:], mlp_terms, (far[c],), chips)
            mlp_sums[c] = scatter4(part).reshape(size, dim)

        for c in range(CHUNKS):
            if c < CHUNKS - 1:
                d_act = d_act_call(order, core_1, g_all[c], w_down)
                acts.append(act_call(order, core_1, z_all[c], d_act, w_gate, w_up, None))
            else:
                acts.append(act_call(order, core_1, z_all[c], g_all[c], *weights))
            part = back_both(c, 1, ())
            far.append(swap(part))
            if c == CHUNKS - 2:
                for earlier in range(c + 1):
                    finish(earlier)
        terms, *d_parts = d_resid_of(0, 1, None)
        grads = terms, d_parts, attn_bwd_of(0, 1, d_parts[1], d_parts[2], None)
        finish_last(CHUNKS - 1)
        shards = [[a.reshape(2 * chips, size, -1) for a in acts[c]] for c in range(CHUNKS)]
        g_gate = wgrad_call(order, core_1, z_all, [a[1] for a in shards], tiles=(0, 1))

        terms, d_resid, d_own, d_oth = d_resid_of(1, CHUNKS - 1, grads)
        norm_terms, (dq_own, dq_oth, dkv_own, dkv_oth) = grads[0] + terms, attn_bwd_of(1, CHUNKS - 1, d_own, d_oth, grads)
        dq_own = dq_own.reshape(tokens, chips * hd)
        dq_oth = dq_oth.reshape(tokens, chips * hd)
        dkv_far = swap(dkv_oth)
        heads_far = head_wgrad(order, (mix_oth, dq_oth), (d_resid, normed_flat), hd)
        dkv_far, dkv_own, _ = lax.optimization_barrier((dkv_far, dkv_own, heads_far))
        dkv = scatter4((dkv_own.astype(F32) + dkv_far.astype(F32)).astype(BF16))
        heads_far = swap(heads_far)

        g_gate = wgrad_call(order, core_1, z_all, [a[1] for a in shards], tiles=(1, 2), earlier=g_gate)
        g_heads_part = head_wgrad(order, (mix_own, dq_own), (d_resid, normed_flat), hd, (heads_far,))
        g_heads = scatter4(g_heads_part)
        dkv, g_heads_part = lax.optimization_barrier((dkv, g_heads_part))
        g_out, g_query = g_heads[0], g_heads[1].T
        d_k_raw = key_pull(dkv[..., :hd].astype(F32))[0]
        dkv = jnp.concatenate([d_k_raw.astype(BF16), dkv[..., hd:]], axis=-1).reshape(tokens, 2 * hd)
        grad_hidden, attn_terms = d_hidden_call(
            order, dq_own, dq_oth, dkv, hidden_flat, d_resid, attn_gain[None, :], wq_own, wq_oth, w_kv, 4 * rows, 2 * rows)
        sums = kv_wgrad(order, normed_flat, dkv, (attn_terms, norm_terms))
        sums = lax.psum(sums, "tp")
        g_attn_norm, g_mlp_norm = sums[dim:].reshape(2, dim)
        hidden_out = add_call(order, resid, mlp_sums).reshape(batch, rows, dim)
        g_up = wgrad_call(order, core_1, z_all, [a[2] for a in shards])
        g_down = wgrad_call(order, core_1, [a[0] for a in shards], g_all)
        return (hidden_out, grad_hidden.reshape(batch, rows, dim), g_attn_norm, g_query, sums[:dim, :hd], sums[:dim, hd:], g_out, g_mlp_norm, g_gate, g_up, g_down)

    return jax.shard_map(local_layer, mesh=mesh, in_specs=in_specs, out_specs=out_specs, check_vma=False)
```
